32 devices in a mesh: gz: 4 (over z), gy: 2 (over y), gx: 4 (over x, core).
Axes of the slice: x: 2, y: 2, z: 4, core: 2. Of those that a mesh axis runs over, the one named last changes fastest.
Arguments:
- k_cell: float32 [192, 192, 192], P('gx', 'gy', 'gz')
- k_ghost: float32 [6, 192, 192], replicated
- f_rhs: float32 [192, 192, 192], P('gx', 'gy', 'gz')
- u_init: float32 [192, 192, 192], P('gx', 'gy', 'gz')
Outputs:
- output 1: float32 [192, 192, 192], P('gx', 'gy', 'gz')
- output 2: float32 [192, 192, 192], P('gx', 'gy', 'gz')
- output 3: float32 [8], replicated
All inputs are finite; a program needn't handle non-finite values.
Results may differ from the reference program's by a relative error of at most 0.001.
Values sent between devices are 32-bit elements.
A program may use at most 1 GiB of HBM per device.

```python
import jax
import jax.numpy as jnp
from jax import lax

GRID_SIDE = 192
CG_ITERS = 8


def setup_inputs(seed: int = 0) -> dict:
    grid_side = GRID_SIDE
    key_list = jax.random.split(jax.random.key(seed), 9)
    block_len = grid_side // 8
    cube_shape = (grid_side, grid_side, grid_side)
    cell_part = jax.random.uniform(key_list[0], cube_shape, jnp.float32, -1.0, 1.0)
    block_part = jax.random.uniform(key_list[1], (8, 8, 8), jnp.float32, -1.0, 1.0)
    block_part = jnp.repeat(jnp.repeat(jnp.repeat(block_part, block_len, axis=0), block_len, axis=1), block_len, axis=2)
    k_cell = jnp.exp(2.302585 * (0.5 * cell_part + 0.5 * block_part))
    k_ghost = jnp.exp(2.302585 * jax.random.uniform(key_list[2], (6, grid_side, grid_side), jnp.float32, -1.0, 1.0))
    coord_1d = jnp.arange(grid_side, dtype=jnp.float32) + 1.0
    wave_num = jax.random.randint(key_list[3], (3, 3), 1, 5).astype(jnp.float32)
    mode_amp = 2.0 * jax.random.normal(key_list[4], (3,), jnp.float32)
    profile = jnp.sin(jnp.pi * wave_num[:, :, None] * coord_1d[None, None, :] / (grid_side + 1.0))
    smooth = jnp.einsum('m,mi,mj,mk->ijk', mode_amp, profile[:, 0], profile[:, 1], profile[:, 2])
    src_pos = jax.random.randint(key_list[5], (64, 3), 1, 8) * block_len + jax.random.randint(key_list[6], (64, 3), -1, 1)
    src_amp = 10.0 * jax.random.normal(key_list[7], (64,), jnp.float32)
    f_rhs = smooth.at[src_pos[:, 0], src_pos[:, 1], src_pos[:, 2]].add(src_amp)
    u_init = 0.3 * jax.random.normal(key_list[8], cube_shape, jnp.float32)
    return {'k_cell': k_cell, 'k_ghost': k_ghost, 'f_rhs': f_rhs, 'u_init': u_init}


def reference(k_cell, k_ghost, f_rhs, u_init):
    k_x = jnp.concatenate([k_ghost[0][None], k_cell, k_ghost[1][None]], axis=0)
    k_y = jnp.concatenate([k_ghost[2][:, None], k_cell, k_ghost[3][:, None]], axis=1)
    k_z = jnp.concatenate([k_ghost[4][:, :, None], k_cell, k_ghost[5][:, :, None]], axis=2)
    coef_x = 2.0 * k_x[:-1] * k_x[1:] / (k_x[:-1] + k_x[1:])
    coef_y = 2.0 * k_y[:, :-1] * k_y[:, 1:] / (k_y[:, :-1] + k_y[:, 1:])
    coef_z = 2.0 * k_z[:, :, :-1] * k_z[:, :, 1:] / (k_z[:, :, :-1] + k_z[:, :, 1:])
    diag_sum = coef_x[:-1] + coef_x[1:] + coef_y[:, :-1] + coef_y[:, 1:] + coef_z[:, :, :-1] + coef_z[:, :, 1:]
    inv_diag = 1.0 / diag_sum

    def apply_op(grid_field):
        pad_x = jnp.pad(grid_field, ((1, 1), (0, 0), (0, 0)))
        pad_y = jnp.pad(grid_field, ((0, 0), (1, 1), (0, 0)))
        pad_z = jnp.pad(grid_field, ((0, 0), (0, 0), (1, 1)))
        flux_x = coef_x * (pad_x[1:] - pad_x[:-1])
        flux_y = coef_y * (pad_y[:, 1:] - pad_y[:, :-1])
        flux_z = coef_z * (pad_z[:, :, 1:] - pad_z[:, :, :-1])
        return (flux_x[:-1] - flux_x[1:]) + (flux_y[:, :-1] - flux_y[:, 1:]) + (flux_z[:, :, :-1] - flux_z[:, :, 1:])

    residual = f_rhs - apply_op(u_init)
    precond = residual * inv_diag
    rz_start = jnp.sum(residual * precond)

    def cg_step(cg_state, unused):
        approx, residual, direction, rz_old = cg_state
        q_vec = apply_op(direction)
        step_alpha = rz_old / jnp.sum(direction * q_vec)
        approx = approx + step_alpha * direction
        residual = residual - step_alpha * q_vec
        precond = residual * inv_diag
        rz_new = jnp.sum(residual * precond)
        direction = precond + (rz_new / rz_old) * direction
        return (approx, residual, direction, rz_new), jnp.sum(residual * residual)

    final_state, history = lax.scan(cg_step, (u_init, residual, precond, rz_start), None, length=CG_ITERS)
    return final_state[0], final_state[1], history
```

```python
import functools

import jax
import jax.numpy as jnp
from jax import lax
from jax.experimental import pallas as pl
from jax.experimental.pallas import tpu as pltpu
from jax.sharding import PartitionSpec as P

CG_ITERS = 8
LANES = 128
PAD = 8
MESH = pl.DeviceIdType.MESH
F32 = jnp.float32


def solve_kernel(dims, counts, kg_ref, k_ref, f_ref, u_ref, x_out, r_out, hist_ref,
                 kp, mp, cx, cy, cz, inv, x, r, w, s, z, p, n,
                 ys, zs, xr, yr, zr, red_s, red_r,
                 xs_sem, ys_sem, zs_sem, xr_sem, yr_sem, zr_sem, rs_sem, rr_sem):
    ni, nl, nj = dims
    ngx, ngy, ngz = counts
    gx, gy, gz = lax.axis_index('gx'), lax.axis_index('gy'), lax.axis_index('gz')
    rows = pl.ds(PAD, nl)
    rows_dn = pl.ds(PAD - 1, nl)
    rows_up = pl.ds(PAD + 1, nl)
    lane = lax.broadcasted_iota(jnp.int32, (nl, LANES), 1)
    lane_row = lax.broadcasted_iota(jnp.int32, (1, LANES), 1)
    inside = lane < nj
    has_xlo, has_xhi = gx > 0, gx < ngx - 1
    has_zlo, has_zhi = gz > 0, gz < ngz - 1
    face_lane = jnp.where(gy == 0, nj - 1, 0)
    halo_lane = jnp.where(gy == 0, nj, LANES - 1)
    wall_lane = jnp.where(gy == 0, LANES - 1, nj)

    def x_copy(ref, slot, up):
        src = ref.at[ni if up else 1, rows]
        return pltpu.make_async_remote_copy(
            src_ref=src, dst_ref=xr.at[slot, 0 if up else 1], send_sem=xs_sem.at[slot, 0 if up else 1],
            recv_sem=xr_sem.at[slot, 0 if up else 1], device_id=(gz, gy, gx + 1 if up else gx - 1), device_id_type=MESH)

    def z_copy(slot, up):
        return pltpu.make_async_remote_copy(
            src_ref=zs.at[slot, 0 if up else 1], dst_ref=zr.at[slot, 0 if up else 1],
            send_sem=zs_sem.at[slot, 0 if up else 1], recv_sem=zr_sem.at[slot, 0 if up else 1],
            device_id=(gz + 1 if up else gz - 1, gy, gx), device_id_type=MESH)

    def y_copy(slot):
        return pltpu.make_async_remote_copy(
            src_ref=ys.at[slot], dst_ref=yr.at[slot], send_sem=ys_sem.at[slot], recv_sem=yr_sem.at[slot],
            device_id=(gz, 1 - gy, gx), device_id_type=MESH)

    def exchange_start(ref, slot):
        pl.when(has_xlo)(lambda: x_copy(ref, slot, False).start())
        pl.when(has_xhi)(lambda: x_copy(ref, slot, True).start())

        def pack(i, acc):
            slab = ref[i + 1, rows, :]
            zs[slot, 1, pl.ds(i, 1), :] = slab[0:1, :]
            zs[slot, 0, pl.ds(i, 1), :] = slab[nl - 1:nl, :]
            shift = lax.rem(i - face_lane + LANES, LANES)
            return jnp.where(lane == i, pltpu.roll(slab, shift, 1), acc)

        ys[slot] = lax.fori_loop(0, ni, pack, jnp.zeros((nl, LANES), F32))
        pl.when(has_zlo)(lambda: z_copy(slot, False).start())
        pl.when(has_zhi)(lambda: z_copy(slot, True).start())
        y_copy(slot).start()

    def exchange_wait(ref, slot):
        @pl.when(has_xlo)
        def _():
            x_copy(ref, slot, False).wait_send()
            x_copy(ref, slot, True).wait_recv()
            ref[0, rows, :] = xr[slot, 0]

        @pl.when(has_xhi)
        def _():
            x_copy(ref, slot, True).wait_send()
            x_copy(ref, slot, False).wait_recv()
            ref[ni + 1, rows, :] = xr[slot, 1]

        @pl.when(has_zlo)
        def _():
            z_copy(slot, False).wait_send()
            z_copy(slot, True).wait_recv()
            for i in range(ni):
                ref[i + 1, PAD - 1:PAD, :] = zr[slot, 0, i:i + 1, :]

        @pl.when(has_zhi)
        def _():
            z_copy(slot, True).wait_send()
            z_copy(slot, False).wait_recv()
            for i in range(ni):
                ref[i + 1, PAD + nl:PAD + nl + 1, :] = zr[slot, 1, i:i + 1, :]

        y_copy(slot).wait()

    def put_lane(slab, column, i, target):
        return jnp.where(lane == target, pltpu.roll(column, lax.rem(target - i + LANES, LANES), 1), slab)

    def stencil(ref, slot, emit, init):
        halo = yr[slot]
        below = ref[0, rows, :]
        first = ref[1, rows, :]

        def step(i, carry):
            v, flux_x, state = carry
            above = ref[i + 2, rows, :]
            flux_next = cx[i + 1] * (above - v)
            flux_zl = cz[i, rows, :] * (v - ref[i + 1, rows_dn, :])
            flux_zh = cz[i, rows_up, :] * (ref[i + 1, rows_up, :] - v)
            vy = put_lane(v, halo, i, halo_lane)
            flux_y = cy[i] * (vy - pltpu.roll(vy, 1, 1))
            total = (flux_x - flux_next) + (flux_y - pltpu.roll(flux_y, LANES - 1, 1)) + (flux_zl - flux_zh)
            state = emit(i, jnp.where(inside, total, 0.0), v, state)
            return above, flux_next, state

        return lax.fori_loop(0, ni, step, (first, cx[0] * (first - below), init))[2]

    def fold(slab):
        out = slab[0:8]
        for part in range(8, nl, 8):
            out = out + slab[part:part + 8]
        return out

    def reduce_start(slot, accs):
        row = jnp.zeros((1, LANES), F32)
        for q, acc in enumerate(accs):
            row = jnp.where(lane_row == q, jnp.sum(jnp.sum(acc, axis=0, keepdims=True), axis=1, keepdims=True), row)
        me = (gz * ngy + gy) * ngx + gx
        red_s[slot] = row
        red_r[slot, me] = row
        for a in reversed(range(ngz)):
            for b in reversed(range(ngy)):
                for c in reversed(range(ngx)):
                    if a or b or c:
                        tgt = (lax.rem(gz + a, ngz), lax.rem(gy + b, ngy), lax.rem(gx + c, ngx))
                        pltpu.make_async_remote_copy(
                            src_ref=red_s.at[slot], dst_ref=red_r.at[slot, me], send_sem=rs_sem.at[slot],
                            recv_sem=rr_sem.at[slot], device_id=tgt, device_id_type=MESH).start()

    def reduce_wait(slot, count):
        others = ngx * ngy * ngz - 1
        whole = red_r.at[slot, pl.ds(0, others)]
        done = pltpu.make_async_remote_copy(
            src_ref=whole, dst_ref=whole, send_sem=rs_sem.at[slot], recv_sem=rr_sem.at[slot],
            device_id=(gz, gy, gx), device_id_type=MESH)
        done.wait_recv()
        done.wait_send()
        total = jnp.sum(red_r[slot], axis=0)
        return [jnp.sum(jnp.where(lane_row == q, total, 0.0), axis=1, keepdims=True) for q in range(count)]

    zero_slab = jnp.zeros((nl, LANES), F32)
    zero_acc = jnp.zeros((8, LANES), F32)

    def load(i, _):
        kp[i + 1, rows, :] = jnp.full((nl, LANES), 1.0, F32)
        kp[i + 1, rows, 0:nj] = k_ref[i]
        kp[i + 1, pl.ds(0, PAD), :] = jnp.ones((PAD, LANES), F32)
        kp[i + 1, pl.ds(PAD + nl, PAD), :] = jnp.ones((PAD, LANES), F32)
        mp[i + 1, rows, :] = zero_slab
        mp[i + 1, rows, 0:nj] = u_ref[i]
        mp[i + 1, pl.ds(0, PAD), :] = jnp.zeros((PAD, LANES), F32)
        mp[i + 1, pl.ds(PAD + nl, PAD), :] = jnp.zeros((PAD, LANES), F32)
        s[i] = zero_slab
        z[i] = zero_slab
        p[i] = zero_slab
        return 0

    lax.fori_loop(0, ni, load, 0)
    for edge in (0, ni + 1):
        mp[edge] = jnp.zeros((nl + 2 * PAD, LANES), F32)
        kp[edge] = jnp.ones((nl + 2 * PAD, LANES), F32)
    exchange_start(kp, 0)
    exchange_start(mp, 1)

    @pl.when(gx == 0)
    def _():
        kp[0, rows, 0:nj] = kg_ref[0, :, 0:nj]

    @pl.when(gx == ngx - 1)
    def _():
        kp[ni + 1, rows, 0:nj] = kg_ref[0, :, 0:nj]

    @pl.when(gz == 0)
    def _():
        for i in range(ni):
            kp[i + 1, PAD - 1:PAD, 0:nj] = kg_ref[2, i:i + 1, 0:nj]

    @pl.when(gz == ngz - 1)
    def _():
        for i in range(ni):
            kp[i + 1, PAD + nl:PAD + nl + 1, 0:nj] = kg_ref[2, i:i + 1, 0:nj]

    exchange_wait(kp, 0)
    wall_y = kg_ref[1, 0:nl, :]
    halo_y = yr[0]

    def harmonic(left, right):
        return 2.0 * left * right / (left + right)

    cx[0] = jnp.where(inside, harmonic(kp[0, rows, :], kp[1, rows, :]), 0.0)

    def coefs(i, _):
        here = kp[i + 1, rows, :]
        x_hi = jnp.where(inside, harmonic(here, kp[i + 2, rows, :]), 0.0)
        cx[i + 1] = x_hi
        z_lo = jnp.where(inside, harmonic(kp[i + 1, rows_dn, :], here), 0.0)
        z_hi = jnp.where(inside, harmonic(here, kp[i + 1, rows_up, :]), 0.0)
        cz[i, rows, :] = z_lo
        cz[i, pl.ds(PAD + nl, 1), :] = z_hi[nl - 1:nl, :]
        ky = put_lane(put_lane(here, halo_y, i, halo_lane), wall_y, i, wall_lane)
        y_lo = jnp.where(lane <= nj, harmonic(pltpu.roll(ky, 1, 1), ky), 0.0)
        cy[i] = y_lo
        diag = cx[i] + x_hi + y_lo + pltpu.roll(y_lo, LANES - 1, 1) + z_lo + z_hi
        inv[i] = jnp.where(inside, 1.0 / jnp.where(inside, diag, 1.0), 0.0)
        return 0

    lax.fori_loop(0, ni, coefs, 0)
    exchange_wait(mp, 1)

    def first_residual(i, av, v, acc):
        x[i] = v
        r[i] = zero_slab
        r[i, :, 0:nj] = f_ref[i]
        res = r[i] - av
        r[i] = res
        u = res * inv[i]
        n[i] = u
        return (acc[0] + fold(res * u),)

    (gamma_acc,) = stencil(mp, 1, first_residual, (zero_acc,))

    def copy_u(i, _):
        mp[i + 1, rows, :] = n[i]
        return 0

    lax.fori_loop(0, ni, copy_u, 0)
    exchange_start(mp, 2)
    exchange_wait(mp, 2)

    def first_w(i, av, v, acc):
        w[i] = av
        n[i] = av * inv[i]
        return (acc[0] + fold(av * v),)

    (delta_acc,) = stencil(mp, 2, first_w, (zero_acc,))
    lax.fori_loop(0, ni, copy_u, 0)

    def scalars(t, sums, gamma_old, pap_old):
        gamma, delta, sigma = sums[0], sums[1], sums[2]
        beta = jnp.where(t == 0, 0.0, gamma / gamma_old)
        pap = delta + 2.0 * beta * sigma + beta * beta * pap_old
        return gamma, pap, beta, gamma / pap

    def advance_x(alpha):
        def step(i, _):
            x[i] = x[i] + alpha * p[i]
            return 0
        lax.fori_loop(0, ni, step, 0)

    def iteration(t, carry):
        accs, gamma_old, pap_old, alpha_old = carry
        reduce_start(t, accs)
        exchange_start(mp, t + 3)
        advance_x(alpha_old)
        exchange_wait(mp, t + 3)

        def store_n(i, av, v, state):
            n[i] = av
            return state

        stencil(mp, t + 3, store_n, 0)
        sums = reduce_wait(t, 4)

        @pl.when(t > 0)
        def _():
            hist_ref[lax.max(t - 1, 0)] = sums[3][0, 0]

        gamma, pap, beta_v, alpha_v = scalars(t, sums, gamma_old, pap_old)
        beta, alpha = beta_v[0, 0], alpha_v[0, 0]

        def update(i, acc):
            iv, r_old, w_old = inv[i], r[i], w[i]
            z_new = n[i] + beta * z[i]
            s_new = w_old + beta * s[i]
            p[i] = iv * r_old + beta * p[i]
            r_new = r_old - alpha * s_new
            w_new = w_old - alpha * z_new
            u_new = iv * r_new
            z[i] = z_new
            s[i] = s_new
            r[i] = r_new
            w[i] = w_new
            mp[i + 1, rows, :] = iv * w_new
            return (acc[0] + fold(r_new * u_new), acc[1] + fold(w_new * u_new),
                    acc[2] + fold(u_new * s_new), acc[3] + fold(r_new * r_new))

        accs = lax.fori_loop(0, ni, update, (zero_acc,) * 4)
        return accs, gamma, pap, alpha

    one = jnp.ones((1, 1), F32)
    accs, gamma_old, pap_old, alpha_old = lax.fori_loop(
        0, CG_ITERS - 1, iteration, ((gamma_acc, delta_acc, zero_acc, zero_acc), one, one, jnp.float32(0.0)))

    last = CG_ITERS - 1
    reduce_start(last, accs)
    advance_x(alpha_old)
    sums = reduce_wait(last, 4)
    hist_ref[last - 1] = sums[3][0, 0]
    _, _, beta_v, alpha_v = scalars(last, sums, gamma_old, pap_old)
    beta, alpha = beta_v[0, 0], alpha_v[0, 0]

    def final(i, acc):
        r_old = r[i]
        s_new = w[i] + beta * s[i]
        p_new = inv[i] * r_old + beta * p[i]
        r_new = r_old - alpha * s_new
        x_new = x[i] + alpha * p_new
        x_out[i] = x_new[:, 0:nj]
        r_out[i] = r_new[:, 0:nj]
        return acc + fold(r_new * r_new)

    acc = lax.fori_loop(0, ni, final, zero_acc)
    reduce_start(CG_ITERS, (acc,))
    hist_ref[last] = reduce_wait(CG_ITERS, 1)[0][0, 0]


def solution(mesh):
    counts = (mesh.shape['gx'], mesh.shape['gy'], mesh.shape['gz'])
    grid_spec = P('gx', 'gy', 'gz')

    def local_solve(k_cell, k_ghost, f_rhs, u_init):
        ni, nj, nl = k_cell.shape
        ngx, ngy, ngz = counts
        gx, gy, gz = lax.axis_index('gx'), lax.axis_index('gy'), lax.axis_index('gz')
        pad_to = lambda a: jnp.pad(a, ((0, max(ni, nl) - a.shape[0]), (0, LANES - a.shape[1])), constant_values=1.0)
        wall = lambda row, start, extent: lax.dynamic_slice(k_ghost, (row,) + start, (1,) + extent)[0]
        wall_x = wall(jnp.where(gx == 0, 0, 1), (gy * nj, gz * nl), (nj, nl)).T
        wall_y = wall(2 + gy, (gx * ni, gz * nl), (ni, nl)).T
        wall_z = wall(jnp.where(gz == 0, 4, 5), (gx * ni, gy * nj), (ni, nj))
        walls = jnp.stack([pad_to(wall_x), pad_to(wall_y), pad_to(wall_z)])
        flip = lambda a: jnp.swapaxes(a, 1, 2)

        slots = CG_ITERS + 2
        whole = (ni, nl, LANES)
        padded = (ni + 2, nl + 2 * PAD, LANES)
        dma = pltpu.SemaphoreType.DMA
        devices = ngx * ngy * ngz
        vmem = pl.BlockSpec(memory_space=pltpu.VMEM)
        out_block = jax.ShapeDtypeStruct((ni, nl, nj), F32)
        x_new, r_new, hist = pl.pallas_call(
            functools.partial(solve_kernel, (ni, nl, nj), counts),
            out_shape=(out_block, out_block, jax.ShapeDtypeStruct((CG_ITERS,), F32)),
            in_specs=[vmem] * 4,
            out_specs=(vmem, vmem, pl.BlockSpec(memory_space=pltpu.SMEM)),
            scratch_shapes=[
                pltpu.VMEM(padded, F32), pltpu.VMEM(padded, F32),
                pltpu.VMEM((ni + 1, nl, LANES), F32), pltpu.VMEM(whole, F32), pltpu.VMEM((ni, nl + 2 * PAD, LANES), F32),
                pltpu.VMEM(whole, F32),
                pltpu.VMEM(whole, F32), pltpu.VMEM(whole, F32), pltpu.VMEM(whole, F32), pltpu.VMEM(whole, F32),
                pltpu.VMEM(whole, F32), pltpu.VMEM(whole, F32), pltpu.VMEM(whole, F32),
                pltpu.VMEM((slots, nl, LANES), F32), pltpu.VMEM((slots, 2, ni, LANES), F32),
                pltpu.VMEM((slots, 2, nl, LANES), F32), pltpu.VMEM((slots, nl, LANES), F32), pltpu.VMEM((slots, 2, ni, LANES), F32),
                pltpu.VMEM((CG_ITERS + 1, 1, LANES), F32), pltpu.VMEM((CG_ITERS + 1, devices, 1, LANES), F32),
                dma((slots, 2)), dma((slots,)), dma((slots, 2)), dma((slots, 2)), dma((slots,)), dma((slots, 2)),
                dma((CG_ITERS + 1,)), dma((CG_ITERS + 1,)),
            ],
            compiler_params=pltpu.CompilerParams(has_side_effects=True),
        )(walls, flip(k_cell), flip(f_rhs), flip(u_init))
        return flip(x_new), flip(r_new), hist

    return jax.shard_map(local_solve, mesh=mesh, in_specs=(grid_spec, P(), grid_spec, grid_spec),
                         out_specs=(grid_spec, grid_spec, P()), check_vma=False)
```

```python
import functools

import jax
import jax.numpy as jnp
from jax import lax
from jax.experimental import pallas as pl
from jax.experimental.pallas import tpu as pltpu
from jax.sharding import PartitionSpec as P

CG_ITERS = 8
LANES = 128
PAD = 8
MESH = pl.DeviceIdType.MESH
F32 = jnp.float32


def solve_kernel(dims, counts, kg_ref, k_ref, f_ref, u_ref, x_out, r_out, hist_ref,
                 kp, mp, cx, cy, cyh, cz, inv, x, r, w, s, z, p, n,
                 ys, zs, xr, yr, zr, red_s, red_r,
                 xs_sem, ys_sem, zs_sem, xr_sem, yr_sem, zr_sem, rs_sem, rr_sem):
    ni, nl, nj = dims
    ngx, ngy, ngz = counts
    gx, gy, gz = lax.axis_index('gx'), lax.axis_index('gy'), lax.axis_index('gz')
    rows = pl.ds(PAD, nl)
    rows_dn = pl.ds(PAD - 1, nl)
    rows_up = pl.ds(PAD + 1, nl)
    lane = lax.broadcasted_iota(jnp.int32, (nl, LANES), 1)
    lane_row = lax.broadcasted_iota(jnp.int32, (1, LANES), 1)
    inside = lane < nj
    has_xlo, has_xhi = gx > 0, gx < ngx - 1
    has_zlo, has_zhi = gz > 0, gz < ngz - 1
    face_lane = jnp.where(gy == 0, nj - 1, 0)

    def column_roll(slab, shift):
        return pltpu.roll(slab, lax.rem(shift + LANES, LANES), 1)

    def slabs(group, step, init):
        def body(g, carry):
            for k in range(group):
                carry = step(g * group + k, carry)
            return carry
        return lax.fori_loop(0, ni // group, body, init)

    def x_copy(ref, slot, up):
        src = ref.at[ni if up else 1, rows]
        return pltpu.make_async_remote_copy(
            src_ref=src, dst_ref=xr.at[slot, 0 if up else 1], send_sem=xs_sem.at[slot, 0 if up else 1],
            recv_sem=xr_sem.at[slot, 0 if up else 1], device_id=(gz, gy, gx + 1 if up else gx - 1), device_id_type=MESH)

    def z_copy(slot, up):
        return pltpu.make_async_remote_copy(
            src_ref=zs.at[slot, 0 if up else 1], dst_ref=zr.at[slot, 0 if up else 1],
            send_sem=zs_sem.at[slot, 0 if up else 1], recv_sem=zr_sem.at[slot, 0 if up else 1],
            device_id=(gz + 1 if up else gz - 1, gy, gx), device_id_type=MESH)

    def y_copy(slot):
        return pltpu.make_async_remote_copy(
            src_ref=ys.at[slot], dst_ref=yr.at[slot], send_sem=ys_sem.at[slot], recv_sem=yr_sem.at[slot],
            device_id=(gz, 1 - gy, gx), device_id_type=MESH)

    def exchange_start(ref, slot):
        pl.when(has_xlo)(lambda: x_copy(ref, slot, False).start())
        pl.when(has_xhi)(lambda: x_copy(ref, slot, True).start())

        def pack(i, acc):
            slab = ref[i + 1, rows, :]
            zs[slot, 1, pl.ds(i, 1), :] = slab[0:1, :]
            zs[slot, 0, pl.ds(i, 1), :] = slab[nl - 1:nl, :]
            return jnp.where(lane == i, column_roll(slab, i - face_lane), acc)

        ys[slot] = slabs(8, pack, jnp.zeros((nl, LANES), F32))
        pl.when(has_zlo)(lambda: z_copy(slot, False).start())
        pl.when(has_zhi)(lambda: z_copy(slot, True).start())
        y_copy(slot).start()

    def exchange_wait(ref, slot):
        @pl.when(has_xlo)
        def _():
            x_copy(ref, slot, False).wait_send()
            x_copy(ref, slot, True).wait_recv()
            ref[0, rows, :] = xr[slot, 0]

        @pl.when(has_xhi)
        def _():
            x_copy(ref, slot, True).wait_send()
            x_copy(ref, slot, False).wait_recv()
            ref[ni + 1, rows, :] = xr[slot, 1]

        @pl.when(has_zlo)
        def _():
            z_copy(slot, False).wait_send()
            z_copy(slot, True).wait_recv()
            for i in range(ni):
                ref[i + 1, PAD - 1:PAD, :] = zr[slot, 0, i:i + 1, :]

        @pl.when(has_zhi)
        def _():
            z_copy(slot, True).wait_send()
            z_copy(slot, False).wait_recv()
            for i in range(ni):
                ref[i + 1, PAD + nl:PAD + nl + 1, :] = zr[slot, 1, i:i + 1, :]

        y_copy(slot).wait()

    def y_sides(slab, below, above, i):
        low = jnp.where(lane == 0, column_roll(below, -i), pltpu.roll(slab, 1, 1))
        high = jnp.where(lane == nj - 1, column_roll(above, nj - 1 - i), pltpu.roll(slab, LANES - 1, 1))
        return low, high

    def stencil(ref, slot, emit, init):
        halo = yr[slot]
        below = ref[0, rows, :]
        lane_lo = jnp.where(gy == 0, -1, 0)
        lane_hi = jnp.where(gy == 0, nj - 1, -1)
        first = ref[1, rows, :]

        def step(i, carry):
            v, flux_x, state = carry
            above = ref[i + 2, rows, :]
            flux_next = cx[i + 1] * (above - v)
            flux_zl = cz[i, rows, :] * (v - ref[i + 1, rows_dn, :])
            flux_zh = cz[i, rows_up, :] * (ref[i + 1, rows_up, :] - v)
            column = column_roll(halo, face_lane - i)
            low = jnp.where(lane == lane_lo, column, pltpu.roll(v, 1, 1))
            high = jnp.where(lane == lane_hi, column, pltpu.roll(v, LANES - 1, 1))
            flux_yl = cy[i] * (v - low)
            flux_yh = cyh[i] * (high - v)
            total = (flux_x - flux_next) + (flux_yl - flux_yh) + (flux_zl - flux_zh)
            state = emit(i, total, v, state)
            return above, flux_next, state

        return slabs(4, step, (first, cx[0] * (first - below), init))[2]

    def fold(slab):
        out = slab[0:8]
        for part in range(8, nl, 8):
            out = out + slab[part:part + 8]
        return out

    def reduce_start(slot, accs):
        row = jnp.zeros((1, LANES), F32)
        for q, acc in enumerate(accs):
            row = jnp.where(lane_row == q, jnp.sum(jnp.sum(acc, axis=0, keepdims=True), axis=1, keepdims=True), row)
        me = (gz * ngy + gy) * ngx + gx
        red_s[slot] = row
        red_r[slot, me] = row
        for a in reversed(range(ngz)):
            for b in reversed(range(ngy)):
                for c in reversed(range(ngx)):
                    if a or b or c:
                        tgt = (lax.rem(gz + a, ngz), lax.rem(gy + b, ngy), lax.rem(gx + c, ngx))
                        pltpu.make_async_remote_copy(
                            src_ref=red_s.at[slot], dst_ref=red_r.at[slot, me], send_sem=rs_sem.at[slot],
                            recv_sem=rr_sem.at[slot], device_id=tgt, device_id_type=MESH).start()

    def reduce_wait(slot, count):
        others = ngx * ngy * ngz - 1
        whole = red_r.at[slot, pl.ds(0, others)]
        done = pltpu.make_async_remote_copy(
            src_ref=whole, dst_ref=whole, send_sem=rs_sem.at[slot], recv_sem=rr_sem.at[slot],
            device_id=(gz, gy, gx), device_id_type=MESH)
        done.wait_recv()
        done.wait_send()
        total = jnp.sum(red_r[slot], axis=0)
        return [jnp.sum(jnp.where(lane_row == q, total, 0.0), axis=1, keepdims=True) for q in range(count)]

    zero_slab = jnp.zeros((nl, LANES), F32)
    zero_acc = jnp.zeros((8, LANES), F32)

    def load(i, _):
        kp[i + 1, rows, :] = jnp.full((nl, LANES), 1.0, F32)
        kp[i + 1, rows, 0:nj] = k_ref[i]
        kp[i + 1, pl.ds(0, PAD), :] = jnp.ones((PAD, LANES), F32)
        kp[i + 1, pl.ds(PAD + nl, PAD), :] = jnp.ones((PAD, LANES), F32)
        mp[i + 1, rows, :] = zero_slab
        mp[i + 1, rows, 0:nj] = u_ref[i]
        mp[i + 1, pl.ds(0, PAD), :] = jnp.zeros((PAD, LANES), F32)
        mp[i + 1, pl.ds(PAD + nl, PAD), :] = jnp.zeros((PAD, LANES), F32)
        s[i] = zero_slab
        z[i] = zero_slab
        p[i] = zero_slab
        return 0

    lax.fori_loop(0, ni, load, 0)
    for edge in (0, ni + 1):
        mp[edge] = jnp.zeros((nl + 2 * PAD, LANES), F32)
        kp[edge] = jnp.ones((nl + 2 * PAD, LANES), F32)
    exchange_start(kp, 0)
    exchange_start(mp, 1)

    @pl.when(gx == 0)
    def _():
        kp[0, rows, 0:nj] = kg_ref[0, :, 0:nj]

    @pl.when(gx == ngx - 1)
    def _():
        kp[ni + 1, rows, 0:nj] = kg_ref[0, :, 0:nj]

    @pl.when(gz == 0)
    def _():
        for i in range(ni):
            kp[i + 1, PAD - 1:PAD, 0:nj] = kg_ref[2, i:i + 1, 0:nj]

    @pl.when(gz == ngz - 1)
    def _():
        for i in range(ni):
            kp[i + 1, PAD + nl:PAD + nl + 1, 0:nj] = kg_ref[2, i:i + 1, 0:nj]

    exchange_wait(kp, 0)
    y_below = jnp.where(gy == 0, kg_ref[1, 0:nl, :], yr[0])
    y_above = jnp.where(gy == 0, yr[0], kg_ref[1, 0:nl, :])

    def harmonic(left, right):
        return 2.0 * left * right / (left + right)

    cx[0] = jnp.where(inside, harmonic(kp[0, rows, :], kp[1, rows, :]), 0.0)

    def coefs(i, _):
        here = kp[i + 1, rows, :]
        x_hi = jnp.where(inside, harmonic(here, kp[i + 2, rows, :]), 0.0)
        cx[i + 1] = x_hi
        z_lo = jnp.where(inside, harmonic(kp[i + 1, rows_dn, :], here), 0.0)
        z_hi = jnp.where(inside, harmonic(here, kp[i + 1, rows_up, :]), 0.0)
        cz[i, rows, :] = z_lo
        cz[i, pl.ds(PAD + nl, 1), :] = z_hi[nl - 1:nl, :]
        low, high = y_sides(here, y_below, y_above, i)
        y_lo = jnp.where(inside, harmonic(low, here), 0.0)
        y_hi = jnp.where(inside, harmonic(here, high), 0.0)
        cy[i] = y_lo
        cyh[i] = y_hi
        diag = cx[i] + x_hi + y_lo + y_hi + z_lo + z_hi
        inv[i] = jnp.where(inside, 1.0 / jnp.where(inside, diag, 1.0), 0.0)
        return 0

    slabs(4, coefs, 0)
    exchange_wait(mp, 1)

    def first_residual(i, av, v, acc):
        x[i] = v
        r[i] = zero_slab
        r[i, :, 0:nj] = f_ref[i]
        res = r[i] - av
        r[i] = res
        u = res * inv[i]
        n[i] = u
        return (acc[0] + fold(res * u),)

    (gamma_acc,) = stencil(mp, 1, first_residual, (zero_acc,))

    def copy_u(i, _):
        mp[i + 1, rows, :] = n[i]
        return 0

    lax.fori_loop(0, ni, copy_u, 0)
    exchange_start(mp, 2)
    exchange_wait(mp, 2)

    def first_w(i, av, v, acc):
        w[i] = av
        n[i] = av * inv[i]
        return (acc[0] + fold(av * v),)

    (delta_acc,) = stencil(mp, 2, first_w, (zero_acc,))
    lax.fori_loop(0, ni, copy_u, 0)

    def scalars(t, sums, gamma_old, pap_old):
        gamma, delta, sigma = sums[0], sums[1], sums[2]
        beta = jnp.where(t == 0, 0.0, gamma / gamma_old)
        pap = delta + 2.0 * beta * sigma + beta * beta * pap_old
        return gamma, pap, beta, gamma / pap

    def advance_x(alpha):
        def step(i, _):
            x[i] = x[i] + alpha * p[i]
            return 0
        lax.fori_loop(0, ni, step, 0)

    def iteration(t, carry):
        accs, gamma_old, pap_old, alpha_old = carry
        reduce_start(t, accs)
        exchange_start(mp, t + 3)
        advance_x(alpha_old)
        exchange_wait(mp, t + 3)

        def store_n(i, av, v, state):
            n[i] = av
            return state

        stencil(mp, t + 3, store_n, 0)
        sums = reduce_wait(t, 4)

        @pl.when(t > 0)
        def _():
            hist_ref[lax.max(t - 1, 0)] = sums[3][0, 0]

        gamma, pap, beta_v, alpha_v = scalars(t, sums, gamma_old, pap_old)
        beta, alpha = beta_v[0, 0], alpha_v[0, 0]

        def update(i, acc):
            iv, r_old, w_old = inv[i], r[i], w[i]
            z_new = n[i] + beta * z[i]
            s_new = w_old + beta * s[i]
            p[i] = iv * r_old + beta * p[i]
            r_new = r_old - alpha * s_new
            w_new = w_old - alpha * z_new
            u_new = iv * r_new
            z[i] = z_new
            s[i] = s_new
            r[i] = r_new
            w[i] = w_new
            mp[i + 1, rows, :] = iv * w_new
            return (acc[0] + fold(r_new * u_new), acc[1] + fold(w_new * u_new),
                    acc[2] + fold(u_new * s_new), acc[3] + fold(r_new * r_new))

        accs = lax.fori_loop(0, ni, update, (zero_acc,) * 4)
        return accs, gamma, pap, alpha

    one = jnp.ones((1, 1), F32)
    accs, gamma_old, pap_old, alpha_old = lax.fori_loop(
        0, CG_ITERS - 1, iteration, ((gamma_acc, delta_acc, zero_acc, zero_acc), one, one, jnp.float32(0.0)))

    last = CG_ITERS - 1
    reduce_start(last, accs)
    advance_x(alpha_old)
    sums = reduce_wait(last, 4)
    hist_ref[last - 1] = sums[3][0, 0]
    _, _, beta_v, alpha_v = scalars(last, sums, gamma_old, pap_old)
    beta, alpha = beta_v[0, 0], alpha_v[0, 0]

    def final(i, acc):
        r_old = r[i]
        s_new = w[i] + beta * s[i]
        p_new = inv[i] * r_old + beta * p[i]
        r_new = r_old - alpha * s_new
        x_new = x[i] + alpha * p_new
        x_out[i] = x_new[:, 0:nj]
        r_out[i] = r_new[:, 0:nj]
        return acc + fold(r_new * r_new)

    acc = lax.fori_loop(0, ni, final, zero_acc)
    reduce_start(CG_ITERS, (acc,))
    hist_ref[last] = reduce_wait(CG_ITERS, 1)[0][0, 0]


def solution(mesh):
    counts = (mesh.shape['gx'], mesh.shape['gy'], mesh.shape['gz'])
    grid_spec = P('gx', 'gy', 'gz')

    def local_solve(k_cell, k_ghost, f_rhs, u_init):
        ni, nj, nl = k_cell.shape
        ngx, ngy, ngz = counts
        gx, gy, gz = lax.axis_index('gx'), lax.axis_index('gy'), lax.axis_index('gz')
        pad_to = lambda a: jnp.pad(a, ((0, max(ni, nl) - a.shape[0]), (0, LANES - a.shape[1])), constant_values=1.0)
        wall = lambda row, start, extent: lax.dynamic_slice(k_ghost, (row,) + start, (1,) + extent)[0]
        wall_x = wall(jnp.where(gx == 0, 0, 1), (gy * nj, gz * nl), (nj, nl)).T
        wall_y = wall(2 + gy, (gx * ni, gz * nl), (ni, nl)).T
        wall_z = wall(jnp.where(gz == 0, 4, 5), (gx * ni, gy * nj), (ni, nj))
        walls = jnp.stack([pad_to(wall_x), pad_to(wall_y), pad_to(wall_z)])
        flip = lambda a: jnp.swapaxes(a, 1, 2)

        slots = CG_ITERS + 2
        whole = (ni, nl, LANES)
        padded = (ni + 2, nl + 2 * PAD, LANES)
        dma = pltpu.SemaphoreType.DMA
        devices = ngx * ngy * ngz
        vmem = pl.BlockSpec(memory_space=pltpu.VMEM)
        out_block = jax.ShapeDtypeStruct((ni, nl, nj), F32)
        x_new, r_new, hist = pl.pallas_call(
            functools.partial(solve_kernel, (ni, nl, nj), counts),
            out_shape=(out_block, out_block, jax.ShapeDtypeStruct((CG_ITERS,), F32)),
            in_specs=[vmem] * 4,
            out_specs=(vmem, vmem, pl.BlockSpec(memory_space=pltpu.SMEM)),
            scratch_shapes=[
                pltpu.VMEM(padded, F32), pltpu.VMEM(padded, F32),
                pltpu.VMEM((ni + 1, nl, LANES), F32), pltpu.VMEM(whole, F32), pltpu.VMEM(whole, F32), pltpu.VMEM((ni, nl + 2 * PAD, LANES), F32),
                pltpu.VMEM(whole, F32),
                pltpu.VMEM(whole, F32), pltpu.VMEM(whole, F32), pltpu.VMEM(whole, F32), pltpu.VMEM(whole, F32),
                pltpu.VMEM(whole, F32), pltpu.VMEM(whole, F32), pltpu.VMEM(whole, F32),
                pltpu.VMEM((slots, nl, LANES), F32), pltpu.VMEM((slots, 2, ni, LANES), F32),
                pltpu.VMEM((slots, 2, nl, LANES), F32), pltpu.VMEM((slots, nl, LANES), F32), pltpu.VMEM((slots, 2, ni, LANES), F32),
                pltpu.VMEM((CG_ITERS + 1, 1, LANES), F32), pltpu.VMEM((CG_ITERS + 1, devices, 1, LANES), F32),
                dma((slots, 2)), dma((slots,)), dma((slots, 2)), dma((slots, 2)), dma((slots,)), dma((slots, 2)),
                dma((CG_ITERS + 1,)), dma((CG_ITERS + 1,)),
            ],
            compiler_params=pltpu.CompilerParams(has_side_effects=True),
        )(walls, flip(k_cell), flip(f_rhs), flip(u_init))
        return flip(x_new), flip(r_new), hist

    return jax.shard_map(local_solve, mesh=mesh, in_specs=(grid_spec, P(), grid_spec, grid_spec),
                         out_specs=(grid_spec, grid_spec, P()), check_vma=False)
```

```python
import functools

import jax
import jax.numpy as jnp
from jax import lax
from jax.experimental import pallas as pl
from jax.experimental.pallas import tpu as pltpu
from jax.sharding import PartitionSpec as P

CG_ITERS = 8
LANES = 128
PAD = 8
GROUP = 4
MESH = pl.DeviceIdType.MESH
F32 = jnp.float32


def solve_kernel(dims, counts, kg_hbm, k_hbm, f_hbm, u_hbm, x_hbm, r_hbm, hist_ref,
                 k_in, f_in, u_in, wall_x, wall_y, wall_z, wall_t, x_stage, r_stage,
                 kp, mp, cx, cy, cyh, cz, inv, x, r, w, s, z, p, n,
                 ys, zs, xr, yr, zr, red_s, red_r,
                 xs_sem, ys_sem, zs_sem, xr_sem, yr_sem, zr_sem, rs_sem, rr_sem, in_sem, out_sem):
    ni, nl, nj = dims
    ngx, ngy, ngz = counts
    half = nl // 2
    gx, gy, gz = lax.axis_index('gx'), lax.axis_index('gy'), lax.axis_index('gz')
    rows = pl.ds(PAD, nl)
    rows_dn = pl.ds(PAD - 1, nl)
    rows_up = pl.ds(PAD + 1, nl)
    lane = lax.broadcasted_iota(jnp.int32, (nl, LANES), 1)
    lane_i = lax.broadcasted_iota(jnp.int32, (ni, LANES), 1)
    lane_half = lax.broadcasted_iota(jnp.int32, (half, LANES), 1)
    lane_row = lax.broadcasted_iota(jnp.int32, (1, LANES), 1)
    inside = lane < nj
    has_xlo, has_xhi = gx > 0, gx < ngx - 1
    has_zlo, has_zhi = gz > 0, gz < ngz - 1
    face_lane = jnp.where(gy == 0, nj - 1, 0)
    lane_lo = jnp.where(gy == 0, -1, 0)
    lane_hi = jnp.where(gy == 0, nj - 1, -1)
    zero_slab = jnp.zeros((nl, LANES), F32)
    zero_acc = jnp.zeros((8, LANES), F32)
    relative = [(a, b, c) for a in reversed(range(ngz)) for b in reversed(range(ngy)) for c in reversed(range(ngx))
                if a or b or c]

    def other(a, b, c):
        return lax.rem(gz + a, ngz), lax.rem(gy + b, ngy), lax.rem(gx + c, ngx)

    def column_roll(slab, shift):
        return pltpu.roll(slab, lax.rem(shift + 2 * LANES, LANES), 1)

    def slabs(group, step, init):
        def body(g, carry):
            for k in range(group):
                carry = step(g * group + k, carry)
            return carry
        return lax.fori_loop(0, ni // group, body, init)

    def x_copy(ref, slot, up):
        src = ref.at[ni if up else 1, rows]
        return pltpu.make_async_remote_copy(
            src_ref=src, dst_ref=xr.at[slot, 0 if up else 1], send_sem=xs_sem.at[slot, 0 if up else 1],
            recv_sem=xr_sem.at[slot, 0 if up else 1], device_id=(gz, gy, gx + 1 if up else gx - 1), device_id_type=MESH)

    def z_copy(slot, up):
        return pltpu.make_async_remote_copy(
            src_ref=zs.at[slot, 0 if up else 1], dst_ref=zr.at[slot, 0 if up else 1],
            send_sem=zs_sem.at[slot, 0 if up else 1], recv_sem=zr_sem.at[slot, 0 if up else 1],
            device_id=(gz + 1 if up else gz - 1, gy, gx), device_id_type=MESH)

    def y_copy(slot):
        return pltpu.make_async_remote_copy(
            src_ref=ys.at[slot], dst_ref=yr.at[slot], send_sem=ys_sem.at[slot], recv_sem=yr_sem.at[slot],
            device_id=(gz, 1 - gy, gx), device_id_type=MESH)

    def pack(ref, slot, i, acc):
        row = lax.max(i, 0) if not isinstance(i, int) else i
        slab = ref[row + 1, rows, :]
        zs[slot, 1, pl.ds(row, 1), :] = slab[0:1, :]
        zs[slot, 0, pl.ds(row, 1), :] = slab[nl - 1:nl, :]
        acc = jnp.where(lane_half == i, column_roll(slab[0:half], row - face_lane), acc)
        return jnp.where(lane_half == i + LANES // 2, column_roll(slab[half:nl], row - face_lane + LANES // 2), acc)

    def packed_pass(ref, slot, step, init):
        def body(g, carry):
            state, acc = carry
            for k in range(GROUP):
                acc = pack(ref, slot, (g - 1) * GROUP + k, acc)
            for k in range(GROUP):
                state = step(g * GROUP + k, state)
            return state, acc
        state, acc = lax.fori_loop(0, ni // GROUP, body, (init, jnp.zeros((half, LANES), F32)))
        for k in range(GROUP):
            acc = pack(ref, slot, ni - GROUP + k, acc)
        ys[slot] = acc
        return state

    def exchange_start(ref, slot):
        pl.when(has_xlo)(lambda: x_copy(ref, slot, False).start())
        pl.when(has_xhi)(lambda: x_copy(ref, slot, True).start())
        pl.when(has_zlo)(lambda: z_copy(slot, False).start())
        pl.when(has_zhi)(lambda: z_copy(slot, True).start())
        y_copy(slot).start()

    def exchange_wait(ref, slot, margins=True):
        @pl.when(has_xlo)
        def _():
            x_copy(ref, slot, False).wait_send()
            x_copy(ref, slot, True).wait_recv()
            if margins:
                ref[0, rows, :] = xr[slot, 0]

        @pl.when(has_xhi)
        def _():
            x_copy(ref, slot, True).wait_send()
            x_copy(ref, slot, False).wait_recv()
            if margins:
                ref[ni + 1, rows, :] = xr[slot, 1]

        @pl.when(has_zlo)
        def _():
            z_copy(slot, False).wait_send()
            z_copy(slot, True).wait_recv()
            if margins:
                for i in range(ni):
                    ref[i + 1, PAD - 1:PAD, :] = zr[slot, 0, i:i + 1, :]

        @pl.when(has_zhi)
        def _():
            z_copy(slot, True).wait_send()
            z_copy(slot, False).wait_recv()
            if margins:
                for i in range(ni):
                    ref[i + 1, PAD + nl:PAD + nl + 1, :] = zr[slot, 1, i:i + 1, :]

        y_copy(slot).wait()

    def face_column(packed, i):
        return jnp.concatenate([column_roll(packed, face_lane - i), column_roll(packed, face_lane - i - LANES // 2)], axis=0)

    def stencil_step(ref, halo, i, v, flux_x, cy_i, cyh_i):
        above = ref[i + 2, rows, :]
        flux_next = cx[i + 1] * (above - v)
        flux_zl = cz[i, rows, :] * (v - ref[i + 1, rows_dn, :])
        flux_zh = cz[i, rows_up, :] * (ref[i + 1, rows_up, :] - v)
        column = face_column(halo, i)
        low = jnp.where(lane == lane_lo, column, pltpu.roll(v, 1, 1))
        high = jnp.where(lane == lane_hi, column, pltpu.roll(v, LANES - 1, 1))
        flux_yl = cy_i * (v - low)
        flux_yh = cyh_i * (high - v)
        return (flux_x - flux_next) + (flux_yl - flux_yh) + (flux_zl - flux_zh), above, flux_next

    def stencil_first(ref):
        first = ref[1, rows, :]
        return first, cx[0] * (first - ref[0, rows, :])

    def fold(slab):
        out = slab[0:8]
        for part in range(8, nl, 8):
            out = out + slab[part:part + 8]
        return out

    def reduce_start(slot, accs):
        row = jnp.zeros((1, LANES), F32)
        for q, acc in enumerate(accs):
            row = jnp.where(lane_row == q, jnp.sum(jnp.sum(acc, axis=0, keepdims=True), axis=1, keepdims=True), row)
        me = (gz * ngy + gy) * ngx + gx
        red_s[slot] = row
        red_r[slot, me] = row
        for delta in relative:
            pltpu.make_async_remote_copy(
                src_ref=red_s.at[slot], dst_ref=red_r.at[slot, me], send_sem=rs_sem.at[slot],
                recv_sem=rr_sem.at[slot], device_id=other(*delta), device_id_type=MESH).start()

    def reduce_wait(slot, count):
        whole = red_r.at[slot, pl.ds(0, len(relative))]
        done = pltpu.make_async_remote_copy(
            src_ref=whole, dst_ref=whole, send_sem=rs_sem.at[slot], recv_sem=rr_sem.at[slot],
            device_id=(gz, gy, gx), device_id_type=MESH)
        done.wait_recv()
        done.wait_send()
        total = jnp.sum(red_r[slot], axis=0)
        return [jnp.sum(jnp.where(lane_row == q, total, 0.0), axis=1, keepdims=True) for q in range(count)]

    x_row, z_row = jnp.where(gx == 0, 0, 1), jnp.where(gz == 0, 4, 5)
    slabs_i = pl.ds(pl.multiple_of(gx * ni, 8), ni)
    inputs = [
        pltpu.make_async_copy(k_hbm, k_in, in_sem.at[0]),
        pltpu.make_async_copy(u_hbm, u_in, in_sem.at[1]),
        pltpu.make_async_copy(kg_hbm.at[x_row, pl.ds(pl.multiple_of(gy * nj, 8), nj)], wall_x, in_sem.at[2]),
        pltpu.make_async_copy(kg_hbm.at[2 + gy, slabs_i], wall_y, in_sem.at[3]),
        pltpu.make_async_copy(kg_hbm.at[z_row, slabs_i], wall_z, in_sem.at[4]),
        pltpu.make_async_copy(f_hbm, f_in, in_sem.at[5]),
    ]
    for copy in inputs:
        copy.start()

    barrier = pltpu.get_barrier_semaphore()
    for delta in relative:
        pl.semaphore_signal(barrier, inc=1, device_id=other(*delta), device_id_type=MESH)

    for edge in (0, ni + 1):
        mp[edge] = jnp.zeros((nl + 2 * PAD, LANES), F32)
        kp[edge] = jnp.ones((nl + 2 * PAD, LANES), F32)

    def clear(i, _):
        mp[i + 1, pl.ds(0, PAD), :] = jnp.zeros((PAD, LANES), F32)
        mp[i + 1, pl.ds(PAD + nl, PAD), :] = jnp.zeros((PAD, LANES), F32)
        kp[i + 1, pl.ds(0, PAD), :] = jnp.ones((PAD, LANES), F32)
        kp[i + 1, pl.ds(PAD + nl, PAD), :] = jnp.ones((PAD, LANES), F32)
        mp[i + 1, rows, :] = zero_slab
        s[i] = zero_slab
        z[i] = zero_slab
        p[i] = zero_slab
        r[1, i] = zero_slab
        r[0, i] = zero_slab
        kp[i + 1, rows, :] = jnp.full((nl, LANES), 1.0, F32)
        return 0

    lax.fori_loop(0, ni, clear, 0)

    def load_k(i, _):
        kp[i + 1, rows, 0:nj] = k_in[i]
        return 0

    def load_u(i, _):
        mp[i + 1, rows, 0:nj] = u_in[i]
        return 0

    inputs[0].wait()
    packed_pass(kp, 0, load_k, 0)
    pl.semaphore_wait(barrier, len(relative))
    exchange_start(kp, 0)
    inputs[1].wait()
    packed_pass(mp, 1, load_u, 0)
    exchange_start(mp, 1)

    for copy in inputs[2:5]:
        copy.wait()
    width = wall_x.shape[1]
    l_rows = pl.ds(pl.multiple_of(gz * nl, 8), nl)

    def flipped(wall, count):
        for start in range(0, width, LANES):
            size = min(LANES, width - start)
            block = jnp.concatenate([wall[:, start:start + size], jnp.ones((LANES - count, size), F32)], axis=0)
            wall_t[start:start + size, :] = block.T
        return wall_t[l_rows, :]

    x_wall = flipped(wall_x, nj)
    y_wall = flipped(wall_y, ni)
    if width > LANES:
        rest = jnp.concatenate([wall_z[:, LANES:width], jnp.ones((ni, 2 * LANES - width), F32)], axis=1)
        whole_z = wall_z[:, 0:LANES]
        turn = LANES - nj
        shifted = jnp.where(lane_i < turn, pltpu.roll(whole_z, turn, 1), pltpu.roll(rest, turn, 1))
    else:
        whole_z = jnp.concatenate([wall_z[...], jnp.ones((ni, LANES - width), F32)], axis=1)
        shifted = pltpu.roll(whole_z, LANES - nj, 1)
    z_wall = jnp.where(gy == 0, whole_z, shifted)

    def harmonic(left, right):
        return 2.0 * left * right / (left + right)

    def coefs(i, _):
        here = kp[i + 1, rows, :]
        cx[i + 1] = jnp.where(inside, harmonic(here, kp[i + 2, rows, :]), 0.0)
        z_hi = jnp.where(inside, harmonic(here, kp[i + 1, rows_up, :]), 0.0)
        cz[i, rows_up, :] = z_hi
        wall = column_roll(y_wall, nj - 1 - face_lane - i)
        low = jnp.where(lane == 0, wall, pltpu.roll(here, 1, 1))
        high = jnp.where(lane == nj - 1, wall, pltpu.roll(here, LANES - 1, 1))
        cy[i] = jnp.where(inside, harmonic(low, here), 0.0)
        cyh[i] = jnp.where(inside, harmonic(here, high), 0.0)
        return 0

    slabs(GROUP, coefs, 0)
    exchange_wait(kp, 0, margins=False)
    cx[0] = jnp.where(inside, harmonic(jnp.where(gx == 0, x_wall, xr[0, 0]), kp[1, rows, :]), 0.0)
    cx[ni] = jnp.where(inside, harmonic(kp[ni, rows, :], jnp.where(gx == ngx - 1, x_wall, xr[0, 1])), 0.0)
    z_low = jnp.where(lane_i < nj, harmonic(jnp.where(gz == 0, z_wall, zr[0, 0]), zs[0, 1]), 0.0)
    z_high = jnp.where(lane_i < nj, harmonic(zs[0, 0], jnp.where(gz == ngz - 1, z_wall, zr[0, 1])), 0.0)
    for i in range(ni):
        cz[i, PAD:PAD + 1, :] = z_low[i:i + 1, :]
        cz[i, PAD + nl:PAD + nl + 1, :] = z_high[i:i + 1, :]
    y_face = harmonic(ys[0], yr[0])
    exchange_wait(mp, 1)
    inputs[5].wait()

    u_halo = yr[1]

    def first_residual(i, carry):
        v, flux_x, acc = carry
        column = face_column(y_face, i)
        cy_i = jnp.where(lane == lane_lo, column, cy[i])
        cyh_i = jnp.where(lane == lane_hi, column, cyh[i])
        cy[i] = cy_i
        cyh[i] = cyh_i
        av, above, flux_next = stencil_step(mp, u_halo, i, v, flux_x, cy_i, cyh_i)
        diag = cx[i] + cx[i + 1] + cy_i + cyh_i + cz[i, rows, :] + cz[i, rows_up, :]
        iv = jnp.where(inside, 1.0 / jnp.where(inside, diag, 1.0), 0.0)
        inv[i] = iv
        x[i] = v
        r[0, i, :, 0:nj] = f_in[i]
        res = r[0, i] - av
        r[0, i] = res
        u = res * iv
        mp[i + 1, rows, :] = u
        return above, flux_next, acc + fold(res * u)

    gamma_acc = packed_pass(mp, 2, first_residual, stencil_first(mp) + (zero_acc,))[2]
    exchange_start(mp, 2)
    exchange_wait(mp, 2)
    z_halo = yr[2]

    def first_w(i, carry):
        v, flux_x, acc = carry
        av, above, flux_next = stencil_step(mp, z_halo, i, v, flux_x, cy[i], cyh[i])
        w[i] = av
        mp[i + 1, rows, :] = av * inv[i]
        return above, flux_next, acc + fold(av * v)

    delta_acc = packed_pass(mp, 3, first_w, stencil_first(mp) + (zero_acc,))[2]

    def scalars(t, sums, gamma_old, pap_old):
        gamma, delta, sigma = sums[0], sums[1], sums[2]
        beta = jnp.where(t == 0, 0.0, gamma / gamma_old)
        pap = delta + 2.0 * beta * sigma + beta * beta * pap_old
        return gamma, pap, beta[0, 0], (gamma / pap)[0, 0]

    def advance_x(now, alpha, beta):
        def step(i, _):
            p_new = inv[i] * r[1 - now, i] + beta * p[i]
            p[i] = p_new
            x[i] = x[i] + alpha * p_new
            return 0
        lax.fori_loop(0, ni, step, 0)

    def iteration(t, carry):
        accs, gamma_old, pap_old, alpha_old, beta_old = carry
        now = lax.rem(t, 2)
        exchange_start(mp, t + 3)
        reduce_start(t, accs)
        advance_x(now, alpha_old, beta_old)
        exchange_wait(mp, t + 3)
        halo = yr[t + 3]

        def apply(i, carry):
            av, above, flux_next = stencil_step(mp, halo, i, carry[0], carry[1], cy[i], cyh[i])
            n[i] = av
            return above, flux_next

        slabs(GROUP, apply, stencil_first(mp))
        sums = reduce_wait(t, 4)
        gamma, pap, beta, alpha = scalars(t, sums, gamma_old, pap_old)

        def update(i, acc):
            iv = inv[i]
            z_new = n[i] + beta * z[i]
            s_new = w[i] + beta * s[i]
            r_new = r[now, i] - alpha * s_new
            w_new = w[i] - alpha * z_new
            u_new = iv * r_new
            z[i] = z_new
            s[i] = s_new
            r[1 - now, i] = r_new
            w[i] = w_new
            mp[i + 1, rows, :] = iv * w_new
            return (acc[0] + fold(r_new * u_new), acc[1] + fold(w_new * u_new),
                    acc[2] + fold(u_new * s_new), acc[3] + fold(r_new * r_new))

        accs = packed_pass(mp, t + 4, update, (zero_acc,) * 4)

        @pl.when(t > 0)
        def _():
            hist_ref[lax.max(t - 1, 0)] = sums[3][0, 0]

        return accs, gamma, pap, alpha, beta

    one = jnp.ones((1, 1), F32)
    last = CG_ITERS - 1
    accs, gamma_old, pap_old, alpha_old, beta_old = lax.fori_loop(
        0, last, iteration, ((gamma_acc, delta_acc, zero_acc, zero_acc), one, one, jnp.float32(0.0), jnp.float32(0.0)))

    now = last % 2
    reduce_start(last, accs)
    advance_x(now, alpha_old, beta_old)
    sums = reduce_wait(last, 4)
    hist_ref[last - 1] = sums[3][0, 0]
    _, _, beta, alpha = scalars(last, sums, gamma_old, pap_old)

    def final(i, acc):
        r_old = r[now, i]
        s_new = w[i] + beta * s[i]
        p_new = inv[i] * r_old + beta * p[i]
        r_new = r_old - alpha * s_new
        x_new = x[i] + alpha * p_new
        x_stage[i] = x_new[:, 0:nj]
        r_stage[i] = r_new[:, 0:nj]
        return acc + fold(r_new * r_new)

    acc = lax.fori_loop(0, ni, final, zero_acc)
    outputs = [pltpu.make_async_copy(x_stage, x_hbm, out_sem.at[0]), pltpu.make_async_copy(r_stage, r_hbm, out_sem.at[1])]
    for copy in outputs:
        copy.start()
    reduce_start(CG_ITERS, (acc,))
    hist_ref[last] = reduce_wait(CG_ITERS, 1)[0][0, 0]
    for copy in outputs:
        copy.wait()


def solution(mesh):
    counts = (mesh.shape['gx'], mesh.shape['gy'], mesh.shape['gz'])
    grid_spec = P('gx', 'gy', 'gz')

    def local_solve(k_cell, k_ghost, f_rhs, u_init):
        ni, nj, nl = k_cell.shape
        flip = lambda a: jnp.swapaxes(a, 1, 2)
        slots = CG_ITERS + 3
        devices = counts[0] * counts[1] * counts[2]
        width = k_ghost.shape[2]
        any_spec = pl.BlockSpec(memory_space=pl.ANY)
        vm = lambda *shape: pltpu.VMEM(shape, F32)
        whole = vm(ni, nl, LANES)
        block = vm(ni, nl, nj)
        padded = vm(ni + 2, nl + 2 * PAD, LANES)
        dma = pltpu.SemaphoreType.DMA
        out_block = jax.ShapeDtypeStruct((ni, nl, nj), F32)
        x_new, r_new, hist = pl.pallas_call(
            functools.partial(solve_kernel, (ni, nl, nj), counts),
            out_shape=(out_block, out_block, jax.ShapeDtypeStruct((CG_ITERS,), F32)),
            in_specs=[any_spec] * 4,
            out_specs=(any_spec, any_spec, pl.BlockSpec(memory_space=pltpu.SMEM)),
            scratch_shapes=[
                block, block, block, vm(nj, width), vm(ni, width), vm(ni, width), vm(-(-width // LANES) * LANES, LANES), block, block,
                padded, padded, vm(ni + 1, nl, LANES), whole, whole, vm(ni, nl + 2 * PAD, LANES), whole,
                whole, vm(2, ni, nl, LANES), whole, whole, whole, whole, whole,
                vm(slots, nl // 2, LANES), vm(slots, 2, ni, LANES),
                vm(slots, 2, nl, LANES), vm(slots, nl // 2, LANES), vm(slots, 2, ni, LANES),
                vm(CG_ITERS + 1, 1, LANES), vm(CG_ITERS + 1, devices, 1, LANES),
                dma((slots, 2)), dma((slots,)), dma((slots, 2)), dma((slots, 2)), dma((slots,)), dma((slots, 2)),
                dma((CG_ITERS + 1,)), dma((CG_ITERS + 1,)), dma((6,)), dma((2,)),
            ],
            compiler_params=pltpu.CompilerParams(has_side_effects=True, collective_id=0),
        )(k_ghost, flip(k_cell), flip(f_rhs), flip(u_init))
        return flip(x_new), flip(r_new), hist

    return jax.shard_map(local_solve, mesh=mesh, in_specs=(grid_spec, P(), grid_spec, grid_spec),
                         out_specs=(grid_spec, grid_spec, P()), check_vma=False)
```

```python
import functools

import jax
import jax.numpy as jnp
from jax import lax
from jax.experimental import pallas as pl
from jax.experimental.pallas import tpu as pltpu
from jax.sharding import PartitionSpec as P

CG_ITERS = 8
LANES = 128
PAD = 8
GROUP = 6
COLUMNS = 16
MESH = pl.DeviceIdType.MESH
F32 = jnp.float32


def solve_kernel(dims, counts, kg_hbm, k_hbm, f_hbm, u_hbm, x_hbm, u_last_hbm, p_hbm, r_hbm, w_hbm, s_hbm, hist_ref, alpha_ref, beta_ref,
                 k_in, f_in, u_in, wall_x, wall_y, wall_z, wall_t, bx, by, bz,
                 kp, mp, cx, cy, cyh, cz, inv, x, r, w, s, z, p, n,
                 ys, zs, xr, yr, zr, red_s, red_r,
                 xs_sem, ys_sem, zs_sem, xr_sem, yr_sem, zr_sem, rs_sem, rr_sem, in_sem, out_sem):
    ni, nl, nj = dims
    ngx, ngy, ngz = counts
    half = nl // 2
    gx, gy, gz = lax.axis_index('gx'), lax.axis_index('gy'), lax.axis_index('gz')
    rows = pl.ds(PAD, nl)
    rows_dn = pl.ds(PAD - 1, nl)
    rows_up = pl.ds(PAD + 1, nl)
    lane = lax.broadcasted_iota(jnp.int32, (nl, LANES), 1)
    lane_i = lax.broadcasted_iota(jnp.int32, (ni, LANES), 1)
    lane_half = lax.broadcasted_iota(jnp.int32, (half, LANES), 1)
    lane_row = lax.broadcasted_iota(jnp.int32, (1, LANES), 1)
    inside = lane < nj
    has_xlo, has_xhi = gx > 0, gx < ngx - 1
    has_zlo, has_zhi = gz > 0, gz < ngz - 1
    face_lane = jnp.where(gy == 0, nj - 1, 0)
    y_low_wall, y_high_wall = gy == 0, gy > 0
    zero_slab = jnp.zeros((nl, LANES), F32)
    zero_acc = jnp.zeros((8, LANES), F32)
    relative = [(a, b, c) for a in reversed(range(ngz)) for b in reversed(range(ngy)) for c in reversed(range(ngx))
                if a or b or c]

    def other(a, b, c):
        return lax.rem(gz + a, ngz), lax.rem(gy + b, ngy), lax.rem(gx + c, ngx)

    def column_roll(slab, shift):
        return pltpu.roll(slab, lax.rem(shift + 2 * LANES, LANES), 1)

    def slabs(group, step, init):
        def body(g, carry):
            for k in range(group):
                carry = step(g * group + k, carry)
            return carry
        return lax.fori_loop(0, ni // group, body, init)

    def x_copy(ref, slot, up):
        src = ref.at[ni if up else 1, rows]
        return pltpu.make_async_remote_copy(
            src_ref=src, dst_ref=xr.at[slot, 0 if up else 1], send_sem=xs_sem.at[slot, 0 if up else 1],
            recv_sem=xr_sem.at[slot, 0 if up else 1], device_id=(gz, gy, gx + 1 if up else gx - 1), device_id_type=MESH)

    def z_copy(slot, up):
        return pltpu.make_async_remote_copy(
            src_ref=zs.at[slot, 0 if up else 1], dst_ref=zr.at[slot, 0 if up else 1],
            send_sem=zs_sem.at[slot, 0 if up else 1], recv_sem=zr_sem.at[slot, 0 if up else 1],
            device_id=(gz + 1 if up else gz - 1, gy, gx), device_id_type=MESH)

    def y_copy(slot):
        return pltpu.make_async_remote_copy(
            src_ref=ys.at[slot], dst_ref=yr.at[slot], send_sem=ys_sem.at[slot], recv_sem=yr_sem.at[slot],
            device_id=(gz, 1 - gy, gx), device_id_type=MESH)

    def pack_rolls(ref, slot, i):
        row = lax.max(i, 0) if not isinstance(i, int) else i
        slab = ref[row + 1, rows, :]
        zs[slot, 1, pl.ds(row, 1), :] = slab[0:1, :]
        zs[slot, 0, pl.ds(row, 1), :] = slab[nl - 1:nl, :]
        return column_roll(slab[0:half], row - face_lane), column_roll(slab[half:nl], row - face_lane + LANES // 2)

    def pack(i, rolled, acc):
        acc = jnp.where(lane_half == i, rolled[0], acc)
        return jnp.where(lane_half == i + LANES // 2, rolled[1], acc)

    def packed_pass(ref, slot, step, init):
        def body(g, carry):
            state, acc = carry
            rolled = [pack_rolls(ref, slot, (g - 1) * GROUP + k) for k in range(GROUP)]
            for k in range(GROUP):
                state = step(g * GROUP + k, state)
            for k in range(GROUP):
                acc = pack((g - 1) * GROUP + k, rolled[k], acc)
            return state, acc
        state, acc = lax.fori_loop(0, ni // GROUP, body, (init, jnp.zeros((half, LANES), F32)))
        rolled = [pack_rolls(ref, slot, ni - GROUP + k) for k in range(GROUP)]
        for k in range(GROUP):
            acc = pack(ni - GROUP + k, rolled[k], acc)
        ys[slot] = acc
        return state

    def exchange_start(ref, slot):
        pl.when(has_xlo)(lambda: x_copy(ref, slot, False).start())
        pl.when(has_xhi)(lambda: x_copy(ref, slot, True).start())
        pl.when(has_zlo)(lambda: z_copy(slot, False).start())
        pl.when(has_zhi)(lambda: z_copy(slot, True).start())
        y_copy(slot).start()

    def exchange_wait(ref, slot):
        @pl.when(has_xlo)
        def _():
            x_copy(ref, slot, False).wait_send()
            x_copy(ref, slot, True).wait_recv()

        @pl.when(has_xhi)
        def _():
            x_copy(ref, slot, True).wait_send()
            x_copy(ref, slot, False).wait_recv()

        @pl.when(has_zlo)
        def _():
            z_copy(slot, False).wait_send()
            z_copy(slot, True).wait_recv()

        @pl.when(has_zhi)
        def _():
            z_copy(slot, True).wait_send()
            z_copy(slot, False).wait_recv()

        y_copy(slot).wait()

    def add_rows(ref, layer, row):
        for i in range(ni):
            ref[i, row:row + 1, :] = ref[i, row:row + 1, :] + layer[i:i + 1, :]

    def add_columns(ref, packed):
        mask = lane == face_lane

        def step(g, _):
            columns = []
            for k in range(min(COLUMNS, ni)):
                i = g * min(COLUMNS, ni) + k
                columns.append((column_roll(packed, face_lane - i), column_roll(packed, face_lane - i - LANES // 2)))
            for k in range(min(COLUMNS, ni)):
                i = g * min(COLUMNS, ni) + k
                ref[i] = ref[i] + jnp.where(mask, jnp.concatenate(columns[k], axis=0), 0.0)
            return 0

        lax.fori_loop(0, ni // min(COLUMNS, ni), step, 0)

    def join_faces(ref, slot):
        y_copy(slot).wait()
        add_columns(n, by[...] * (ys[slot] - yr[slot]))

        @pl.when(has_xlo)
        def _():
            x_copy(ref, slot, False).wait_send()
            x_copy(ref, slot, True).wait_recv()
            n[0] = n[0] + bx[0] * (ref[1, rows, :] - xr[slot, 0])

        @pl.when(has_xhi)
        def _():
            x_copy(ref, slot, True).wait_send()
            x_copy(ref, slot, False).wait_recv()
            n[ni - 1] = n[ni - 1] + bx[1] * (ref[ni, rows, :] - xr[slot, 1])

        @pl.when(has_zlo)
        def _():
            z_copy(slot, False).wait_send()
            z_copy(slot, True).wait_recv()
            add_rows(n, bz[0] * (zs[slot, 1] - zr[slot, 0]), 0)

        @pl.when(has_zhi)
        def _():
            z_copy(slot, True).wait_send()
            z_copy(slot, False).wait_recv()
            add_rows(n, bz[1] * (zs[slot, 0] - zr[slot, 1]), nl - 1)

    def stencil(ref):
        def step(i, carry):
            v, flux_x = carry
            above = ref[i + 2, rows, :]
            flux_next = cx[i + 1] * (above - v)
            flux_zl = cz[i, rows, :] * (v - ref[i + 1, rows_dn, :])
            flux_zh = cz[i, rows_up, :] * (ref[i + 1, rows_up, :] - v)
            flux_yl = cy[i] * (v - pltpu.roll(v, 1, 1))
            flux_yh = cyh[i] * (pltpu.roll(v, LANES - 1, 1) - v)
            n[i] = (flux_x - flux_next) + (flux_yl - flux_yh) + (flux_zl - flux_zh)
            return above, flux_next

        first = ref[1, rows, :]
        slabs(GROUP, step, (first, cx[0] * (first - ref[0, rows, :])))

    def fold(slab):
        out = slab[0:8]
        for part in range(8, nl, 8):
            out = out + slab[part:part + 8]
        return out

    def reduce_start(slot, accs):
        row = jnp.zeros((1, LANES), F32)
        for q, acc in enumerate(accs):
            row = jnp.where(lane_row == q, jnp.sum(jnp.sum(acc, axis=0, keepdims=True), axis=1, keepdims=True), row)
        me = (gz * ngy + gy) * ngx + gx
        red_s[slot] = row
        red_r[slot, me] = row
        for delta in relative:
            pltpu.make_async_remote_copy(
                src_ref=red_s.at[slot], dst_ref=red_r.at[slot, me], send_sem=rs_sem.at[slot],
                recv_sem=rr_sem.at[slot], device_id=other(*delta), device_id_type=MESH).start()

    def reduce_wait(slot, count):
        whole = red_r.at[slot, pl.ds(0, len(relative))]
        done = pltpu.make_async_remote_copy(
            src_ref=whole, dst_ref=whole, send_sem=rs_sem.at[slot], recv_sem=rr_sem.at[slot],
            device_id=(gz, gy, gx), device_id_type=MESH)
        done.wait_recv()
        done.wait_send()
        total = jnp.sum(red_r[slot], axis=0)
        return [jnp.sum(jnp.where(lane_row == q, total, 0.0), axis=1, keepdims=True) for q in range(count)]

    x_row, z_row = jnp.where(gx == 0, 0, 1), jnp.where(gz == 0, 4, 5)
    slabs_i = pl.ds(pl.multiple_of(gx * ni, 8), ni)
    inputs = [
        pltpu.make_async_copy(k_hbm, k_in, in_sem.at[0]),
        pltpu.make_async_copy(u_hbm, u_in, in_sem.at[1]),
        pltpu.make_async_copy(kg_hbm.at[x_row, pl.ds(pl.multiple_of(gy * nj, 8), nj)], wall_x, in_sem.at[2]),
        pltpu.make_async_copy(kg_hbm.at[2 + gy, slabs_i], wall_y, in_sem.at[3]),
        pltpu.make_async_copy(kg_hbm.at[z_row, slabs_i], wall_z, in_sem.at[4]),
        pltpu.make_async_copy(f_hbm, f_in, in_sem.at[5]),
    ]
    for copy in inputs:
        copy.start()

    barrier = pltpu.get_barrier_semaphore()
    for delta in relative:
        pl.semaphore_signal(barrier, inc=1, device_id=other(*delta), device_id_type=MESH)

    for edge in (0, ni + 1):
        mp[edge] = jnp.zeros((nl + 2 * PAD, LANES), F32)
        kp[edge] = jnp.ones((nl + 2 * PAD, LANES), F32)

    def clear(i, _):
        mp[i + 1, pl.ds(0, PAD), :] = jnp.zeros((PAD, LANES), F32)
        mp[i + 1, pl.ds(PAD + nl, PAD), :] = jnp.zeros((PAD, LANES), F32)
        kp[i + 1, pl.ds(0, PAD), :] = jnp.ones((PAD, LANES), F32)
        kp[i + 1, pl.ds(PAD + nl, PAD), :] = jnp.ones((PAD, LANES), F32)
        mp[i + 1, rows, :] = zero_slab
        s[i] = zero_slab
        z[i] = zero_slab
        p[i] = zero_slab
        r[1, i] = zero_slab
        r[0, i] = zero_slab
        kp[i + 1, rows, :] = jnp.full((nl, LANES), 1.0, F32)
        return 0

    lax.fori_loop(0, ni, clear, 0)

    def load_k(i, _):
        kp[i + 1, rows, 0:nj] = k_in[i]
        return 0

    def load_u(i, _):
        mp[i + 1, rows, 0:nj] = u_in[i]
        return 0

    inputs[0].wait()
    packed_pass(kp, 0, load_k, 0)
    pl.semaphore_wait(barrier, len(relative))
    exchange_start(kp, 0)
    inputs[1].wait()
    packed_pass(mp, 1, load_u, 0)
    exchange_start(mp, 1)

    for copy in inputs[2:5]:
        copy.wait()
    width = wall_x.shape[1]
    l_rows = pl.ds(pl.multiple_of(gz * nl, 8), nl)

    def flipped(wall, count):
        for start in range(0, width, LANES):
            size = min(LANES, width - start)
            block = jnp.concatenate([wall[:, start:start + size], jnp.ones((LANES - count, size), F32)], axis=0)
            wall_t[start:start + size, :] = block.T
        return wall_t[l_rows, :]

    x_wall = flipped(wall_x, nj)
    y_wall = flipped(wall_y, ni)
    if width > LANES:
        rest = jnp.concatenate([wall_z[:, LANES:width], jnp.ones((ni, 2 * LANES - width), F32)], axis=1)
        whole_z = wall_z[:, 0:LANES]
        turn = LANES - nj
        shifted = jnp.where(lane_i < turn, pltpu.roll(whole_z, turn, 1), pltpu.roll(rest, turn, 1))
    else:
        whole_z = jnp.concatenate([wall_z[...], jnp.ones((ni, LANES - width), F32)], axis=1)
        shifted = pltpu.roll(whole_z, LANES - nj, 1)
    z_wall = jnp.where(gy == 0, whole_z, shifted)

    def harmonic(left, right):
        return 2.0 * left * right / (left + right)

    in_i = lane_i < nj
    cx[0] = jnp.where(jnp.logical_and(inside, gx == 0), harmonic(x_wall, kp[1, rows, :]), 0.0)
    z_low = jnp.where(jnp.logical_and(in_i, gz == 0), harmonic(z_wall, zs[0, 1]), 0.0)
    z_high = jnp.where(jnp.logical_and(in_i, gz == ngz - 1), harmonic(zs[0, 0], z_wall), 0.0)
    y_low_mask = jnp.logical_and(inside, jnp.logical_or(lane > 0, y_low_wall))
    y_high_mask = jnp.logical_and(inside, jnp.logical_or(lane < nj - 1, y_high_wall))
    wall_lane = nj - 1 - face_lane

    def coefs(i, _):
        here = kp[i + 1, rows, :]
        cx[i + 1] = jnp.where(inside, harmonic(here, kp[i + 2, rows, :]), 0.0)
        cz[i, rows_up, :] = jnp.where(inside, harmonic(here, kp[i + 1, rows_up, :]), 0.0)
        wall = column_roll(y_wall, wall_lane - i)
        low = jnp.where(lane == 0, wall, pltpu.roll(here, 1, 1))
        high = jnp.where(lane == nj - 1, wall, pltpu.roll(here, LANES - 1, 1))
        cy[i] = jnp.where(y_low_mask, harmonic(low, here), 0.0)
        cyh[i] = jnp.where(y_high_mask, harmonic(here, high), 0.0)
        return 0

    slabs(GROUP, coefs, 0)
    cx[ni] = jnp.where(jnp.logical_and(inside, gx == ngx - 1), harmonic(kp[ni, rows, :], x_wall), 0.0)
    for i in range(ni):
        cz[i, PAD:PAD + 1, :] = z_low[i:i + 1, :]
        cz[i, PAD + nl:PAD + nl + 1, :] = z_high[i:i + 1, :]

    stencil(mp)

    def diagonal(i, _):
        inv[i] = cx[i] + cx[i + 1] + cy[i] + cyh[i] + cz[i, rows, :] + cz[i, rows_up, :]
        return 0

    lax.fori_loop(0, ni, diagonal, 0)

    exchange_wait(kp, 0)

    @pl.when(has_xlo)
    def _():
        bx[0] = jnp.where(inside, harmonic(xr[0, 0], kp[1, rows, :]), 0.0)
        inv[0] = inv[0] + bx[0]

    @pl.when(has_xhi)
    def _():
        bx[1] = jnp.where(inside, harmonic(kp[ni, rows, :], xr[0, 1]), 0.0)
        inv[ni - 1] = inv[ni - 1] + bx[1]

    @pl.when(has_zlo)
    def _():
        bz[0] = jnp.where(in_i, harmonic(zr[0, 0], zs[0, 1]), 0.0)
        add_rows(inv, bz[0], 0)

    @pl.when(has_zhi)
    def _():
        bz[1] = jnp.where(in_i, harmonic(zs[0, 0], zr[0, 1]), 0.0)
        add_rows(inv, bz[1], nl - 1)

    y_face = jnp.where(lax.rem(lane_half, LANES // 2) < ni, harmonic(ys[0], yr[0]), 0.0)
    by[...] = y_face
    add_columns(inv, y_face)
    join_faces(mp, 1)
    inputs[5].wait()

    def first_residual(i, acc):
        iv = jnp.where(inside, 1.0 / jnp.where(inside, inv[i], 1.0), 0.0)
        inv[i] = iv
        x[i] = mp[i + 1, rows, :]
        r[0, i, :, 0:nj] = f_in[i]
        res = r[0, i] - n[i]
        r[0, i] = res
        u = res * iv
        mp[i + 1, rows, :] = u
        return acc + fold(res * u)

    gamma_acc = packed_pass(mp, 2, first_residual, zero_acc)
    exchange_start(mp, 2)
    stencil(mp)
    join_faces(mp, 2)

    def first_w(i, acc):
        av = n[i]
        w[i] = av
        acc = acc + fold(av * mp[i + 1, rows, :])
        mp[i + 1, rows, :] = av * inv[i]
        return acc

    delta_acc = packed_pass(mp, 3, first_w, zero_acc)

    def scalars(t, sums, gamma_old, pap_old):
        gamma, delta, sigma = sums[0], sums[1], sums[2]
        beta = jnp.where(t == 0, 0.0, gamma / gamma_old)
        pap = delta + 2.0 * beta * sigma + beta * beta * pap_old
        return gamma, pap, beta[0, 0], (gamma / pap)[0, 0]

    def advance_x(now, alpha, beta):
        def step(i, _):
            p_new = inv[i] * r[1 - now, i] + beta * p[i]
            p[i] = p_new
            x[i] = x[i] + alpha * p_new
            return 0
        lax.fori_loop(0, ni, step, 0)

    def iteration(t, carry):
        accs, gamma_old, pap_old, alpha_old, beta_old = carry
        now = lax.rem(t, 2)
        reduce_start(t, accs)
        exchange_start(mp, t + 3)
        stencil(mp)
        advance_x(now, alpha_old, beta_old)
        join_faces(mp, t + 3)
        sums = reduce_wait(t, 4)
        gamma, pap, beta, alpha = scalars(t, sums, gamma_old, pap_old)

        def update(i, acc):
            iv = inv[i]
            z_new = n[i] + beta * z[i]
            s_new = w[i] + beta * s[i]
            r_new = r[now, i] - alpha * s_new
            w_new = w[i] - alpha * z_new
            u_new = iv * r_new
            z[i] = z_new
            s[i] = s_new
            r[1 - now, i] = r_new
            w[i] = w_new
            mp[i + 1, rows, :] = iv * w_new
            return (acc[0] + fold(r_new * u_new), acc[1] + fold(w_new * u_new),
                    acc[2] + fold(u_new * s_new), acc[3] + fold(r_new * r_new))

        accs = packed_pass(mp, t + 4, update, (zero_acc,) * 4)

        @pl.when(t > 0)
        def _():
            hist_ref[lax.max(t - 1, 0)] = sums[3][0, 0]

        return accs, gamma, pap, alpha, beta

    one = jnp.ones((1, 1), F32)
    last = CG_ITERS - 1
    accs, gamma_old, pap_old, alpha_old, beta_old = lax.fori_loop(
        0, last, iteration, ((gamma_acc, delta_acc, zero_acc, zero_acc), one, one, jnp.float32(0.0), jnp.float32(0.0)))

    now = last % 2
    reduce_start(last, accs)
    outputs = [pltpu.make_async_copy(src, dst, out_sem.at[j]) for j, (src, dst) in enumerate((
        (r.at[now], r_hbm), (w, w_hbm), (s, s_hbm), (p, p_hbm), (x, x_hbm), (n, u_last_hbm)))]
    for copy in outputs[:3]:
        copy.start()

    def last_dots(i, acc):
        rv, wv, sv = r[now, i], w[i], s[i]
        n[i] = inv[i] * rv
        pairs = ((rv, wv), (rv, sv), (wv, wv), (wv, sv), (sv, sv))
        return tuple(a + fold(b * c) for a, (b, c) in zip(acc, pairs))

    dots = lax.fori_loop(0, ni, last_dots, (zero_acc,) * 5)
    reduce_start(CG_ITERS, dots)
    advance_x(now, alpha_old, beta_old)
    for copy in outputs[3:]:
        copy.start()
    sums = reduce_wait(last, 4)
    hist_ref[last - 1] = sums[3][0, 0]
    gamma = sums[0]
    beta = gamma / gamma_old
    alpha = gamma / (sums[1] + 2.0 * beta * sums[2] + beta * beta * pap_old)
    alpha_ref[0] = alpha[0, 0]
    beta_ref[0] = beta[0, 0]
    rw, rs, ww, ws, ss = reduce_wait(CG_ITERS, 5)
    hist_ref[last] = (sums[3] - 2.0 * alpha * (rw + beta * rs) + alpha * alpha * (ww + 2.0 * beta * ws + beta * beta * ss))[0, 0]
    for copy in outputs:
        copy.wait()


def solution(mesh):
    counts = (mesh.shape['gx'], mesh.shape['gy'], mesh.shape['gz'])
    grid_spec = P('gx', 'gy', 'gz')

    def local_solve(k_cell, k_ghost, f_rhs, u_init):
        ni, nj, nl = k_cell.shape
        flip = lambda a: jnp.swapaxes(a, 1, 2)
        slots = CG_ITERS + 3
        devices = counts[0] * counts[1] * counts[2]
        width = k_ghost.shape[2]
        any_spec = pl.BlockSpec(memory_space=pl.ANY)
        vm = lambda *shape: pltpu.VMEM(shape, F32)
        whole = vm(ni, nl, LANES)
        block = vm(ni, nl, nj)
        padded = vm(ni + 2, nl + 2 * PAD, LANES)
        dma = pltpu.SemaphoreType.DMA
        out_block = jax.ShapeDtypeStruct((ni, nl, LANES), F32)
        scalar_out = jax.ShapeDtypeStruct((1,), F32)
        x_old, u, p, r_old, w, s, hist, alpha, beta = pl.pallas_call(
            functools.partial(solve_kernel, (ni, nl, nj), counts),
            out_shape=(out_block,) * 6 + (jax.ShapeDtypeStruct((CG_ITERS,), F32), scalar_out, scalar_out),
            in_specs=[any_spec] * 4,
            out_specs=(any_spec,) * 6 + (pl.BlockSpec(memory_space=pltpu.SMEM),) * 3,
            scratch_shapes=[
                block, block, block, vm(nj, width), vm(ni, width), vm(ni, width), vm(-(-width // LANES) * LANES, LANES),
                vm(2, nl, LANES), vm(nl // 2, LANES), vm(2, ni, LANES),
                padded, padded, vm(ni + 1, nl, LANES), whole, whole, vm(ni, nl + 2 * PAD, LANES), whole,
                whole, vm(2, ni, nl, LANES), whole, whole, whole, whole, whole,
                vm(slots, nl // 2, LANES), vm(slots, 2, ni, LANES),
                vm(slots, 2, nl, LANES), vm(slots, nl // 2, LANES), vm(slots, 2, ni, LANES),
                vm(CG_ITERS + 1, 1, LANES), vm(CG_ITERS + 1, devices, 1, LANES),
                dma((slots, 2)), dma((slots,)), dma((slots, 2)), dma((slots, 2)), dma((slots,)), dma((slots, 2)),
                dma((CG_ITERS + 1,)), dma((CG_ITERS + 1,)), dma((6,)), dma((6,)),
            ],
            compiler_params=pltpu.CompilerParams(has_side_effects=True, collective_id=0),
        )(k_ghost, flip(k_cell), flip(f_rhs), flip(u_init))
        alpha, beta = alpha[0], beta[0]
        x_new = (x_old + alpha * (u + beta * p))[:, :, 0:nj]
        r_new = (r_old - alpha * (w + beta * s))[:, :, 0:nj]
        return flip(x_new), flip(r_new), hist

    return jax.shard_map(local_solve, mesh=mesh, in_specs=(grid_spec, P(), grid_spec, grid_spec),
                         out_specs=(grid_spec, grid_spec, P()), check_vma=False)
```

```python
import functools

import jax
import jax.numpy as jnp
from jax import lax
from jax.experimental import pallas as pl
from jax.experimental.pallas import tpu as pltpu
from jax.sharding import PartitionSpec as P

CG_ITERS = 8
LANES = 128
PAD = 8
GROUP = 6
COLUMNS = 16
MESH = pl.DeviceIdType.MESH
F32 = jnp.float32


def solve_kernel(dims, counts, kg_hbm, k_hbm, f_hbm, u_hbm, x, n, p, r, w, s, hist_ref, alpha_ref, beta_ref,
                 k_in, f_in, u_in, wall_x, wall_y, wall_z, wall_t, bx, by, bz,
                 kp, mp, cx, cy, cyh, cz, inv, z,
                 ys, zs, xr, yr, zr, red_s, red_r,
                 xs_sem, ys_sem, zs_sem, xr_sem, yr_sem, zr_sem, rs_sem, rr_sem, in_sem):
    ni, nl, nj = dims
    ngx, ngy, ngz = counts
    half = nl // 2
    gx, gy, gz = lax.axis_index('gx'), lax.axis_index('gy'), lax.axis_index('gz')
    rows = pl.ds(PAD, nl)
    rows_dn = pl.ds(PAD - 1, nl)
    rows_up = pl.ds(PAD + 1, nl)
    lane = lax.broadcasted_iota(jnp.int32, (nl, LANES), 1)
    lane_i = lax.broadcasted_iota(jnp.int32, (ni, LANES), 1)
    lane_half = lax.broadcasted_iota(jnp.int32, (half, LANES), 1)
    lane_row = lax.broadcasted_iota(jnp.int32, (1, LANES), 1)
    inside = lane < nj
    has_xlo, has_xhi = gx > 0, gx < ngx - 1
    has_zlo, has_zhi = gz > 0, gz < ngz - 1
    face_lane = jnp.where(gy == 0, nj - 1, 0)
    y_low_wall, y_high_wall = gy == 0, gy > 0
    zero_slab = jnp.zeros((nl, LANES), F32)
    zero_acc = jnp.zeros((8, LANES), F32)
    relative = [(a, b, c) for a in reversed(range(ngz)) for b in reversed(range(ngy)) for c in reversed(range(ngx))
                if a or b or c]

    def other(a, b, c):
        return lax.rem(gz + a, ngz), lax.rem(gy + b, ngy), lax.rem(gx + c, ngx)

    def column_roll(slab, shift):
        return pltpu.roll(slab, lax.rem(shift + 2 * LANES, LANES), 1)

    def slabs(group, step, init):
        def body(g, carry):
            for k in range(group):
                carry = step(g * group + k, carry)
            return carry
        return lax.fori_loop(0, ni // group, body, init)

    def x_copy(ref, slot, up):
        src = ref.at[ni if up else 1, rows]
        return pltpu.make_async_remote_copy(
            src_ref=src, dst_ref=xr.at[slot, 0 if up else 1], send_sem=xs_sem.at[slot, 0 if up else 1],
            recv_sem=xr_sem.at[slot, 0 if up else 1], device_id=(gz, gy, gx + 1 if up else gx - 1), device_id_type=MESH)

    def z_copy(slot, up):
        return pltpu.make_async_remote_copy(
            src_ref=zs.at[slot, 0 if up else 1], dst_ref=zr.at[slot, 0 if up else 1],
            send_sem=zs_sem.at[slot, 0 if up else 1], recv_sem=zr_sem.at[slot, 0 if up else 1],
            device_id=(gz + 1 if up else gz - 1, gy, gx), device_id_type=MESH)

    def y_copy(slot):
        return pltpu.make_async_remote_copy(
            src_ref=ys.at[slot], dst_ref=yr.at[slot], send_sem=ys_sem.at[slot], recv_sem=yr_sem.at[slot],
            device_id=(gz, 1 - gy, gx), device_id_type=MESH)

    def pack_rolls(ref, slot, i):
        row = lax.max(i, 0) if not isinstance(i, int) else i
        slab = ref[row + 1, rows, :]
        zs[slot, 1, pl.ds(row, 1), :] = slab[0:1, :]
        zs[slot, 0, pl.ds(row, 1), :] = slab[nl - 1:nl, :]
        return column_roll(slab[0:half], row - face_lane), column_roll(slab[half:nl], row - face_lane + LANES // 2)

    def pack(i, rolled, acc):
        acc = jnp.where(lane_half == i, rolled[0], acc)
        return jnp.where(lane_half == i + LANES // 2, rolled[1], acc)

    def packed_pass(ref, slot, step, init):
        def body(g, carry):
            state, acc = carry
            rolled = [pack_rolls(ref, slot, (g - 1) * GROUP + k) for k in range(GROUP)]
            for k in range(GROUP):
                state = step(g * GROUP + k, state)
            for k in range(GROUP):
                acc = pack((g - 1) * GROUP + k, rolled[k], acc)
            return state, acc
        state, acc = lax.fori_loop(0, ni // GROUP, body, (init, jnp.zeros((half, LANES), F32)))
        rolled = [pack_rolls(ref, slot, ni - GROUP + k) for k in range(GROUP)]
        for k in range(GROUP):
            acc = pack(ni - GROUP + k, rolled[k], acc)
        ys[slot] = acc
        return state

    def exchange_start(ref, slot):
        pl.when(has_xlo)(lambda: x_copy(ref, slot, False).start())
        pl.when(has_xhi)(lambda: x_copy(ref, slot, True).start())
        pl.when(has_zlo)(lambda: z_copy(slot, False).start())
        pl.when(has_zhi)(lambda: z_copy(slot, True).start())
        y_copy(slot).start()

    def exchange_wait(ref, slot):
        @pl.when(has_xlo)
        def _():
            x_copy(ref, slot, False).wait_send()
            x_copy(ref, slot, True).wait_recv()

        @pl.when(has_xhi)
        def _():
            x_copy(ref, slot, True).wait_send()
            x_copy(ref, slot, False).wait_recv()

        @pl.when(has_zlo)
        def _():
            z_copy(slot, False).wait_send()
            z_copy(slot, True).wait_recv()

        @pl.when(has_zhi)
        def _():
            z_copy(slot, True).wait_send()
            z_copy(slot, False).wait_recv()

        y_copy(slot).wait()

    def add_rows(ref, layer, row):
        for i in range(ni):
            ref[i, row:row + 1, :] = ref[i, row:row + 1, :] + layer[i:i + 1, :]

    def add_columns(ref, packed):
        mask = lane == face_lane

        def step(g, _):
            columns = []
            for k in range(min(COLUMNS, ni)):
                i = g * min(COLUMNS, ni) + k
                columns.append((column_roll(packed, face_lane - i), column_roll(packed, face_lane - i - LANES // 2)))
            for k in range(min(COLUMNS, ni)):
                i = g * min(COLUMNS, ni) + k
                ref[i] = ref[i] + jnp.where(mask, jnp.concatenate(columns[k], axis=0), 0.0)
            return 0

        lax.fori_loop(0, ni // min(COLUMNS, ni), step, 0)

    def join_faces(ref, slot):
        y_copy(slot).wait()
        add_columns(n, by[...] * (ys[slot] - yr[slot]))

        @pl.when(has_xlo)
        def _():
            x_copy(ref, slot, False).wait_send()
            x_copy(ref, slot, True).wait_recv()
            n[0] = n[0] + bx[0] * (ref[1, rows, :] - xr[slot, 0])

        @pl.when(has_xhi)
        def _():
            x_copy(ref, slot, True).wait_send()
            x_copy(ref, slot, False).wait_recv()
            n[ni - 1] = n[ni - 1] + bx[1] * (ref[ni, rows, :] - xr[slot, 1])

        @pl.when(has_zlo)
        def _():
            z_copy(slot, False).wait_send()
            z_copy(slot, True).wait_recv()
            add_rows(n, bz[0] * (zs[slot, 1] - zr[slot, 0]), 0)

        @pl.when(has_zhi)
        def _():
            z_copy(slot, True).wait_send()
            z_copy(slot, False).wait_recv()
            add_rows(n, bz[1] * (zs[slot, 0] - zr[slot, 1]), nl - 1)

    def stencil(ref):
        def step(i, carry):
            v, flux_x = carry
            above = ref[i + 2, rows, :]
            flux_next = cx[i + 1] * (above - v)
            flux_zl = cz[i, rows, :] * (v - ref[i + 1, rows_dn, :])
            flux_zh = cz[i, rows_up, :] * (ref[i + 1, rows_up, :] - v)
            flux_yl = cy[i] * (v - pltpu.roll(v, 1, 1))
            flux_yh = cyh[i] * (pltpu.roll(v, LANES - 1, 1) - v)
            n[i] = (flux_x - flux_next) + (flux_yl - flux_yh) + (flux_zl - flux_zh)
            return above, flux_next

        first = ref[1, rows, :]
        slabs(GROUP, step, (first, cx[0] * (first - ref[0, rows, :])))

    def fold(slab):
        out = slab[0:8]
        for part in range(8, nl, 8):
            out = out + slab[part:part + 8]
        return out

    def reduce_start(slot, accs):
        row = jnp.zeros((1, LANES), F32)
        for q, acc in enumerate(accs):
            row = jnp.where(lane_row == q, jnp.sum(jnp.sum(acc, axis=0, keepdims=True), axis=1, keepdims=True), row)
        me = (gz * ngy + gy) * ngx + gx
        red_s[slot] = row
        red_r[slot, me] = row
        for delta in relative:
            pltpu.make_async_remote_copy(
                src_ref=red_s.at[slot], dst_ref=red_r.at[slot, me], send_sem=rs_sem.at[slot],
                recv_sem=rr_sem.at[slot], device_id=other(*delta), device_id_type=MESH).start()

    def reduce_wait(slot, count):
        whole = red_r.at[slot, pl.ds(0, len(relative))]
        done = pltpu.make_async_remote_copy(
            src_ref=whole, dst_ref=whole, send_sem=rs_sem.at[slot], recv_sem=rr_sem.at[slot],
            device_id=(gz, gy, gx), device_id_type=MESH)
        done.wait_recv()
        done.wait_send()
        total = jnp.sum(red_r[slot], axis=0)
        return [jnp.sum(jnp.where(lane_row == q, total, 0.0), axis=1, keepdims=True) for q in range(count)]

    x_row, z_row = jnp.where(gx == 0, 0, 1), jnp.where(gz == 0, 4, 5)
    slabs_i = pl.ds(pl.multiple_of(gx * ni, 8), ni)
    inputs = [
        pltpu.make_async_copy(k_hbm, k_in, in_sem.at[0]),
        pltpu.make_async_copy(u_hbm, u_in, in_sem.at[1]),
        pltpu.make_async_copy(kg_hbm.at[x_row, pl.ds(pl.multiple_of(gy * nj, 8), nj)], wall_x, in_sem.at[2]),
        pltpu.make_async_copy(kg_hbm.at[2 + gy, slabs_i], wall_y, in_sem.at[3]),
        pltpu.make_async_copy(kg_hbm.at[z_row, slabs_i], wall_z, in_sem.at[4]),
        pltpu.make_async_copy(f_hbm, f_in, in_sem.at[5]),
    ]
    for copy in inputs:
        copy.start()

    barrier = pltpu.get_barrier_semaphore()
    for delta in relative:
        pl.semaphore_signal(barrier, inc=1, device_id=other(*delta), device_id_type=MESH)

    for edge in (0, ni + 1):
        mp[edge] = jnp.zeros((nl + 2 * PAD, LANES), F32)
        kp[edge] = jnp.ones((nl + 2 * PAD, LANES), F32)

    def clear(i, _):
        mp[i + 1, pl.ds(0, PAD), :] = jnp.zeros((PAD, LANES), F32)
        mp[i + 1, pl.ds(PAD + nl, PAD), :] = jnp.zeros((PAD, LANES), F32)
        kp[i + 1, pl.ds(0, PAD), :] = jnp.ones((PAD, LANES), F32)
        kp[i + 1, pl.ds(PAD + nl, PAD), :] = jnp.ones((PAD, LANES), F32)
        mp[i + 1, rows, :] = zero_slab
        s[i] = zero_slab
        z[i] = zero_slab
        p[i] = zero_slab
        r[1, i] = zero_slab
        r[0, i] = zero_slab
        kp[i + 1, rows, :] = jnp.full((nl, LANES), 1.0, F32)
        return 0

    lax.fori_loop(0, ni, clear, 0)

    def load_k(i, _):
        kp[i + 1, rows, 0:nj] = k_in[i]
        return 0

    def load_u(i, _):
        mp[i + 1, rows, 0:nj] = u_in[i]
        return 0

    inputs[0].wait()
    packed_pass(kp, 0, load_k, 0)
    pl.semaphore_wait(barrier, len(relative))
    exchange_start(kp, 0)
    inputs[1].wait()
    packed_pass(mp, 1, load_u, 0)
    exchange_start(mp, 1)

    for copy in inputs[2:5]:
        copy.wait()
    width = wall_x.shape[1]
    l_rows = pl.ds(pl.multiple_of(gz * nl, 8), nl)

    def flipped(wall, count):
        for start in range(0, width, LANES):
            size = min(LANES, width - start)
            block = jnp.concatenate([wall[:, start:start + size], jnp.ones((LANES - count, size), F32)], axis=0)
            wall_t[start:start + size, :] = block.T
        return wall_t[l_rows, :]

    x_wall = flipped(wall_x, nj)
    y_wall = flipped(wall_y, ni)
    if width > LANES:
        rest = jnp.concatenate([wall_z[:, LANES:width], jnp.ones((ni, 2 * LANES - width), F32)], axis=1)
        whole_z = wall_z[:, 0:LANES]
        turn = LANES - nj
        shifted = jnp.where(lane_i < turn, pltpu.roll(whole_z, turn, 1), pltpu.roll(rest, turn, 1))
    else:
        whole_z = jnp.concatenate([wall_z[...], jnp.ones((ni, LANES - width), F32)], axis=1)
        shifted = pltpu.roll(whole_z, LANES - nj, 1)
    z_wall = jnp.where(gy == 0, whole_z, shifted)

    def harmonic(left, right):
        return 2.0 * left * right / (left + right)

    in_i = lane_i < nj
    cx[0] = jnp.where(jnp.logical_and(inside, gx == 0), harmonic(x_wall, kp[1, rows, :]), 0.0)
    z_low = jnp.where(jnp.logical_and(in_i, gz == 0), harmonic(z_wall, zs[0, 1]), 0.0)
    z_high = jnp.where(jnp.logical_and(in_i, gz == ngz - 1), harmonic(zs[0, 0], z_wall), 0.0)
    y_low_mask = jnp.logical_and(inside, jnp.logical_or(lane > 0, y_low_wall))
    y_high_mask = jnp.logical_and(inside, jnp.logical_or(lane < nj - 1, y_high_wall))
    wall_lane = nj - 1 - face_lane

    def coefs(i, _):
        here = kp[i + 1, rows, :]
        cx[i + 1] = jnp.where(inside, harmonic(here, kp[i + 2, rows, :]), 0.0)
        cz[i, rows_up, :] = jnp.where(inside, harmonic(here, kp[i + 1, rows_up, :]), 0.0)
        wall = column_roll(y_wall, wall_lane - i)
        low = jnp.where(lane == 0, wall, pltpu.roll(here, 1, 1))
        high = jnp.where(lane == nj - 1, wall, pltpu.roll(here, LANES - 1, 1))
        cy[i] = jnp.where(y_low_mask, harmonic(low, here), 0.0)
        cyh[i] = jnp.where(y_high_mask, harmonic(here, high), 0.0)
        return 0

    slabs(GROUP, coefs, 0)
    cx[ni] = jnp.where(jnp.logical_and(inside, gx == ngx - 1), harmonic(kp[ni, rows, :], x_wall), 0.0)
    for i in range(ni):
        cz[i, PAD:PAD + 1, :] = z_low[i:i + 1, :]
        cz[i, PAD + nl:PAD + nl + 1, :] = z_high[i:i + 1, :]

    stencil(mp)

    def diagonal(i, _):
        inv[i] = cx[i] + cx[i + 1] + cy[i] + cyh[i] + cz[i, rows, :] + cz[i, rows_up, :]
        return 0

    lax.fori_loop(0, ni, diagonal, 0)

    exchange_wait(kp, 0)

    @pl.when(has_xlo)
    def _():
        bx[0] = jnp.where(inside, harmonic(xr[0, 0], kp[1, rows, :]), 0.0)
        inv[0] = inv[0] + bx[0]

    @pl.when(has_xhi)
    def _():
        bx[1] = jnp.where(inside, harmonic(kp[ni, rows, :], xr[0, 1]), 0.0)
        inv[ni - 1] = inv[ni - 1] + bx[1]

    @pl.when(has_zlo)
    def _():
        bz[0] = jnp.where(in_i, harmonic(zr[0, 0], zs[0, 1]), 0.0)
        add_rows(inv, bz[0], 0)

    @pl.when(has_zhi)
    def _():
        bz[1] = jnp.where(in_i, harmonic(zs[0, 0], zr[0, 1]), 0.0)
        add_rows(inv, bz[1], nl - 1)

    y_face = jnp.where(lax.rem(lane_half, LANES // 2) < ni, harmonic(ys[0], yr[0]), 0.0)
    by[...] = y_face
    add_columns(inv, y_face)
    join_faces(mp, 1)
    inputs[5].wait()

    def first_residual(i, acc):
        iv = jnp.where(inside, 1.0 / jnp.where(inside, inv[i], 1.0), 0.0)
        inv[i] = iv
        x[i] = mp[i + 1, rows, :]
        r[0, i, :, 0:nj] = f_in[i]
        res = r[0, i] - n[i]
        r[0, i] = res
        u = res * iv
        mp[i + 1, rows, :] = u
        return acc + fold(res * u)

    gamma_acc = packed_pass(mp, 2, first_residual, zero_acc)
    exchange_start(mp, 2)
    stencil(mp)
    join_faces(mp, 2)

    def first_w(i, acc):
        av = n[i]
        w[i] = av
        acc = acc + fold(av * mp[i + 1, rows, :])
        mp[i + 1, rows, :] = av * inv[i]
        return acc

    delta_acc = packed_pass(mp, 3, first_w, zero_acc)

    def scalars(t, sums, gamma_old, pap_old):
        gamma, delta, sigma = sums[0], sums[1], sums[2]
        beta = jnp.where(t == 0, 0.0, gamma / gamma_old)
        pap = delta + 2.0 * beta * sigma + beta * beta * pap_old
        return gamma, pap, beta[0, 0], (gamma / pap)[0, 0]

    def advance_x(now, alpha, beta):
        def step(i, _):
            p_new = inv[i] * r[1 - now, i] + beta * p[i]
            p[i] = p_new
            x[i] = x[i] + alpha * p_new
            return 0
        lax.fori_loop(0, ni, step, 0)

    def iteration(t, carry):
        accs, gamma_old, pap_old, alpha_old, beta_old = carry
        now = lax.rem(t, 2)
        reduce_start(t, accs)
        exchange_start(mp, t + 3)
        stencil(mp)
        advance_x(now, alpha_old, beta_old)
        join_faces(mp, t + 3)
        sums = reduce_wait(t, 4)
        gamma, pap, beta, alpha = scalars(t, sums, gamma_old, pap_old)

        def update(i, acc):
            iv = inv[i]
            z_new = n[i] + beta * z[i]
            s_new = w[i] + beta * s[i]
            r_new = r[now, i] - alpha * s_new
            w_new = w[i] - alpha * z_new
            u_new = iv * r_new
            z[i] = z_new
            s[i] = s_new
            r[1 - now, i] = r_new
            w[i] = w_new
            mp[i + 1, rows, :] = iv * w_new
            return (acc[0] + fold(r_new * u_new), acc[1] + fold(w_new * u_new),
                    acc[2] + fold(u_new * s_new), acc[3] + fold(r_new * r_new))

        accs = packed_pass(mp, t + 4, update, (zero_acc,) * 4)

        @pl.when(t > 0)
        def _():
            hist_ref[lax.max(t - 1, 0)] = sums[3][0, 0]

        return accs, gamma, pap, alpha, beta

    one = jnp.ones((1, 1), F32)
    last = CG_ITERS - 1
    accs, gamma_old, pap_old, alpha_old, beta_old = lax.fori_loop(
        0, last, iteration, ((gamma_acc, delta_acc, zero_acc, zero_acc), one, one, jnp.float32(0.0), jnp.float32(0.0)))

    now = last % 2
    reduce_start(last, accs)

    def last_dots(i, acc):
        rv, wv, sv = r[now, i], w[i], s[i]
        n[i] = inv[i] * rv
        pairs = ((rv, wv), (rv, sv), (wv, wv), (wv, sv), (sv, sv))
        return tuple(a + fold(b * c) for a, (b, c) in zip(acc, pairs))

    dots = lax.fori_loop(0, ni, last_dots, (zero_acc,) * 5)
    reduce_start(CG_ITERS, dots)
    advance_x(now, alpha_old, beta_old)
    sums = reduce_wait(last, 4)
    hist_ref[last - 1] = sums[3][0, 0]
    gamma = sums[0]
    beta = gamma / gamma_old
    alpha = gamma / (sums[1] + 2.0 * beta * sums[2] + beta * beta * pap_old)
    alpha_ref[0] = alpha[0, 0]
    beta_ref[0] = beta[0, 0]
    rw, rs, ww, ws, ss = reduce_wait(CG_ITERS, 5)
    hist_ref[last] = (sums[3] - 2.0 * alpha * (rw + beta * rs) + alpha * alpha * (ww + 2.0 * beta * ws + beta * beta * ss))[0, 0]


def finish_kernel(chunk, alpha_ref, beta_ref, hist_ref, x, u, p, r, w, s, x_hbm, r_hbm, hist_hbm, x_new, r_new, sem, hist_sem):
    ni, _, nj = x_new.shape
    alpha, beta = alpha_ref[0], beta_ref[0]
    copies = [pltpu.make_async_copy(hist_ref, hist_hbm, hist_sem)]
    copies[0].start()
    for g in range(ni // chunk):
        def step(i, _):
            x_new[i] = (x[i] + alpha * (u[i] + beta * p[i]))[:, 0:nj]
            r_new[i] = (r[1, i] - alpha * (w[i] + beta * s[i]))[:, 0:nj]
            return 0
        lax.fori_loop(g * chunk, (g + 1) * chunk, step, 0)
        part = pl.ds(g * chunk, chunk)
        for j, (src, dst) in enumerate(((x_new, x_hbm), (r_new, r_hbm))):
            copies.append(pltpu.make_async_copy(src.at[part], dst.at[part], sem.at[j, g]))
            copies[-1].start()
    for copy in copies:
        copy.wait()


def solution(mesh):
    counts = (mesh.shape['gx'], mesh.shape['gy'], mesh.shape['gz'])
    grid_spec = P('gx', 'gy', 'gz')

    def local_solve(k_cell, k_ghost, f_rhs, u_init):
        ni, nj, nl = k_cell.shape
        flip = lambda a: jnp.swapaxes(a, 1, 2)
        slots = CG_ITERS + 3
        devices = counts[0] * counts[1] * counts[2]
        width = k_ghost.shape[2]
        any_spec = pl.BlockSpec(memory_space=pl.ANY)
        vm = lambda *shape: pltpu.VMEM(shape, F32)
        whole = vm(ni, nl, LANES)
        block = vm(ni, nl, nj)
        padded = vm(ni + 2, nl + 2 * PAD, LANES)
        dma = pltpu.SemaphoreType.DMA
        kept = pltpu.VMEM((ni, nl, LANES), F32)
        scalar_out = jax.ShapeDtypeStruct((1,), F32)
        vmem_spec, smem_spec = pl.BlockSpec(memory_space=pltpu.VMEM), pl.BlockSpec(memory_space=pltpu.SMEM)
        *state, hist, alpha, beta = pl.pallas_call(
            functools.partial(solve_kernel, (ni, nl, nj), counts),
            out_shape=(kept, kept, kept, pltpu.VMEM((2, ni, nl, LANES), F32), kept, kept,
                       jax.ShapeDtypeStruct((CG_ITERS,), F32), scalar_out, scalar_out),
            in_specs=[any_spec] * 4,
            out_specs=(vmem_spec,) * 6 + (smem_spec,) * 3,
            scratch_shapes=[
                block, block, block, vm(nj, width), vm(ni, width), vm(ni, width), vm(-(-width // LANES) * LANES, LANES),
                vm(2, nl, LANES), vm(nl // 2, LANES), vm(2, ni, LANES),
                padded, padded, vm(ni + 1, nl, LANES), whole, whole, vm(ni, nl + 2 * PAD, LANES), whole,
                whole,
                vm(slots, nl // 2, LANES), vm(slots, 2, ni, LANES),
                vm(slots, 2, nl, LANES), vm(slots, nl // 2, LANES), vm(slots, 2, ni, LANES),
                vm(CG_ITERS + 1, 1, LANES), vm(CG_ITERS + 1, devices, 1, LANES),
                dma((slots, 2)), dma((slots,)), dma((slots, 2)), dma((slots, 2)), dma((slots,)), dma((slots, 2)),
                dma((CG_ITERS + 1,)), dma((CG_ITERS + 1,)), dma((6,)),
            ],
            compiler_params=pltpu.CompilerParams(has_side_effects=True, collective_id=0, vmem_limit_bytes=28 << 20),
        )(*(pltpu.with_memory_space_constraint(a, pltpu.HBM) for a in (k_ghost, flip(k_cell), flip(f_rhs), flip(u_init))))
        chunk = ni // 4
        out_block = jax.ShapeDtypeStruct((ni, nl, nj), F32)
        x_new, r_new, hist = pl.pallas_call(
            functools.partial(finish_kernel, chunk),
            out_shape=(out_block, out_block, jax.ShapeDtypeStruct((CG_ITERS,), F32)),
            in_specs=[smem_spec] * 3 + [vmem_spec] * 6,
            out_specs=(any_spec,) * 3,
            scratch_shapes=[block, block, dma((2, ni // chunk)), dma],
            compiler_params=pltpu.CompilerParams(vmem_limit_bytes=28 << 20),
        )(alpha, beta, hist, *state)
        return flip(x_new), flip(r_new), hist

    return jax.shard_map(local_solve, mesh=mesh, in_specs=(grid_spec, P(), grid_spec, grid_spec),
                         out_specs=(grid_spec, grid_spec, P()), check_vma=False)
```

```python
import functools

import jax
import jax.numpy as jnp
from jax import lax
from jax.experimental import pallas as pl
from jax.experimental.pallas import tpu as pltpu
from jax.sharding import PartitionSpec as P

CG_ITERS = 8
LANES = 128
PAD = 8
GROUP = 6
COLUMNS = 16
MESH = pl.DeviceIdType.MESH
F32 = jnp.float32


def solve_kernel(dims, counts, kg_hbm, k_hbm, f_hbm, u_hbm, x, n, p, r, w, s, scal_ref,
                 k_in, f_in, u_in, wall_x, wall_y, wall_z, wall_t, bx, by, bz,
                 kp, mp, cx, cy, cyh, cz, inv, z,
                 ys, zs, xr, yr, zr, red_s, red_r,
                 xs_sem, ys_sem, zs_sem, xr_sem, yr_sem, zr_sem, rs_sem, rr_sem, in_sem, near_sem):
    ni, nl, nj = dims
    ngx, ngy, ngz = counts
    half = nl // 2
    gx, gy, gz = lax.axis_index('gx'), lax.axis_index('gy'), lax.axis_index('gz')
    rows = pl.ds(PAD, nl)
    rows_dn = pl.ds(PAD - 1, nl)
    rows_up = pl.ds(PAD + 1, nl)
    lane = lax.broadcasted_iota(jnp.int32, (nl, LANES), 1)
    lane_i = lax.broadcasted_iota(jnp.int32, (ni, LANES), 1)
    lane_half = lax.broadcasted_iota(jnp.int32, (half, LANES), 1)
    lane_row = lax.broadcasted_iota(jnp.int32, (1, LANES), 1)
    inside = lane < nj
    has_xlo, has_xhi = gx > 0, gx < ngx - 1
    has_zlo, has_zhi = gz > 0, gz < ngz - 1
    face_lane = jnp.where(gy == 0, nj - 1, 0)
    y_low_wall, y_high_wall = gy == 0, gy > 0
    zero_slab = jnp.zeros((nl, LANES), F32)
    zero_acc = jnp.zeros((8, LANES), F32)
    relative = [(a, b, c) for a in reversed(range(ngz)) for b in reversed(range(ngy)) for c in reversed(range(ngx))
                if a or b or c]

    def other(a, b, c):
        return lax.rem(gz + a, ngz), lax.rem(gy + b, ngy), lax.rem(gx + c, ngx)

    def column_roll(slab, shift):
        return pltpu.roll(slab, lax.rem(shift + 2 * LANES, LANES), 1)

    def slabs(group, step, init):
        def body(g, carry):
            for k in range(group):
                carry = step(g * group + k, carry)
            return carry
        return lax.fori_loop(0, ni // group, body, init)

    def x_copy(ref, slot, up):
        src = ref.at[ni if up else 1, rows]
        return pltpu.make_async_remote_copy(
            src_ref=src, dst_ref=xr.at[slot, 0 if up else 1], send_sem=xs_sem.at[slot, 0 if up else 1],
            recv_sem=xr_sem.at[slot, 0 if up else 1], device_id=(gz, gy, gx + 1 if up else gx - 1), device_id_type=MESH)

    def z_copy(slot, up):
        return pltpu.make_async_remote_copy(
            src_ref=zs.at[slot, 0 if up else 1], dst_ref=zr.at[slot, 0 if up else 1],
            send_sem=zs_sem.at[slot, 0 if up else 1], recv_sem=zr_sem.at[slot, 0 if up else 1],
            device_id=(gz + 1 if up else gz - 1, gy, gx), device_id_type=MESH)

    def y_copy(slot):
        return pltpu.make_async_remote_copy(
            src_ref=ys.at[slot], dst_ref=yr.at[slot], send_sem=ys_sem.at[slot], recv_sem=yr_sem.at[slot],
            device_id=(gz, 1 - gy, gx), device_id_type=MESH)

    def pack_rolls(ref, slot, i):
        row = lax.max(i, 0) if not isinstance(i, int) else i
        slab = ref[row + 1, rows, :]
        zs[slot, 1, pl.ds(row, 1), :] = slab[0:1, :]
        zs[slot, 0, pl.ds(row, 1), :] = slab[nl - 1:nl, :]
        return column_roll(slab[0:half], row - face_lane), column_roll(slab[half:nl], row - face_lane + LANES // 2)

    def pack(i, rolled, acc):
        acc = jnp.where(lane_half == i, rolled[0], acc)
        return jnp.where(lane_half == i + LANES // 2, rolled[1], acc)

    def packed_pass(ref, slot, step, init):
        def body(g, carry):
            state, acc = carry
            rolled = [pack_rolls(ref, slot, (g - 1) * GROUP + k) for k in range(GROUP)]
            for k in range(GROUP):
                state = step(g * GROUP + k, state)
            for k in range(GROUP):
                acc = pack((g - 1) * GROUP + k, rolled[k], acc)
            return state, acc
        state, acc = lax.fori_loop(0, ni // GROUP, body, (init, jnp.zeros((half, LANES), F32)))
        rolled = [pack_rolls(ref, slot, ni - GROUP + k) for k in range(GROUP)]
        for k in range(GROUP):
            acc = pack(ni - GROUP + k, rolled[k], acc)
        ys[slot] = acc
        return state

    def exchange_start(ref, slot):
        pl.when(has_xlo)(lambda: x_copy(ref, slot, False).start())
        pl.when(has_xhi)(lambda: x_copy(ref, slot, True).start())
        pl.when(has_zlo)(lambda: z_copy(slot, False).start())
        pl.when(has_zhi)(lambda: z_copy(slot, True).start())
        y_copy(slot).start()

    def exchange_wait(ref, slot):
        @pl.when(has_xlo)
        def _():
            x_copy(ref, slot, False).wait_send()
            x_copy(ref, slot, True).wait_recv()

        @pl.when(has_xhi)
        def _():
            x_copy(ref, slot, True).wait_send()
            x_copy(ref, slot, False).wait_recv()

        @pl.when(has_zlo)
        def _():
            z_copy(slot, False).wait_send()
            z_copy(slot, True).wait_recv()

        @pl.when(has_zhi)
        def _():
            z_copy(slot, True).wait_send()
            z_copy(slot, False).wait_recv()

        y_copy(slot).wait()

    def add_rows(ref, layer, row):
        for i in range(ni):
            ref[i, row:row + 1, :] = ref[i, row:row + 1, :] + layer[i:i + 1, :]

    def add_columns(ref, packed):
        mask = lane == face_lane

        def step(g, _):
            columns = []
            for k in range(min(COLUMNS, ni)):
                i = g * min(COLUMNS, ni) + k
                columns.append((column_roll(packed, face_lane - i), column_roll(packed, face_lane - i - LANES // 2)))
            for k in range(min(COLUMNS, ni)):
                i = g * min(COLUMNS, ni) + k
                ref[i] = ref[i] + jnp.where(mask, jnp.concatenate(columns[k], axis=0), 0.0)
            return 0

        lax.fori_loop(0, ni // min(COLUMNS, ni), step, 0)

    def join_faces(ref, slot):
        y_copy(slot).wait()
        add_columns(n, by[...] * (ys[slot] - yr[slot]))

        @pl.when(has_xlo)
        def _():
            x_copy(ref, slot, False).wait_send()
            x_copy(ref, slot, True).wait_recv()
            n[0] = n[0] + bx[0] * (ref[1, rows, :] - xr[slot, 0])

        @pl.when(has_xhi)
        def _():
            x_copy(ref, slot, True).wait_send()
            x_copy(ref, slot, False).wait_recv()
            n[ni - 1] = n[ni - 1] + bx[1] * (ref[ni, rows, :] - xr[slot, 1])

        @pl.when(has_zlo)
        def _():
            z_copy(slot, False).wait_send()
            z_copy(slot, True).wait_recv()
            add_rows(n, bz[0] * (zs[slot, 1] - zr[slot, 0]), 0)

        @pl.when(has_zhi)
        def _():
            z_copy(slot, True).wait_send()
            z_copy(slot, False).wait_recv()
            add_rows(n, bz[1] * (zs[slot, 0] - zr[slot, 1]), nl - 1)

    def stencil(ref):
        def step(i, carry):
            v, flux_x = carry
            above = ref[i + 2, rows, :]
            flux_next = cx[i + 1] * (above - v)
            flux_zl = cz[i, rows, :] * (v - ref[i + 1, rows_dn, :])
            flux_zh = cz[i, rows_up, :] * (ref[i + 1, rows_up, :] - v)
            flux_yl = cy[i] * (v - pltpu.roll(v, 1, 1))
            flux_yh = cyh[i] * (pltpu.roll(v, LANES - 1, 1) - v)
            n[i] = (flux_x - flux_next) + (flux_yl - flux_yh) + (flux_zl - flux_zh)
            return above, flux_next

        first = ref[1, rows, :]
        slabs(GROUP, step, (first, cx[0] * (first - ref[0, rows, :])))

    def fold(slab):
        out = slab[0:8]
        for part in range(8, nl, 8):
            out = out + slab[part:part + 8]
        return out

    def reduce_start(slot, accs):
        row = jnp.zeros((1, LANES), F32)
        for q, acc in enumerate(accs):
            row = jnp.where(lane_row == q, jnp.sum(jnp.sum(acc, axis=0, keepdims=True), axis=1, keepdims=True), row)
        me = (gz * ngy + gy) * ngx + gx
        red_s[slot] = row
        red_r[slot, me] = row
        for delta in relative:
            pltpu.make_async_remote_copy(
                src_ref=red_s.at[slot], dst_ref=red_r.at[slot, me], send_sem=rs_sem.at[slot],
                recv_sem=rr_sem.at[slot], device_id=other(*delta), device_id_type=MESH).start()

    def reduce_wait(slot, count):
        whole = red_r.at[slot, pl.ds(0, len(relative))]
        done = pltpu.make_async_remote_copy(
            src_ref=whole, dst_ref=whole, send_sem=rs_sem.at[slot], recv_sem=rr_sem.at[slot],
            device_id=(gz, gy, gx), device_id_type=MESH)
        done.wait_recv()
        done.wait_send()
        total = jnp.sum(red_r[slot], axis=0)
        return [jnp.sum(jnp.where(lane_row == q, total, 0.0), axis=1, keepdims=True) for q in range(count)]

    x_row, z_row = jnp.where(gx == 0, 0, 1), jnp.where(gz == 0, 4, 5)
    slabs_i = pl.ds(pl.multiple_of(gx * ni, 8), ni)
    inputs = [
        pltpu.make_async_copy(k_hbm, k_in, in_sem.at[0]),
        pltpu.make_async_copy(u_hbm, u_in, in_sem.at[1]),
        pltpu.make_async_copy(kg_hbm.at[x_row, pl.ds(pl.multiple_of(gy * nj, 8), nj)], wall_x, in_sem.at[2]),
        pltpu.make_async_copy(kg_hbm.at[2 + gy, slabs_i], wall_y, in_sem.at[3]),
        pltpu.make_async_copy(kg_hbm.at[z_row, slabs_i], wall_z, in_sem.at[4]),
        pltpu.make_async_copy(f_hbm, f_in, in_sem.at[5]),
    ]
    for copy in inputs:
        copy.start()

    def tell_neighbours(sem):
        tell = lambda *target: pl.semaphore_signal(sem, inc=1, device_id=target, device_id_type=MESH)
        pl.when(has_xlo)(lambda: tell(gz, gy, gx - 1))
        pl.when(has_xhi)(lambda: tell(gz, gy, gx + 1))
        pl.when(has_zlo)(lambda: tell(gz - 1, gy, gx))
        pl.when(has_zhi)(lambda: tell(gz + 1, gy, gx))
        tell(gz, 1 - gy, gx)

    neighbours = 5 - jnp.where(has_xlo, 0, 1) - jnp.where(has_xhi, 0, 1) - jnp.where(has_zlo, 0, 1) - jnp.where(has_zhi, 0, 1)
    rounds = (ngx - 1) + (ngy - 1) + (ngz - 1) - 1

    def next_round(k):
        pl.semaphore_wait(near_sem.at[k], neighbours)
        if k + 1 < rounds:
            tell_neighbours(near_sem.at[k + 1])

    barrier = pltpu.get_barrier_semaphore()
    tell_neighbours(barrier)

    for edge in (0, ni + 1):
        mp[edge] = jnp.zeros((nl + 2 * PAD, LANES), F32)
        kp[edge] = jnp.ones((nl + 2 * PAD, LANES), F32)

    def clear(i, _):
        mp[i + 1, pl.ds(0, PAD), :] = jnp.zeros((PAD, LANES), F32)
        mp[i + 1, pl.ds(PAD + nl, PAD), :] = jnp.zeros((PAD, LANES), F32)
        kp[i + 1, pl.ds(0, PAD), :] = jnp.ones((PAD, LANES), F32)
        kp[i + 1, pl.ds(PAD + nl, PAD), :] = jnp.ones((PAD, LANES), F32)
        mp[i + 1, rows, :] = zero_slab
        s[i] = zero_slab
        z[i] = zero_slab
        p[i] = zero_slab
        r[1, i] = zero_slab
        r[0, i] = zero_slab
        kp[i + 1, rows, :] = jnp.full((nl, LANES), 1.0, F32)
        return 0

    lax.fori_loop(0, ni, clear, 0)

    def load_k(i, _):
        kp[i + 1, rows, 0:nj] = k_in[i]
        return 0

    def load_u(i, _):
        mp[i + 1, rows, 0:nj] = u_in[i]
        return 0

    inputs[0].wait()
    packed_pass(kp, 0, load_k, 0)
    pl.semaphore_wait(barrier, neighbours)
    tell_neighbours(near_sem.at[0])
    exchange_start(kp, 0)
    inputs[1].wait()
    packed_pass(mp, 1, load_u, 0)
    exchange_start(mp, 1)
    next_round(0)

    for copy in inputs[2:5]:
        copy.wait()
    width = wall_x.shape[1]
    l_rows = pl.ds(pl.multiple_of(gz * nl, 8), nl)

    def flipped(wall, count):
        for start in range(0, width, LANES):
            size = min(LANES, width - start)
            block = jnp.concatenate([wall[:, start:start + size], jnp.ones((LANES - count, size), F32)], axis=0)
            wall_t[start:start + size, :] = block.T
        return wall_t[l_rows, :]

    x_wall = flipped(wall_x, nj)
    y_wall = flipped(wall_y, ni)
    if width > LANES:
        rest = jnp.concatenate([wall_z[:, LANES:width], jnp.ones((ni, 2 * LANES - width), F32)], axis=1)
        whole_z = wall_z[:, 0:LANES]
        turn = LANES - nj
        shifted = jnp.where(lane_i < turn, pltpu.roll(whole_z, turn, 1), pltpu.roll(rest, turn, 1))
    else:
        whole_z = jnp.concatenate([wall_z[...], jnp.ones((ni, LANES - width), F32)], axis=1)
        shifted = pltpu.roll(whole_z, LANES - nj, 1)
    z_wall = jnp.where(gy == 0, whole_z, shifted)

    def harmonic(left, right):
        return 2.0 * left * right / (left + right)

    next_round(1)

    in_i = lane_i < nj
    cx[0] = jnp.where(jnp.logical_and(inside, gx == 0), harmonic(x_wall, kp[1, rows, :]), 0.0)
    z_low = jnp.where(jnp.logical_and(in_i, gz == 0), harmonic(z_wall, zs[0, 1]), 0.0)
    z_high = jnp.where(jnp.logical_and(in_i, gz == ngz - 1), harmonic(zs[0, 0], z_wall), 0.0)
    y_low_mask = jnp.logical_and(inside, jnp.logical_or(lane > 0, y_low_wall))
    y_high_mask = jnp.logical_and(inside, jnp.logical_or(lane < nj - 1, y_high_wall))
    wall_lane = nj - 1 - face_lane

    def coefs(i, _):
        here = kp[i + 1, rows, :]
        cx[i + 1] = jnp.where(inside, harmonic(here, kp[i + 2, rows, :]), 0.0)
        cz[i, rows_up, :] = jnp.where(inside, harmonic(here, kp[i + 1, rows_up, :]), 0.0)
        wall = column_roll(y_wall, wall_lane - i)
        low = jnp.where(lane == 0, wall, pltpu.roll(here, 1, 1))
        high = jnp.where(lane == nj - 1, wall, pltpu.roll(here, LANES - 1, 1))
        cy[i] = jnp.where(y_low_mask, harmonic(low, here), 0.0)
        cyh[i] = jnp.where(y_high_mask, harmonic(here, high), 0.0)
        return 0

    slabs(GROUP, coefs, 0)
    next_round(2)
    cx[ni] = jnp.where(jnp.logical_and(inside, gx == ngx - 1), harmonic(kp[ni, rows, :], x_wall), 0.0)
    for i in range(ni):
        cz[i, PAD:PAD + 1, :] = z_low[i:i + 1, :]
        cz[i, PAD + nl:PAD + nl + 1, :] = z_high[i:i + 1, :]

    stencil(mp)

    def diagonal(i, _):
        inv[i] = cx[i] + cx[i + 1] + cy[i] + cyh[i] + cz[i, rows, :] + cz[i, rows_up, :]
        return 0

    lax.fori_loop(0, ni, diagonal, 0)
    next_round(3)

    exchange_wait(kp, 0)

    @pl.when(has_xlo)
    def _():
        bx[0] = jnp.where(inside, harmonic(xr[0, 0], kp[1, rows, :]), 0.0)
        inv[0] = inv[0] + bx[0]

    @pl.when(has_xhi)
    def _():
        bx[1] = jnp.where(inside, harmonic(kp[ni, rows, :], xr[0, 1]), 0.0)
        inv[ni - 1] = inv[ni - 1] + bx[1]

    @pl.when(has_zlo)
    def _():
        bz[0] = jnp.where(in_i, harmonic(zr[0, 0], zs[0, 1]), 0.0)
        add_rows(inv, bz[0], 0)

    @pl.when(has_zhi)
    def _():
        bz[1] = jnp.where(in_i, harmonic(zs[0, 0], zr[0, 1]), 0.0)
        add_rows(inv, bz[1], nl - 1)

    y_face = jnp.where(lax.rem(lane_half, LANES // 2) < ni, harmonic(ys[0], yr[0]), 0.0)
    by[...] = y_face
    add_columns(inv, y_face)
    join_faces(mp, 1)
    inputs[5].wait()

    def first_residual(i, acc):
        iv = jnp.where(inside, 1.0 / jnp.where(inside, inv[i], 1.0), 0.0)
        inv[i] = iv
        x[i] = mp[i + 1, rows, :]
        r[0, i, :, 0:nj] = f_in[i]
        res = r[0, i] - n[i]
        r[0, i] = res
        u = res * iv
        mp[i + 1, rows, :] = u
        return acc + fold(res * u)

    gamma_acc = packed_pass(mp, 2, first_residual, zero_acc)
    exchange_start(mp, 2)
    next_round(4)
    stencil(mp)
    for k in range(5, rounds):
        next_round(k)
    join_faces(mp, 2)

    def first_w(i, acc):
        av = n[i]
        w[i] = av
        acc = acc + fold(av * mp[i + 1, rows, :])
        mp[i + 1, rows, :] = av * inv[i]
        return acc

    delta_acc = packed_pass(mp, 3, first_w, zero_acc)

    def scalars(t, sums, gamma_old, pap_old):
        gamma, delta, sigma = sums[0], sums[1], sums[2]
        beta = jnp.where(t == 0, 0.0, gamma / gamma_old)
        pap = delta + 2.0 * beta * sigma + beta * beta * pap_old
        return gamma, pap, beta[0, 0], (gamma / pap)[0, 0]

    def advance_x(now, alpha, beta):
        def step(i, _):
            p_new = inv[i] * r[1 - now, i] + beta * p[i]
            p[i] = p_new
            x[i] = x[i] + alpha * p_new
            return 0
        lax.fori_loop(0, ni, step, 0)

    def iteration(t, carry):
        accs, gamma_old, pap_old, alpha_old, beta_old = carry
        now = lax.rem(t, 2)
        reduce_start(t, accs)
        exchange_start(mp, t + 3)
        stencil(mp)
        advance_x(now, alpha_old, beta_old)
        join_faces(mp, t + 3)
        sums = reduce_wait(t, 4)
        gamma, pap, beta, alpha = scalars(t, sums, gamma_old, pap_old)

        def update(i, acc):
            iv = inv[i]
            z_new = n[i] + beta * z[i]
            s_new = w[i] + beta * s[i]
            r_new = r[now, i] - alpha * s_new
            w_new = w[i] - alpha * z_new
            u_new = iv * r_new
            z[i] = z_new
            s[i] = s_new
            r[1 - now, i] = r_new
            w[i] = w_new
            mp[i + 1, rows, :] = iv * w_new
            return (acc[0] + fold(r_new * u_new), acc[1] + fold(w_new * u_new),
                    acc[2] + fold(u_new * s_new), acc[3] + fold(r_new * r_new))

        accs = packed_pass(mp, t + 4, update, (zero_acc,) * 4)

        scal_ref[lax.rem(t + CG_ITERS - 1, CG_ITERS)] = jnp.broadcast_to(sums[3], (1, LANES))

        return accs, gamma, pap, alpha, beta

    one = jnp.ones((1, 1), F32)
    last = CG_ITERS - 1
    accs, gamma_old, pap_old, alpha_old, beta_old = lax.fori_loop(
        0, last, iteration, ((gamma_acc, delta_acc, zero_acc, zero_acc), one, one, jnp.float32(0.0), jnp.float32(0.0)))

    now = last % 2
    reduce_start(last, accs)

    def last_dots(i, acc):
        rv, wv, sv = r[now, i], w[i], s[i]
        n[i] = inv[i] * rv
        pairs = ((rv, wv), (rv, sv), (wv, wv), (wv, sv), (sv, sv))
        return tuple(a + fold(b * c) for a, (b, c) in zip(acc, pairs))

    dots = lax.fori_loop(0, ni, last_dots, (zero_acc,) * 5)
    reduce_start(CG_ITERS, dots)
    advance_x(now, alpha_old, beta_old)
    sums = reduce_wait(last, 4)
    wide = lambda value: jnp.broadcast_to(value, (1, LANES))
    scal_ref[last - 1] = wide(sums[3])
    gamma = sums[0]
    beta = gamma / gamma_old
    alpha = gamma / (sums[1] + 2.0 * beta * sums[2] + beta * beta * pap_old)
    scal_ref[CG_ITERS] = wide(alpha)
    scal_ref[CG_ITERS + 1] = wide(beta)
    rw, rs, ww, ws, ss = reduce_wait(CG_ITERS, 5)
    scal_ref[last] = wide(sums[3] - 2.0 * alpha * (rw + beta * rs) + alpha * alpha * (ww + 2.0 * beta * ws + beta * beta * ss))


def finish_kernel(chunk, scal, x, u, p, r, w, s, x_hbm, r_hbm, hist_hbm, x_new, r_new, hist, sem, hist_sem):
    ni, nl, nj = x_new.shape
    alpha = jnp.broadcast_to(scal[CG_ITERS], (nl, LANES))
    beta = jnp.broadcast_to(scal[CG_ITERS + 1], (nl, LANES))
    copies = []

    def step(i, _):
        x_new[i] = (x[i] + alpha * (u[i] + beta * p[i]))[:, 0:nj]
        r_new[i] = (r[1, i] - alpha * (w[i] + beta * s[i]))[:, 0:nj]
        return 0

    for g in range(ni // chunk):
        lax.fori_loop(g * chunk, (g + 1) * chunk, step, 0)
        part = pl.ds(g * chunk, chunk)
        for j, (src, dst) in enumerate(((x_new, x_hbm), (r_new, r_hbm))):
            copies.append(pltpu.make_async_copy(src.at[part], dst.at[part], sem.at[j, g]))
            copies[-1].start()
        if g == 0:
            for t in range(CG_ITERS):
                hist[t] = scal[t, 0, 0]
            copies.append(pltpu.make_async_copy(hist, hist_hbm, hist_sem))
            copies[-1].start()
    for copy in copies:
        copy.wait()


def solution(mesh):
    counts = (mesh.shape['gx'], mesh.shape['gy'], mesh.shape['gz'])
    grid_spec = P('gx', 'gy', 'gz')

    def local_solve(k_cell, k_ghost, f_rhs, u_init):
        ni, nj, nl = k_cell.shape
        flip = lambda a: jnp.swapaxes(a, 1, 2)
        slots = CG_ITERS + 3
        devices = counts[0] * counts[1] * counts[2]
        width = k_ghost.shape[2]
        any_spec = pl.BlockSpec(memory_space=pl.ANY)
        vm = lambda *shape: pltpu.VMEM(shape, F32)
        whole = vm(ni, nl, LANES)
        block = vm(ni, nl, nj)
        padded = vm(ni + 2, nl + 2 * PAD, LANES)
        dma = pltpu.SemaphoreType.DMA
        kept = pltpu.VMEM((ni, nl, LANES), F32)
        vmem_spec = pl.BlockSpec(memory_space=pltpu.VMEM)
        *state, scal = pl.pallas_call(
            functools.partial(solve_kernel, (ni, nl, nj), counts),
            out_shape=(kept, kept, kept, pltpu.VMEM((2, ni, nl, LANES), F32), kept, kept,
                       pltpu.VMEM((CG_ITERS + 2, 1, LANES), F32)),
            in_specs=[any_spec] * 4,
            out_specs=(vmem_spec,) * 7,
            scratch_shapes=[
                block, block, block, vm(nj, width), vm(ni, width), vm(ni, width), vm(-(-width // LANES) * LANES, LANES),
                vm(2, nl, LANES), vm(nl // 2, LANES), vm(2, ni, LANES),
                padded, padded, vm(ni + 1, nl, LANES), whole, whole, vm(ni, nl + 2 * PAD, LANES), whole,
                whole,
                vm(slots, nl // 2, LANES), vm(slots, 2, ni, LANES),
                vm(slots, 2, nl, LANES), vm(slots, nl // 2, LANES), vm(slots, 2, ni, LANES),
                vm(CG_ITERS + 1, 1, LANES), vm(CG_ITERS + 1, devices, 1, LANES),
                dma((slots, 2)), dma((slots,)), dma((slots, 2)), dma((slots, 2)), dma((slots,)), dma((slots, 2)),
                dma((CG_ITERS + 1,)), dma((CG_ITERS + 1,)), dma((6,)), pltpu.SemaphoreType.REGULAR((6,)),
            ],
            compiler_params=pltpu.CompilerParams(has_side_effects=True, collective_id=0, vmem_limit_bytes=28 << 20),
        )(*(pltpu.with_memory_space_constraint(a, pltpu.HBM) for a in (k_ghost, flip(k_cell), flip(f_rhs), flip(u_init))))
        chunk = ni // 4
        out_block = jax.ShapeDtypeStruct((ni, nl, nj), F32)
        x_new, r_new, hist = pl.pallas_call(
            functools.partial(finish_kernel, chunk),
            out_shape=(out_block, out_block, jax.ShapeDtypeStruct((CG_ITERS,), F32)),
            in_specs=[vmem_spec] * 7,
            out_specs=(any_spec,) * 3,
            scratch_shapes=[block, block, pltpu.SMEM((CG_ITERS,), F32), dma((2, ni // chunk)), dma],
            compiler_params=pltpu.CompilerParams(vmem_limit_bytes=28 << 20),
        )(scal, *state)
        return flip(x_new), flip(r_new), hist

    return jax.shard_map(local_solve, mesh=mesh, in_specs=(grid_spec, P(), grid_spec, grid_spec),
                         out_specs=(grid_spec, grid_spec, P()), check_vma=False)
```

```python
import functools

import jax
import jax.numpy as jnp
from jax import lax
from jax.experimental import pallas as pl
from jax.experimental.pallas import tpu as pltpu
from jax.sharding import PartitionSpec as P

CG_ITERS = 8
LANES = 128
PAD = 8
GROUP = 6
COLUMNS = 16
MESH = pl.DeviceIdType.MESH
F32 = jnp.float32


def solve_kernel(dims, counts, kg_hbm, k_hbm, f_hbm, u_hbm, x, n, p, r, w, s, scal_ref,
                 k_in, f_in, u_in, wall_x, wall_y, wall_z, wall_t, bx, by, bz,
                 kp, mp, cx, cy, cyh, cz, inv, dg, z,
                 ys, zs, xr, yr, zr, red_s, red_r,
                 xs_sem, ys_sem, zs_sem, xr_sem, yr_sem, zr_sem, rs_sem, rr_sem, in_sem, near_sem):
    ni, nl, nj = dims
    ngx, ngy, ngz = counts
    half = nl // 2
    gx, gy, gz = lax.axis_index('gx'), lax.axis_index('gy'), lax.axis_index('gz')
    rows = pl.ds(PAD, nl)
    rows_dn = pl.ds(PAD - 1, nl)
    rows_up = pl.ds(PAD + 1, nl)
    lane = lax.broadcasted_iota(jnp.int32, (nl, LANES), 1)
    lane_i = lax.broadcasted_iota(jnp.int32, (ni, LANES), 1)
    lane_half = lax.broadcasted_iota(jnp.int32, (half, LANES), 1)
    lane_row = lax.broadcasted_iota(jnp.int32, (1, LANES), 1)
    inside = lane < nj
    has_xlo, has_xhi = gx > 0, gx < ngx - 1
    has_zlo, has_zhi = gz > 0, gz < ngz - 1
    face_lane = jnp.where(gy == 0, nj - 1, 0)
    y_low_wall, y_high_wall = gy == 0, gy > 0
    zero_slab = jnp.zeros((nl, LANES), F32)
    zero_acc = jnp.zeros((8, LANES), F32)
    relative = [(a, b, c) for a in reversed(range(ngz)) for b in reversed(range(ngy)) for c in reversed(range(ngx))
                if a or b or c]

    def other(a, b, c):
        return lax.rem(gz + a, ngz), lax.rem(gy + b, ngy), lax.rem(gx + c, ngx)

    def column_roll(slab, shift):
        return pltpu.roll(slab, lax.rem(shift + 2 * LANES, LANES), 1)

    def slabs(group, step, init):
        def body(g, carry):
            for k in range(group):
                carry = step(g * group + k, carry)
            return carry
        return lax.fori_loop(0, ni // group, body, init)

    def x_copy(ref, slot, up):
        src = ref.at[ni if up else 1, rows]
        return pltpu.make_async_remote_copy(
            src_ref=src, dst_ref=xr.at[slot, 0 if up else 1], send_sem=xs_sem.at[slot, 0 if up else 1],
            recv_sem=xr_sem.at[slot, 0 if up else 1], device_id=(gz, gy, gx + 1 if up else gx - 1), device_id_type=MESH)

    def z_copy(slot, up):
        return pltpu.make_async_remote_copy(
            src_ref=zs.at[slot, 0 if up else 1], dst_ref=zr.at[slot, 0 if up else 1],
            send_sem=zs_sem.at[slot, 0 if up else 1], recv_sem=zr_sem.at[slot, 0 if up else 1],
            device_id=(gz + 1 if up else gz - 1, gy, gx), device_id_type=MESH)

    def y_copy(slot):
        return pltpu.make_async_remote_copy(
            src_ref=ys.at[slot], dst_ref=yr.at[slot], send_sem=ys_sem.at[slot], recv_sem=yr_sem.at[slot],
            device_id=(gz, 1 - gy, gx), device_id_type=MESH)

    def pack_rolls(ref, slot, i):
        row = lax.max(i, 0) if not isinstance(i, int) else i
        slab = ref[row + 1, rows, :]
        zs[slot, 1, pl.ds(row, 1), :] = slab[0:1, :]
        zs[slot, 0, pl.ds(row, 1), :] = slab[nl - 1:nl, :]
        return column_roll(slab[0:half], row - face_lane), column_roll(slab[half:nl], row - face_lane + LANES // 2)

    def pack(i, rolled, acc):
        acc = jnp.where(lane_half == i, rolled[0], acc)
        return jnp.where(lane_half == i + LANES // 2, rolled[1], acc)

    def packed_pass(ref, slot, step, init, tail=lambda state: state):
        def body(g, carry):
            state, acc = carry
            rolled = [pack_rolls(ref, slot, (g - 1) * GROUP + k) for k in range(GROUP)]
            for k in range(GROUP):
                state = step(g * GROUP + k, state)
            for k in range(GROUP):
                acc = pack((g - 1) * GROUP + k, rolled[k], acc)
            return state, acc
        state, acc = lax.fori_loop(0, ni // GROUP, body, (init, jnp.zeros((half, LANES), F32)))
        rolled = [pack_rolls(ref, slot, ni - GROUP + k) for k in range(GROUP)]
        state = tail(state)
        for k in range(GROUP):
            acc = pack(ni - GROUP + k, rolled[k], acc)
        ys[slot] = acc
        return state

    def exchange_start(ref, slot):
        pl.when(has_xlo)(lambda: x_copy(ref, slot, False).start())
        pl.when(has_xhi)(lambda: x_copy(ref, slot, True).start())
        pl.when(has_zlo)(lambda: z_copy(slot, False).start())
        pl.when(has_zhi)(lambda: z_copy(slot, True).start())
        y_copy(slot).start()

    def exchange_wait(ref, slot):
        @pl.when(has_xlo)
        def _():
            x_copy(ref, slot, False).wait_send()
            x_copy(ref, slot, True).wait_recv()

        @pl.when(has_xhi)
        def _():
            x_copy(ref, slot, True).wait_send()
            x_copy(ref, slot, False).wait_recv()

        @pl.when(has_zlo)
        def _():
            z_copy(slot, False).wait_send()
            z_copy(slot, True).wait_recv()

        @pl.when(has_zhi)
        def _():
            z_copy(slot, True).wait_send()
            z_copy(slot, False).wait_recv()

        y_copy(slot).wait()

    def add_rows(ref, layer, row):
        for i in range(ni):
            ref[i, row:row + 1, :] = ref[i, row:row + 1, :] + layer[i:i + 1, :]

    def add_columns(ref, packed):
        mask = lane == face_lane

        def step(g, _):
            columns = []
            for k in range(min(COLUMNS, ni)):
                i = g * min(COLUMNS, ni) + k
                columns.append((column_roll(packed, face_lane - i), column_roll(packed, face_lane - i - LANES // 2)))
            for k in range(min(COLUMNS, ni)):
                i = g * min(COLUMNS, ni) + k
                ref[i] = ref[i] + jnp.where(mask, jnp.concatenate(columns[k], axis=0), 0.0)
            return 0

        lax.fori_loop(0, ni // min(COLUMNS, ni), step, 0)

    def join_faces(ref, slot):
        y_copy(slot).wait()
        add_columns(n, by[...] * (ys[slot] - yr[slot]))

        @pl.when(has_xlo)
        def _():
            x_copy(ref, slot, False).wait_send()
            x_copy(ref, slot, True).wait_recv()
            n[0] = n[0] + bx[0] * (ref[1, rows, :] - xr[slot, 0])

        @pl.when(has_xhi)
        def _():
            x_copy(ref, slot, True).wait_send()
            x_copy(ref, slot, False).wait_recv()
            n[ni - 1] = n[ni - 1] + bx[1] * (ref[ni, rows, :] - xr[slot, 1])

        @pl.when(has_zlo)
        def _():
            z_copy(slot, False).wait_send()
            z_copy(slot, True).wait_recv()
            add_rows(n, bz[0] * (zs[slot, 1] - zr[slot, 0]), 0)

        @pl.when(has_zhi)
        def _():
            z_copy(slot, True).wait_send()
            z_copy(slot, False).wait_recv()
            add_rows(n, bz[1] * (zs[slot, 0] - zr[slot, 1]), nl - 1)

    def stencil(ref):
        def step(i, carry):
            v, flux_x = carry
            above = ref[i + 2, rows, :]
            flux_next = cx[i + 1] * (above - v)
            flux_zl = cz[i, rows, :] * (v - ref[i + 1, rows_dn, :])
            flux_zh = cz[i, rows_up, :] * (ref[i + 1, rows_up, :] - v)
            flux_yl = cy[i] * (v - pltpu.roll(v, 1, 1))
            flux_yh = cyh[i] * (pltpu.roll(v, LANES - 1, 1) - v)
            n[i] = (flux_x - flux_next) + (flux_yl - flux_yh) + (flux_zl - flux_zh)
            return above, flux_next

        first = ref[1, rows, :]
        slabs(GROUP, step, (first, cx[0] * (first - ref[0, rows, :])))

    def fold(slab):
        out = slab[0:8]
        for part in range(8, nl, 8):
            out = out + slab[part:part + 8]
        return out

    def reduce_row(slot, accs):
        row = jnp.zeros((1, LANES), F32)
        for q, acc in enumerate(accs):
            row = jnp.where(lane_row == q, jnp.sum(jnp.sum(acc, axis=0, keepdims=True), axis=1, keepdims=True), row)
        red_s[slot] = row
        red_r[slot, (gz * ngy + gy) * ngx + gx] = row

    def reduce_send(slot):
        me = (gz * ngy + gy) * ngx + gx
        for delta in relative:
            pltpu.make_async_remote_copy(
                src_ref=red_s.at[slot], dst_ref=red_r.at[slot, me], send_sem=rs_sem.at[slot],
                recv_sem=rr_sem.at[slot], device_id=other(*delta), device_id_type=MESH).start()

    def reduce_wait(slot, count):
        whole = red_r.at[slot, pl.ds(0, len(relative))]
        done = pltpu.make_async_remote_copy(
            src_ref=whole, dst_ref=whole, send_sem=rs_sem.at[slot], recv_sem=rr_sem.at[slot],
            device_id=(gz, gy, gx), device_id_type=MESH)
        done.wait_recv()
        done.wait_send()
        total = jnp.sum(red_r[slot], axis=0)
        return [jnp.sum(jnp.where(lane_row == q, total, 0.0), axis=1, keepdims=True) for q in range(count)]

    x_row, z_row = jnp.where(gx == 0, 0, 1), jnp.where(gz == 0, 4, 5)
    slabs_i = pl.ds(pl.multiple_of(gx * ni, 8), ni)
    inputs = [
        pltpu.make_async_copy(k_hbm, k_in, in_sem.at[0]),
        pltpu.make_async_copy(u_hbm, u_in, in_sem.at[1]),
        pltpu.make_async_copy(kg_hbm.at[x_row, pl.ds(pl.multiple_of(gy * nj, 8), nj)], wall_x, in_sem.at[2]),
        pltpu.make_async_copy(kg_hbm.at[2 + gy, slabs_i], wall_y, in_sem.at[3]),
        pltpu.make_async_copy(kg_hbm.at[z_row, slabs_i], wall_z, in_sem.at[4]),
        pltpu.make_async_copy(f_hbm, f_in, in_sem.at[5]),
    ]
    for copy in inputs[:5]:
        copy.start()

    def tell_neighbours(sem):
        tell = lambda *target: pl.semaphore_signal(sem, inc=1, device_id=target, device_id_type=MESH)
        pl.when(has_xlo)(lambda: tell(gz, gy, gx - 1))
        pl.when(has_xhi)(lambda: tell(gz, gy, gx + 1))
        pl.when(has_zlo)(lambda: tell(gz - 1, gy, gx))
        pl.when(has_zhi)(lambda: tell(gz + 1, gy, gx))
        tell(gz, 1 - gy, gx)

    neighbours = 5 - jnp.where(has_xlo, 0, 1) - jnp.where(has_xhi, 0, 1) - jnp.where(has_zlo, 0, 1) - jnp.where(has_zhi, 0, 1)
    rounds = (ngx - 1) + (ngy - 1) + (ngz - 1) - 1

    def next_round(k):
        pl.semaphore_wait(near_sem.at[k], neighbours)
        if k + 1 < rounds:
            tell_neighbours(near_sem.at[k + 1])

    barrier = pltpu.get_barrier_semaphore()
    tell_neighbours(barrier)

    for edge in (0, ni + 1):
        mp[edge] = jnp.zeros((nl + 2 * PAD, LANES), F32)
        kp[edge] = jnp.ones((nl + 2 * PAD, LANES), F32)

    def clear(i, _):
        mp[i + 1, pl.ds(0, PAD), :] = jnp.zeros((PAD, LANES), F32)
        mp[i + 1, pl.ds(PAD + nl, PAD), :] = jnp.zeros((PAD, LANES), F32)
        kp[i + 1, pl.ds(0, PAD), :] = jnp.ones((PAD, LANES), F32)
        kp[i + 1, pl.ds(PAD + nl, PAD), :] = jnp.ones((PAD, LANES), F32)
        mp[i + 1, rows, :] = zero_slab
        s[i] = zero_slab
        z[i] = zero_slab
        p[i] = zero_slab
        r[1, i] = zero_slab
        r[0, i] = zero_slab
        kp[i + 1, rows, :] = jnp.full((nl, LANES), 1.0, F32)
        return 0

    lax.fori_loop(0, ni, clear, 0)

    def load_k(i, _):
        kp[i + 1, rows, 0:nj] = k_in[i]
        return 0

    def load_u(i, _):
        mp[i + 1, rows, 0:nj] = u_in[i]
        return 0

    inputs[0].wait()
    inputs[5].start()
    packed_pass(kp, 0, load_k, 0)
    pl.semaphore_wait(barrier, neighbours)
    tell_neighbours(near_sem.at[0])
    exchange_start(kp, 0)
    inputs[1].wait()
    packed_pass(mp, 1, load_u, 0)
    exchange_start(mp, 1)
    next_round(0)

    for copy in inputs[2:5]:
        copy.wait()
    width = wall_x.shape[1]
    l_rows = pl.ds(pl.multiple_of(gz * nl, 8), nl)

    def flipped(wall, count):
        for start in range(0, width, LANES):
            size = min(LANES, width - start)
            block = jnp.concatenate([wall[:, start:start + size], jnp.ones((LANES - count, size), F32)], axis=0)
            wall_t[start:start + size, :] = block.T
        return wall_t[l_rows, :]

    x_wall = flipped(wall_x, nj)
    y_wall = flipped(wall_y, ni)
    if width > LANES:
        rest = jnp.concatenate([wall_z[:, LANES:width], jnp.ones((ni, 2 * LANES - width), F32)], axis=1)
        whole_z = wall_z[:, 0:LANES]
        turn = LANES - nj
        shifted = jnp.where(lane_i < turn, pltpu.roll(whole_z, turn, 1), pltpu.roll(rest, turn, 1))
    else:
        whole_z = jnp.concatenate([wall_z[...], jnp.ones((ni, LANES - width), F32)], axis=1)
        shifted = pltpu.roll(whole_z, LANES - nj, 1)
    z_wall = jnp.where(gy == 0, whole_z, shifted)

    def harmonic(left, right):
        return 2.0 * left * right / (left + right)

    next_round(1)

    in_i = lane_i < nj
    cx[0] = jnp.where(jnp.logical_and(inside, gx == 0), harmonic(x_wall, kp[1, rows, :]), 0.0)
    z_low = jnp.where(jnp.logical_and(in_i, gz == 0), harmonic(z_wall, zs[0, 1]), 0.0)
    z_high = jnp.where(jnp.logical_and(in_i, gz == ngz - 1), harmonic(zs[0, 0], z_wall), 0.0)
    y_low_mask = jnp.logical_and(inside, jnp.logical_or(lane > 0, y_low_wall))
    y_high_mask = jnp.logical_and(inside, jnp.logical_or(lane < nj - 1, y_high_wall))
    wall_lane = nj - 1 - face_lane

    def coefs(i, _):
        here = kp[i + 1, rows, :]
        cx[i + 1] = jnp.where(inside, harmonic(here, kp[i + 2, rows, :]), 0.0)
        cz[i, rows_up, :] = jnp.where(inside, harmonic(here, kp[i + 1, rows_up, :]), 0.0)
        wall = column_roll(y_wall, wall_lane - i)
        low = jnp.where(lane == 0, wall, pltpu.roll(here, 1, 1))
        high = jnp.where(lane == nj - 1, wall, pltpu.roll(here, LANES - 1, 1))
        cy[i] = jnp.where(y_low_mask, harmonic(low, here), 0.0)
        cyh[i] = jnp.where(y_high_mask, harmonic(here, high), 0.0)
        return 0

    slabs(GROUP, coefs, 0)
    next_round(2)
    cx[ni] = jnp.where(jnp.logical_and(inside, gx == ngx - 1), harmonic(kp[ni, rows, :], x_wall), 0.0)
    for i in range(ni):
        cz[i, PAD:PAD + 1, :] = z_low[i:i + 1, :]
        cz[i, PAD + nl:PAD + nl + 1, :] = z_high[i:i + 1, :]

    stencil(mp)

    def diagonal(i, _):
        dg[i] = cx[i] + cx[i + 1] + cy[i] + cyh[i] + cz[i, rows, :] + cz[i, rows_up, :]
        return 0

    lax.fori_loop(0, ni, diagonal, 0)
    next_round(3)

    exchange_wait(kp, 0)

    @pl.when(has_xlo)
    def _():
        bx[0] = jnp.where(inside, harmonic(xr[0, 0], kp[1, rows, :]), 0.0)
        dg[0] = dg[0] + bx[0]

    @pl.when(has_xhi)
    def _():
        bx[1] = jnp.where(inside, harmonic(kp[ni, rows, :], xr[0, 1]), 0.0)
        dg[ni - 1] = dg[ni - 1] + bx[1]

    @pl.when(has_zlo)
    def _():
        bz[0] = jnp.where(in_i, harmonic(zr[0, 0], zs[0, 1]), 0.0)
        add_rows(dg, bz[0], 0)

    @pl.when(has_zhi)
    def _():
        bz[1] = jnp.where(in_i, harmonic(zs[0, 0], zr[0, 1]), 0.0)
        add_rows(dg, bz[1], nl - 1)

    y_face = jnp.where(lax.rem(lane_half, LANES // 2) < ni, harmonic(ys[0], yr[0]), 0.0)
    by[...] = y_face
    add_columns(dg, y_face)
    join_faces(mp, 1)
    inputs[5].wait()

    def first_residual(i, acc):
        iv = jnp.where(inside, 1.0 / jnp.where(inside, dg[i], 1.0), 0.0)
        inv[i] = iv
        x[i] = mp[i + 1, rows, :]
        r[0, i, :, 0:nj] = f_in[i]
        res = r[0, i] - n[i]
        r[0, i] = res
        u = res * iv
        mp[i + 1, rows, :] = u
        return acc + fold(res * u)

    gamma_acc = packed_pass(mp, 2, first_residual, zero_acc)
    exchange_start(mp, 2)
    next_round(4)
    stencil(mp)
    for k in range(5, rounds):
        next_round(k)
    join_faces(mp, 2)

    def first_w(i, acc):
        av = n[i]
        acc = acc + fold(av * mp[i + 1, rows, :])
        mp[i + 1, rows, :] = av * inv[i]
        return acc

    packed_pass(mp, 3, first_w, zero_acc, lambda delta_acc: reduce_row(0, (gamma_acc, delta_acc)))

    def scalars(t, sums, gamma_old, pap_old):
        gamma, delta, sigma = sums[0], sums[1], sums[2]
        beta = jnp.where(t == 0, 0.0, gamma / gamma_old)
        pap = delta + 2.0 * beta * sigma + beta * beta * pap_old
        return gamma, pap, beta[0, 0], (gamma / pap)[0, 0]

    def advance_x(now, alpha, beta):
        def step(i, acc):
            p_new = inv[i] * r[1 - now, i] + beta * p[i]
            p[i] = p_new
            x[i] = x[i] + alpha * p_new
            return acc + fold(r[now, i] * r[now, i])
        return lax.fori_loop(0, ni, step, zero_acc)

    def iteration(t, carry):
        gamma_old, pap_old, alpha_old, beta_old = carry
        now = lax.rem(t, 2)
        exchange_start(mp, t + 3)
        reduce_send(t)
        stencil(mp)
        rr_acc = advance_x(now, alpha_old, beta_old)
        join_faces(mp, t + 3)
        sums = reduce_wait(t, 4)
        gamma, pap, beta, alpha = scalars(t, sums, gamma_old, pap_old)

        def update(i, acc):
            iv = inv[i]
            w_old = dg[i] * mp[i + 1, rows, :]
            z_new = n[i] + beta * z[i]
            s_new = w_old + beta * s[i]
            r_new = r[now, i] - alpha * s_new
            w_new = w_old - alpha * z_new
            u_new = iv * r_new
            z[i] = z_new
            s[i] = s_new
            r[1 - now, i] = r_new
            mp[i + 1, rows, :] = iv * w_new
            return acc[0] + fold(r_new * u_new), acc[1] + fold(w_new * u_new), acc[2] + fold(u_new * s_new)

        packed_pass(mp, t + 4, update, (zero_acc,) * 3, lambda accs: reduce_row(t + 1, accs + (rr_acc,)))
        scal_ref[lax.rem(t + CG_ITERS - 2, CG_ITERS)] = jnp.broadcast_to(sums[3], (1, LANES))
        return gamma, pap, alpha, beta

    one = jnp.ones((1, 1), F32)
    last = CG_ITERS - 1
    gamma_old, pap_old, alpha_old, beta_old = lax.fori_loop(
        0, last, iteration, (one, one, jnp.float32(0.0), jnp.float32(0.0)))

    now = last % 2
    reduce_send(last)

    def last_dots(i, acc):
        rv, sv = r[now, i], s[i]
        wv = dg[i] * mp[i + 1, rows, :]
        w[i] = wv
        n[i] = inv[i] * rv
        pairs = ((rv, rv), (rv, wv), (rv, sv), (wv, wv), (wv, sv), (sv, sv))
        return tuple(a + fold(b * c) for a, (b, c) in zip(acc, pairs))

    reduce_row(CG_ITERS, slabs(2, last_dots, (zero_acc,) * 6))
    reduce_send(CG_ITERS)
    advance_x(now, alpha_old, beta_old)
    sums = reduce_wait(last, 4)
    wide = lambda value: jnp.broadcast_to(value, (1, LANES))
    scal_ref[last - 2] = wide(sums[3])
    gamma = sums[0]
    beta = gamma / gamma_old
    alpha = gamma / (sums[1] + 2.0 * beta * sums[2] + beta * beta * pap_old)
    scal_ref[CG_ITERS] = wide(alpha)
    scal_ref[CG_ITERS + 1] = wide(beta)
    rr, rw, rs, ww, ws, ss = reduce_wait(CG_ITERS, 6)
    scal_ref[last - 1] = wide(rr)
    scal_ref[last] = wide(rr - 2.0 * alpha * (rw + beta * rs) + alpha * alpha * (ww + 2.0 * beta * ws + beta * beta * ss))


def finish_kernel(chunk, scal, x, u, p, r, w, s, x_hbm, r_hbm, hist_hbm, x_new, r_new, hist, sem, hist_sem):
    ni, nl, nj = x_new.shape
    alpha = jnp.broadcast_to(scal[CG_ITERS], (nl, LANES))
    beta = jnp.broadcast_to(scal[CG_ITERS + 1], (nl, LANES))
    copies = []

    def step(i, _):
        x_new[i] = (x[i] + alpha * (u[i] + beta * p[i]))[:, 0:nj]
        r_new[i] = (r[1, i] - alpha * (w[i] + beta * s[i]))[:, 0:nj]
        return 0

    for g in range(ni // chunk):
        lax.fori_loop(g * chunk, (g + 1) * chunk, step, 0)
        part = pl.ds(g * chunk, chunk)
        for j, (src, dst) in enumerate(((x_new, x_hbm), (r_new, r_hbm))):
            copies.append(pltpu.make_async_copy(src.at[part], dst.at[part], sem.at[j, g]))
            copies[-1].start()
        if g == 0:
            for t in range(CG_ITERS):
                hist[t] = scal[t, 0, 0]
            copies.append(pltpu.make_async_copy(hist, hist_hbm, hist_sem))
            copies[-1].start()
    for copy in copies:
        copy.wait()


def solution(mesh):
    counts = (mesh.shape['gx'], mesh.shape['gy'], mesh.shape['gz'])
    grid_spec = P('gx', 'gy', 'gz')

    def local_solve(k_cell, k_ghost, f_rhs, u_init):
        ni, nj, nl = k_cell.shape
        flip = lambda a: jnp.swapaxes(a, 1, 2)
        slots = CG_ITERS + 3
        devices = counts[0] * counts[1] * counts[2]
        width = k_ghost.shape[2]
        any_spec = pl.BlockSpec(memory_space=pl.ANY)
        vm = lambda *shape: pltpu.VMEM(shape, F32)
        whole = vm(ni, nl, LANES)
        block = vm(ni, nl, nj)
        padded = vm(ni + 2, nl + 2 * PAD, LANES)
        dma = pltpu.SemaphoreType.DMA
        kept = pltpu.VMEM((ni, nl, LANES), F32)
        vmem_spec = pl.BlockSpec(memory_space=pltpu.VMEM)
        *state, scal = pl.pallas_call(
            functools.partial(solve_kernel, (ni, nl, nj), counts),
            out_shape=(kept, kept, kept, pltpu.VMEM((2, ni, nl, LANES), F32), kept, kept,
                       pltpu.VMEM((CG_ITERS + 2, 1, LANES), F32)),
            in_specs=[any_spec] * 4,
            out_specs=(vmem_spec,) * 7,
            scratch_shapes=[
                block, block, block, vm(nj, width), vm(ni, width), vm(ni, width), vm(-(-width // LANES) * LANES, LANES),
                vm(2, nl, LANES), vm(nl // 2, LANES), vm(2, ni, LANES),
                padded, padded, vm(ni + 1, nl, LANES), whole, whole, vm(ni, nl + 2 * PAD, LANES), whole,
                whole, whole,
                vm(slots, nl // 2, LANES), vm(slots, 2, ni, LANES),
                vm(slots, 2, nl, LANES), vm(slots, nl // 2, LANES), vm(slots, 2, ni, LANES),
                vm(CG_ITERS + 1, 1, LANES), vm(CG_ITERS + 1, devices, 1, LANES),
                dma((slots, 2)), dma((slots,)), dma((slots, 2)), dma((slots, 2)), dma((slots,)), dma((slots, 2)),
                dma((CG_ITERS + 1,)), dma((CG_ITERS + 1,)), dma((6,)), pltpu.SemaphoreType.REGULAR((6,)),
            ],
            compiler_params=pltpu.CompilerParams(has_side_effects=True, collective_id=0, vmem_limit_bytes=28 << 20),
        )(*(pltpu.with_memory_space_constraint(a, pltpu.HBM) for a in (k_ghost, flip(k_cell), flip(f_rhs), flip(u_init))))
        chunk = ni // 4
        out_block = jax.ShapeDtypeStruct((ni, nl, nj), F32)
        x_new, r_new, hist = pl.pallas_call(
            functools.partial(finish_kernel, chunk),
            out_shape=(out_block, out_block, jax.ShapeDtypeStruct((CG_ITERS,), F32)),
            in_specs=[vmem_spec] * 7,
            out_specs=(any_spec,) * 3,
            scratch_shapes=[block, block, pltpu.SMEM((CG_ITERS,), F32), dma((2, ni // chunk)), dma],
            compiler_params=pltpu.CompilerParams(vmem_limit_bytes=28 << 20),
        )(scal, *state)
        return flip(x_new), flip(r_new), hist

    return jax.shard_map(local_solve, mesh=mesh, in_specs=(grid_spec, P(), grid_spec, grid_spec),
                         out_specs=(grid_spec, grid_spec, P()), check_vma=False)
```

```python
import functools

import jax
import jax.numpy as jnp
from jax import lax
from jax.experimental import pallas as pl
from jax.experimental.pallas import tpu as pltpu
from jax.sharding import PartitionSpec as P

CG_ITERS = 8
LANES = 128
PAD = 8
GROUP = 6
COLUMNS = 16
MESH = pl.DeviceIdType.MESH
F32 = jnp.float32


def solve_kernel(dims, counts, kg_hbm, k_hbm, f_hbm, u_hbm, x, n, p, r, w, s, scal_ref,
                 k_in, f_in, u_in, wall_x, wall_y, wall_z, wall_t, bx, by, bz,
                 kp, mp, cx, cy, cyh, cz, inv, z,
                 ys, zs, xr, yr, zr, red_s, red_r,
                 xs_sem, ys_sem, zs_sem, xr_sem, yr_sem, zr_sem, rs_sem, rr_sem, in_sem, near_sem):
    ni, nl, nj = dims
    ngx, ngy, ngz = counts
    half = nl // 2
    gx, gy, gz = lax.axis_index('gx'), lax.axis_index('gy'), lax.axis_index('gz')
    rows = pl.ds(PAD, nl)
    rows_dn = pl.ds(PAD - 1, nl)
    rows_up = pl.ds(PAD + 1, nl)
    lane = lax.broadcasted_iota(jnp.int32, (nl, LANES), 1)
    lane_i = lax.broadcasted_iota(jnp.int32, (ni, LANES), 1)
    lane_half = lax.broadcasted_iota(jnp.int32, (half, LANES), 1)
    lane_row = lax.broadcasted_iota(jnp.int32, (1, LANES), 1)
    inside = lane < nj
    has_xlo, has_xhi = gx > 0, gx < ngx - 1
    has_zlo, has_zhi = gz > 0, gz < ngz - 1
    face_lane = jnp.where(gy == 0, nj - 1, 0)
    y_low_wall, y_high_wall = gy == 0, gy > 0
    zero_slab = jnp.zeros((nl, LANES), F32)
    zero_acc = jnp.zeros((8, LANES), F32)
    relative = [(a, b, c) for a in reversed(range(ngz)) for b in reversed(range(ngy)) for c in reversed(range(ngx))
                if a or b or c]

    def other(a, b, c):
        return lax.rem(gz + a, ngz), lax.rem(gy + b, ngy), lax.rem(gx + c, ngx)

    def column_roll(slab, shift):
        return pltpu.roll(slab, shift + 2 * LANES, 1)

    def slabs(group, step, init):
        def body(g, carry):
            for k in range(group):
                carry = step(g * group + k, carry)
            return carry
        return lax.fori_loop(0, ni // group, body, init)

    def x_copy(ref, slot, up):
        src = ref.at[ni if up else 1, rows]
        return pltpu.make_async_remote_copy(
            src_ref=src, dst_ref=xr.at[slot, 0 if up else 1], send_sem=xs_sem.at[slot, 0 if up else 1],
            recv_sem=xr_sem.at[slot, 0 if up else 1], device_id=(gz, gy, gx + 1 if up else gx - 1), device_id_type=MESH)

    def z_copy(slot, up):
        return pltpu.make_async_remote_copy(
            src_ref=zs.at[slot, 0 if up else 1], dst_ref=zr.at[slot, 0 if up else 1],
            send_sem=zs_sem.at[slot, 0 if up else 1], recv_sem=zr_sem.at[slot, 0 if up else 1],
            device_id=(gz + 1 if up else gz - 1, gy, gx), device_id_type=MESH)

    def y_copy(slot):
        return pltpu.make_async_remote_copy(
            src_ref=ys.at[slot], dst_ref=yr.at[slot], send_sem=ys_sem.at[slot], recv_sem=yr_sem.at[slot],
            device_id=(gz, 1 - gy, gx), device_id_type=MESH)

    def pack_rolls(ref, slot, i):
        row = lax.max(i, 0) if not isinstance(i, int) else i
        slab = ref[row + 1, rows, :]
        zs[slot, 1, pl.ds(row, 1), :] = slab[0:1, :]
        zs[slot, 0, pl.ds(row, 1), :] = slab[nl - 1:nl, :]
        return column_roll(slab[0:half], row - face_lane), column_roll(slab[half:nl], row - face_lane + LANES // 2)

    def pack(i, rolled, acc):
        acc = jnp.where(lane_half == i, rolled[0], acc)
        return jnp.where(lane_half == i + LANES // 2, rolled[1], acc)

    def packed_pass(ref, slot, step, init, tail=lambda state: state):
        def body(g, carry):
            state, acc = carry
            rolled = [pack_rolls(ref, slot, (g - 1) * GROUP + k) for k in range(GROUP)]
            for k in range(GROUP):
                state = step(g * GROUP + k, state)
            for k in range(GROUP):
                acc = pack((g - 1) * GROUP + k, rolled[k], acc)
            return state, acc
        state, acc = lax.fori_loop(0, ni // GROUP, body, (init, jnp.zeros((half, LANES), F32)))
        rolled = [pack_rolls(ref, slot, ni - GROUP + k) for k in range(GROUP)]
        state = tail(state)
        for k in range(GROUP):
            acc = pack(ni - GROUP + k, rolled[k], acc)
        ys[slot] = acc
        return state

    def exchange_start(ref, slot):
        pl.when(has_xlo)(lambda: x_copy(ref, slot, False).start())
        pl.when(has_xhi)(lambda: x_copy(ref, slot, True).start())
        pl.when(has_zlo)(lambda: z_copy(slot, False).start())
        pl.when(has_zhi)(lambda: z_copy(slot, True).start())
        y_copy(slot).start()

    def exchange_wait(ref, slot):
        @pl.when(has_xlo)
        def _():
            x_copy(ref, slot, False).wait_send()
            x_copy(ref, slot, True).wait_recv()

        @pl.when(has_xhi)
        def _():
            x_copy(ref, slot, True).wait_send()
            x_copy(ref, slot, False).wait_recv()

        @pl.when(has_zlo)
        def _():
            z_copy(slot, False).wait_send()
            z_copy(slot, True).wait_recv()

        @pl.when(has_zhi)
        def _():
            z_copy(slot, True).wait_send()
            z_copy(slot, False).wait_recv()

        y_copy(slot).wait()

    def add_rows(ref, layer, row):
        for i in range(ni):
            ref[i, row:row + 1, :] = ref[i, row:row + 1, :] + layer[i:i + 1, :]

    def add_columns(ref, packed):
        mask = lane == face_lane

        def step(g, _):
            columns = []
            for k in range(min(COLUMNS, ni)):
                i = g * min(COLUMNS, ni) + k
                columns.append((column_roll(packed, face_lane - i), column_roll(packed, face_lane - i - LANES // 2)))
            for k in range(min(COLUMNS, ni)):
                i = g * min(COLUMNS, ni) + k
                ref[i] = ref[i] + jnp.where(mask, jnp.concatenate(columns[k], axis=0), 0.0)
            return 0

        lax.fori_loop(0, ni // min(COLUMNS, ni), step, 0)

    def join_faces(ref, slot):
        y_copy(slot).wait()
        add_columns(n, by[...] * (ys[slot] - yr[slot]))

        @pl.when(has_xlo)
        def _():
            x_copy(ref, slot, False).wait_send()
            x_copy(ref, slot, True).wait_recv()
            n[0] = n[0] + bx[0] * (ref[1, rows, :] - xr[slot, 0])

        @pl.when(has_xhi)
        def _():
            x_copy(ref, slot, True).wait_send()
            x_copy(ref, slot, False).wait_recv()
            n[ni - 1] = n[ni - 1] + bx[1] * (ref[ni, rows, :] - xr[slot, 1])

        @pl.when(has_zlo)
        def _():
            z_copy(slot, False).wait_send()
            z_copy(slot, True).wait_recv()
            add_rows(n, bz[0] * (zs[slot, 1] - zr[slot, 0]), 0)

        @pl.when(has_zhi)
        def _():
            z_copy(slot, True).wait_send()
            z_copy(slot, False).wait_recv()
            add_rows(n, bz[1] * (zs[slot, 0] - zr[slot, 1]), nl - 1)

    def stencil(ref):
        def step(i, carry):
            v, flux_x = carry
            above = ref[i + 2, rows, :]
            flux_next = cx[i + 1] * (above - v)
            flux_zl = cz[i, rows, :] * (v - ref[i + 1, rows_dn, :])
            flux_zh = cz[i, rows_up, :] * (ref[i + 1, rows_up, :] - v)
            flux_yl = cy[i] * (v - pltpu.roll(v, 1, 1))
            flux_yh = cyh[i] * (pltpu.roll(v, LANES - 1, 1) - v)
            n[i] = (flux_x - flux_next) + (flux_yl - flux_yh) + (flux_zl - flux_zh)
            return above, flux_next

        first = ref[1, rows, :]
        slabs(GROUP, step, (first, cx[0] * (first - ref[0, rows, :])))

    def fold(slab):
        out = slab[0:8]
        for part in range(8, nl, 8):
            out = out + slab[part:part + 8]
        return out

    def reduce_row(slot, accs):
        row = jnp.zeros((1, LANES), F32)
        for q, acc in enumerate(accs):
            row = jnp.where(lane_row == q, jnp.sum(jnp.sum(acc, axis=0, keepdims=True), axis=1, keepdims=True), row)
        red_s[slot] = row
        red_r[slot, (gz * ngy + gy) * ngx + gx] = row

    def reduce_send(slot):
        me = (gz * ngy + gy) * ngx + gx
        for delta in relative:
            pltpu.make_async_remote_copy(
                src_ref=red_s.at[slot], dst_ref=red_r.at[slot, me], send_sem=rs_sem.at[slot],
                recv_sem=rr_sem.at[slot], device_id=other(*delta), device_id_type=MESH).start()

    def reduce_wait(slot, count):
        whole = red_r.at[slot, pl.ds(0, len(relative))]
        done = pltpu.make_async_remote_copy(
            src_ref=whole, dst_ref=whole, send_sem=rs_sem.at[slot], recv_sem=rr_sem.at[slot],
            device_id=(gz, gy, gx), device_id_type=MESH)
        done.wait_recv()
        done.wait_send()
        total = jnp.sum(red_r[slot], axis=0)
        return [jnp.sum(jnp.where(lane_row == q, total, 0.0), axis=1, keepdims=True) for q in range(count)]

    x_row, z_row = jnp.where(gx == 0, 0, 1), jnp.where(gz == 0, 4, 5)
    slabs_i = pl.ds(pl.multiple_of(gx * ni, 8), ni)
    inputs = [
        pltpu.make_async_copy(k_hbm, k_in, in_sem.at[0]),
        pltpu.make_async_copy(u_hbm, u_in, in_sem.at[1]),
        pltpu.make_async_copy(kg_hbm.at[x_row, pl.ds(pl.multiple_of(gy * nj, 8), nj)], wall_x, in_sem.at[2]),
        pltpu.make_async_copy(kg_hbm.at[2 + gy, slabs_i], wall_y, in_sem.at[3]),
        pltpu.make_async_copy(kg_hbm.at[z_row, slabs_i], wall_z, in_sem.at[4]),
        pltpu.make_async_copy(f_hbm, f_in, in_sem.at[5]),
    ]
    for copy in inputs[:5]:
        copy.start()

    def tell_neighbours(sem):
        tell = lambda *target: pl.semaphore_signal(sem, inc=1, device_id=target, device_id_type=MESH)
        pl.when(has_xlo)(lambda: tell(gz, gy, gx - 1))
        pl.when(has_xhi)(lambda: tell(gz, gy, gx + 1))
        pl.when(has_zlo)(lambda: tell(gz - 1, gy, gx))
        pl.when(has_zhi)(lambda: tell(gz + 1, gy, gx))
        tell(gz, 1 - gy, gx)

    neighbours = 5 - jnp.where(has_xlo, 0, 1) - jnp.where(has_xhi, 0, 1) - jnp.where(has_zlo, 0, 1) - jnp.where(has_zhi, 0, 1)
    rounds = (ngx - 1) + (ngy - 1) + (ngz - 1) - 1

    def next_round(k):
        pl.semaphore_wait(near_sem.at[k], neighbours)
        if k + 1 < rounds:
            tell_neighbours(near_sem.at[k + 1])

    barrier = pltpu.get_barrier_semaphore()
    tell_neighbours(barrier)

    for edge in (0, ni + 1):
        mp[edge] = jnp.zeros((nl + 2 * PAD, LANES), F32)
        kp[edge] = jnp.ones((nl + 2 * PAD, LANES), F32)

    def clear(i, _):
        mp[i + 1, pl.ds(0, PAD), :] = jnp.zeros((PAD, LANES), F32)
        mp[i + 1, pl.ds(PAD + nl, PAD), :] = jnp.zeros((PAD, LANES), F32)
        kp[i + 1, pl.ds(0, PAD), :] = jnp.ones((PAD, LANES), F32)
        kp[i + 1, pl.ds(PAD + nl, PAD), :] = jnp.ones((PAD, LANES), F32)
        mp[i + 1, rows, :] = zero_slab
        s[i] = zero_slab
        z[i] = zero_slab
        p[i] = zero_slab
        r[1, i] = zero_slab
        r[0, i] = zero_slab
        kp[i + 1, rows, :] = jnp.full((nl, LANES), 1.0, F32)
        return 0

    lax.fori_loop(0, ni, clear, 0)

    def load_k(i, _):
        kp[i + 1, rows, 0:nj] = k_in[i]
        return 0

    def load_u(i, _):
        mp[i + 1, rows, 0:nj] = u_in[i]
        return 0

    inputs[0].wait()
    inputs[5].start()
    packed_pass(kp, 0, load_k, 0)
    pl.semaphore_wait(barrier, neighbours)
    tell_neighbours(near_sem.at[0])
    exchange_start(kp, 0)
    inputs[1].wait()
    packed_pass(mp, 1, load_u, 0)
    exchange_start(mp, 1)
    next_round(0)

    for copy in inputs[2:5]:
        copy.wait()
    width = wall_x.shape[1]
    l_rows = pl.ds(pl.multiple_of(gz * nl, 8), nl)

    def flipped(wall, count):
        for start in range(0, width, LANES):
            size = min(LANES, width - start)
            block = jnp.concatenate([wall[:, start:start + size], jnp.ones((LANES - count, size), F32)], axis=0)
            wall_t[start:start + size, :] = block.T
        return wall_t[l_rows, :]

    x_wall = flipped(wall_x, nj)
    y_wall = flipped(wall_y, ni)
    if width > LANES:
        rest = jnp.concatenate([wall_z[:, LANES:width], jnp.ones((ni, 2 * LANES - width), F32)], axis=1)
        whole_z = wall_z[:, 0:LANES]
        turn = LANES - nj
        shifted = jnp.where(lane_i < turn, pltpu.roll(whole_z, turn, 1), pltpu.roll(rest, turn, 1))
    else:
        whole_z = jnp.concatenate([wall_z[...], jnp.ones((ni, LANES - width), F32)], axis=1)
        shifted = pltpu.roll(whole_z, LANES - nj, 1)
    z_wall = jnp.where(gy == 0, whole_z, shifted)

    def harmonic(left, right):
        return 2.0 * left * right / (left + right)

    next_round(1)

    in_i = lane_i < nj
    cx[0] = jnp.where(jnp.logical_and(inside, gx == 0), harmonic(x_wall, kp[1, rows, :]), 0.0)
    z_low = jnp.where(jnp.logical_and(in_i, gz == 0), harmonic(z_wall, zs[0, 1]), 0.0)
    z_high = jnp.where(jnp.logical_and(in_i, gz == ngz - 1), harmonic(zs[0, 0], z_wall), 0.0)
    y_low_mask = jnp.logical_and(inside, jnp.logical_or(lane > 0, y_low_wall))
    y_high_mask = jnp.logical_and(inside, jnp.logical_or(lane < nj - 1, y_high_wall))
    wall_lane = nj - 1 - face_lane

    def coefs(i, _):
        here = kp[i + 1, rows, :]
        cx[i + 1] = jnp.where(inside, harmonic(here, kp[i + 2, rows, :]), 0.0)
        cz[i, rows_up, :] = jnp.where(inside, harmonic(here, kp[i + 1, rows_up, :]), 0.0)
        wall = column_roll(y_wall, wall_lane - i)
        low = jnp.where(lane == 0, wall, pltpu.roll(here, 1, 1))
        high = jnp.where(lane == nj - 1, wall, pltpu.roll(here, LANES - 1, 1))
        cy[i] = jnp.where(y_low_mask, harmonic(low, here), 0.0)
        cyh[i] = jnp.where(y_high_mask, harmonic(here, high), 0.0)
        return 0

    slabs(GROUP, coefs, 0)
    next_round(2)
    cx[ni] = jnp.where(jnp.logical_and(inside, gx == ngx - 1), harmonic(kp[ni, rows, :], x_wall), 0.0)
    for i in range(ni):
        cz[i, PAD:PAD + 1, :] = z_low[i:i + 1, :]
        cz[i, PAD + nl:PAD + nl + 1, :] = z_high[i:i + 1, :]

    stencil(mp)

    def diagonal(i, _):
        inv[i] = cx[i] + cx[i + 1] + cy[i] + cyh[i] + cz[i, rows, :] + cz[i, rows_up, :]
        return 0

    lax.fori_loop(0, ni, diagonal, 0)
    next_round(3)

    exchange_wait(kp, 0)

    @pl.when(has_xlo)
    def _():
        bx[0] = jnp.where(inside, harmonic(xr[0, 0], kp[1, rows, :]), 0.0)
        inv[0] = inv[0] + bx[0]

    @pl.when(has_xhi)
    def _():
        bx[1] = jnp.where(inside, harmonic(kp[ni, rows, :], xr[0, 1]), 0.0)
        inv[ni - 1] = inv[ni - 1] + bx[1]

    @pl.when(has_zlo)
    def _():
        bz[0] = jnp.where(in_i, harmonic(zr[0, 0], zs[0, 1]), 0.0)
        add_rows(inv, bz[0], 0)

    @pl.when(has_zhi)
    def _():
        bz[1] = jnp.where(in_i, harmonic(zs[0, 0], zr[0, 1]), 0.0)
        add_rows(inv, bz[1], nl - 1)

    y_face = jnp.where(lax.rem(lane_half, LANES // 2) < ni, harmonic(ys[0], yr[0]), 0.0)
    by[...] = y_face
    add_columns(inv, y_face)
    join_faces(mp, 1)
    inputs[5].wait()

    def first_residual(i, acc):
        iv = jnp.where(inside, 1.0 / jnp.where(inside, inv[i], 1.0), 0.0)
        inv[i] = iv
        x[i] = mp[i + 1, rows, :]
        r[0, i, :, 0:nj] = f_in[i]
        res = r[0, i] - n[i]
        r[0, i] = res
        u = res * iv
        mp[i + 1, rows, :] = u
        return acc + fold(res * u)

    gamma_acc = packed_pass(mp, 2, first_residual, zero_acc)
    exchange_start(mp, 2)
    next_round(4)
    stencil(mp)
    for k in range(5, rounds):
        next_round(k)
    join_faces(mp, 2)

    def first_w(i, acc):
        av = n[i]
        w[i] = av
        acc = acc + fold(av * mp[i + 1, rows, :])
        mp[i + 1, rows, :] = av * inv[i]
        return acc

    packed_pass(mp, 3, first_w, zero_acc, lambda delta_acc: reduce_row(0, (gamma_acc, delta_acc)))

    def scalars(t, sums, gamma_old, pap_old):
        gamma, delta, sigma = sums[0], sums[1], sums[2]
        beta = jnp.where(t == 0, 0.0, gamma / gamma_old)
        pap = delta + 2.0 * beta * sigma + beta * beta * pap_old
        return gamma, pap, beta[0, 0], (gamma / pap)[0, 0]

    def advance_x(now, alpha, beta):
        def step(i, acc):
            p_new = inv[i] * r[1 - now, i] + beta * p[i]
            p[i] = p_new
            x[i] = x[i] + alpha * p_new
            return acc + fold(r[now, i] * r[now, i])
        return lax.fori_loop(0, ni, step, zero_acc)

    def iteration(t, carry):
        gamma_old, pap_old, alpha_old, beta_old = carry
        now = lax.rem(t, 2)
        reduce_send(t)
        exchange_start(mp, t + 3)
        stencil(mp)
        rr_acc = advance_x(now, alpha_old, beta_old)
        join_faces(mp, t + 3)
        sums = reduce_wait(t, 4)
        gamma, pap, beta, alpha = scalars(t, sums, gamma_old, pap_old)

        def update(i, acc):
            iv = inv[i]
            w_old = w[i]
            z_new = n[i] + beta * z[i]
            s_new = w_old + beta * s[i]
            r_new = r[now, i] - alpha * s_new
            w_new = w_old - alpha * z_new
            u_new = iv * r_new
            z[i] = z_new
            s[i] = s_new
            r[1 - now, i] = r_new
            w[i] = w_new
            mp[i + 1, rows, :] = iv * w_new
            return acc[0] + fold(r_new * u_new), acc[1] + fold(w_new * u_new), acc[2] + fold(u_new * s_new)

        packed_pass(mp, t + 4, update, (zero_acc,) * 3, lambda accs: reduce_row(t + 1, accs + (rr_acc,)))
        scal_ref[lax.rem(t + CG_ITERS - 2, CG_ITERS)] = jnp.broadcast_to(sums[3], (1, LANES))
        return gamma, pap, alpha, beta

    one = jnp.ones((1, 1), F32)
    last = CG_ITERS - 1
    gamma_old, pap_old, alpha_old, beta_old = lax.fori_loop(
        0, last, iteration, (one, one, jnp.float32(0.0), jnp.float32(0.0)))

    now = last % 2
    reduce_send(last)

    def last_dots(i, acc):
        rv, sv = r[now, i], s[i]
        wv = w[i]
        n[i] = inv[i] * rv
        pairs = ((rv, rv), (rv, wv), (rv, sv), (wv, wv), (wv, sv), (sv, sv))
        return tuple(a + fold(b * c) for a, (b, c) in zip(acc, pairs))

    reduce_row(CG_ITERS, slabs(2, last_dots, (zero_acc,) * 6))
    reduce_send(CG_ITERS)
    advance_x(now, alpha_old, beta_old)
    sums = reduce_wait(last, 4)
    wide = lambda value: jnp.broadcast_to(value, (1, LANES))
    scal_ref[last - 2] = wide(sums[3])
    gamma = sums[0]
    beta = gamma / gamma_old
    alpha = gamma / (sums[1] + 2.0 * beta * sums[2] + beta * beta * pap_old)
    scal_ref[CG_ITERS] = wide(alpha)
    scal_ref[CG_ITERS + 1] = wide(beta)
    rr, rw, rs, ww, ws, ss = reduce_wait(CG_ITERS, 6)
    scal_ref[last - 1] = wide(rr)
    scal_ref[last] = wide(rr - 2.0 * alpha * (rw + beta * rs) + alpha * alpha * (ww + 2.0 * beta * ws + beta * beta * ss))


def finish_kernel(chunk, scal, x, u, p, r, w, s, x_hbm, r_hbm, hist_hbm, x_new, r_new, hist, sem, hist_sem):
    ni, nl, nj = x_new.shape
    alpha = jnp.broadcast_to(scal[CG_ITERS], (nl, LANES))
    beta = jnp.broadcast_to(scal[CG_ITERS + 1], (nl, LANES))
    copies = []

    def step(i, _):
        x_new[i] = (x[i] + alpha * (u[i] + beta * p[i]))[:, 0:nj]
        r_new[i] = (r[1, i] - alpha * (w[i] + beta * s[i]))[:, 0:nj]
        return 0

    for g in range(ni // chunk):
        lax.fori_loop(g * chunk, (g + 1) * chunk, step, 0)
        part = pl.ds(g * chunk, chunk)
        for j, (src, dst) in enumerate(((x_new, x_hbm), (r_new, r_hbm))):
            copies.append(pltpu.make_async_copy(src.at[part], dst.at[part], sem.at[j, g]))
            copies[-1].start()
        if g == 0:
            for t in range(CG_ITERS):
                hist[t] = scal[t, 0, 0]
            copies.append(pltpu.make_async_copy(hist, hist_hbm, hist_sem))
            copies[-1].start()
    for copy in copies:
        copy.wait()


def solution(mesh):
    counts = (mesh.shape['gx'], mesh.shape['gy'], mesh.shape['gz'])
    grid_spec = P('gx', 'gy', 'gz')

    def local_solve(k_cell, k_ghost, f_rhs, u_init):
        ni, nj, nl = k_cell.shape
        flip = lambda a: jnp.swapaxes(a, 1, 2)
        slots = CG_ITERS + 3
        devices = counts[0] * counts[1] * counts[2]
        width = k_ghost.shape[2]
        any_spec = pl.BlockSpec(memory_space=pl.ANY)
        vm = lambda *shape: pltpu.VMEM(shape, F32)
        whole = vm(ni, nl, LANES)
        block = vm(ni, nl, nj)
        padded = vm(ni + 2, nl + 2 * PAD, LANES)
        dma = pltpu.SemaphoreType.DMA
        kept = pltpu.VMEM((ni, nl, LANES), F32)
        vmem_spec = pl.BlockSpec(memory_space=pltpu.VMEM)
        *state, scal = pl.pallas_call(
            functools.partial(solve_kernel, (ni, nl, nj), counts),
            out_shape=(kept, kept, kept, pltpu.VMEM((2, ni, nl, LANES), F32), kept, kept,
                       pltpu.VMEM((CG_ITERS + 2, 1, LANES), F32)),
            in_specs=[any_spec] * 4,
            out_specs=(vmem_spec,) * 7,
            scratch_shapes=[
                block, block, block, vm(nj, width), vm(ni, width), vm(ni, width), vm(-(-width // LANES) * LANES, LANES),
                vm(2, nl, LANES), vm(nl // 2, LANES), vm(2, ni, LANES),
                padded, padded, vm(ni + 1, nl, LANES), whole, whole, vm(ni, nl + 2 * PAD, LANES), whole,
                whole,
                vm(slots, nl // 2, LANES), vm(slots, 2, ni, LANES),
                vm(slots, 2, nl, LANES), vm(slots, nl // 2, LANES), vm(slots, 2, ni, LANES),
                vm(CG_ITERS + 1, 1, LANES), vm(CG_ITERS + 1, devices, 1, LANES),
                dma((slots, 2)), dma((slots,)), dma((slots, 2)), dma((slots, 2)), dma((slots,)), dma((slots, 2)),
                dma((CG_ITERS + 1,)), dma((CG_ITERS + 1,)), dma((6,)), pltpu.SemaphoreType.REGULAR((6,)),
            ],
            compiler_params=pltpu.CompilerParams(has_side_effects=True, collective_id=0, vmem_limit_bytes=28 << 20),
        )(*(pltpu.with_memory_space_constraint(a, pltpu.HBM) for a in (k_ghost, flip(k_cell), flip(f_rhs), flip(u_init))))
        chunk = ni // 4
        out_block = jax.ShapeDtypeStruct((ni, nl, nj), F32)
        x_new, r_new, hist = pl.pallas_call(
            functools.partial(finish_kernel, chunk),
            out_shape=(out_block, out_block, jax.ShapeDtypeStruct((CG_ITERS,), F32)),
            in_specs=[vmem_spec] * 7,
            out_specs=(any_spec,) * 3,
            scratch_shapes=[block, block, pltpu.SMEM((CG_ITERS,), F32), dma((2, ni // chunk)), dma],
            compiler_params=pltpu.CompilerParams(vmem_limit_bytes=28 << 20),
        )(scal, *state)
        return flip(x_new), flip(r_new), hist

    return jax.shard_map(local_solve, mesh=mesh, in_specs=(grid_spec, P(), grid_spec, grid_spec),
                         out_specs=(grid_spec, grid_spec, P()), check_vma=False)
```

```python
import functools

import jax
import jax.numpy as jnp
from jax import lax
from jax.experimental import pallas as pl
from jax.experimental.pallas import tpu as pltpu
from jax.sharding import PartitionSpec as P

CG_ITERS = 8
LANES = 128
PAD = 8
GROUP = 6
COLUMNS = 16
MESH = pl.DeviceIdType.MESH
F32 = jnp.float32


def solve_kernel(dims, counts, kg_hbm, k_hbm, f_hbm, u_hbm, x, n, p, r, w, s, scal_ref,
                 k_in, f_in, u_in, wall_x, wall_y, wall_z, wall_t, bx, by, bz,
                 kp, mp, cx, cy, cyh, cz, inv, z,
                 ys, zs, xr, yr, zr, red_s, red_r,
                 xs_sem, ys_sem, zs_sem, xr_sem, yr_sem, zr_sem, rs_sem, rr_sem, in_sem, near_sem):
    ni, nl, nj = dims
    ngx, ngy, ngz = counts
    half = nl // 2
    gx, gy, gz = lax.axis_index('gx'), lax.axis_index('gy'), lax.axis_index('gz')
    rows = pl.ds(PAD, nl)
    rows_dn = pl.ds(PAD - 1, nl)
    rows_up = pl.ds(PAD + 1, nl)
    lane = lax.broadcasted_iota(jnp.int32, (nl, LANES), 1)
    lane_i = lax.broadcasted_iota(jnp.int32, (ni, LANES), 1)
    lane_half = lax.broadcasted_iota(jnp.int32, (half, LANES), 1)
    lane_row = lax.broadcasted_iota(jnp.int32, (1, LANES), 1)
    inside = lane < nj
    has_xlo, has_xhi = gx > 0, gx < ngx - 1
    has_zlo, has_zhi = gz > 0, gz < ngz - 1
    face_lane = jnp.where(gy == 0, nj - 1, 0)
    y_low_wall, y_high_wall = gy == 0, gy > 0
    zero_slab = jnp.zeros((nl, LANES), F32)
    zero_acc = jnp.zeros((8, LANES), F32)
    others = ngx * ngy * ngz - 1

    def column_roll(slab, shift):
        return pltpu.roll(slab, shift + 2 * LANES, 1)

    def slabs(group, step, init):
        def body(g, carry):
            for k in range(group):
                carry = step(g * group + k, carry)
            return carry
        return lax.fori_loop(0, ni // group, body, init)

    def x_copy(ref, slot, up):
        src = ref.at[ni if up else 1, rows]
        return pltpu.make_async_remote_copy(
            src_ref=src, dst_ref=xr.at[slot, 0 if up else 1], send_sem=xs_sem.at[slot, 0 if up else 1],
            recv_sem=xr_sem.at[slot, 0 if up else 1], device_id=(gz, gy, gx + 1 if up else gx - 1), device_id_type=MESH)

    def z_copy(slot, up):
        return pltpu.make_async_remote_copy(
            src_ref=zs.at[slot, 0 if up else 1], dst_ref=zr.at[slot, 0 if up else 1],
            send_sem=zs_sem.at[slot, 0 if up else 1], recv_sem=zr_sem.at[slot, 0 if up else 1],
            device_id=(gz + 1 if up else gz - 1, gy, gx), device_id_type=MESH)

    def y_copy(slot):
        return pltpu.make_async_remote_copy(
            src_ref=ys.at[slot], dst_ref=yr.at[slot], send_sem=ys_sem.at[slot], recv_sem=yr_sem.at[slot],
            device_id=(gz, 1 - gy, gx), device_id_type=MESH)

    def pack_rolls(ref, slot, i):
        row = lax.max(i, 0) if not isinstance(i, int) else i
        slab = ref[row + 1, rows, :]
        zs[slot, 1, pl.ds(row, 1), :] = slab[0:1, :]
        zs[slot, 0, pl.ds(row, 1), :] = slab[nl - 1:nl, :]
        return column_roll(slab[0:half], row - face_lane), column_roll(slab[half:nl], row - face_lane + LANES // 2)

    def pack(i, rolled, acc):
        acc = jnp.where(lane_half == i, rolled[0], acc)
        return jnp.where(lane_half == i + LANES // 2, rolled[1], acc)

    def packed_pass(ref, slot, step, init, tail=lambda state: state):
        def body(g, carry):
            state, acc = carry
            rolled = [pack_rolls(ref, slot, (g - 1) * GROUP + k) for k in range(GROUP)]
            for k in range(GROUP):
                state = step(g * GROUP + k, state)
            for k in range(GROUP):
                acc = pack((g - 1) * GROUP + k, rolled[k], acc)
            return state, acc
        state, acc = lax.fori_loop(0, ni // GROUP, body, (init, jnp.zeros((half, LANES), F32)))
        rolled = [pack_rolls(ref, slot, ni - GROUP + k) for k in range(GROUP)]
        state = tail(state)
        for k in range(GROUP):
            acc = pack(ni - GROUP + k, rolled[k], acc)
        ys[slot] = acc
        return state

    def exchange_start(ref, slot):
        y_copy(slot).start()
        pl.when(has_zlo)(lambda: z_copy(slot, False).start())
        pl.when(has_zhi)(lambda: z_copy(slot, True).start())
        pl.when(has_xlo)(lambda: x_copy(ref, slot, False).start())
        pl.when(has_xhi)(lambda: x_copy(ref, slot, True).start())

    def exchange_wait(ref, slot):
        @pl.when(has_xlo)
        def _():
            x_copy(ref, slot, False).wait_send()
            x_copy(ref, slot, True).wait_recv()

        @pl.when(has_xhi)
        def _():
            x_copy(ref, slot, True).wait_send()
            x_copy(ref, slot, False).wait_recv()

        @pl.when(has_zlo)
        def _():
            z_copy(slot, False).wait_send()
            z_copy(slot, True).wait_recv()

        @pl.when(has_zhi)
        def _():
            z_copy(slot, True).wait_send()
            z_copy(slot, False).wait_recv()

        y_copy(slot).wait()

    def add_rows(ref, layer, row):
        for i in range(ni):
            ref[i, row:row + 1, :] = ref[i, row:row + 1, :] + layer[i:i + 1, :]

    def add_columns(ref, packed):
        mask = lane == face_lane

        def step(g, _):
            columns = []
            for k in range(min(COLUMNS, ni)):
                i = g * min(COLUMNS, ni) + k
                columns.append((column_roll(packed, face_lane - i), column_roll(packed, face_lane - i - LANES // 2)))
            for k in range(min(COLUMNS, ni)):
                i = g * min(COLUMNS, ni) + k
                ref[i] = ref[i] + jnp.where(mask, jnp.concatenate(columns[k], axis=0), 0.0)
            return 0

        lax.fori_loop(0, ni // min(COLUMNS, ni), step, 0)

    def join_faces(ref, slot):
        y_copy(slot).wait()
        add_columns(n, by[...] * (ys[slot] - yr[slot]))

        @pl.when(has_xlo)
        def _():
            x_copy(ref, slot, False).wait_send()
            x_copy(ref, slot, True).wait_recv()
            n[0] = n[0] + bx[0] * (ref[1, rows, :] - xr[slot, 0])

        @pl.when(has_xhi)
        def _():
            x_copy(ref, slot, True).wait_send()
            x_copy(ref, slot, False).wait_recv()
            n[ni - 1] = n[ni - 1] + bx[1] * (ref[ni, rows, :] - xr[slot, 1])

        @pl.when(has_zlo)
        def _():
            z_copy(slot, False).wait_send()
            z_copy(slot, True).wait_recv()
            add_rows(n, bz[0] * (zs[slot, 1] - zr[slot, 0]), 0)

        @pl.when(has_zhi)
        def _():
            z_copy(slot, True).wait_send()
            z_copy(slot, False).wait_recv()
            add_rows(n, bz[1] * (zs[slot, 0] - zr[slot, 1]), nl - 1)

    def stencil(ref):
        def step(i, carry):
            v, flux_x = carry
            above = ref[i + 2, rows, :]
            flux_next = cx[i + 1] * (above - v)
            flux_zl = cz[i, rows, :] * (v - ref[i + 1, rows_dn, :])
            flux_zh = cz[i, rows_up, :] * (ref[i + 1, rows_up, :] - v)
            flux_yl = cy[i] * (v - pltpu.roll(v, 1, 1))
            flux_yh = cyh[i] * (pltpu.roll(v, LANES - 1, 1) - v)
            n[i] = (flux_x - flux_next) + (flux_yl - flux_yh) + (flux_zl - flux_zh)
            return above, flux_next

        first = ref[1, rows, :]
        slabs(GROUP, step, (first, cx[0] * (first - ref[0, rows, :])))

    def fold(slab):
        out = slab[0:8]
        for part in range(8, nl, 8):
            out = out + slab[part:part + 8]
        return out

    def reduce_row(slot, accs):
        row = jnp.zeros((1, LANES), F32)
        for q, acc in enumerate(accs):
            row = jnp.where(lane_row == q, jnp.sum(jnp.sum(acc, axis=0, keepdims=True), axis=1, keepdims=True), row)
        red_s[slot] = row
        red_r[slot, (gz * ngy + gy) * ngx + gx] = row

    def reduce_send(slot, planes):
        me = (gz * ngy + gy) * ngx + gx
        for k in planes:
            z_to = jnp.where(2 * gz < ngz, ngz - 1 - k, k)
            for b in reversed(range(ngy)):
                for c in (2, 3, 1, 0):
                    copy = pltpu.make_async_remote_copy(
                        src_ref=red_s.at[slot], dst_ref=red_r.at[slot, me], send_sem=rs_sem.at[slot], recv_sem=rr_sem.at[slot],
                        device_id=(z_to, lax.rem(gy + b, ngy), lax.rem(gx + c, ngx)), device_id_type=MESH)
                    if b or c:
                        copy.start()
                    else:
                        pl.when(z_to != gz)(copy.start)

    def reduce_wait(slot, count):
        whole = red_r.at[slot, pl.ds(0, others)]
        done = pltpu.make_async_remote_copy(
            src_ref=whole, dst_ref=whole, send_sem=rs_sem.at[slot], recv_sem=rr_sem.at[slot],
            device_id=(gz, gy, gx), device_id_type=MESH)
        done.wait_recv()
        done.wait_send()
        total = jnp.sum(red_r[slot], axis=0)
        return [jnp.sum(jnp.where(lane_row == q, total, 0.0), axis=1, keepdims=True) for q in range(count)]

    x_row, z_row = jnp.where(gx == 0, 0, 1), jnp.where(gz == 0, 4, 5)
    slabs_i = pl.ds(pl.multiple_of(gx * ni, 8), ni)
    inputs = [
        pltpu.make_async_copy(k_hbm, k_in, in_sem.at[0]),
        pltpu.make_async_copy(u_hbm, u_in, in_sem.at[1]),
        pltpu.make_async_copy(kg_hbm.at[x_row, pl.ds(pl.multiple_of(gy * nj, 8), nj)], wall_x, in_sem.at[2]),
        pltpu.make_async_copy(kg_hbm.at[2 + gy, slabs_i], wall_y, in_sem.at[3]),
        pltpu.make_async_copy(kg_hbm.at[z_row, slabs_i], wall_z, in_sem.at[4]),
        pltpu.make_async_copy(f_hbm, f_in, in_sem.at[5]),
    ]
    for copy in inputs[:5]:
        copy.start()

    def tell_neighbours(sem):
        tell = lambda *target: pl.semaphore_signal(sem, inc=1, device_id=target, device_id_type=MESH)
        pl.when(has_xlo)(lambda: tell(gz, gy, gx - 1))
        pl.when(has_xhi)(lambda: tell(gz, gy, gx + 1))
        pl.when(has_zlo)(lambda: tell(gz - 1, gy, gx))
        pl.when(has_zhi)(lambda: tell(gz + 1, gy, gx))
        tell(gz, 1 - gy, gx)

    neighbours = 5 - jnp.where(has_xlo, 0, 1) - jnp.where(has_xhi, 0, 1) - jnp.where(has_zlo, 0, 1) - jnp.where(has_zhi, 0, 1)
    rounds = (ngx - 1) + (ngy - 1) + (ngz - 1) - 1

    def next_round(k):
        pl.semaphore_wait(near_sem.at[k], neighbours)
        if k + 1 < rounds:
            tell_neighbours(near_sem.at[k + 1])

    barrier = pltpu.get_barrier_semaphore()
    tell_neighbours(barrier)

    for edge in (0, ni + 1):
        mp[edge] = jnp.zeros((nl + 2 * PAD, LANES), F32)
        kp[edge] = jnp.ones((nl + 2 * PAD, LANES), F32)

    def clear(i, _):
        mp[i + 1, pl.ds(0, PAD), :] = jnp.zeros((PAD, LANES), F32)
        mp[i + 1, pl.ds(PAD + nl, PAD), :] = jnp.zeros((PAD, LANES), F32)
        kp[i + 1, pl.ds(0, PAD), :] = jnp.ones((PAD, LANES), F32)
        kp[i + 1, pl.ds(PAD + nl, PAD), :] = jnp.ones((PAD, LANES), F32)
        mp[i + 1, rows, :] = zero_slab
        s[i] = zero_slab
        z[i] = zero_slab
        p[i] = zero_slab
        r[1, i] = zero_slab
        r[0, i] = zero_slab
        kp[i + 1, rows, :] = jnp.full((nl, LANES), 1.0, F32)
        return 0

    lax.fori_loop(0, ni, clear, 0)

    def load_k(i, _):
        kp[i + 1, rows, 0:nj] = k_in[i]
        return 0

    def load_u(i, _):
        mp[i + 1, rows, 0:nj] = u_in[i]
        return 0

    inputs[0].wait()
    inputs[5].start()
    packed_pass(kp, 0, load_k, 0)
    pl.semaphore_wait(barrier, neighbours)
    tell_neighbours(near_sem.at[0])
    exchange_start(kp, 0)
    inputs[1].wait()
    packed_pass(mp, 1, load_u, 0)
    exchange_start(mp, 1)
    next_round(0)

    for copy in inputs[2:5]:
        copy.wait()
    width = wall_x.shape[1]
    l_rows = pl.ds(pl.multiple_of(gz * nl, 8), nl)

    def flipped(wall, count):
        for start in range(0, width, LANES):
            size = min(LANES, width - start)
            block = jnp.concatenate([wall[:, start:start + size], jnp.ones((LANES - count, size), F32)], axis=0)
            wall_t[start:start + size, :] = block.T
        return wall_t[l_rows, :]

    x_wall = flipped(wall_x, nj)
    y_wall = flipped(wall_y, ni)
    if width > LANES:
        rest = jnp.concatenate([wall_z[:, LANES:width], jnp.ones((ni, 2 * LANES - width), F32)], axis=1)
        whole_z = wall_z[:, 0:LANES]
        turn = LANES - nj
        shifted = jnp.where(lane_i < turn, pltpu.roll(whole_z, turn, 1), pltpu.roll(rest, turn, 1))
    else:
        whole_z = jnp.concatenate([wall_z[...], jnp.ones((ni, LANES - width), F32)], axis=1)
        shifted = pltpu.roll(whole_z, LANES - nj, 1)
    z_wall = jnp.where(gy == 0, whole_z, shifted)

    def harmonic(left, right):
        return 2.0 * left * right / (left + right)

    next_round(1)

    in_i = lane_i < nj
    cx[0] = jnp.where(jnp.logical_and(inside, gx == 0), harmonic(x_wall, kp[1, rows, :]), 0.0)
    z_low = jnp.where(jnp.logical_and(in_i, gz == 0), harmonic(z_wall, zs[0, 1]), 0.0)
    z_high = jnp.where(jnp.logical_and(in_i, gz == ngz - 1), harmonic(zs[0, 0], z_wall), 0.0)
    y_low_mask = jnp.logical_and(inside, jnp.logical_or(lane > 0, y_low_wall))
    y_high_mask = jnp.logical_and(inside, jnp.logical_or(lane < nj - 1, y_high_wall))
    wall_lane = nj - 1 - face_lane

    def coefs(i, _):
        here = kp[i + 1, rows, :]
        cx[i + 1] = jnp.where(inside, harmonic(here, kp[i + 2, rows, :]), 0.0)
        cz[i, rows_up, :] = jnp.where(inside, harmonic(here, kp[i + 1, rows_up, :]), 0.0)
        wall = column_roll(y_wall, wall_lane - i)
        low = jnp.where(lane == 0, wall, pltpu.roll(here, 1, 1))
        high = jnp.where(lane == nj - 1, wall, pltpu.roll(here, LANES - 1, 1))
        cy[i] = jnp.where(y_low_mask, harmonic(low, here), 0.0)
        cyh[i] = jnp.where(y_high_mask, harmonic(here, high), 0.0)
        return 0

    slabs(GROUP, coefs, 0)
    next_round(2)
    cx[ni] = jnp.where(jnp.logical_and(inside, gx == ngx - 1), harmonic(kp[ni, rows, :], x_wall), 0.0)
    for i in range(ni):
        cz[i, PAD:PAD + 1, :] = z_low[i:i + 1, :]
        cz[i, PAD + nl:PAD + nl + 1, :] = z_high[i:i + 1, :]

    stencil(mp)

    def diagonal(i, _):
        inv[i] = cx[i] + cx[i + 1] + cy[i] + cyh[i] + cz[i, rows, :] + cz[i, rows_up, :]
        return 0

    lax.fori_loop(0, ni, diagonal, 0)
    next_round(3)

    exchange_wait(kp, 0)

    @pl.when(has_xlo)
    def _():
        bx[0] = jnp.where(inside, harmonic(xr[0, 0], kp[1, rows, :]), 0.0)
        inv[0] = inv[0] + bx[0]

    @pl.when(has_xhi)
    def _():
        bx[1] = jnp.where(inside, harmonic(kp[ni, rows, :], xr[0, 1]), 0.0)
        inv[ni - 1] = inv[ni - 1] + bx[1]

    @pl.when(has_zlo)
    def _():
        bz[0] = jnp.where(in_i, harmonic(zr[0, 0], zs[0, 1]), 0.0)
        add_rows(inv, bz[0], 0)

    @pl.when(has_zhi)
    def _():
        bz[1] = jnp.where(in_i, harmonic(zs[0, 0], zr[0, 1]), 0.0)
        add_rows(inv, bz[1], nl - 1)

    y_face = jnp.where(lax.rem(lane_half, LANES // 2) < ni, harmonic(ys[0], yr[0]), 0.0)
    by[...] = y_face
    add_columns(inv, y_face)
    join_faces(mp, 1)
    inputs[5].wait()

    def first_residual(i, acc):
        iv = jnp.where(inside, 1.0 / jnp.where(inside, inv[i], 1.0), 0.0)
        inv[i] = iv
        x[i] = mp[i + 1, rows, :]
        r[0, i, :, 0:nj] = f_in[i]
        res = r[0, i] - n[i]
        r[0, i] = res
        u = res * iv
        mp[i + 1, rows, :] = u
        return acc + fold(res * u)

    gamma_acc = packed_pass(mp, 2, first_residual, zero_acc)
    exchange_start(mp, 2)
    next_round(4)
    stencil(mp)
    for k in range(5, rounds):
        next_round(k)
    join_faces(mp, 2)

    def first_w(i, acc):
        av = n[i]
        w[i] = av
        acc = acc + fold(av * mp[i + 1, rows, :])
        mp[i + 1, rows, :] = av * inv[i]
        return acc

    packed_pass(mp, 3, first_w, zero_acc, lambda delta_acc: reduce_row(0, (gamma_acc, delta_acc)))

    def scalars(t, sums, gamma_old, pap_old):
        gamma, delta, sigma = sums[0], sums[1], sums[2]
        beta = jnp.where(t == 0, 0.0, gamma / gamma_old)
        pap = delta + 2.0 * beta * sigma + beta * beta * pap_old
        return gamma, pap, beta[0, 0], (gamma / pap)[0, 0]

    def advance_x(now, alpha, beta):
        def step(i, acc):
            p_new = inv[i] * r[1 - now, i] + beta * p[i]
            p[i] = p_new
            x[i] = x[i] + alpha * p_new
            return acc + fold(r[now, i] * r[now, i])
        return lax.fori_loop(0, ni, step, zero_acc)

    def iteration(t, carry):
        gamma_old, pap_old, alpha_old, beta_old = carry
        now = lax.rem(t, 2)
        reduce_send(t, (0,))
        exchange_start(mp, t + 3)
        reduce_send(t, range(1, ngz))
        stencil(mp)
        rr_acc = advance_x(now, alpha_old, beta_old)
        join_faces(mp, t + 3)
        sums = reduce_wait(t, 4)
        gamma, pap, beta, alpha = scalars(t, sums, gamma_old, pap_old)

        def update(i, acc):
            iv = inv[i]
            w_old = w[i]
            z_new = n[i] + beta * z[i]
            s_new = w_old + beta * s[i]
            r_new = r[now, i] - alpha * s_new
            w_new = w_old - alpha * z_new
            u_new = iv * r_new
            z[i] = z_new
            s[i] = s_new
            r[1 - now, i] = r_new
            w[i] = w_new
            mp[i + 1, rows, :] = iv * w_new
            return acc[0] + fold(r_new * u_new), acc[1] + fold(w_new * u_new), acc[2] + fold(u_new * s_new)

        packed_pass(mp, t + 4, update, (zero_acc,) * 3, lambda accs: reduce_row(t + 1, accs + (rr_acc,)))
        scal_ref[lax.rem(t + CG_ITERS - 2, CG_ITERS)] = jnp.broadcast_to(sums[3], (1, LANES))
        return gamma, pap, alpha, beta

    one = jnp.ones((1, 1), F32)
    last = CG_ITERS - 1
    gamma_old, pap_old, alpha_old, beta_old = lax.fori_loop(
        0, last, iteration, (one, one, jnp.float32(0.0), jnp.float32(0.0)))

    now = last % 2
    reduce_send(last, range(ngz))

    def last_dots(i, acc):
        rv, sv = r[now, i], s[i]
        wv = w[i]
        n[i] = inv[i] * rv
        pairs = ((rv, rv), (rv, wv), (rv, sv), (wv, wv), (wv, sv), (sv, sv))
        return tuple(a + fold(b * c) for a, (b, c) in zip(acc, pairs))

    reduce_row(CG_ITERS, slabs(2, last_dots, (zero_acc,) * 6))
    reduce_send(CG_ITERS, range(ngz))
    advance_x(now, alpha_old, beta_old)
    sums = reduce_wait(last, 4)
    wide = lambda value: jnp.broadcast_to(value, (1, LANES))
    scal_ref[last - 2] = wide(sums[3])
    gamma = sums[0]
    beta = gamma / gamma_old
    alpha = gamma / (sums[1] + 2.0 * beta * sums[2] + beta * beta * pap_old)
    scal_ref[CG_ITERS] = wide(alpha)
    scal_ref[CG_ITERS + 1] = wide(beta)
    rr, rw, rs, ww, ws, ss = reduce_wait(CG_ITERS, 6)
    scal_ref[last - 1] = wide(rr)
    scal_ref[last] = wide(rr - 2.0 * alpha * (rw + beta * rs) + alpha * alpha * (ww + 2.0 * beta * ws + beta * beta * ss))


def finish_kernel(chunk, scal, x, u, p, r, w, s, x_hbm, r_hbm, hist_hbm, x_new, r_new, hist, sem, hist_sem):
    ni, nl, nj = x_new.shape
    alpha = jnp.broadcast_to(scal[CG_ITERS], (nl, LANES))
    beta = jnp.broadcast_to(scal[CG_ITERS + 1], (nl, LANES))
    copies = []

    def step(i, _):
        x_new[i] = (x[i] + alpha * (u[i] + beta * p[i]))[:, 0:nj]
        r_new[i] = (r[1, i] - alpha * (w[i] + beta * s[i]))[:, 0:nj]
        return 0

    for g in range(ni // chunk):
        lax.fori_loop(g * chunk, (g + 1) * chunk, step, 0)
        part = pl.ds(g * chunk, chunk)
        for j, (src, dst) in enumerate(((x_new, x_hbm), (r_new, r_hbm))):
            copies.append(pltpu.make_async_copy(src.at[part], dst.at[part], sem.at[j, g]))
            copies[-1].start()
        if g == 0:
            for t in range(CG_ITERS):
                hist[t] = scal[t, 0, 0]
            copies.append(pltpu.make_async_copy(hist, hist_hbm, hist_sem))
            copies[-1].start()
    for copy in copies:
        copy.wait()


def solution(mesh):
    counts = (mesh.shape['gx'], mesh.shape['gy'], mesh.shape['gz'])
    grid_spec = P('gx', 'gy', 'gz')

    def local_solve(k_cell, k_ghost, f_rhs, u_init):
        ni, nj, nl = k_cell.shape
        flip = lambda a: jnp.swapaxes(a, 1, 2)
        slots = CG_ITERS + 3
        devices = counts[0] * counts[1] * counts[2]
        width = k_ghost.shape[2]
        any_spec = pl.BlockSpec(memory_space=pl.ANY)
        vm = lambda *shape: pltpu.VMEM(shape, F32)
        whole = vm(ni, nl, LANES)
        block = vm(ni, nl, nj)
        padded = vm(ni + 2, nl + 2 * PAD, LANES)
        dma = pltpu.SemaphoreType.DMA
        kept = pltpu.VMEM((ni, nl, LANES), F32)
        vmem_spec = pl.BlockSpec(memory_space=pltpu.VMEM)
        *state, scal = pl.pallas_call(
            functools.partial(solve_kernel, (ni, nl, nj), counts),
            out_shape=(kept, kept, kept, pltpu.VMEM((2, ni, nl, LANES), F32), kept, kept,
                       pltpu.VMEM((CG_ITERS + 2, 1, LANES), F32)),
            in_specs=[any_spec] * 4,
            out_specs=(vmem_spec,) * 7,
            scratch_shapes=[
                block, block, block, vm(nj, width), vm(ni, width), vm(ni, width), vm(-(-width // LANES) * LANES, LANES),
                vm(2, nl, LANES), vm(nl // 2, LANES), vm(2, ni, LANES),
                padded, padded, vm(ni + 1, nl, LANES), whole, whole, vm(ni, nl + 2 * PAD, LANES), whole,
                whole,
                vm(slots, nl // 2, LANES), vm(slots, 2, ni, LANES),
                vm(slots, 2, nl, LANES), vm(slots, nl // 2, LANES), vm(slots, 2, ni, LANES),
                vm(CG_ITERS + 1, 1, LANES), vm(CG_ITERS + 1, devices, 1, LANES),
                dma((slots, 2)), dma((slots,)), dma((slots, 2)), dma((slots, 2)), dma((slots,)), dma((slots, 2)),
                dma((CG_ITERS + 1,)), dma((CG_ITERS + 1,)), dma((6,)), pltpu.SemaphoreType.REGULAR((6,)),
            ],
            compiler_params=pltpu.CompilerParams(has_side_effects=True, collective_id=0, vmem_limit_bytes=28 << 20),
        )(*(pltpu.with_memory_space_constraint(a, pltpu.HBM) for a in (k_ghost, flip(k_cell), flip(f_rhs), flip(u_init))))
        chunk = ni // 4
        out_block = jax.ShapeDtypeStruct((ni, nl, nj), F32)
        x_new, r_new, hist = pl.pallas_call(
            functools.partial(finish_kernel, chunk),
            out_shape=(out_block, out_block, jax.ShapeDtypeStruct((CG_ITERS,), F32)),
            in_specs=[vmem_spec] * 7,
            out_specs=(any_spec,) * 3,
            scratch_shapes=[block, block, pltpu.SMEM((CG_ITERS,), F32), dma((2, ni // chunk)), dma],
            compiler_params=pltpu.CompilerParams(vmem_limit_bytes=28 << 20),
        )(scal, *state)
        return flip(x_new), flip(r_new), hist

    return jax.shard_map(local_solve, mesh=mesh, in_specs=(grid_spec, P(), grid_spec, grid_spec),
                         out_specs=(grid_spec, grid_spec, P()), check_vma=False)
```

```python
import functools

import jax
import jax.numpy as jnp
from jax import lax
from jax.experimental import pallas as pl
from jax.experimental.pallas import tpu as pltpu
from jax.sharding import PartitionSpec as P

CG_ITERS = 8
LANES = 128
PAD = 8
GROUP = 6
COLUMNS = 16
UPDATE = 4
MESH = pl.DeviceIdType.MESH
F32 = jnp.float32


def solve_kernel(dims, counts, kg_hbm, k_hbm, f_hbm, u_hbm, x, n, p, r, w, s, scal_ref,
                 k_in, f_in, u_in, wall_x, wall_y, wall_z, wall_t, bx, by, bz,
                 kp, mp, cx, cy, cyh, cz, inv, z,
                 ys, zs, xr, yr, zr, red_s, red_r,
                 xs_sem, ys_sem, zs_sem, xr_sem, yr_sem, zr_sem, rs_sem, rr_sem, in_sem, near_sem):
    ni, nl, nj = dims
    ngx, ngy, ngz = counts
    half = nl // 2
    gx, gy, gz = lax.axis_index('gx'), lax.axis_index('gy'), lax.axis_index('gz')
    rows = pl.ds(PAD, nl)
    rows_dn = pl.ds(PAD - 1, nl)
    rows_up = pl.ds(PAD + 1, nl)
    lane = lax.broadcasted_iota(jnp.int32, (nl, LANES), 1)
    lane_i = lax.broadcasted_iota(jnp.int32, (ni, LANES), 1)
    lane_half = lax.broadcasted_iota(jnp.int32, (half, LANES), 1)
    lane_row = lax.broadcasted_iota(jnp.int32, (1, LANES), 1)
    inside = lane < nj
    has_xlo, has_xhi = gx > 0, gx < ngx - 1
    has_zlo, has_zhi = gz > 0, gz < ngz - 1
    face_lane = jnp.where(gy == 0, nj - 1, 0)
    y_low_wall, y_high_wall = gy == 0, gy > 0
    zero_slab = jnp.zeros((nl, LANES), F32)
    zero_acc = jnp.zeros((8, LANES), F32)
    others = ngx * ngy * ngz - 1

    def column_roll(slab, shift):
        return pltpu.roll(slab, shift + 2 * LANES, 1)

    def slabs(group, step, init):
        def body(g, carry):
            for k in range(group):
                carry = step(g * group + k, carry)
            return carry
        return lax.fori_loop(0, ni // group, body, init)

    def x_copy(ref, slot, up):
        src = ref.at[ni if up else 1, rows]
        return pltpu.make_async_remote_copy(
            src_ref=src, dst_ref=xr.at[slot, 0 if up else 1], send_sem=xs_sem.at[slot, 0 if up else 1],
            recv_sem=xr_sem.at[slot, 0 if up else 1], device_id=(gz, gy, gx + 1 if up else gx - 1), device_id_type=MESH)

    def z_copy(slot, up):
        return pltpu.make_async_remote_copy(
            src_ref=zs.at[slot, 0 if up else 1], dst_ref=zr.at[slot, 0 if up else 1],
            send_sem=zs_sem.at[slot, 0 if up else 1], recv_sem=zr_sem.at[slot, 0 if up else 1],
            device_id=(gz + 1 if up else gz - 1, gy, gx), device_id_type=MESH)

    def y_copy(slot):
        return pltpu.make_async_remote_copy(
            src_ref=ys.at[slot], dst_ref=yr.at[slot], send_sem=ys_sem.at[slot], recv_sem=yr_sem.at[slot],
            device_id=(gz, 1 - gy, gx), device_id_type=MESH)

    def pack_rolls(ref, slot, i, behind=False):
        row = lax.max(i, 0) if behind else i
        slab = ref[row + 1, rows, :]
        zs[slot, 1, pl.ds(row, 1), :] = slab[0:1, :]
        zs[slot, 0, pl.ds(row, 1), :] = slab[nl - 1:nl, :]
        return column_roll(slab[0:half], row - face_lane), column_roll(slab[half:nl], row - face_lane + LANES // 2)

    def pack(i, rolled, acc):
        acc = jnp.where(lane_half == i, rolled[0], acc)
        return jnp.where(lane_half == i + LANES // 2, rolled[1], acc)

    def packed_pass(ref, slot, step, init):
        def body(g, carry):
            state, acc = carry
            rolled = [pack_rolls(ref, slot, (g - 1) * GROUP + k, behind=True) for k in range(GROUP)]
            for k in range(GROUP):
                state = step(g * GROUP + k, state)
            for k in range(GROUP):
                acc = pack((g - 1) * GROUP + k, rolled[k], acc)
            return state, acc
        state, acc = lax.fori_loop(0, ni // GROUP, body, (init, jnp.zeros((half, LANES), F32)))
        rolled = [pack_rolls(ref, slot, ni - GROUP + k) for k in range(GROUP)]
        for k in range(GROUP):
            acc = pack(ni - GROUP + k, rolled[k], acc)
        ys[slot] = acc
        return state

    def pack_faces(ref, slot):
        group = min(COLUMNS, ni)

        def body(g, acc):
            rolled = [pack_rolls(ref, slot, g * group + k) for k in range(group)]
            for k in range(group):
                acc = pack(g * group + k, rolled[k], acc)
            return acc

        ys[slot] = lax.fori_loop(0, ni // group, body, jnp.zeros((half, LANES), F32))

    def exchange_start(ref, slot):
        y_copy(slot).start()
        pl.when(has_zlo)(lambda: z_copy(slot, False).start())
        pl.when(has_zhi)(lambda: z_copy(slot, True).start())
        pl.when(has_xlo)(lambda: x_copy(ref, slot, False).start())
        pl.when(has_xhi)(lambda: x_copy(ref, slot, True).start())

    def exchange_wait(ref, slot):
        @pl.when(has_xlo)
        def _():
            x_copy(ref, slot, False).wait_send()
            x_copy(ref, slot, True).wait_recv()

        @pl.when(has_xhi)
        def _():
            x_copy(ref, slot, True).wait_send()
            x_copy(ref, slot, False).wait_recv()

        @pl.when(has_zlo)
        def _():
            z_copy(slot, False).wait_send()
            z_copy(slot, True).wait_recv()

        @pl.when(has_zhi)
        def _():
            z_copy(slot, True).wait_send()
            z_copy(slot, False).wait_recv()

        y_copy(slot).wait()

    def add_rows(ref, layer, row):
        for i in range(ni):
            ref[i, row:row + 1, :] = ref[i, row:row + 1, :] + layer[i:i + 1, :]

    def add_columns(ref, packed):
        mask = lane == face_lane

        def step(g, _):
            columns = []
            for k in range(min(COLUMNS, ni)):
                i = g * min(COLUMNS, ni) + k
                columns.append((column_roll(packed, face_lane - i), column_roll(packed, face_lane - i - LANES // 2)))
            for k in range(min(COLUMNS, ni)):
                i = g * min(COLUMNS, ni) + k
                ref[i] = ref[i] + jnp.where(mask, jnp.concatenate(columns[k], axis=0), 0.0)
            return 0

        lax.fori_loop(0, ni // min(COLUMNS, ni), step, 0)

    def join_faces(ref, slot):
        y_copy(slot).wait()
        add_columns(n, by[...] * (ys[slot] - yr[slot]))

        @pl.when(has_xlo)
        def _():
            x_copy(ref, slot, False).wait_send()
            x_copy(ref, slot, True).wait_recv()
            n[0] = n[0] + bx[0] * (ref[1, rows, :] - xr[slot, 0])

        @pl.when(has_xhi)
        def _():
            x_copy(ref, slot, True).wait_send()
            x_copy(ref, slot, False).wait_recv()
            n[ni - 1] = n[ni - 1] + bx[1] * (ref[ni, rows, :] - xr[slot, 1])

        @pl.when(has_zlo)
        def _():
            z_copy(slot, False).wait_send()
            z_copy(slot, True).wait_recv()
            add_rows(n, bz[0] * (zs[slot, 1] - zr[slot, 0]), 0)

        @pl.when(has_zhi)
        def _():
            z_copy(slot, True).wait_send()
            z_copy(slot, False).wait_recv()
            add_rows(n, bz[1] * (zs[slot, 0] - zr[slot, 1]), nl - 1)

    def stencil(ref):
        def step(i, carry):
            v, flux_x = carry
            above = ref[i + 2, rows, :]
            flux_next = cx[i + 1] * (above - v)
            flux_zl = cz[i, rows, :] * (v - ref[i + 1, rows_dn, :])
            flux_zh = cz[i, rows_up, :] * (ref[i + 1, rows_up, :] - v)
            flux_yl = cy[i] * (v - pltpu.roll(v, 1, 1))
            flux_yh = cyh[i] * (pltpu.roll(v, LANES - 1, 1) - v)
            n[i] = (flux_x - flux_next) + (flux_yl - flux_yh) + (flux_zl - flux_zh)
            return above, flux_next

        first = ref[1, rows, :]
        slabs(GROUP, step, (first, cx[0] * (first - ref[0, rows, :])))

    def fold(slab):
        out = slab[0:8]
        for part in range(8, nl, 8):
            out = out + slab[part:part + 8]
        return out

    def reduce_row(slot, accs):
        row = jnp.zeros((1, LANES), F32)
        for q, acc in enumerate(accs):
            row = jnp.where(lane_row == q, jnp.sum(jnp.sum(acc, axis=0, keepdims=True), axis=1, keepdims=True), row)
        red_s[slot] = row
        red_r[slot, (gz * ngy + gy) * ngx + gx] = row

    def reduce_send(slot, planes):
        me = (gz * ngy + gy) * ngx + gx
        for k in planes:
            z_to = jnp.where(2 * gz < ngz, ngz - 1 - k, k)
            for b in reversed(range(ngy)):
                for c in (2, 3, 1, 0):
                    copy = pltpu.make_async_remote_copy(
                        src_ref=red_s.at[slot], dst_ref=red_r.at[slot, me], send_sem=rs_sem.at[slot], recv_sem=rr_sem.at[slot],
                        device_id=(z_to, lax.rem(gy + b, ngy), lax.rem(gx + c, ngx)), device_id_type=MESH)
                    if b or c:
                        copy.start()
                    else:
                        pl.when(z_to != gz)(copy.start)

    def reduce_wait(slot, count):
        whole = red_r.at[slot, pl.ds(0, others)]
        done = pltpu.make_async_remote_copy(
            src_ref=whole, dst_ref=whole, send_sem=rs_sem.at[slot], recv_sem=rr_sem.at[slot],
            device_id=(gz, gy, gx), device_id_type=MESH)
        done.wait_recv()
        done.wait_send()
        total = jnp.sum(red_r[slot], axis=0)
        return [jnp.sum(jnp.where(lane_row == q, total, 0.0), axis=1, keepdims=True) for q in range(count)]

    x_row, z_row = jnp.where(gx == 0, 0, 1), jnp.where(gz == 0, 4, 5)
    slabs_i = pl.ds(pl.multiple_of(gx * ni, 8), ni)
    inputs = [
        pltpu.make_async_copy(k_hbm, k_in, in_sem.at[0]),
        pltpu.make_async_copy(u_hbm, u_in, in_sem.at[1]),
        pltpu.make_async_copy(kg_hbm.at[x_row, pl.ds(pl.multiple_of(gy * nj, 8), nj)], wall_x, in_sem.at[2]),
        pltpu.make_async_copy(kg_hbm.at[2 + gy, slabs_i], wall_y, in_sem.at[3]),
        pltpu.make_async_copy(kg_hbm.at[z_row, slabs_i], wall_z, in_sem.at[4]),
        pltpu.make_async_copy(f_hbm, f_in, in_sem.at[5]),
    ]
    for copy in inputs[:5]:
        copy.start()

    def tell_neighbours(sem):
        tell = lambda *target: pl.semaphore_signal(sem, inc=1, device_id=target, device_id_type=MESH)
        pl.when(has_xlo)(lambda: tell(gz, gy, gx - 1))
        pl.when(has_xhi)(lambda: tell(gz, gy, gx + 1))
        pl.when(has_zlo)(lambda: tell(gz - 1, gy, gx))
        pl.when(has_zhi)(lambda: tell(gz + 1, gy, gx))
        tell(gz, 1 - gy, gx)

    neighbours = 5 - jnp.where(has_xlo, 0, 1) - jnp.where(has_xhi, 0, 1) - jnp.where(has_zlo, 0, 1) - jnp.where(has_zhi, 0, 1)
    rounds = (ngx - 1) + (ngy - 1) + (ngz - 1) - 1

    def next_round(k):
        pl.semaphore_wait(near_sem.at[k], neighbours)
        if k + 1 < rounds:
            tell_neighbours(near_sem.at[k + 1])

    barrier = pltpu.get_barrier_semaphore()
    tell_neighbours(barrier)

    for edge in (0, ni + 1):
        mp[edge] = jnp.zeros((nl + 2 * PAD, LANES), F32)
        kp[edge] = jnp.ones((nl + 2 * PAD, LANES), F32)

    def clear(i, _):
        mp[i + 1, pl.ds(0, PAD), :] = jnp.zeros((PAD, LANES), F32)
        mp[i + 1, pl.ds(PAD + nl, PAD), :] = jnp.zeros((PAD, LANES), F32)
        kp[i + 1, pl.ds(0, PAD), :] = jnp.ones((PAD, LANES), F32)
        kp[i + 1, pl.ds(PAD + nl, PAD), :] = jnp.ones((PAD, LANES), F32)
        mp[i + 1, rows, :] = zero_slab
        s[i] = zero_slab
        z[i] = zero_slab
        p[i] = zero_slab
        r[1, i] = zero_slab
        r[0, i] = zero_slab
        kp[i + 1, rows, :] = jnp.full((nl, LANES), 1.0, F32)
        return 0

    lax.fori_loop(0, ni, clear, 0)

    def load_k(i, _):
        kp[i + 1, rows, 0:nj] = k_in[i]
        return 0

    def load_u(i, _):
        mp[i + 1, rows, 0:nj] = u_in[i]
        return 0

    inputs[0].wait()
    inputs[5].start()
    packed_pass(kp, 0, load_k, 0)
    pl.semaphore_wait(barrier, neighbours)
    tell_neighbours(near_sem.at[0])
    exchange_start(kp, 0)
    inputs[1].wait()
    packed_pass(mp, 1, load_u, 0)
    exchange_start(mp, 1)
    next_round(0)

    for copy in inputs[2:5]:
        copy.wait()
    width = wall_x.shape[1]
    l_rows = pl.ds(pl.multiple_of(gz * nl, 8), nl)

    def flipped(wall, count):
        for start in range(0, width, LANES):
            size = min(LANES, width - start)
            block = jnp.concatenate([wall[:, start:start + size], jnp.ones((LANES - count, size), F32)], axis=0)
            wall_t[start:start + size, :] = block.T
        return wall_t[l_rows, :]

    x_wall = flipped(wall_x, nj)
    y_wall = flipped(wall_y, ni)
    if width > LANES:
        rest = jnp.concatenate([wall_z[:, LANES:width], jnp.ones((ni, 2 * LANES - width), F32)], axis=1)
        whole_z = wall_z[:, 0:LANES]
        turn = LANES - nj
        shifted = jnp.where(lane_i < turn, pltpu.roll(whole_z, turn, 1), pltpu.roll(rest, turn, 1))
    else:
        whole_z = jnp.concatenate([wall_z[...], jnp.ones((ni, LANES - width), F32)], axis=1)
        shifted = pltpu.roll(whole_z, LANES - nj, 1)
    z_wall = jnp.where(gy == 0, whole_z, shifted)

    def harmonic(left, right):
        return 2.0 * left * right / (left + right)

    next_round(1)

    in_i = lane_i < nj
    cx[0] = jnp.where(jnp.logical_and(inside, gx == 0), harmonic(x_wall, kp[1, rows, :]), 0.0)
    z_low = jnp.where(jnp.logical_and(in_i, gz == 0), harmonic(z_wall, zs[0, 1]), 0.0)
    z_high = jnp.where(jnp.logical_and(in_i, gz == ngz - 1), harmonic(zs[0, 0], z_wall), 0.0)
    y_low_mask = jnp.logical_and(inside, jnp.logical_or(lane > 0, y_low_wall))
    y_high_mask = jnp.logical_and(inside, jnp.logical_or(lane < nj - 1, y_high_wall))
    wall_lane = nj - 1 - face_lane

    def coefs(i, _):
        here = kp[i + 1, rows, :]
        cx[i + 1] = jnp.where(inside, harmonic(here, kp[i + 2, rows, :]), 0.0)
        cz[i, rows_up, :] = jnp.where(inside, harmonic(here, kp[i + 1, rows_up, :]), 0.0)
        wall = column_roll(y_wall, wall_lane - i)
        low = jnp.where(lane == 0, wall, pltpu.roll(here, 1, 1))
        high = jnp.where(lane == nj - 1, wall, pltpu.roll(here, LANES - 1, 1))
        cy[i] = jnp.where(y_low_mask, harmonic(low, here), 0.0)
        cyh[i] = jnp.where(y_high_mask, harmonic(here, high), 0.0)
        return 0

    slabs(GROUP, coefs, 0)
    next_round(2)
    cx[ni] = jnp.where(jnp.logical_and(inside, gx == ngx - 1), harmonic(kp[ni, rows, :], x_wall), 0.0)
    for i in range(ni):
        cz[i, PAD:PAD + 1, :] = z_low[i:i + 1, :]
        cz[i, PAD + nl:PAD + nl + 1, :] = z_high[i:i + 1, :]

    stencil(mp)

    def diagonal(i, _):
        inv[i] = cx[i] + cx[i + 1] + cy[i] + cyh[i] + cz[i, rows, :] + cz[i, rows_up, :]
        return 0

    lax.fori_loop(0, ni, diagonal, 0)
    next_round(3)

    exchange_wait(kp, 0)

    @pl.when(has_xlo)
    def _():
        bx[0] = jnp.where(inside, harmonic(xr[0, 0], kp[1, rows, :]), 0.0)
        inv[0] = inv[0] + bx[0]

    @pl.when(has_xhi)
    def _():
        bx[1] = jnp.where(inside, harmonic(kp[ni, rows, :], xr[0, 1]), 0.0)
        inv[ni - 1] = inv[ni - 1] + bx[1]

    @pl.when(has_zlo)
    def _():
        bz[0] = jnp.where(in_i, harmonic(zr[0, 0], zs[0, 1]), 0.0)
        add_rows(inv, bz[0], 0)

    @pl.when(has_zhi)
    def _():
        bz[1] = jnp.where(in_i, harmonic(zs[0, 0], zr[0, 1]), 0.0)
        add_rows(inv, bz[1], nl - 1)

    y_face = jnp.where(lax.rem(lane_half, LANES // 2) < ni, harmonic(ys[0], yr[0]), 0.0)
    by[...] = y_face
    add_columns(inv, y_face)
    join_faces(mp, 1)
    inputs[5].wait()

    def first_residual(i, acc):
        iv = jnp.where(inside, 1.0 / jnp.where(inside, inv[i], 1.0), 0.0)
        inv[i] = iv
        x[i] = mp[i + 1, rows, :]
        r[0, i, :, 0:nj] = f_in[i]
        res = r[0, i] - n[i]
        r[0, i] = res
        u = res * iv
        mp[i + 1, rows, :] = u
        return acc + fold(res * u)

    gamma_acc = packed_pass(mp, 2, first_residual, zero_acc)
    exchange_start(mp, 2)
    next_round(4)
    stencil(mp)
    for k in range(5, rounds):
        next_round(k)
    join_faces(mp, 2)

    def first_w(i, acc):
        av = n[i]
        w[i] = av
        acc = acc + fold(av * mp[i + 1, rows, :])
        mp[i + 1, rows, :] = av * inv[i]
        return acc

    reduce_row(0, (gamma_acc, slabs(GROUP, first_w, zero_acc)))

    def scalars(t, sums, gamma_old, pap_old):
        gamma, delta, sigma = sums[0], sums[1], sums[2]
        beta = jnp.where(t == 0, 0.0, gamma / gamma_old)
        pap = delta + 2.0 * beta * sigma + beta * beta * pap_old
        return gamma, pap, beta[0, 0], (gamma / pap)[0, 0]

    def advance_x(now, alpha, beta):
        def step(i, acc):
            p_new = inv[i] * r[1 - now, i] + beta * p[i]
            p[i] = p_new
            x[i] = x[i] + alpha * p_new
            return acc + fold(r[now, i] * r[now, i])
        return lax.fori_loop(0, ni, step, zero_acc)

    def iteration(t, carry):
        gamma_old, pap_old, alpha_old, beta_old = carry
        now = lax.rem(t, 2)
        reduce_send(t, range(0, ngz // 2))
        pack_faces(mp, t + 3)
        exchange_start(mp, t + 3)
        reduce_send(t, range(ngz // 2, ngz))
        stencil(mp)
        rr_acc = advance_x(now, alpha_old, beta_old)
        join_faces(mp, t + 3)
        sums = reduce_wait(t, 4)
        gamma, pap, beta, alpha = scalars(t, sums, gamma_old, pap_old)

        def update(i, acc):
            iv = inv[i]
            w_old = w[i]
            z_new = n[i] + beta * z[i]
            s_new = w_old + beta * s[i]
            r_new = r[now, i] - alpha * s_new
            w_new = w_old - alpha * z_new
            u_new = iv * r_new
            z[i] = z_new
            s[i] = s_new
            r[1 - now, i] = r_new
            w[i] = w_new
            mp[i + 1, rows, :] = iv * w_new
            return acc[0] + fold(r_new * u_new), acc[1] + fold(w_new * u_new), acc[2] + fold(u_new * s_new)

        reduce_row(t + 1, slabs(UPDATE, update, (zero_acc,) * 3) + (rr_acc,))
        scal_ref[lax.rem(t + CG_ITERS - 2, CG_ITERS)] = jnp.broadcast_to(sums[3], (1, LANES))
        return gamma, pap, alpha, beta

    one = jnp.ones((1, 1), F32)
    last = CG_ITERS - 1
    gamma_old, pap_old, alpha_old, beta_old = lax.fori_loop(
        0, last, iteration, (one, one, jnp.float32(0.0), jnp.float32(0.0)))

    now = last % 2
    reduce_send(last, range(ngz))

    def last_dots(i, acc):
        rv, sv = r[now, i], s[i]
        wv = w[i]
        n[i] = inv[i] * rv
        pairs = ((rv, rv), (rv, wv), (rv, sv), (wv, wv), (wv, sv), (sv, sv))
        return tuple(a + fold(b * c) for a, (b, c) in zip(acc, pairs))

    reduce_row(CG_ITERS, slabs(2, last_dots, (zero_acc,) * 6))
    reduce_send(CG_ITERS, range(ngz))
    advance_x(now, alpha_old, beta_old)
    sums = reduce_wait(last, 4)
    wide = lambda value: jnp.broadcast_to(value, (1, LANES))
    scal_ref[last - 2] = wide(sums[3])
    gamma = sums[0]
    beta = gamma / gamma_old
    alpha = gamma / (sums[1] + 2.0 * beta * sums[2] + beta * beta * pap_old)
    scal_ref[CG_ITERS] = wide(alpha)
    scal_ref[CG_ITERS + 1] = wide(beta)
    rr, rw, rs, ww, ws, ss = reduce_wait(CG_ITERS, 6)
    scal_ref[last - 1] = wide(rr)
    scal_ref[last] = wide(rr - 2.0 * alpha * (rw + beta * rs) + alpha * alpha * (ww + 2.0 * beta * ws + beta * beta * ss))


def finish_kernel(chunk, scal, x, u, p, r, w, s, x_hbm, r_hbm, hist_hbm, x_new, r_new, hist, sem, hist_sem):
    ni, nl, nj = x_new.shape
    alpha = jnp.broadcast_to(scal[CG_ITERS], (nl, LANES))
    beta = jnp.broadcast_to(scal[CG_ITERS + 1], (nl, LANES))
    copies = []

    def step(i, _):
        x_new[i] = (x[i] + alpha * (u[i] + beta * p[i]))[:, 0:nj]
        r_new[i] = (r[1, i] - alpha * (w[i] + beta * s[i]))[:, 0:nj]
        return 0

    for g in range(ni // chunk):
        lax.fori_loop(g * chunk, (g + 1) * chunk, step, 0)
        part = pl.ds(g * chunk, chunk)
        for j, (src, dst) in enumerate(((x_new, x_hbm), (r_new, r_hbm))):
            copies.append(pltpu.make_async_copy(src.at[part], dst.at[part], sem.at[j, g]))
            copies[-1].start()
        if g == 0:
            for t in range(CG_ITERS):
                hist[t] = scal[t, 0, 0]
            copies.append(pltpu.make_async_copy(hist, hist_hbm, hist_sem))
            copies[-1].start()
    for copy in copies:
        copy.wait()


def solution(mesh):
    counts = (mesh.shape['gx'], mesh.shape['gy'], mesh.shape['gz'])
    grid_spec = P('gx', 'gy', 'gz')

    def local_solve(k_cell, k_ghost, f_rhs, u_init):
        ni, nj, nl = k_cell.shape
        flip = lambda a: jnp.swapaxes(a, 1, 2)
        slots = CG_ITERS + 3
        devices = counts[0] * counts[1] * counts[2]
        width = k_ghost.shape[2]
        any_spec = pl.BlockSpec(memory_space=pl.ANY)
        vm = lambda *shape: pltpu.VMEM(shape, F32)
        whole = vm(ni, nl, LANES)
        block = vm(ni, nl, nj)
        padded = vm(ni + 2, nl + 2 * PAD, LANES)
        dma = pltpu.SemaphoreType.DMA
        kept = pltpu.VMEM((ni, nl, LANES), F32)
        vmem_spec = pl.BlockSpec(memory_space=pltpu.VMEM)
        *state, scal = pl.pallas_call(
            functools.partial(solve_kernel, (ni, nl, nj), counts),
            out_shape=(kept, kept, kept, pltpu.VMEM((2, ni, nl, LANES), F32), kept, kept,
                       pltpu.VMEM((CG_ITERS + 2, 1, LANES), F32)),
            in_specs=[any_spec] * 4,
            out_specs=(vmem_spec,) * 7,
            scratch_shapes=[
                block, block, block, vm(nj, width), vm(ni, width), vm(ni, width), vm(-(-width // LANES) * LANES, LANES),
                vm(2, nl, LANES), vm(nl // 2, LANES), vm(2, ni, LANES),
                padded, padded, vm(ni + 1, nl, LANES), whole, whole, vm(ni, nl + 2 * PAD, LANES), whole,
                whole,
                vm(slots, nl // 2, LANES), vm(slots, 2, ni, LANES),
                vm(slots, 2, nl, LANES), vm(slots, nl // 2, LANES), vm(slots, 2, ni, LANES),
                vm(CG_ITERS + 1, 1, LANES), vm(CG_ITERS + 1, devices, 1, LANES),
                dma((slots, 2)), dma((slots,)), dma((slots, 2)), dma((slots, 2)), dma((slots,)), dma((slots, 2)),
                dma((CG_ITERS + 1,)), dma((CG_ITERS + 1,)), dma((6,)), pltpu.SemaphoreType.REGULAR((6,)),
            ],
            compiler_params=pltpu.CompilerParams(has_side_effects=True, collective_id=0, vmem_limit_bytes=28 << 20),
        )(*(pltpu.with_memory_space_constraint(a, pltpu.HBM) for a in (k_ghost, flip(k_cell), flip(f_rhs), flip(u_init))))
        chunk = ni // 4
        out_block = jax.ShapeDtypeStruct((ni, nl, nj), F32)
        x_new, r_new, hist = pl.pallas_call(
            functools.partial(finish_kernel, chunk),
            out_shape=(out_block, out_block, jax.ShapeDtypeStruct((CG_ITERS,), F32)),
            in_specs=[vmem_spec] * 7,
            out_specs=(any_spec,) * 3,
            scratch_shapes=[block, block, pltpu.SMEM((CG_ITERS,), F32), dma((2, ni // chunk)), dma],
            compiler_params=pltpu.CompilerParams(vmem_limit_bytes=28 << 20),
        )(scal, *state)
        return flip(x_new), flip(r_new), hist

    return jax.shard_map(local_solve, mesh=mesh, in_specs=(grid_spec, P(), grid_spec, grid_spec),
                         out_specs=(grid_spec, grid_spec, P()), check_vma=False)
```

```python
import functools

import jax
import jax.numpy as jnp
from jax import lax
from jax.experimental import pallas as pl
from jax.experimental.pallas import tpu as pltpu
from jax.sharding import PartitionSpec as P

CG_ITERS = 8
LANES = 128
PAD = 8
GROUP = 6
COLUMNS = 16
UPDATE = 4
MESH = pl.DeviceIdType.MESH
F32 = jnp.float32


def solve_kernel(dims, counts, kg_hbm, k_hbm, f_hbm, u_hbm, x, n, p, r, w, s, scal_ref,
                 k_in, f_in, u_in, wall_x, wall_y, wall_z, wall_t, bx, by, bz,
                 kp, mp, cx, cy, cyh, cz, inv, z,
                 ys, zs, xr, yr, zr, red_s, red_r,
                 xs_sem, ys_sem, zs_sem, xr_sem, yr_sem, zr_sem, rs_sem, rr_sem, in_sem, near_sem):
    ni, nl, nj = dims
    ngx, ngy, ngz = counts
    half = nl // 2
    gx, gy, gz = lax.axis_index('gx'), lax.axis_index('gy'), lax.axis_index('gz')
    rows = pl.ds(PAD, nl)
    rows_dn = pl.ds(PAD - 1, nl)
    rows_up = pl.ds(PAD + 1, nl)
    lane = lax.broadcasted_iota(jnp.int32, (nl, LANES), 1)
    lane_i = lax.broadcasted_iota(jnp.int32, (ni, LANES), 1)
    lane_half = lax.broadcasted_iota(jnp.int32, (half, LANES), 1)
    lane_row = lax.broadcasted_iota(jnp.int32, (1, LANES), 1)
    inside = lane < nj
    has_xlo, has_xhi = gx > 0, gx < ngx - 1
    has_zlo, has_zhi = gz > 0, gz < ngz - 1
    face_lane = jnp.where(gy == 0, nj - 1, 0)
    y_low_wall, y_high_wall = gy == 0, gy > 0
    zero_slab = jnp.zeros((nl, LANES), F32)
    zero_acc = jnp.zeros((8, LANES), F32)
    others = ngx * ngy * ngz - 1

    def column_roll(slab, shift):
        return pltpu.roll(slab, shift + 2 * LANES, 1)

    def slabs(group, step, init):
        def body(g, carry):
            for k in range(group):
                carry = step(g * group + k, carry)
            return carry
        return lax.fori_loop(0, ni // group, body, init)

    def x_copy(ref, slot, up):
        src = ref.at[ni if up else 1, rows]
        return pltpu.make_async_remote_copy(
            src_ref=src, dst_ref=xr.at[slot, 0 if up else 1], send_sem=xs_sem.at[slot, 0 if up else 1],
            recv_sem=xr_sem.at[slot, 0 if up else 1], device_id=(gz, gy, gx + 1 if up else gx - 1), device_id_type=MESH)

    def z_copy(slot, up):
        return pltpu.make_async_remote_copy(
            src_ref=zs.at[slot, 0 if up else 1], dst_ref=zr.at[slot, 0 if up else 1],
            send_sem=zs_sem.at[slot, 0 if up else 1], recv_sem=zr_sem.at[slot, 0 if up else 1],
            device_id=(gz + 1 if up else gz - 1, gy, gx), device_id_type=MESH)

    def y_copy(slot):
        return pltpu.make_async_remote_copy(
            src_ref=ys.at[slot], dst_ref=yr.at[slot], send_sem=ys_sem.at[slot], recv_sem=yr_sem.at[slot],
            device_id=(gz, 1 - gy, gx), device_id_type=MESH)

    def pack_slab(slot, i, slab):
        zs[slot, 1, pl.ds(i, 1), :] = slab[0:1, :]
        zs[slot, 0, pl.ds(i, 1), :] = slab[nl - 1:nl, :]
        return column_roll(slab[0:half], i - face_lane), column_roll(slab[half:nl], i - face_lane + LANES // 2)

    def pack_rolls(ref, slot, i, behind=False):
        row = lax.max(i, 0) if behind else i
        return pack_slab(slot, row, ref[row + 1, rows, :])

    def pack(i, rolled, acc):
        acc = jnp.where(lane_half == i, rolled[0], acc)
        return jnp.where(lane_half == i + LANES // 2, rolled[1], acc)

    def packed_pass(ref, slot, step, init):
        def body(g, carry):
            state, acc = carry
            rolled = [pack_rolls(ref, slot, (g - 1) * GROUP + k, behind=True) for k in range(GROUP)]
            for k in range(GROUP):
                state = step(g * GROUP + k, state)
            for k in range(GROUP):
                acc = pack((g - 1) * GROUP + k, rolled[k], acc)
            return state, acc
        state, acc = lax.fori_loop(0, ni // GROUP, body, (init, jnp.zeros((half, LANES), F32)))
        rolled = [pack_rolls(ref, slot, ni - GROUP + k) for k in range(GROUP)]
        for k in range(GROUP):
            acc = pack(ni - GROUP + k, rolled[k], acc)
        ys[slot] = acc
        return state

    def scale_and_pack(slot):
        group = min(COLUMNS, ni)

        def body(g, acc):
            rolled = []
            for k in range(group):
                i = g * group + k
                m = inv[i] * w[i]
                mp[i + 1, rows, :] = m
                rolled.append(pack_slab(slot, i, m))
            for k in range(group):
                acc = pack(g * group + k, rolled[k], acc)
            return acc

        ys[slot] = lax.fori_loop(0, ni // group, body, jnp.zeros((half, LANES), F32))

    def exchange_start(ref, slot):
        y_copy(slot).start()
        pl.when(has_zlo)(lambda: z_copy(slot, False).start())
        pl.when(has_zhi)(lambda: z_copy(slot, True).start())
        pl.when(has_xlo)(lambda: x_copy(ref, slot, False).start())
        pl.when(has_xhi)(lambda: x_copy(ref, slot, True).start())

    def exchange_wait(ref, slot):
        @pl.when(has_xlo)
        def _():
            x_copy(ref, slot, False).wait_send()
            x_copy(ref, slot, True).wait_recv()

        @pl.when(has_xhi)
        def _():
            x_copy(ref, slot, True).wait_send()
            x_copy(ref, slot, False).wait_recv()

        @pl.when(has_zlo)
        def _():
            z_copy(slot, False).wait_send()
            z_copy(slot, True).wait_recv()

        @pl.when(has_zhi)
        def _():
            z_copy(slot, True).wait_send()
            z_copy(slot, False).wait_recv()

        y_copy(slot).wait()

    def add_rows(ref, layer, row):
        for i in range(ni):
            ref[i, row:row + 1, :] = ref[i, row:row + 1, :] + layer[i:i + 1, :]

    def add_columns(ref, packed):
        mask = lane == face_lane

        def step(g, _):
            columns = []
            for k in range(min(COLUMNS, ni)):
                i = g * min(COLUMNS, ni) + k
                columns.append((column_roll(packed, face_lane - i), column_roll(packed, face_lane - i - LANES // 2)))
            for k in range(min(COLUMNS, ni)):
                i = g * min(COLUMNS, ni) + k
                ref[i] = ref[i] + jnp.where(mask, jnp.concatenate(columns[k], axis=0), 0.0)
            return 0

        lax.fori_loop(0, ni // min(COLUMNS, ni), step, 0)

    def join_faces(ref, slot):
        y_copy(slot).wait()
        add_columns(n, by[...] * (ys[slot] - yr[slot]))

        @pl.when(has_xlo)
        def _():
            x_copy(ref, slot, False).wait_send()
            x_copy(ref, slot, True).wait_recv()
            n[0] = n[0] + bx[0] * (ref[1, rows, :] - xr[slot, 0])

        @pl.when(has_xhi)
        def _():
            x_copy(ref, slot, True).wait_send()
            x_copy(ref, slot, False).wait_recv()
            n[ni - 1] = n[ni - 1] + bx[1] * (ref[ni, rows, :] - xr[slot, 1])

        @pl.when(has_zlo)
        def _():
            z_copy(slot, False).wait_send()
            z_copy(slot, True).wait_recv()
            add_rows(n, bz[0] * (zs[slot, 1] - zr[slot, 0]), 0)

        @pl.when(has_zhi)
        def _():
            z_copy(slot, True).wait_send()
            z_copy(slot, False).wait_recv()
            add_rows(n, bz[1] * (zs[slot, 0] - zr[slot, 1]), nl - 1)

    def stencil(ref, diagonal=False):
        def step(i, carry):
            v, flux_x = carry
            above = ref[i + 2, rows, :]
            if diagonal:
                inv[i] = cx[i] + cx[i + 1] + cy[i] + cyh[i] + cz[i, rows, :] + cz[i, rows_up, :]
            flux_next = cx[i + 1] * (above - v)
            flux_zl = cz[i, rows, :] * (v - ref[i + 1, rows_dn, :])
            flux_zh = cz[i, rows_up, :] * (ref[i + 1, rows_up, :] - v)
            flux_yl = cy[i] * (v - pltpu.roll(v, 1, 1))
            flux_yh = cyh[i] * (pltpu.roll(v, LANES - 1, 1) - v)
            n[i] = (flux_x - flux_next) + (flux_yl - flux_yh) + (flux_zl - flux_zh)
            return above, flux_next

        first = ref[1, rows, :]
        slabs(GROUP, step, (first, cx[0] * (first - ref[0, rows, :])))

    def fold(slab):
        out = slab[0:8]
        for part in range(8, nl, 8):
            out = out + slab[part:part + 8]
        return out

    def reduce_row(slot, accs):
        row = jnp.zeros((1, LANES), F32)
        for q, acc in enumerate(accs):
            row = jnp.where(lane_row == q, jnp.sum(jnp.sum(acc, axis=0, keepdims=True), axis=1, keepdims=True), row)
        red_s[slot] = row
        red_r[slot, (gz * ngy + gy) * ngx + gx] = row

    def reduce_send(slot, planes):
        me = (gz * ngy + gy) * ngx + gx
        for k in planes:
            z_to = jnp.where(2 * gz < ngz, ngz - 1 - k, k)
            for b in reversed(range(ngy)):
                for c in (2, 3, 1, 0):
                    copy = pltpu.make_async_remote_copy(
                        src_ref=red_s.at[slot], dst_ref=red_r.at[slot, me], send_sem=rs_sem.at[slot], recv_sem=rr_sem.at[slot],
                        device_id=(z_to, lax.rem(gy + b, ngy), lax.rem(gx + c, ngx)), device_id_type=MESH)
                    if b or c:
                        copy.start()
                    else:
                        pl.when(z_to != gz)(copy.start)

    def reduce_wait(slot, count):
        whole = red_r.at[slot, pl.ds(0, others)]
        done = pltpu.make_async_remote_copy(
            src_ref=whole, dst_ref=whole, send_sem=rs_sem.at[slot], recv_sem=rr_sem.at[slot],
            device_id=(gz, gy, gx), device_id_type=MESH)
        done.wait_recv()
        done.wait_send()
        total = jnp.sum(red_r[slot], axis=0)
        return [jnp.sum(jnp.where(lane_row == q, total, 0.0), axis=1, keepdims=True) for q in range(count)]

    x_row, z_row = jnp.where(gx == 0, 0, 1), jnp.where(gz == 0, 4, 5)
    slabs_i = pl.ds(pl.multiple_of(gx * ni, 8), ni)
    inputs = [
        pltpu.make_async_copy(k_hbm, k_in, in_sem.at[0]),
        pltpu.make_async_copy(u_hbm, u_in, in_sem.at[1]),
        pltpu.make_async_copy(kg_hbm.at[x_row, pl.ds(pl.multiple_of(gy * nj, 8), nj)], wall_x, in_sem.at[2]),
        pltpu.make_async_copy(kg_hbm.at[2 + gy, slabs_i], wall_y, in_sem.at[3]),
        pltpu.make_async_copy(kg_hbm.at[z_row, slabs_i], wall_z, in_sem.at[4]),
        pltpu.make_async_copy(f_hbm, f_in, in_sem.at[5]),
    ]
    for copy in inputs[:5]:
        copy.start()

    def tell_neighbours(sem):
        tell = lambda *target: pl.semaphore_signal(sem, inc=1, device_id=target, device_id_type=MESH)
        pl.when(has_xlo)(lambda: tell(gz, gy, gx - 1))
        pl.when(has_xhi)(lambda: tell(gz, gy, gx + 1))
        pl.when(has_zlo)(lambda: tell(gz - 1, gy, gx))
        pl.when(has_zhi)(lambda: tell(gz + 1, gy, gx))
        tell(gz, 1 - gy, gx)

    neighbours = 5 - jnp.where(has_xlo, 0, 1) - jnp.where(has_xhi, 0, 1) - jnp.where(has_zlo, 0, 1) - jnp.where(has_zhi, 0, 1)
    rounds = (ngx - 1) + (ngy - 1) + (ngz - 1) - 1

    def next_round(k):
        pl.semaphore_wait(near_sem.at[k], neighbours)
        if k + 1 < rounds:
            tell_neighbours(near_sem.at[k + 1])

    barrier = pltpu.get_barrier_semaphore()
    tell_neighbours(barrier)

    for edge in (0, ni + 1):
        mp[edge] = jnp.zeros((nl + 2 * PAD, LANES), F32)
        kp[edge] = jnp.ones((nl + 2 * PAD, LANES), F32)

    def clear(i, _):
        mp[i + 1, pl.ds(0, PAD), :] = jnp.zeros((PAD, LANES), F32)
        mp[i + 1, pl.ds(PAD + nl, PAD), :] = jnp.zeros((PAD, LANES), F32)
        kp[i + 1, pl.ds(0, PAD), :] = jnp.ones((PAD, LANES), F32)
        kp[i + 1, pl.ds(PAD + nl, PAD), :] = jnp.ones((PAD, LANES), F32)
        mp[i + 1, rows, :] = zero_slab
        s[i] = zero_slab
        z[i] = zero_slab
        p[i] = zero_slab
        r[1, i] = zero_slab
        r[0, i] = zero_slab
        kp[i + 1, rows, :] = jnp.full((nl, LANES), 1.0, F32)
        return 0

    lax.fori_loop(0, ni, clear, 0)

    def load_k(i, _):
        kp[i + 1, rows, 0:nj] = k_in[i]
        return 0

    def load_u(i, _):
        mp[i + 1, rows, 0:nj] = u_in[i]
        return 0

    inputs[0].wait()
    inputs[5].start()
    packed_pass(kp, 0, load_k, 0)
    pl.semaphore_wait(barrier, neighbours)
    tell_neighbours(near_sem.at[0])
    exchange_start(kp, 0)
    inputs[1].wait()
    packed_pass(mp, 1, load_u, 0)
    exchange_start(mp, 1)
    next_round(0)

    for copy in inputs[2:5]:
        copy.wait()
    width = wall_x.shape[1]
    l_rows = pl.ds(pl.multiple_of(gz * nl, 8), nl)

    def flipped(wall, count):
        for start in range(0, width, LANES):
            size = min(LANES, width - start)
            block = jnp.concatenate([wall[:, start:start + size], jnp.ones((LANES - count, size), F32)], axis=0)
            wall_t[start:start + size, :] = block.T
        return wall_t[l_rows, :]

    x_wall = flipped(wall_x, nj)
    y_wall = flipped(wall_y, ni)
    if width > LANES:
        rest = jnp.concatenate([wall_z[:, LANES:width], jnp.ones((ni, 2 * LANES - width), F32)], axis=1)
        whole_z = wall_z[:, 0:LANES]
        turn = LANES - nj
        shifted = jnp.where(lane_i < turn, pltpu.roll(whole_z, turn, 1), pltpu.roll(rest, turn, 1))
    else:
        whole_z = jnp.concatenate([wall_z[...], jnp.ones((ni, LANES - width), F32)], axis=1)
        shifted = pltpu.roll(whole_z, LANES - nj, 1)
    z_wall = jnp.where(gy == 0, whole_z, shifted)

    def harmonic(left, right):
        return 2.0 * left * right / (left + right)

    next_round(1)

    in_i = lane_i < nj
    cx[0] = jnp.where(jnp.logical_and(inside, gx == 0), harmonic(x_wall, kp[1, rows, :]), 0.0)
    z_low = jnp.where(jnp.logical_and(in_i, gz == 0), harmonic(z_wall, zs[0, 1]), 0.0)
    z_high = jnp.where(jnp.logical_and(in_i, gz == ngz - 1), harmonic(zs[0, 0], z_wall), 0.0)
    y_low_mask = jnp.logical_and(inside, jnp.logical_or(lane > 0, y_low_wall))
    y_high_mask = jnp.logical_and(inside, jnp.logical_or(lane < nj - 1, y_high_wall))
    wall_lane = nj - 1 - face_lane

    def coefs(i, _):
        here = kp[i + 1, rows, :]
        cx[i + 1] = jnp.where(inside, harmonic(here, kp[i + 2, rows, :]), 0.0)
        cz[i, rows_up, :] = jnp.where(inside, harmonic(here, kp[i + 1, rows_up, :]), 0.0)
        wall = column_roll(y_wall, wall_lane - i)
        low = jnp.where(lane == 0, wall, pltpu.roll(here, 1, 1))
        high = jnp.where(lane == nj - 1, wall, pltpu.roll(here, LANES - 1, 1))
        cy[i] = jnp.where(y_low_mask, harmonic(low, here), 0.0)
        cyh[i] = jnp.where(y_high_mask, harmonic(here, high), 0.0)
        return 0

    slabs(GROUP, coefs, 0)
    next_round(2)
    cx[ni] = jnp.where(jnp.logical_and(inside, gx == ngx - 1), harmonic(kp[ni, rows, :], x_wall), 0.0)
    for i in range(ni):
        cz[i, PAD:PAD + 1, :] = z_low[i:i + 1, :]
        cz[i, PAD + nl:PAD + nl + 1, :] = z_high[i:i + 1, :]

    stencil(mp, diagonal=True)
    next_round(3)

    exchange_wait(kp, 0)

    @pl.when(has_xlo)
    def _():
        bx[0] = jnp.where(inside, harmonic(xr[0, 0], kp[1, rows, :]), 0.0)
        inv[0] = inv[0] + bx[0]

    @pl.when(has_xhi)
    def _():
        bx[1] = jnp.where(inside, harmonic(kp[ni, rows, :], xr[0, 1]), 0.0)
        inv[ni - 1] = inv[ni - 1] + bx[1]

    @pl.when(has_zlo)
    def _():
        bz[0] = jnp.where(in_i, harmonic(zr[0, 0], zs[0, 1]), 0.0)
        add_rows(inv, bz[0], 0)

    @pl.when(has_zhi)
    def _():
        bz[1] = jnp.where(in_i, harmonic(zs[0, 0], zr[0, 1]), 0.0)
        add_rows(inv, bz[1], nl - 1)

    y_face = jnp.where(lax.rem(lane_half, LANES // 2) < ni, harmonic(ys[0], yr[0]), 0.0)
    by[...] = y_face
    add_columns(inv, y_face)
    join_faces(mp, 1)
    inputs[5].wait()

    def first_residual(i, acc):
        iv = jnp.where(inside, 1.0 / jnp.where(inside, inv[i], 1.0), 0.0)
        inv[i] = iv
        x[i] = mp[i + 1, rows, :]
        r[0, i, :, 0:nj] = f_in[i]
        res = r[0, i] - n[i]
        r[0, i] = res
        u = res * iv
        mp[i + 1, rows, :] = u
        return acc + fold(res * u)

    gamma_acc = packed_pass(mp, 2, first_residual, zero_acc)
    exchange_start(mp, 2)
    next_round(4)
    stencil(mp)
    for k in range(5, rounds):
        next_round(k)
    join_faces(mp, 2)

    def first_w(i, acc):
        av = n[i]
        w[i] = av
        return acc + fold(av * mp[i + 1, rows, :])

    reduce_row(0, (gamma_acc, slabs(GROUP, first_w, zero_acc)))

    def scalars(t, sums, gamma_old, pap_old):
        gamma, delta, sigma = sums[0], sums[1], sums[2]
        beta = jnp.where(t == 0, 0.0, gamma / gamma_old)
        pap = delta + 2.0 * beta * sigma + beta * beta * pap_old
        return gamma, pap, beta[0, 0], (gamma / pap)[0, 0]

    def advance_x(now, alpha, beta):
        def step(i, acc):
            p_new = inv[i] * r[1 - now, i] + beta * p[i]
            p[i] = p_new
            x[i] = x[i] + alpha * p_new
            return acc + fold(r[now, i] * r[now, i])
        return lax.fori_loop(0, ni, step, zero_acc)

    def iteration(t, carry):
        gamma_old, pap_old, alpha_old, beta_old = carry
        now = lax.rem(t, 2)
        reduce_send(t, range(0, ngz // 2))
        scale_and_pack(t + 3)
        exchange_start(mp, t + 3)
        reduce_send(t, range(ngz // 2, ngz))
        stencil(mp)
        rr_acc = advance_x(now, alpha_old, beta_old)
        join_faces(mp, t + 3)
        sums = reduce_wait(t, 4)
        gamma, pap, beta, alpha = scalars(t, sums, gamma_old, pap_old)

        def update(i, acc):
            iv = inv[i]
            w_old = w[i]
            z_new = n[i] + beta * z[i]
            s_new = w_old + beta * s[i]
            r_new = r[now, i] - alpha * s_new
            w_new = w_old - alpha * z_new
            u_new = iv * r_new
            z[i] = z_new
            s[i] = s_new
            r[1 - now, i] = r_new
            w[i] = w_new
            return acc[0] + fold(r_new * u_new), acc[1] + fold(w_new * u_new), acc[2] + fold(u_new * s_new)

        reduce_row(t + 1, slabs(UPDATE, update, (zero_acc,) * 3) + (rr_acc,))
        scal_ref[lax.rem(t + CG_ITERS - 2, CG_ITERS)] = jnp.broadcast_to(sums[3], (1, LANES))
        return gamma, pap, alpha, beta

    one = jnp.ones((1, 1), F32)
    last = CG_ITERS - 1
    gamma_old, pap_old, alpha_old, beta_old = lax.fori_loop(
        0, last, iteration, (one, one, jnp.float32(0.0), jnp.float32(0.0)))

    now = last % 2
    reduce_send(last, range(ngz))

    def last_dots(i, acc):
        rv, sv = r[now, i], s[i]
        wv = w[i]
        pairs = ((rv, rv), (rv, wv), (rv, sv), (wv, wv), (wv, sv), (sv, sv))
        return tuple(a + fold(b * c) for a, (b, c) in zip(acc, pairs))

    reduce_row(CG_ITERS, slabs(3, last_dots, (zero_acc,) * 6))
    reduce_send(CG_ITERS, range(ngz))
    advance_x(now, alpha_old, beta_old)

    def last_u(i, _):
        n[i] = inv[i] * r[now, i]
        return 0

    lax.fori_loop(0, ni, last_u, 0)
    sums = reduce_wait(last, 4)
    wide = lambda value: jnp.broadcast_to(value, (1, LANES))
    scal_ref[last - 2] = wide(sums[3])
    gamma = sums[0]
    beta = gamma / gamma_old
    alpha = gamma / (sums[1] + 2.0 * beta * sums[2] + beta * beta * pap_old)
    scal_ref[CG_ITERS] = wide(alpha)
    scal_ref[CG_ITERS + 1] = wide(beta)
    rr, rw, rs, ww, ws, ss = reduce_wait(CG_ITERS, 6)
    scal_ref[last - 1] = wide(rr)
    scal_ref[last] = wide(rr - 2.0 * alpha * (rw + beta * rs) + alpha * alpha * (ww + 2.0 * beta * ws + beta * beta * ss))


def finish_kernel(chunk, scal, x, u, p, r, w, s, x_hbm, r_hbm, hist_hbm, x_new, r_new, hist, sem, hist_sem):
    ni, nl, nj = x_new.shape
    alpha = jnp.broadcast_to(scal[CG_ITERS], (nl, LANES))
    beta = jnp.broadcast_to(scal[CG_ITERS + 1], (nl, LANES))
    copies = []

    def step(i, _):
        x_new[i] = (x[i] + alpha * (u[i] + beta * p[i]))[:, 0:nj]
        r_new[i] = (r[1, i] - alpha * (w[i] + beta * s[i]))[:, 0:nj]
        return 0

    for g in range(ni // chunk):
        lax.fori_loop(g * chunk, (g + 1) * chunk, step, 0)
        part = pl.ds(g * chunk, chunk)
        for j, (src, dst) in enumerate(((x_new, x_hbm), (r_new, r_hbm))):
            copies.append(pltpu.make_async_copy(src.at[part], dst.at[part], sem.at[j, g]))
            copies[-1].start()
        if g == 0:
            for t in range(CG_ITERS):
                hist[t] = scal[t, 0, 0]
            copies.append(pltpu.make_async_copy(hist, hist_hbm, hist_sem))
            copies[-1].start()
    for copy in copies:
        copy.wait()


def solution(mesh):
    counts = (mesh.shape['gx'], mesh.shape['gy'], mesh.shape['gz'])
    grid_spec = P('gx', 'gy', 'gz')

    def local_solve(k_cell, k_ghost, f_rhs, u_init):
        ni, nj, nl = k_cell.shape
        flip = lambda a: jnp.swapaxes(a, 1, 2)
        slots = CG_ITERS + 3
        devices = counts[0] * counts[1] * counts[2]
        width = k_ghost.shape[2]
        any_spec = pl.BlockSpec(memory_space=pl.ANY)
        vm = lambda *shape: pltpu.VMEM(shape, F32)
        whole = vm(ni, nl, LANES)
        block = vm(ni, nl, nj)
        padded = vm(ni + 2, nl + 2 * PAD, LANES)
        dma = pltpu.SemaphoreType.DMA
        kept = pltpu.VMEM((ni, nl, LANES), F32)
        vmem_spec = pl.BlockSpec(memory_space=pltpu.VMEM)
        *state, scal = pl.pallas_call(
            functools.partial(solve_kernel, (ni, nl, nj), counts),
            out_shape=(kept, kept, kept, pltpu.VMEM((2, ni, nl, LANES), F32), kept, kept,
                       pltpu.VMEM((CG_ITERS + 2, 1, LANES), F32)),
            in_specs=[any_spec] * 4,
            out_specs=(vmem_spec,) * 7,
            scratch_shapes=[
                block, block, block, vm(nj, width), vm(ni, width), vm(ni, width), vm(-(-width // LANES) * LANES, LANES),
                vm(2, nl, LANES), vm(nl // 2, LANES), vm(2, ni, LANES),
                padded, padded, vm(ni + 1, nl, LANES), whole, whole, vm(ni, nl + 2 * PAD, LANES), whole,
                whole,
                vm(slots, nl // 2, LANES), vm(slots, 2, ni, LANES),
                vm(slots, 2, nl, LANES), vm(slots, nl // 2, LANES), vm(slots, 2, ni, LANES),
                vm(CG_ITERS + 1, 1, LANES), vm(CG_ITERS + 1, devices, 1, LANES),
                dma((slots, 2)), dma((slots,)), dma((slots, 2)), dma((slots, 2)), dma((slots,)), dma((slots, 2)),
                dma((CG_ITERS + 1,)), dma((CG_ITERS + 1,)), dma((6,)), pltpu.SemaphoreType.REGULAR((6,)),
            ],
            compiler_params=pltpu.CompilerParams(has_side_effects=True, collective_id=0, vmem_limit_bytes=28 << 20),
        )(*(pltpu.with_memory_space_constraint(a, pltpu.HBM) for a in (k_ghost, flip(k_cell), flip(f_rhs), flip(u_init))))
        chunk = ni // 4
        out_block = jax.ShapeDtypeStruct((ni, nl, nj), F32)
        x_new, r_new, hist = pl.pallas_call(
            functools.partial(finish_kernel, chunk),
            out_shape=(out_block, out_block, jax.ShapeDtypeStruct((CG_ITERS,), F32)),
            in_specs=[vmem_spec] * 7,
            out_specs=(any_spec,) * 3,
            scratch_shapes=[block, block, pltpu.SMEM((CG_ITERS,), F32), dma((2, ni // chunk)), dma],
            compiler_params=pltpu.CompilerParams(vmem_limit_bytes=28 << 20),
        )(scal, *state)
        return flip(x_new), flip(r_new), hist

    return jax.shard_map(local_solve, mesh=mesh, in_specs=(grid_spec, P(), grid_spec, grid_spec),
                         out_specs=(grid_spec, grid_spec, P()), check_vma=False)
```

```python
import functools

import jax
import jax.numpy as jnp
from jax import lax
from jax.experimental import pallas as pl
from jax.experimental.pallas import tpu as pltpu
from jax.sharding import PartitionSpec as P

CG_ITERS = 8
LANES = 128
PAD = 8
GROUP = 6
COLUMNS = 16
UPDATE = 4
MESH = pl.DeviceIdType.MESH
F32 = jnp.float32


def solve_kernel(dims, counts, kg_hbm, k_hbm, f_hbm, u_hbm, x_last, r_last, scal_ref,
                 k_in, f_in, u_in, wall_x, wall_y, wall_z, wall_t, bx, by, bz,
                 kp, mp, cx, cy, cyh, cz, inv, x, r, w, s, z, p, n,
                 ys, zs, xr, yr, zr, red_s, red_r,
                 xs_sem, ys_sem, zs_sem, xr_sem, yr_sem, zr_sem, rs_sem, rr_sem, in_sem, near_sem):
    ni, nl, nj = dims
    ngx, ngy, ngz = counts
    half = nl // 2
    gx, gy, gz = lax.axis_index('gx'), lax.axis_index('gy'), lax.axis_index('gz')
    rows = pl.ds(PAD, nl)
    rows_dn = pl.ds(PAD - 1, nl)
    rows_up = pl.ds(PAD + 1, nl)
    lane = lax.broadcasted_iota(jnp.int32, (nl, LANES), 1)
    lane_i = lax.broadcasted_iota(jnp.int32, (ni, LANES), 1)
    lane_half = lax.broadcasted_iota(jnp.int32, (half, LANES), 1)
    lane_row = lax.broadcasted_iota(jnp.int32, (1, LANES), 1)
    inside = lane < nj
    has_xlo, has_xhi = gx > 0, gx < ngx - 1
    has_zlo, has_zhi = gz > 0, gz < ngz - 1
    face_lane = jnp.where(gy == 0, nj - 1, 0)
    y_low_wall, y_high_wall = gy == 0, gy > 0
    zero_slab = jnp.zeros((nl, LANES), F32)
    zero_acc = jnp.zeros((8, LANES), F32)
    others = ngx * ngy * ngz - 1

    def column_roll(slab, shift):
        return pltpu.roll(slab, shift + 2 * LANES, 1)

    def slabs(group, step, init):
        def body(g, carry):
            for k in range(group):
                carry = step(g * group + k, carry)
            return carry
        return lax.fori_loop(0, ni // group, body, init)

    def x_copy(ref, slot, up):
        src = ref.at[ni if up else 1, rows]
        return pltpu.make_async_remote_copy(
            src_ref=src, dst_ref=xr.at[slot, 0 if up else 1], send_sem=xs_sem.at[slot, 0 if up else 1],
            recv_sem=xr_sem.at[slot, 0 if up else 1], device_id=(gz, gy, gx + 1 if up else gx - 1), device_id_type=MESH)

    def z_copy(slot, up):
        return pltpu.make_async_remote_copy(
            src_ref=zs.at[slot, 0 if up else 1], dst_ref=zr.at[slot, 0 if up else 1],
            send_sem=zs_sem.at[slot, 0 if up else 1], recv_sem=zr_sem.at[slot, 0 if up else 1],
            device_id=(gz + 1 if up else gz - 1, gy, gx), device_id_type=MESH)

    def y_copy(slot):
        return pltpu.make_async_remote_copy(
            src_ref=ys.at[slot], dst_ref=yr.at[slot], send_sem=ys_sem.at[slot], recv_sem=yr_sem.at[slot],
            device_id=(gz, 1 - gy, gx), device_id_type=MESH)

    def pack_slab(slot, i, slab):
        zs[slot, 1, pl.ds(i, 1), :] = slab[0:1, :]
        zs[slot, 0, pl.ds(i, 1), :] = slab[nl - 1:nl, :]
        return column_roll(slab[0:half], i - face_lane), column_roll(slab[half:nl], i - face_lane + LANES // 2)

    def pack_rolls(ref, slot, i, behind=False):
        row = lax.max(i, 0) if behind else i
        return pack_slab(slot, row, ref[row + 1, rows, :])

    def pack(i, rolled, acc):
        acc = jnp.where(lane_half == i, rolled[0], acc)
        return jnp.where(lane_half == i + LANES // 2, rolled[1], acc)

    def packed_pass(ref, slot, step, init):
        def body(g, carry):
            state, acc = carry
            rolled = [pack_rolls(ref, slot, (g - 1) * GROUP + k, behind=True) for k in range(GROUP)]
            for k in range(GROUP):
                state = step(g * GROUP + k, state)
            for k in range(GROUP):
                acc = pack((g - 1) * GROUP + k, rolled[k], acc)
            return state, acc
        state, acc = lax.fori_loop(0, ni // GROUP, body, (init, jnp.zeros((half, LANES), F32)))
        rolled = [pack_rolls(ref, slot, ni - GROUP + k) for k in range(GROUP)]
        for k in range(GROUP):
            acc = pack(ni - GROUP + k, rolled[k], acc)
        ys[slot] = acc
        return state

    def scale_and_pack(slot):
        group = min(COLUMNS, ni)

        def body(g, acc):
            rolled = []
            for k in range(group):
                i = g * group + k
                m = inv[i] * w[i]
                mp[i + 1, rows, :] = m
                rolled.append(pack_slab(slot, i, m))
            for k in range(group):
                acc = pack(g * group + k, rolled[k], acc)
            return acc

        ys[slot] = lax.fori_loop(0, ni // group, body, jnp.zeros((half, LANES), F32))

    def exchange_start(ref, slot):
        y_copy(slot).start()
        pl.when(has_zlo)(lambda: z_copy(slot, False).start())
        pl.when(has_zhi)(lambda: z_copy(slot, True).start())
        pl.when(has_xlo)(lambda: x_copy(ref, slot, False).start())
        pl.when(has_xhi)(lambda: x_copy(ref, slot, True).start())

    def exchange_wait(ref, slot):
        @pl.when(has_xlo)
        def _():
            x_copy(ref, slot, False).wait_send()
            x_copy(ref, slot, True).wait_recv()

        @pl.when(has_xhi)
        def _():
            x_copy(ref, slot, True).wait_send()
            x_copy(ref, slot, False).wait_recv()

        @pl.when(has_zlo)
        def _():
            z_copy(slot, False).wait_send()
            z_copy(slot, True).wait_recv()

        @pl.when(has_zhi)
        def _():
            z_copy(slot, True).wait_send()
            z_copy(slot, False).wait_recv()

        y_copy(slot).wait()

    def add_rows(ref, layer, row):
        for i in range(ni):
            ref[i, row:row + 1, :] = ref[i, row:row + 1, :] + layer[i:i + 1, :]

    def add_columns(ref, packed):
        mask = lane == face_lane

        def step(g, _):
            columns = []
            for k in range(min(COLUMNS, ni)):
                i = g * min(COLUMNS, ni) + k
                columns.append((column_roll(packed, face_lane - i), column_roll(packed, face_lane - i - LANES // 2)))
            for k in range(min(COLUMNS, ni)):
                i = g * min(COLUMNS, ni) + k
                ref[i] = ref[i] + jnp.where(mask, jnp.concatenate(columns[k], axis=0), 0.0)
            return 0

        lax.fori_loop(0, ni // min(COLUMNS, ni), step, 0)

    def join_faces(ref, slot):
        y_copy(slot).wait()
        add_columns(n, by[...] * (ys[slot] - yr[slot]))

        @pl.when(has_xlo)
        def _():
            x_copy(ref, slot, False).wait_send()
            x_copy(ref, slot, True).wait_recv()
            n[0] = n[0] + bx[0] * (ref[1, rows, :] - xr[slot, 0])

        @pl.when(has_xhi)
        def _():
            x_copy(ref, slot, True).wait_send()
            x_copy(ref, slot, False).wait_recv()
            n[ni - 1] = n[ni - 1] + bx[1] * (ref[ni, rows, :] - xr[slot, 1])

        @pl.when(has_zlo)
        def _():
            z_copy(slot, False).wait_send()
            z_copy(slot, True).wait_recv()
            add_rows(n, bz[0] * (zs[slot, 1] - zr[slot, 0]), 0)

        @pl.when(has_zhi)
        def _():
            z_copy(slot, True).wait_send()
            z_copy(slot, False).wait_recv()
            add_rows(n, bz[1] * (zs[slot, 0] - zr[slot, 1]), nl - 1)

    def stencil(ref, diagonal=False):
        def step(i, carry):
            v, flux_x = carry
            above = ref[i + 2, rows, :]
            if diagonal:
                inv[i] = cx[i] + cx[i + 1] + cy[i] + cyh[i] + cz[i, rows, :] + cz[i, rows_up, :]
            flux_next = cx[i + 1] * (above - v)
            flux_zl = cz[i, rows, :] * (v - ref[i + 1, rows_dn, :])
            flux_zh = cz[i, rows_up, :] * (ref[i + 1, rows_up, :] - v)
            flux_yl = cy[i] * (v - pltpu.roll(v, 1, 1))
            flux_yh = cyh[i] * (pltpu.roll(v, LANES - 1, 1) - v)
            n[i] = (flux_x - flux_next) + (flux_yl - flux_yh) + (flux_zl - flux_zh)
            return above, flux_next

        first = ref[1, rows, :]
        slabs(GROUP, step, (first, cx[0] * (first - ref[0, rows, :])))

    def fold(slab):
        out = slab[0:8]
        for part in range(8, nl, 8):
            out = out + slab[part:part + 8]
        return out

    def reduce_row(slot, accs):
        row = jnp.zeros((1, LANES), F32)
        for q, acc in enumerate(accs):
            row = jnp.where(lane_row == q, jnp.sum(jnp.sum(acc, axis=0, keepdims=True), axis=1, keepdims=True), row)
        red_s[slot] = row
        red_r[slot, (gz * ngy + gy) * ngx + gx] = row

    def reduce_send(slot, planes):
        me = (gz * ngy + gy) * ngx + gx
        for k in planes:
            z_to = jnp.where(2 * gz < ngz, ngz - 1 - k, k)
            for b in reversed(range(ngy)):
                for c in (2, 3, 1, 0):
                    copy = pltpu.make_async_remote_copy(
                        src_ref=red_s.at[slot], dst_ref=red_r.at[slot, me], send_sem=rs_sem.at[slot], recv_sem=rr_sem.at[slot],
                        device_id=(z_to, lax.rem(gy + b, ngy), lax.rem(gx + c, ngx)), device_id_type=MESH)
                    if b or c:
                        copy.start()
                    else:
                        pl.when(z_to != gz)(copy.start)

    def reduce_wait(slot, count):
        whole = red_r.at[slot, pl.ds(0, others)]
        done = pltpu.make_async_remote_copy(
            src_ref=whole, dst_ref=whole, send_sem=rs_sem.at[slot], recv_sem=rr_sem.at[slot],
            device_id=(gz, gy, gx), device_id_type=MESH)
        done.wait_recv()
        done.wait_send()
        parts = [red_r[slot, device] for device in range(others + 1)]
        while len(parts) > 1:
            parts = [a + b for a, b in zip(parts[0::2], parts[1::2])]
        total = parts[0]
        return [jnp.sum(jnp.where(lane_row == q, total, 0.0), axis=1, keepdims=True) for q in range(count)]

    x_row, z_row = jnp.where(gx == 0, 0, 1), jnp.where(gz == 0, 4, 5)
    slabs_i = pl.ds(pl.multiple_of(gx * ni, 8), ni)
    inputs = [
        pltpu.make_async_copy(k_hbm, k_in, in_sem.at[0]),
        pltpu.make_async_copy(u_hbm, u_in, in_sem.at[1]),
        pltpu.make_async_copy(kg_hbm.at[x_row, pl.ds(pl.multiple_of(gy * nj, 8), nj)], wall_x, in_sem.at[2]),
        pltpu.make_async_copy(kg_hbm.at[2 + gy, slabs_i], wall_y, in_sem.at[3]),
        pltpu.make_async_copy(kg_hbm.at[z_row, slabs_i], wall_z, in_sem.at[4]),
        pltpu.make_async_copy(f_hbm, f_in, in_sem.at[5]),
    ]
    for copy in inputs[:5]:
        copy.start()

    def tell_neighbours(sem):
        tell = lambda *target: pl.semaphore_signal(sem, inc=1, device_id=target, device_id_type=MESH)
        pl.when(has_xlo)(lambda: tell(gz, gy, gx - 1))
        pl.when(has_xhi)(lambda: tell(gz, gy, gx + 1))
        pl.when(has_zlo)(lambda: tell(gz - 1, gy, gx))
        pl.when(has_zhi)(lambda: tell(gz + 1, gy, gx))
        tell(gz, 1 - gy, gx)

    neighbours = 5 - jnp.where(has_xlo, 0, 1) - jnp.where(has_xhi, 0, 1) - jnp.where(has_zlo, 0, 1) - jnp.where(has_zhi, 0, 1)
    rounds = (ngx - 1) + (ngy - 1) + (ngz - 1) - 1

    def next_round(k):
        pl.semaphore_wait(near_sem.at[k], neighbours)
        if k + 1 < rounds:
            tell_neighbours(near_sem.at[k + 1])

    barrier = pltpu.get_barrier_semaphore()
    tell_neighbours(barrier)

    for edge in (0, ni + 1):
        mp[edge] = jnp.zeros((nl + 2 * PAD, LANES), F32)
        kp[edge] = jnp.ones((nl + 2 * PAD, LANES), F32)

    def clear(i, _):
        mp[i + 1, pl.ds(0, PAD), :] = jnp.zeros((PAD, LANES), F32)
        mp[i + 1, pl.ds(PAD + nl, PAD), :] = jnp.zeros((PAD, LANES), F32)
        kp[i + 1, pl.ds(0, PAD), :] = jnp.ones((PAD, LANES), F32)
        kp[i + 1, pl.ds(PAD + nl, PAD), :] = jnp.ones((PAD, LANES), F32)
        mp[i + 1, rows, :] = zero_slab
        s[i] = zero_slab
        z[i] = zero_slab
        p[i] = zero_slab
        r[1, i] = zero_slab
        r[0, i] = zero_slab
        kp[i + 1, rows, :] = jnp.full((nl, LANES), 1.0, F32)
        return 0

    lax.fori_loop(0, ni, clear, 0)

    def load_k(i, _):
        kp[i + 1, rows, 0:nj] = k_in[i]
        return 0

    def load_u(i, _):
        mp[i + 1, rows, 0:nj] = u_in[i]
        return 0

    inputs[0].wait()
    inputs[5].start()
    packed_pass(kp, 0, load_k, 0)
    pl.semaphore_wait(barrier, neighbours)
    tell_neighbours(near_sem.at[0])
    exchange_start(kp, 0)
    inputs[1].wait()
    packed_pass(mp, 1, load_u, 0)
    exchange_start(mp, 1)
    next_round(0)

    for copy in inputs[2:5]:
        copy.wait()
    width = wall_x.shape[1]
    l_rows = pl.ds(pl.multiple_of(gz * nl, 8), nl)

    def flipped(wall, count):
        for start in range(0, width, LANES):
            size = min(LANES, width - start)
            block = jnp.concatenate([wall[:, start:start + size], jnp.ones((LANES - count, size), F32)], axis=0)
            wall_t[start:start + size, :] = block.T
        return wall_t[l_rows, :]

    x_wall = flipped(wall_x, nj)
    y_wall = flipped(wall_y, ni)
    if width > LANES:
        rest = jnp.concatenate([wall_z[:, LANES:width], jnp.ones((ni, 2 * LANES - width), F32)], axis=1)
        whole_z = wall_z[:, 0:LANES]
        turn = LANES - nj
        shifted = jnp.where(lane_i < turn, pltpu.roll(whole_z, turn, 1), pltpu.roll(rest, turn, 1))
    else:
        whole_z = jnp.concatenate([wall_z[...], jnp.ones((ni, LANES - width), F32)], axis=1)
        shifted = pltpu.roll(whole_z, LANES - nj, 1)
    z_wall = jnp.where(gy == 0, whole_z, shifted)

    def harmonic(left, right):
        return 2.0 * left * right / (left + right)

    next_round(1)

    in_i = lane_i < nj
    cx[0] = jnp.where(jnp.logical_and(inside, gx == 0), harmonic(x_wall, kp[1, rows, :]), 0.0)
    z_low = jnp.where(jnp.logical_and(in_i, gz == 0), harmonic(z_wall, zs[0, 1]), 0.0)
    z_high = jnp.where(jnp.logical_and(in_i, gz == ngz - 1), harmonic(zs[0, 0], z_wall), 0.0)
    y_low_mask = jnp.logical_and(inside, jnp.logical_or(lane > 0, y_low_wall))
    y_high_mask = jnp.logical_and(inside, jnp.logical_or(lane < nj - 1, y_high_wall))
    wall_lane = jnp.where(gy == 0, 0, nj)

    def coefs(i, _):
        here = kp[i + 1, rows, :]
        cx[i + 1] = jnp.where(inside, harmonic(here, kp[i + 2, rows, :]), 0.0)
        cz[i, rows_up, :] = jnp.where(inside, harmonic(here, kp[i + 1, rows_up, :]), 0.0)
        wall = column_roll(y_wall, wall_lane - i)
        low = jnp.where(jnp.logical_and(lane == 0, y_low_wall), wall, pltpu.roll(here, 1, 1))
        faces = harmonic(low, jnp.where(jnp.logical_and(lane == nj, y_high_wall), wall, here))
        cy[i] = jnp.where(y_low_mask, faces, 0.0)
        cyh[i] = jnp.where(y_high_mask, pltpu.roll(faces, LANES - 1, 1), 0.0)
        return 0

    slabs(GROUP, coefs, 0)
    next_round(2)
    cx[ni] = jnp.where(jnp.logical_and(inside, gx == ngx - 1), harmonic(kp[ni, rows, :], x_wall), 0.0)
    for i in range(ni):
        cz[i, PAD:PAD + 1, :] = z_low[i:i + 1, :]
        cz[i, PAD + nl:PAD + nl + 1, :] = z_high[i:i + 1, :]

    stencil(mp, diagonal=True)
    next_round(3)

    exchange_wait(kp, 0)

    @pl.when(has_xlo)
    def _():
        bx[0] = jnp.where(inside, harmonic(xr[0, 0], kp[1, rows, :]), 0.0)
        inv[0] = inv[0] + bx[0]

    @pl.when(has_xhi)
    def _():
        bx[1] = jnp.where(inside, harmonic(kp[ni, rows, :], xr[0, 1]), 0.0)
        inv[ni - 1] = inv[ni - 1] + bx[1]

    @pl.when(has_zlo)
    def _():
        bz[0] = jnp.where(in_i, harmonic(zr[0, 0], zs[0, 1]), 0.0)
        add_rows(inv, bz[0], 0)

    @pl.when(has_zhi)
    def _():
        bz[1] = jnp.where(in_i, harmonic(zs[0, 0], zr[0, 1]), 0.0)
        add_rows(inv, bz[1], nl - 1)

    y_face = jnp.where(lax.rem(lane_half, LANES // 2) < ni, harmonic(ys[0], yr[0]), 0.0)
    by[...] = y_face
    add_columns(inv, y_face)
    join_faces(mp, 1)
    inputs[5].wait()

    def first_residual(i, acc):
        iv = jnp.where(inside, 1.0 / jnp.where(inside, inv[i], 1.0), 0.0)
        inv[i] = iv
        x[i] = mp[i + 1, rows, :]
        r[0, i, :, 0:nj] = f_in[i]
        res = r[0, i] - n[i]
        r[0, i] = res
        u = res * iv
        mp[i + 1, rows, :] = u
        return acc + fold(res * u)

    gamma_acc = packed_pass(mp, 2, first_residual, zero_acc)
    exchange_start(mp, 2)
    next_round(4)
    stencil(mp)
    for k in range(5, rounds):
        next_round(k)
    join_faces(mp, 2)

    def first_w(i, acc):
        av = n[i]
        w[i] = av
        return acc + fold(av * mp[i + 1, rows, :])

    reduce_row(0, (gamma_acc, slabs(GROUP, first_w, zero_acc)))

    def scalars(t, sums, gamma_old, pap_old):
        gamma, delta, sigma = sums[0], sums[1], sums[2]
        beta = jnp.where(t == 0, 0.0, gamma / gamma_old)
        pap = delta + 2.0 * beta * sigma + beta * beta * pap_old
        return gamma, pap, beta, gamma / pap

    def wide(value):
        return jnp.broadcast_to(value, (nl, LANES))

    def advance_x(now, alpha, beta):
        alpha, beta = wide(alpha), wide(beta)

        def step(i, acc):
            p_new = inv[i] * r[1 - now, i] + beta * p[i]
            p[i] = p_new
            x[i] = x[i] + alpha * p_new
            return acc + fold(r[now, i] * r[now, i])
        return lax.fori_loop(0, ni, step, zero_acc)

    def iteration(t, carry):
        gamma_old, pap_old, alpha_old, beta_old = carry
        now = lax.rem(t, 2)
        reduce_send(t, range(0, ngz // 2))
        scale_and_pack(t + 3)
        exchange_start(mp, t + 3)
        reduce_send(t, range(ngz // 2, ngz))
        stencil(mp)
        rr_acc = advance_x(now, alpha_old, beta_old)
        join_faces(mp, t + 3)
        sums = reduce_wait(t, 4)
        gamma, pap, beta, alpha = scalars(t, sums, gamma_old, pap_old)

        alpha_w, beta_w = wide(alpha), wide(beta)

        def update(i, acc):
            iv = inv[i]
            w_old = w[i]
            z_new = n[i] + beta_w * z[i]
            s_new = w_old + beta_w * s[i]
            r_new = r[now, i] - alpha_w * s_new
            w_new = w_old - alpha_w * z_new
            u_new = iv * r_new
            z[i] = z_new
            s[i] = s_new
            r[1 - now, i] = r_new
            w[i] = w_new
            return acc[0] + fold(r_new * u_new), acc[1] + fold(w_new * u_new), acc[2] + fold(u_new * s_new)

        reduce_row(t + 1, slabs(UPDATE, update, (zero_acc,) * 3) + (rr_acc,))
        scal_ref[lax.rem(t + CG_ITERS - 2, CG_ITERS)] = jnp.broadcast_to(sums[3], (1, LANES))
        return gamma, pap, alpha, beta

    one = jnp.ones((1, 1), F32)
    last = CG_ITERS - 1
    gamma_old, pap_old, alpha_old, beta_old = lax.fori_loop(
        0, last, iteration, (one, one, 0.0 * one, 0.0 * one))

    now = last % 2
    reduce_send(last, range(ngz))

    def last_dots(i, acc):
        rv, sv = r[now, i], s[i]
        wv = w[i]
        pairs = ((rv, rv), (rv, wv), (rv, sv), (wv, wv), (wv, sv), (sv, sv))
        return tuple(a + fold(b * c) for a, (b, c) in zip(acc, pairs))

    reduce_row(CG_ITERS, slabs(3, last_dots, (zero_acc,) * 6))
    reduce_send(CG_ITERS, range(ngz))
    advance_x(now, alpha_old, beta_old)

    sums = reduce_wait(last, 4)
    line = lambda value: jnp.broadcast_to(value, (1, LANES))
    scal_ref[last - 2] = line(sums[3])
    gamma = sums[0]
    beta = gamma / gamma_old
    alpha = gamma / (sums[1] + 2.0 * beta * sums[2] + beta * beta * pap_old)
    alpha_w, beta_w = wide(alpha), wide(beta)

    def final(i, _):
        r_old = r[now, i]
        x_last[i] = (x[i] + alpha_w * (inv[i] * r_old + beta_w * p[i]))[:, 0:nj]
        r_last[i] = (r_old - alpha_w * (w[i] + beta_w * s[i]))[:, 0:nj]
        return 0

    slabs(2, final, 0)
    rr, rw, rs, ww, ws, ss = reduce_wait(CG_ITERS, 6)
    scal_ref[last - 1] = line(rr)
    scal_ref[last] = line(rr - 2.0 * alpha * (rw + beta * rs) + alpha * alpha * (ww + 2.0 * beta * ws + beta * beta * ss))


def finish_kernel(scal, x, r, x_hbm, r_hbm, hist_hbm, hist, sem):
    copies = [pltpu.make_async_copy(x, x_hbm, sem.at[0]), pltpu.make_async_copy(r, r_hbm, sem.at[1]),
              pltpu.make_async_copy(hist, hist_hbm, sem.at[2])]
    copies[0].start()
    copies[1].start()
    for t in range(CG_ITERS):
        hist[t] = scal[t, 0, 0]
    copies[2].start()
    for copy in copies:
        copy.wait()


def solution(mesh):
    counts = (mesh.shape['gx'], mesh.shape['gy'], mesh.shape['gz'])
    grid_spec = P('gx', 'gy', 'gz')

    def local_solve(k_cell, k_ghost, f_rhs, u_init):
        ni, nj, nl = k_cell.shape
        flip = lambda a: jnp.swapaxes(a, 1, 2)
        slots = CG_ITERS + 3
        devices = counts[0] * counts[1] * counts[2]
        width = k_ghost.shape[2]
        any_spec = pl.BlockSpec(memory_space=pl.ANY)
        vm = lambda *shape: pltpu.VMEM(shape, F32)
        whole = vm(ni, nl, LANES)
        block = vm(ni, nl, nj)
        padded = vm(ni + 2, nl + 2 * PAD, LANES)
        dma = pltpu.SemaphoreType.DMA
        kept = pltpu.VMEM((ni, nl, nj), F32)
        vmem_spec = pl.BlockSpec(memory_space=pltpu.VMEM)
        x_last, r_last, scal = pl.pallas_call(
            functools.partial(solve_kernel, (ni, nl, nj), counts),
            out_shape=(kept, kept, pltpu.VMEM((CG_ITERS, 1, LANES), F32)),
            in_specs=[any_spec] * 4,
            out_specs=(vmem_spec,) * 3,
            scratch_shapes=[
                block, block, block, vm(nj, width), vm(ni, width), vm(ni, width), vm(-(-width // LANES) * LANES, LANES),
                vm(2, nl, LANES), vm(nl // 2, LANES), vm(2, ni, LANES),
                padded, padded, vm(ni + 1, nl, LANES), whole, whole, vm(ni, nl + 2 * PAD, LANES), whole,
                whole, vm(2, ni, nl, LANES), whole, whole, whole, whole, whole,
                vm(slots, nl // 2, LANES), vm(slots, 2, ni, LANES),
                vm(slots, 2, nl, LANES), vm(slots, nl // 2, LANES), vm(slots, 2, ni, LANES),
                vm(CG_ITERS + 1, 1, LANES), vm(CG_ITERS + 1, devices, 1, LANES),
                dma((slots, 2)), dma((slots,)), dma((slots, 2)), dma((slots, 2)), dma((slots,)), dma((slots, 2)),
                dma((CG_ITERS + 1,)), dma((CG_ITERS + 1,)), dma((6,)), pltpu.SemaphoreType.REGULAR((6,)),
            ],
            compiler_params=pltpu.CompilerParams(has_side_effects=True, collective_id=0, vmem_limit_bytes=28 << 20),
        )(*(pltpu.with_memory_space_constraint(a, pltpu.HBM) for a in (k_ghost, flip(k_cell), flip(f_rhs), flip(u_init))))
        out_block = jax.ShapeDtypeStruct((ni, nl, nj), F32)
        x_new, r_new, hist = pl.pallas_call(
            finish_kernel,
            out_shape=(out_block, out_block, jax.ShapeDtypeStruct((CG_ITERS,), F32)),
            in_specs=[vmem_spec] * 3,
            out_specs=(any_spec,) * 3,
            scratch_shapes=[pltpu.SMEM((CG_ITERS,), F32), dma((3,))],
            compiler_params=pltpu.CompilerParams(vmem_limit_bytes=28 << 20),
        )(scal, x_last, r_last)
        return flip(x_new), flip(r_new), hist

    return jax.shard_map(local_solve, mesh=mesh, in_specs=(grid_spec, P(), grid_spec, grid_spec),
                         out_specs=(grid_spec, grid_spec, P()), check_vma=False)
```

```python
import functools

import jax
import jax.numpy as jnp
from jax import lax
from jax.experimental import pallas as pl
from jax.experimental.pallas import tpu as pltpu
from jax.sharding import PartitionSpec as P

CG_ITERS = 8
LANES = 128
PAD = 8
GROUP = 6
COLUMNS = 16
UPDATE = 4
MESH = pl.DeviceIdType.MESH
F32 = jnp.float32


def solve_kernel(dims, counts, kg_hbm, k_hbm, f_hbm, u_hbm, x_last, r_last, scal_ref,
                 k_in, f_in, u_in, wall_x, wall_y, wall_z, wall_t, bx, by, bz,
                 kp, mp, cx, cy, cyh, cz, inv, x, r, w, s, z, p, n,
                 ys, zs, xr, yr, zr, red_s, red_r,
                 xs_sem, ys_sem, zs_sem, xr_sem, yr_sem, zr_sem, rs_sem, rr_sem, in_sem, near_sem):
    ni, nl, nj = dims
    ngx, ngy, ngz = counts
    half = nl // 2
    gx, gy, gz = lax.axis_index('gx'), lax.axis_index('gy'), lax.axis_index('gz')
    rows = pl.ds(PAD, nl)
    rows_dn = pl.ds(PAD - 1, nl)
    rows_up = pl.ds(PAD + 1, nl)
    lane = lax.broadcasted_iota(jnp.int32, (nl, LANES), 1)
    lane_i = lax.broadcasted_iota(jnp.int32, (ni, LANES), 1)
    lane_half = lax.broadcasted_iota(jnp.int32, (half, LANES), 1)
    lane_row = lax.broadcasted_iota(jnp.int32, (1, LANES), 1)
    inside = lane < nj
    has_xlo, has_xhi = gx > 0, gx < ngx - 1
    has_zlo, has_zhi = gz > 0, gz < ngz - 1
    face_lane = jnp.where(gy == 0, nj - 1, 0)
    y_low_wall, y_high_wall = gy == 0, gy > 0
    zero_slab = jnp.zeros((nl, LANES), F32)
    zero_acc = jnp.zeros((8, LANES), F32)
    others = ngx * ngy * ngz - 1

    def column_roll(slab, shift):
        return pltpu.roll(slab, shift + 2 * LANES, 1)

    def slabs(group, step, init):
        def body(g, carry):
            for k in range(group):
                carry = step(g * group + k, carry)
            return carry
        return lax.fori_loop(0, ni // group, body, init)

    def x_copy(ref, slot, up):
        src = ref.at[ni if up else 1, rows]
        return pltpu.make_async_remote_copy(
            src_ref=src, dst_ref=xr.at[slot, 0 if up else 1], send_sem=xs_sem.at[slot, 0 if up else 1],
            recv_sem=xr_sem.at[slot, 0 if up else 1], device_id=(gz, gy, gx + 1 if up else gx - 1), device_id_type=MESH)

    def z_copy(slot, up):
        return pltpu.make_async_remote_copy(
            src_ref=zs.at[slot, 0 if up else 1], dst_ref=zr.at[slot, 0 if up else 1],
            send_sem=zs_sem.at[slot, 0 if up else 1], recv_sem=zr_sem.at[slot, 0 if up else 1],
            device_id=(gz + 1 if up else gz - 1, gy, gx), device_id_type=MESH)

    def y_copy(slot):
        return pltpu.make_async_remote_copy(
            src_ref=ys.at[slot], dst_ref=yr.at[slot], send_sem=ys_sem.at[slot], recv_sem=yr_sem.at[slot],
            device_id=(gz, 1 - gy, gx), device_id_type=MESH)

    def pack_slab(slot, i, slab):
        zs[slot, 1, pl.ds(i, 1), :] = slab[0:1, :]
        zs[slot, 0, pl.ds(i, 1), :] = slab[nl - 1:nl, :]
        return column_roll(slab[0:half], i - face_lane), column_roll(slab[half:nl], i - face_lane + LANES // 2)

    def pack_rolls(ref, slot, i, behind=False):
        row = lax.max(i, 0) if behind else i
        return pack_slab(slot, row, ref[row + 1, rows, :])

    def pack(i, rolled, acc):
        acc = jnp.where(lane_half == i, rolled[0], acc)
        return jnp.where(lane_half == i + LANES // 2, rolled[1], acc)

    def packed_pass(ref, slot, step, init):
        def body(g, carry):
            state, acc = carry
            rolled = [pack_rolls(ref, slot, (g - 1) * GROUP + k, behind=True) for k in range(GROUP)]
            for k in range(GROUP):
                state = step(g * GROUP + k, state)
            for k in range(GROUP):
                acc = pack((g - 1) * GROUP + k, rolled[k], acc)
            return state, acc
        state, acc = lax.fori_loop(0, ni // GROUP, body, (init, jnp.zeros((half, LANES), F32)))
        rolled = [pack_rolls(ref, slot, ni - GROUP + k) for k in range(GROUP)]
        for k in range(GROUP):
            acc = pack(ni - GROUP + k, rolled[k], acc)
        ys[slot] = acc
        return state

    def scale_and_pack(slot):
        group = min(COLUMNS, ni)

        def body(g, acc):
            rolled = []
            for k in range(group):
                i = g * group + k
                m = inv[i] * w[i]
                mp[i + 1, rows, :] = m
                rolled.append(pack_slab(slot, i, m))
            for k in range(group):
                acc = pack(g * group + k, rolled[k], acc)
            return acc

        ys[slot] = lax.fori_loop(0, ni // group, body, jnp.zeros((half, LANES), F32))

    def exchange_start(ref, slot):
        y_copy(slot).start()
        pl.when(has_zlo)(lambda: z_copy(slot, False).start())
        pl.when(has_zhi)(lambda: z_copy(slot, True).start())
        pl.when(has_xlo)(lambda: x_copy(ref, slot, False).start())
        pl.when(has_xhi)(lambda: x_copy(ref, slot, True).start())

    def exchange_wait(ref, slot):
        @pl.when(has_xlo)
        def _():
            x_copy(ref, slot, False).wait_send()
            x_copy(ref, slot, True).wait_recv()

        @pl.when(has_xhi)
        def _():
            x_copy(ref, slot, True).wait_send()
            x_copy(ref, slot, False).wait_recv()

        @pl.when(has_zlo)
        def _():
            z_copy(slot, False).wait_send()
            z_copy(slot, True).wait_recv()

        @pl.when(has_zhi)
        def _():
            z_copy(slot, True).wait_send()
            z_copy(slot, False).wait_recv()

        y_copy(slot).wait()

    def add_rows(ref, layer, row):
        for i in range(ni):
            ref[i, row:row + 1, :] = ref[i, row:row + 1, :] + layer[i:i + 1, :]

    def add_columns(ref, packed):
        mask = lane == face_lane

        def step(g, _):
            columns = []
            for k in range(min(COLUMNS, ni)):
                i = g * min(COLUMNS, ni) + k
                columns.append((column_roll(packed, face_lane - i), column_roll(packed, face_lane - i - LANES // 2)))
            for k in range(min(COLUMNS, ni)):
                i = g * min(COLUMNS, ni) + k
                ref[i] = ref[i] + jnp.where(mask, jnp.concatenate(columns[k], axis=0), 0.0)
            return 0

        lax.fori_loop(0, ni // min(COLUMNS, ni), step, 0)

    def join_faces(ref, slot):
        y_copy(slot).wait()
        add_columns(n, by[...] * (ys[slot] - yr[slot]))

        @pl.when(has_xlo)
        def _():
            x_copy(ref, slot, False).wait_send()
            x_copy(ref, slot, True).wait_recv()
            n[0] = n[0] + bx[0] * (ref[1, rows, :] - xr[slot, 0])

        @pl.when(has_xhi)
        def _():
            x_copy(ref, slot, True).wait_send()
            x_copy(ref, slot, False).wait_recv()
            n[ni - 1] = n[ni - 1] + bx[1] * (ref[ni, rows, :] - xr[slot, 1])

        @pl.when(has_zlo)
        def _():
            z_copy(slot, False).wait_send()
            z_copy(slot, True).wait_recv()
            add_rows(n, bz[0] * (zs[slot, 1] - zr[slot, 0]), 0)

        @pl.when(has_zhi)
        def _():
            z_copy(slot, True).wait_send()
            z_copy(slot, False).wait_recv()
            add_rows(n, bz[1] * (zs[slot, 0] - zr[slot, 1]), nl - 1)

    def stencil(ref, diagonal=False):
        def step(i, carry):
            v, flux_x = carry
            above = ref[i + 2, rows, :]
            if diagonal:
                inv[i] = cx[i] + cx[i + 1] + cy[i] + cyh[i] + cz[i, rows, :] + cz[i, rows_up, :]
            flux_next = cx[i + 1] * (above - v)
            flux_zl = cz[i, rows, :] * (v - ref[i + 1, rows_dn, :])
            flux_zh = cz[i, rows_up, :] * (ref[i + 1, rows_up, :] - v)
            flux_yl = cy[i] * (v - pltpu.roll(v, 1, 1))
            flux_yh = cyh[i] * (pltpu.roll(v, LANES - 1, 1) - v)
            n[i] = (flux_x - flux_next) + (flux_yl - flux_yh) + (flux_zl - flux_zh)
            return above, flux_next

        first = ref[1, rows, :]
        slabs(GROUP, step, (first, cx[0] * (first - ref[0, rows, :])))

    def fold(slab):
        out = slab[0:8]
        for part in range(8, nl, 8):
            out = out + slab[part:part + 8]
        return out

    def reduce_row(slot, accs):
        row = jnp.zeros((1, LANES), F32)
        for q, acc in enumerate(accs):
            row = jnp.where(lane_row == q, jnp.sum(jnp.sum(acc, axis=0, keepdims=True), axis=1, keepdims=True), row)
        red_s[slot] = row
        red_r[slot, (gz * ngy + gy) * ngx + gx] = row

    def reduce_send(slot, planes):
        me = (gz * ngy + gy) * ngx + gx
        far, next_far = jnp.where(gz < 2, 3, 0), jnp.where(gz < 2, 2, 1)
        order = (far, next_far, 6 - gz - far - next_far, gz)
        for k in planes:
            z_to = order[k]
            for b in reversed(range(ngy)):
                for c in (2, 3, 1, 0):
                    copy = pltpu.make_async_remote_copy(
                        src_ref=red_s.at[slot], dst_ref=red_r.at[slot, me], send_sem=rs_sem.at[slot], recv_sem=rr_sem.at[slot],
                        device_id=(z_to, lax.rem(gy + b, ngy), lax.rem(gx + c, ngx)), device_id_type=MESH)
                    if b or c or k < ngz - 1:
                        copy.start()

    def reduce_wait(slot, count):
        whole = red_r.at[slot, pl.ds(0, others)]
        done = pltpu.make_async_remote_copy(
            src_ref=whole, dst_ref=whole, send_sem=rs_sem.at[slot], recv_sem=rr_sem.at[slot],
            device_id=(gz, gy, gx), device_id_type=MESH)
        done.wait_recv()
        done.wait_send()
        parts = [red_r[slot, device] for device in range(others + 1)]
        while len(parts) > 1:
            parts = [a + b for a, b in zip(parts[0::2], parts[1::2])]
        total = parts[0]
        return [jnp.sum(jnp.where(lane_row == q, total, 0.0), axis=1, keepdims=True) for q in range(count)]

    x_row, z_row = jnp.where(gx == 0, 0, 1), jnp.where(gz == 0, 4, 5)
    slabs_i = pl.ds(pl.multiple_of(gx * ni, 8), ni)
    inputs = [
        pltpu.make_async_copy(k_hbm, k_in, in_sem.at[0]),
        pltpu.make_async_copy(u_hbm, u_in, in_sem.at[1]),
        pltpu.make_async_copy(kg_hbm.at[x_row, pl.ds(pl.multiple_of(gy * nj, 8), nj)], wall_x, in_sem.at[2]),
        pltpu.make_async_copy(kg_hbm.at[2 + gy, slabs_i], wall_y, in_sem.at[3]),
        pltpu.make_async_copy(kg_hbm.at[z_row, slabs_i], wall_z, in_sem.at[4]),
        pltpu.make_async_copy(f_hbm, f_in, in_sem.at[5]),
    ]
    for copy in inputs[:5]:
        copy.start()

    def tell_neighbours(sem):
        tell = lambda *target: pl.semaphore_signal(sem, inc=1, device_id=target, device_id_type=MESH)
        pl.when(has_xlo)(lambda: tell(gz, gy, gx - 1))
        pl.when(has_xhi)(lambda: tell(gz, gy, gx + 1))
        pl.when(has_zlo)(lambda: tell(gz - 1, gy, gx))
        pl.when(has_zhi)(lambda: tell(gz + 1, gy, gx))
        tell(gz, 1 - gy, gx)

    neighbours = 5 - jnp.where(has_xlo, 0, 1) - jnp.where(has_xhi, 0, 1) - jnp.where(has_zlo, 0, 1) - jnp.where(has_zhi, 0, 1)
    rounds = (ngx - 1) + (ngy - 1) + (ngz - 1) - 1

    def next_round(k):
        pl.semaphore_wait(near_sem.at[k], neighbours)
        if k + 1 < rounds:
            tell_neighbours(near_sem.at[k + 1])

    barrier = pltpu.get_barrier_semaphore()
    tell_neighbours(barrier)

    for edge in (0, ni + 1):
        mp[edge] = jnp.zeros((nl + 2 * PAD, LANES), F32)
        kp[edge] = jnp.ones((nl + 2 * PAD, LANES), F32)

    def clear(i, _):
        mp[i + 1, pl.ds(0, PAD), :] = jnp.zeros((PAD, LANES), F32)
        mp[i + 1, pl.ds(PAD + nl, PAD), :] = jnp.zeros((PAD, LANES), F32)
        kp[i + 1, pl.ds(0, PAD), :] = jnp.ones((PAD, LANES), F32)
        kp[i + 1, pl.ds(PAD + nl, PAD), :] = jnp.ones((PAD, LANES), F32)
        mp[i + 1, rows, :] = zero_slab
        s[i] = zero_slab
        z[i] = zero_slab
        p[i] = zero_slab
        r[1, i] = zero_slab
        r[0, i] = zero_slab
        kp[i + 1, rows, :] = jnp.full((nl, LANES), 1.0, F32)
        return 0

    lax.fori_loop(0, ni, clear, 0)

    def load_k(i, _):
        kp[i + 1, rows, 0:nj] = k_in[i]
        return 0

    def load_u(i, _):
        mp[i + 1, rows, 0:nj] = u_in[i]
        return 0

    inputs[0].wait()
    inputs[5].start()
    packed_pass(kp, 0, load_k, 0)
    pl.semaphore_wait(barrier, neighbours)
    tell_neighbours(near_sem.at[0])
    exchange_start(kp, 0)
    inputs[1].wait()
    packed_pass(mp, 1, load_u, 0)
    exchange_start(mp, 1)
    next_round(0)

    for copy in inputs[2:5]:
        copy.wait()
    width = wall_x.shape[1]
    l_rows = pl.ds(pl.multiple_of(gz * nl, 8), nl)

    def flipped(wall, count):
        for start in range(0, width, LANES):
            size = min(LANES, width - start)
            block = jnp.concatenate([wall[:, start:start + size], jnp.ones((LANES - count, size), F32)], axis=0)
            wall_t[start:start + size, :] = block.T
        return wall_t[l_rows, :]

    x_wall = flipped(wall_x, nj)
    y_wall = flipped(wall_y, ni)
    if width > LANES:
        rest = jnp.concatenate([wall_z[:, LANES:width], jnp.ones((ni, 2 * LANES - width), F32)], axis=1)
        whole_z = wall_z[:, 0:LANES]
        turn = LANES - nj
        shifted = jnp.where(lane_i < turn, pltpu.roll(whole_z, turn, 1), pltpu.roll(rest, turn, 1))
    else:
        whole_z = jnp.concatenate([wall_z[...], jnp.ones((ni, LANES - width), F32)], axis=1)
        shifted = pltpu.roll(whole_z, LANES - nj, 1)
    z_wall = jnp.where(gy == 0, whole_z, shifted)

    def harmonic(left, right):
        return 2.0 * left * right / (left + right)

    next_round(1)

    in_i = lane_i < nj
    cx[0] = jnp.where(jnp.logical_and(inside, gx == 0), harmonic(x_wall, kp[1, rows, :]), 0.0)
    z_low = jnp.where(jnp.logical_and(in_i, gz == 0), harmonic(z_wall, zs[0, 1]), 0.0)
    z_high = jnp.where(jnp.logical_and(in_i, gz == ngz - 1), harmonic(zs[0, 0], z_wall), 0.0)
    y_low_mask = jnp.logical_and(inside, jnp.logical_or(lane > 0, y_low_wall))
    y_high_mask = jnp.logical_and(inside, jnp.logical_or(lane < nj - 1, y_high_wall))
    wall_lane = jnp.where(gy == 0, 0, nj)

    def coefs(i, _):
        here = kp[i + 1, rows, :]
        cx[i + 1] = jnp.where(inside, harmonic(here, kp[i + 2, rows, :]), 0.0)
        cz[i, rows_up, :] = jnp.where(inside, harmonic(here, kp[i + 1, rows_up, :]), 0.0)
        wall = column_roll(y_wall, wall_lane - i)
        low = jnp.where(jnp.logical_and(lane == 0, y_low_wall), wall, pltpu.roll(here, 1, 1))
        faces = harmonic(low, jnp.where(jnp.logical_and(lane == nj, y_high_wall), wall, here))
        cy[i] = jnp.where(y_low_mask, faces, 0.0)
        cyh[i] = jnp.where(y_high_mask, pltpu.roll(faces, LANES - 1, 1), 0.0)
        return 0

    slabs(GROUP, coefs, 0)
    next_round(2)
    cx[ni] = jnp.where(jnp.logical_and(inside, gx == ngx - 1), harmonic(kp[ni, rows, :], x_wall), 0.0)
    for i in range(ni):
        cz[i, PAD:PAD + 1, :] = z_low[i:i + 1, :]
        cz[i, PAD + nl:PAD + nl + 1, :] = z_high[i:i + 1, :]

    stencil(mp, diagonal=True)
    next_round(3)

    exchange_wait(kp, 0)

    @pl.when(has_xlo)
    def _():
        bx[0] = jnp.where(inside, harmonic(xr[0, 0], kp[1, rows, :]), 0.0)
        inv[0] = inv[0] + bx[0]

    @pl.when(has_xhi)
    def _():
        bx[1] = jnp.where(inside, harmonic(kp[ni, rows, :], xr[0, 1]), 0.0)
        inv[ni - 1] = inv[ni - 1] + bx[1]

    @pl.when(has_zlo)
    def _():
        bz[0] = jnp.where(in_i, harmonic(zr[0, 0], zs[0, 1]), 0.0)
        add_rows(inv, bz[0], 0)

    @pl.when(has_zhi)
    def _():
        bz[1] = jnp.where(in_i, harmonic(zs[0, 0], zr[0, 1]), 0.0)
        add_rows(inv, bz[1], nl - 1)

    y_face = jnp.where(lax.rem(lane_half, LANES // 2) < ni, harmonic(ys[0], yr[0]), 0.0)
    by[...] = y_face
    add_columns(inv, y_face)
    join_faces(mp, 1)
    inputs[5].wait()

    def first_residual(i, acc):
        iv = jnp.where(inside, 1.0 / jnp.where(inside, inv[i], 1.0), 0.0)
        inv[i] = iv
        x[i] = mp[i + 1, rows, :]
        r[0, i, :, 0:nj] = f_in[i]
        res = r[0, i] - n[i]
        r[0, i] = res
        u = res * iv
        mp[i + 1, rows, :] = u
        return acc + fold(res * u)

    gamma_acc = packed_pass(mp, 2, first_residual, zero_acc)
    exchange_start(mp, 2)
    next_round(4)
    stencil(mp)
    for k in range(5, rounds):
        next_round(k)
    join_faces(mp, 2)

    def first_w(i, acc):
        av = n[i]
        w[i] = av
        return acc + fold(av * mp[i + 1, rows, :])

    reduce_row(0, (gamma_acc, slabs(GROUP, first_w, zero_acc)))

    def scalars(t, sums, gamma_old, pap_old):
        gamma, delta, sigma = sums[0], sums[1], sums[2]
        beta = jnp.where(t == 0, 0.0, gamma / gamma_old)
        pap = delta + 2.0 * beta * sigma + beta * beta * pap_old
        return gamma, pap, beta, gamma / pap

    def wide(value):
        return jnp.broadcast_to(value, (nl, LANES))

    def advance_x(now, alpha, beta):
        alpha, beta = wide(alpha), wide(beta)

        def step(i, acc):
            p_new = inv[i] * r[1 - now, i] + beta * p[i]
            p[i] = p_new
            x[i] = x[i] + alpha * p_new
            return acc + fold(r[now, i] * r[now, i])
        return lax.fori_loop(0, ni, step, zero_acc)

    def iteration(t, carry):
        gamma_old, pap_old, alpha_old, beta_old = carry
        now = lax.rem(t, 2)
        reduce_send(t, range(0, ngz - 1))
        scale_and_pack(t + 3)
        exchange_start(mp, t + 3)
        reduce_send(t, (ngz - 1,))
        stencil(mp)
        rr_acc = advance_x(now, alpha_old, beta_old)
        join_faces(mp, t + 3)
        sums = reduce_wait(t, 4)
        gamma, pap, beta, alpha = scalars(t, sums, gamma_old, pap_old)

        alpha_w, beta_w = wide(alpha), wide(beta)

        def update(i, acc):
            iv = inv[i]
            w_old = w[i]
            z_new = n[i] + beta_w * z[i]
            s_new = w_old + beta_w * s[i]
            r_new = r[now, i] - alpha_w * s_new
            w_new = w_old - alpha_w * z_new
            u_new = iv * r_new
            z[i] = z_new
            s[i] = s_new
            r[1 - now, i] = r_new
            w[i] = w_new
            return acc[0] + fold(r_new * u_new), acc[1] + fold(w_new * u_new), acc[2] + fold(u_new * s_new)

        reduce_row(t + 1, slabs(UPDATE, update, (zero_acc,) * 3) + (rr_acc,))
        scal_ref[lax.rem(t + CG_ITERS - 2, CG_ITERS)] = jnp.broadcast_to(sums[3], (1, LANES))
        return gamma, pap, alpha, beta

    one = jnp.ones((1, 1), F32)
    last = CG_ITERS - 1
    gamma_old, pap_old, alpha_old, beta_old = lax.fori_loop(
        0, last, iteration, (one, one, 0.0 * one, 0.0 * one))

    now = last % 2
    reduce_send(last, range(ngz))

    def last_dots(i, acc):
        rv, sv = r[now, i], s[i]
        wv = w[i]
        pairs = ((rv, rv), (rv, wv), (rv, sv), (wv, wv), (wv, sv), (sv, sv))
        return tuple(a + fold(b * c) for a, (b, c) in zip(acc, pairs))

    reduce_row(CG_ITERS, slabs(3, last_dots, (zero_acc,) * 6))
    reduce_send(CG_ITERS, range(ngz))
    advance_x(now, alpha_old, beta_old)

    sums = reduce_wait(last, 4)
    line = lambda value: jnp.broadcast_to(value, (1, LANES))
    scal_ref[last - 2] = line(sums[3])
    gamma = sums[0]
    beta = gamma / gamma_old
    alpha = gamma / (sums[1] + 2.0 * beta * sums[2] + beta * beta * pap_old)
    alpha_w, beta_w = wide(alpha), wide(beta)

    def final(i, _):
        r_old = r[now, i]
        x_last[i] = (x[i] + alpha_w * (inv[i] * r_old + beta_w * p[i]))[:, 0:nj]
        r_last[i] = (r_old - alpha_w * (w[i] + beta_w * s[i]))[:, 0:nj]
        return 0

    slabs(2, final, 0)
    rr, rw, rs, ww, ws, ss = reduce_wait(CG_ITERS, 6)
    scal_ref[last - 1] = line(rr)
    scal_ref[last] = line(rr - 2.0 * alpha * (rw + beta * rs) + alpha * alpha * (ww + 2.0 * beta * ws + beta * beta * ss))


def finish_kernel(scal, x, r, x_hbm, r_hbm, hist_hbm, hist, sem):
    copies = [pltpu.make_async_copy(x, x_hbm, sem.at[0]), pltpu.make_async_copy(r, r_hbm, sem.at[1]),
              pltpu.make_async_copy(hist, hist_hbm, sem.at[2])]
    copies[0].start()
    copies[1].start()
    for t in range(CG_ITERS):
        hist[t] = scal[t, 0, 0]
    copies[2].start()
    for copy in copies:
        copy.wait()


def solution(mesh):
    counts = (mesh.shape['gx'], mesh.shape['gy'], mesh.shape['gz'])
    grid_spec = P('gx', 'gy', 'gz')

    def local_solve(k_cell, k_ghost, f_rhs, u_init):
        ni, nj, nl = k_cell.shape
        flip = lambda a: jnp.swapaxes(a, 1, 2)
        slots = CG_ITERS + 3
        devices = counts[0] * counts[1] * counts[2]
        width = k_ghost.shape[2]
        any_spec = pl.BlockSpec(memory_space=pl.ANY)
        vm = lambda *shape: pltpu.VMEM(shape, F32)
        whole = vm(ni, nl, LANES)
        block = vm(ni, nl, nj)
        padded = vm(ni + 2, nl + 2 * PAD, LANES)
        dma = pltpu.SemaphoreType.DMA
        kept = pltpu.VMEM((ni, nl, nj), F32)
        vmem_spec = pl.BlockSpec(memory_space=pltpu.VMEM)
        x_last, r_last, scal = pl.pallas_call(
            functools.partial(solve_kernel, (ni, nl, nj), counts),
            out_shape=(kept, kept, pltpu.VMEM((CG_ITERS, 1, LANES), F32)),
            in_specs=[any_spec] * 4,
            out_specs=(vmem_spec,) * 3,
            scratch_shapes=[
                block, block, block, vm(nj, width), vm(ni, width), vm(ni, width), vm(-(-width // LANES) * LANES, LANES),
                vm(2, nl, LANES), vm(nl // 2, LANES), vm(2, ni, LANES),
                padded, padded, vm(ni + 1, nl, LANES), whole, whole, vm(ni, nl + 2 * PAD, LANES), whole,
                whole, vm(2, ni, nl, LANES), whole, whole, whole, whole, whole,
                vm(slots, nl // 2, LANES), vm(slots, 2, ni, LANES),
                vm(slots, 2, nl, LANES), vm(slots, nl // 2, LANES), vm(slots, 2, ni, LANES),
                vm(CG_ITERS + 1, 1, LANES), vm(CG_ITERS + 1, devices, 1, LANES),
                dma((slots, 2)), dma((slots,)), dma((slots, 2)), dma((slots, 2)), dma((slots,)), dma((slots, 2)),
                dma((CG_ITERS + 1,)), dma((CG_ITERS + 1,)), dma((6,)), pltpu.SemaphoreType.REGULAR((6,)),
            ],
            compiler_params=pltpu.CompilerParams(has_side_effects=True, collective_id=0, vmem_limit_bytes=28 << 20),
        )(*(pltpu.with_memory_space_constraint(a, pltpu.HBM) for a in (k_ghost, flip(k_cell), flip(f_rhs), flip(u_init))))
        out_block = jax.ShapeDtypeStruct((ni, nl, nj), F32)
        x_new, r_new, hist = pl.pallas_call(
            finish_kernel,
            out_shape=(out_block, out_block, jax.ShapeDtypeStruct((CG_ITERS,), F32)),
            in_specs=[vmem_spec] * 3,
            out_specs=(any_spec,) * 3,
            scratch_shapes=[pltpu.SMEM((CG_ITERS,), F32), dma((3,))],
            compiler_params=pltpu.CompilerParams(vmem_limit_bytes=28 << 20),
        )(scal, x_last, r_last)
        return flip(x_new), flip(r_new), hist

    return jax.shard_map(local_solve, mesh=mesh, in_specs=(grid_spec, P(), grid_spec, grid_spec),
                         out_specs=(grid_spec, grid_spec, P()), check_vma=False)
```

```python
import functools

import jax
import jax.numpy as jnp
from jax import lax
from jax.experimental import pallas as pl
from jax.experimental.pallas import tpu as pltpu
from jax.sharding import PartitionSpec as P

CG_ITERS = 8
LANES = 128
PAD = 8
GROUP = 6
COLUMNS = 24
UPDATE = 4
MESH = pl.DeviceIdType.MESH
F32 = jnp.float32


def solve_kernel(dims, counts, kg_hbm, k_hbm, f_hbm, u_hbm, x_last, r_last, scal_ref,
                 k_in, f_in, u_in, wall_x, wall_y, wall_z, wall_t, bx, by, bz,
                 kp, mp, cx, cy, cyh, cz, inv, x, r, w, s, z, p, n,
                 ys, zs, xr, yr, zr, red_s, red_r,
                 xs_sem, ys_sem, zs_sem, xr_sem, yr_sem, zr_sem, rs_sem, rr_sem, in_sem, near_sem):
    ni, nl, nj = dims
    ngx, ngy, ngz = counts
    half = nl // 2
    gx, gy, gz = lax.axis_index('gx'), lax.axis_index('gy'), lax.axis_index('gz')
    rows = pl.ds(PAD, nl)
    rows_dn = pl.ds(PAD - 1, nl)
    rows_up = pl.ds(PAD + 1, nl)
    lane = lax.broadcasted_iota(jnp.int32, (nl, LANES), 1)
    lane_i = lax.broadcasted_iota(jnp.int32, (ni, LANES), 1)
    lane_half = lax.broadcasted_iota(jnp.int32, (half, LANES), 1)
    lane_row = lax.broadcasted_iota(jnp.int32, (1, LANES), 1)
    inside = lane < nj
    has_xlo, has_xhi = gx > 0, gx < ngx - 1
    has_zlo, has_zhi = gz > 0, gz < ngz - 1
    face_lane = jnp.where(gy == 0, nj - 1, 0)
    y_low_wall, y_high_wall = gy == 0, gy > 0
    zero_slab = jnp.zeros((nl, LANES), F32)
    zero_acc = jnp.zeros((8, LANES), F32)
    others = ngx * ngy * ngz - 1

    def column_roll(slab, shift):
        return pltpu.roll(slab, shift + 2 * LANES, 1)

    def slabs(group, step, init):
        def body(g, carry):
            for k in range(group):
                carry = step(g * group + k, carry)
            return carry
        return lax.fori_loop(0, ni // group, body, init)

    def x_copy(ref, slot, up):
        src = ref.at[ni if up else 1, rows]
        return pltpu.make_async_remote_copy(
            src_ref=src, dst_ref=xr.at[slot, 0 if up else 1], send_sem=xs_sem.at[slot, 0 if up else 1],
            recv_sem=xr_sem.at[slot, 0 if up else 1], device_id=(gz, gy, gx + 1 if up else gx - 1), device_id_type=MESH)

    def z_copy(slot, up):
        return pltpu.make_async_remote_copy(
            src_ref=zs.at[slot, 0 if up else 1], dst_ref=zr.at[slot, 0 if up else 1],
            send_sem=zs_sem.at[slot, 0 if up else 1], recv_sem=zr_sem.at[slot, 0 if up else 1],
            device_id=(gz + 1 if up else gz - 1, gy, gx), device_id_type=MESH)

    def y_copy(slot):
        return pltpu.make_async_remote_copy(
            src_ref=ys.at[slot], dst_ref=yr.at[slot], send_sem=ys_sem.at[slot], recv_sem=yr_sem.at[slot],
            device_id=(gz, 1 - gy, gx), device_id_type=MESH)

    def pack_slab(slot, i, slab):
        zs[slot, 1, pl.ds(i, 1), :] = slab[0:1, :]
        zs[slot, 0, pl.ds(i, 1), :] = slab[nl - 1:nl, :]
        return column_roll(slab[0:half], i - face_lane), column_roll(slab[half:nl], i - face_lane + LANES // 2)

    def pack_rolls(ref, slot, i, behind=False):
        row = lax.max(i, 0) if behind else i
        return pack_slab(slot, row, ref[row + 1, rows, :])

    def pack(i, rolled, acc):
        acc = jnp.where(lane_half == i, rolled[0], acc)
        return jnp.where(lane_half == i + LANES // 2, rolled[1], acc)

    def packed_pass(ref, slot, step, init):
        def body(g, carry):
            state, acc = carry
            rolled = [pack_rolls(ref, slot, (g - 1) * GROUP + k, behind=True) for k in range(GROUP)]
            for k in range(GROUP):
                state = step(g * GROUP + k, state)
            for k in range(GROUP):
                acc = pack((g - 1) * GROUP + k, rolled[k], acc)
            return state, acc
        state, acc = lax.fori_loop(0, ni // GROUP, body, (init, jnp.zeros((half, LANES), F32)))
        rolled = [pack_rolls(ref, slot, ni - GROUP + k) for k in range(GROUP)]
        for k in range(GROUP):
            acc = pack(ni - GROUP + k, rolled[k], acc)
        ys[slot] = acc
        return state

    def scale_and_pack(slot):
        group = min(COLUMNS, ni)

        def body(g, acc):
            rolled = []
            for k in range(group):
                i = g * group + k
                m = inv[i] * w[i]
                mp[i + 1, rows, :] = m
                rolled.append(pack_slab(slot, i, m))
            for k in range(group):
                acc = pack(g * group + k, rolled[k], acc)
            return acc

        ys[slot] = lax.fori_loop(0, ni // group, body, jnp.zeros((half, LANES), F32))

    def exchange_start(ref, slot):
        y_copy(slot).start()
        pl.when(has_zlo)(lambda: z_copy(slot, False).start())
        pl.when(has_zhi)(lambda: z_copy(slot, True).start())
        pl.when(has_xlo)(lambda: x_copy(ref, slot, False).start())
        pl.when(has_xhi)(lambda: x_copy(ref, slot, True).start())

    def exchange_wait(ref, slot):
        @pl.when(has_xlo)
        def _():
            x_copy(ref, slot, False).wait_send()
            x_copy(ref, slot, True).wait_recv()

        @pl.when(has_xhi)
        def _():
            x_copy(ref, slot, True).wait_send()
            x_copy(ref, slot, False).wait_recv()

        @pl.when(has_zlo)
        def _():
            z_copy(slot, False).wait_send()
            z_copy(slot, True).wait_recv()

        @pl.when(has_zhi)
        def _():
            z_copy(slot, True).wait_send()
            z_copy(slot, False).wait_recv()

        y_copy(slot).wait()

    def add_rows(ref, layer, row):
        for i in range(ni):
            ref[i, row:row + 1, :] = ref[i, row:row + 1, :] + layer[i:i + 1, :]

    def add_columns(ref, packed):
        mask = lane == face_lane

        def step(g, _):
            columns = []
            for k in range(min(COLUMNS, ni)):
                i = g * min(COLUMNS, ni) + k
                columns.append((column_roll(packed, face_lane - i), column_roll(packed, face_lane - i - LANES // 2)))
            for k in range(min(COLUMNS, ni)):
                i = g * min(COLUMNS, ni) + k
                ref[i] = ref[i] + jnp.where(mask, jnp.concatenate(columns[k], axis=0), 0.0)
            return 0

        lax.fori_loop(0, ni // min(COLUMNS, ni), step, 0)

    def join_faces(ref, slot):
        y_copy(slot).wait()
        add_columns(n, by[...] * (ys[slot] - yr[slot]))

        @pl.when(has_xlo)
        def _():
            x_copy(ref, slot, False).wait_send()
            x_copy(ref, slot, True).wait_recv()
            n[0] = n[0] + bx[0] * (ref[1, rows, :] - xr[slot, 0])

        @pl.when(has_xhi)
        def _():
            x_copy(ref, slot, True).wait_send()
            x_copy(ref, slot, False).wait_recv()
            n[ni - 1] = n[ni - 1] + bx[1] * (ref[ni, rows, :] - xr[slot, 1])

        @pl.when(has_zlo)
        def _():
            z_copy(slot, False).wait_send()
            z_copy(slot, True).wait_recv()
            add_rows(n, bz[0] * (zs[slot, 1] - zr[slot, 0]), 0)

        @pl.when(has_zhi)
        def _():
            z_copy(slot, True).wait_send()
            z_copy(slot, False).wait_recv()
            add_rows(n, bz[1] * (zs[slot, 0] - zr[slot, 1]), nl - 1)

    def stencil(ref, diagonal=False):
        def step(i, carry):
            v, flux_x = carry
            above = ref[i + 2, rows, :]
            if diagonal:
                inv[i] = cx[i] + cx[i + 1] + cy[i] + cyh[i] + cz[i, rows, :] + cz[i, rows_up, :]
            flux_next = cx[i + 1] * (above - v)
            flux_zl = cz[i, rows, :] * (v - ref[i + 1, rows_dn, :])
            flux_zh = cz[i, rows_up, :] * (ref[i + 1, rows_up, :] - v)
            flux_yl = cy[i] * (v - pltpu.roll(v, 1, 1))
            flux_yh = cyh[i] * (pltpu.roll(v, LANES - 1, 1) - v)
            n[i] = (flux_x - flux_next) + (flux_yl - flux_yh) + (flux_zl - flux_zh)
            return above, flux_next

        first = ref[1, rows, :]
        slabs(GROUP, step, (first, cx[0] * (first - ref[0, rows, :])))

    def fold(slab):
        out = slab[0:8]
        for part in range(8, nl, 8):
            out = out + slab[part:part + 8]
        return out

    def reduce_row(slot, accs):
        row = jnp.zeros((1, LANES), F32)
        for q, acc in enumerate(accs):
            row = jnp.where(lane_row == q, jnp.sum(jnp.sum(acc, axis=0, keepdims=True), axis=1, keepdims=True), row)
        red_s[slot] = row
        red_r[slot, (gz * ngy + gy) * ngx + gx] = row

    def reduce_send(slot, planes):
        me = (gz * ngy + gy) * ngx + gx
        far, next_far = jnp.where(gz < 2, 3, 0), jnp.where(gz < 2, 2, 1)
        order = (far, next_far, 6 - gz - far - next_far, gz)
        for k in planes:
            z_to = order[k]
            for b in reversed(range(ngy)):
                for c in (2, 3, 1, 0):
                    copy = pltpu.make_async_remote_copy(
                        src_ref=red_s.at[slot], dst_ref=red_r.at[slot, me], send_sem=rs_sem.at[slot], recv_sem=rr_sem.at[slot],
                        device_id=(z_to, lax.rem(gy + b, ngy), lax.rem(gx + c, ngx)), device_id_type=MESH)
                    if b or c or k < ngz - 1:
                        copy.start()

    def reduce_wait(slot, count):
        whole = red_r.at[slot, pl.ds(0, others)]
        done = pltpu.make_async_remote_copy(
            src_ref=whole, dst_ref=whole, send_sem=rs_sem.at[slot], recv_sem=rr_sem.at[slot],
            device_id=(gz, gy, gx), device_id_type=MESH)
        done.wait_recv()
        done.wait_send()
        parts = [red_r[slot, device] for device in range(others + 1)]
        while len(parts) > 1:
            parts = [a + b for a, b in zip(parts[0::2], parts[1::2])]
        total = parts[0]
        return [jnp.sum(jnp.where(lane_row == q, total, 0.0), axis=1, keepdims=True) for q in range(count)]

    x_row, z_row = jnp.where(gx == 0, 0, 1), jnp.where(gz == 0, 4, 5)
    slabs_i = pl.ds(pl.multiple_of(gx * ni, 8), ni)
    inputs = [
        pltpu.make_async_copy(k_hbm, k_in, in_sem.at[0]),
        pltpu.make_async_copy(u_hbm, u_in, in_sem.at[1]),
        pltpu.make_async_copy(kg_hbm.at[x_row, pl.ds(pl.multiple_of(gy * nj, 8), nj)], wall_x, in_sem.at[2]),
        pltpu.make_async_copy(kg_hbm.at[2 + gy, slabs_i], wall_y, in_sem.at[3]),
        pltpu.make_async_copy(kg_hbm.at[z_row, slabs_i], wall_z, in_sem.at[4]),
        pltpu.make_async_copy(f_hbm, f_in, in_sem.at[5]),
    ]
    for copy in inputs[:5]:
        copy.start()

    def tell_neighbours(sem):
        tell = lambda *target: pl.semaphore_signal(sem, inc=1, device_id=target, device_id_type=MESH)
        pl.when(has_xlo)(lambda: tell(gz, gy, gx - 1))
        pl.when(has_xhi)(lambda: tell(gz, gy, gx + 1))
        pl.when(has_zlo)(lambda: tell(gz - 1, gy, gx))
        pl.when(has_zhi)(lambda: tell(gz + 1, gy, gx))
        tell(gz, 1 - gy, gx)

    neighbours = 5 - jnp.where(has_xlo, 0, 1) - jnp.where(has_xhi, 0, 1) - jnp.where(has_zlo, 0, 1) - jnp.where(has_zhi, 0, 1)
    rounds = (ngx - 1) + (ngy - 1) + (ngz - 1) - 1

    def next_round(k):
        pl.semaphore_wait(near_sem.at[k], neighbours)
        if k + 1 < rounds:
            tell_neighbours(near_sem.at[k + 1])

    barrier = pltpu.get_barrier_semaphore()
    tell_neighbours(barrier)

    for edge in (0, ni + 1):
        mp[edge] = jnp.zeros((nl + 2 * PAD, LANES), F32)
        kp[edge] = jnp.ones((nl + 2 * PAD, LANES), F32)

    def clear(i, _):
        mp[i + 1, pl.ds(0, PAD), :] = jnp.zeros((PAD, LANES), F32)
        mp[i + 1, pl.ds(PAD + nl, PAD), :] = jnp.zeros((PAD, LANES), F32)
        kp[i + 1, pl.ds(0, PAD), :] = jnp.ones((PAD, LANES), F32)
        kp[i + 1, pl.ds(PAD + nl, PAD), :] = jnp.ones((PAD, LANES), F32)
        mp[i + 1, rows, :] = zero_slab
        s[i] = zero_slab
        z[i] = zero_slab
        p[i] = zero_slab
        r[1, i] = zero_slab
        r[0, i] = zero_slab
        kp[i + 1, rows, :] = jnp.full((nl, LANES), 1.0, F32)
        return 0

    lax.fori_loop(0, ni, clear, 0)

    def load_k(i, _):
        kp[i + 1, rows, 0:nj] = k_in[i]
        return 0

    def load_u(i, _):
        mp[i + 1, rows, 0:nj] = u_in[i]
        return 0

    inputs[0].wait()
    inputs[5].start()
    packed_pass(kp, 0, load_k, 0)
    pl.semaphore_wait(barrier, neighbours)
    tell_neighbours(near_sem.at[0])
    exchange_start(kp, 0)
    inputs[1].wait()
    packed_pass(mp, 1, load_u, 0)
    exchange_start(mp, 1)
    next_round(0)

    for copy in inputs[2:5]:
        copy.wait()
    width = wall_x.shape[1]
    l_rows = pl.ds(pl.multiple_of(gz * nl, 8), nl)

    def flipped(wall, count):
        for start in range(0, width, LANES):
            size = min(LANES, width - start)
            block = jnp.concatenate([wall[:, start:start + size], jnp.ones((LANES - count, size), F32)], axis=0)
            wall_t[start:start + size, :] = block.T
        return wall_t[l_rows, :]

    x_wall = flipped(wall_x, nj)
    y_wall = flipped(wall_y, ni)
    if width > LANES:
        rest = jnp.concatenate([wall_z[:, LANES:width], jnp.ones((ni, 2 * LANES - width), F32)], axis=1)
        whole_z = wall_z[:, 0:LANES]
        turn = LANES - nj
        shifted = jnp.where(lane_i < turn, pltpu.roll(whole_z, turn, 1), pltpu.roll(rest, turn, 1))
    else:
        whole_z = jnp.concatenate([wall_z[...], jnp.ones((ni, LANES - width), F32)], axis=1)
        shifted = pltpu.roll(whole_z, LANES - nj, 1)
    z_wall = jnp.where(gy == 0, whole_z, shifted)

    def harmonic(left, right):
        return 2.0 * left * right / (left + right)

    next_round(1)

    in_i = lane_i < nj
    cx[0] = jnp.where(jnp.logical_and(inside, gx == 0), harmonic(x_wall, kp[1, rows, :]), 0.0)
    z_low = jnp.where(jnp.logical_and(in_i, gz == 0), harmonic(z_wall, zs[0, 1]), 0.0)
    z_high = jnp.where(jnp.logical_and(in_i, gz == ngz - 1), harmonic(zs[0, 0], z_wall), 0.0)
    y_low_mask = jnp.logical_and(inside, jnp.logical_or(lane > 0, y_low_wall))
    y_high_mask = jnp.logical_and(inside, jnp.logical_or(lane < nj - 1, y_high_wall))
    wall_lane = jnp.where(gy == 0, 0, nj)

    def coefs(i, _):
        here = kp[i + 1, rows, :]
        cx[i + 1] = jnp.where(inside, harmonic(here, kp[i + 2, rows, :]), 0.0)
        cz[i, rows_up, :] = jnp.where(inside, harmonic(here, kp[i + 1, rows_up, :]), 0.0)
        wall = column_roll(y_wall, wall_lane - i)
        low = jnp.where(jnp.logical_and(lane == 0, y_low_wall), wall, pltpu.roll(here, 1, 1))
        faces = harmonic(low, jnp.where(jnp.logical_and(lane == nj, y_high_wall), wall, here))
        cy[i] = jnp.where(y_low_mask, faces, 0.0)
        cyh[i] = jnp.where(y_high_mask, pltpu.roll(faces, LANES - 1, 1), 0.0)
        return 0

    slabs(GROUP, coefs, 0)
    next_round(2)
    cx[ni] = jnp.where(jnp.logical_and(inside, gx == ngx - 1), harmonic(kp[ni, rows, :], x_wall), 0.0)
    for i in range(ni):
        cz[i, PAD:PAD + 1, :] = z_low[i:i + 1, :]
        cz[i, PAD + nl:PAD + nl + 1, :] = z_high[i:i + 1, :]

    stencil(mp, diagonal=True)
    next_round(3)

    exchange_wait(kp, 0)

    @pl.when(has_xlo)
    def _():
        bx[0] = jnp.where(inside, harmonic(xr[0, 0], kp[1, rows, :]), 0.0)
        inv[0] = inv[0] + bx[0]

    @pl.when(has_xhi)
    def _():
        bx[1] = jnp.where(inside, harmonic(kp[ni, rows, :], xr[0, 1]), 0.0)
        inv[ni - 1] = inv[ni - 1] + bx[1]

    @pl.when(has_zlo)
    def _():
        bz[0] = jnp.where(in_i, harmonic(zr[0, 0], zs[0, 1]), 0.0)
        add_rows(inv, bz[0], 0)

    @pl.when(has_zhi)
    def _():
        bz[1] = jnp.where(in_i, harmonic(zs[0, 0], zr[0, 1]), 0.0)
        add_rows(inv, bz[1], nl - 1)

    y_face = jnp.where(lax.rem(lane_half, LANES // 2) < ni, harmonic(ys[0], yr[0]), 0.0)
    by[...] = y_face
    add_columns(inv, y_face)
    join_faces(mp, 1)
    inputs[5].wait()

    def first_residual(i, acc):
        iv = jnp.where(inside, 1.0 / jnp.where(inside, inv[i], 1.0), 0.0)
        inv[i] = iv
        x[i] = mp[i + 1, rows, :]
        r[0, i, :, 0:nj] = f_in[i]
        res = r[0, i] - n[i]
        r[0, i] = res
        u = res * iv
        mp[i + 1, rows, :] = u
        return acc + fold(res * u)

    gamma_acc = packed_pass(mp, 2, first_residual, zero_acc)
    exchange_start(mp, 2)
    next_round(4)
    stencil(mp)
    for k in range(5, rounds):
        next_round(k)
    join_faces(mp, 2)

    def first_w(i, acc):
        av = n[i]
        w[i] = av
        return acc + fold(av * mp[i + 1, rows, :])

    reduce_row(0, (gamma_acc, slabs(GROUP, first_w, zero_acc)))

    def scalars(t, sums, gamma_old, pap_old):
        gamma, delta, sigma = sums[0], sums[1], sums[2]
        beta = jnp.where(t == 0, 0.0, gamma / gamma_old)
        pap = delta + 2.0 * beta * sigma + beta * beta * pap_old
        return gamma, pap, beta, gamma / pap

    def wide(value):
        return jnp.broadcast_to(value, (nl, LANES))

    def advance_x(now, alpha, beta):
        alpha, beta = wide(alpha), wide(beta)

        def step(i, acc):
            p_new = inv[i] * r[1 - now, i] + beta * p[i]
            p[i] = p_new
            x[i] = x[i] + alpha * p_new
            return acc + fold(r[now, i] * r[now, i])
        return lax.fori_loop(0, ni, step, zero_acc)

    def iteration(t, carry):
        gamma_old, pap_old, alpha_old, beta_old = carry
        now = lax.rem(t, 2)
        reduce_send(t, range(0, ngz - 1))
        scale_and_pack(t + 3)
        exchange_start(mp, t + 3)
        reduce_send(t, (ngz - 1,))
        stencil(mp)
        rr_acc = advance_x(now, alpha_old, beta_old)
        join_faces(mp, t + 3)
        sums = reduce_wait(t, 4)
        gamma, pap, beta, alpha = scalars(t, sums, gamma_old, pap_old)

        alpha_w, beta_w = wide(alpha), wide(beta)

        def update(i, acc):
            iv = inv[i]
            w_old = w[i]
            z_new = n[i] + beta_w * z[i]
            s_new = w_old + beta_w * s[i]
            r_new = r[now, i] - alpha_w * s_new
            w_new = w_old - alpha_w * z_new
            u_new = iv * r_new
            z[i] = z_new
            s[i] = s_new
            r[1 - now, i] = r_new
            w[i] = w_new
            return acc[0] + fold(r_new * u_new), acc[1] + fold(w_new * u_new), acc[2] + fold(u_new * s_new)

        reduce_row(t + 1, slabs(UPDATE, update, (zero_acc,) * 3) + (rr_acc,))
        scal_ref[lax.rem(t + CG_ITERS - 2, CG_ITERS)] = jnp.broadcast_to(sums[3], (1, LANES))
        return gamma, pap, alpha, beta

    one = jnp.ones((1, 1), F32)
    last = CG_ITERS - 1
    gamma_old, pap_old, alpha_old, beta_old = lax.fori_loop(
        0, last, iteration, (one, one, 0.0 * one, 0.0 * one))

    now = last % 2
    reduce_send(last, range(ngz))

    def last_dots(i, acc):
        rv, sv = r[now, i], s[i]
        wv = w[i]
        pairs = ((rv, rv), (rv, wv), (rv, sv), (wv, wv), (wv, sv), (sv, sv))
        return tuple(a + fold(b * c) for a, (b, c) in zip(acc, pairs))

    reduce_row(CG_ITERS, slabs(3, last_dots, (zero_acc,) * 6))
    reduce_send(CG_ITERS, range(ngz))
    advance_x(now, alpha_old, beta_old)

    sums = reduce_wait(last, 4)
    line = lambda value: jnp.broadcast_to(value, (1, LANES))
    scal_ref[last - 2] = line(sums[3])
    gamma = sums[0]
    beta = gamma / gamma_old
    alpha = gamma / (sums[1] + 2.0 * beta * sums[2] + beta * beta * pap_old)
    alpha_w, beta_w = wide(alpha), wide(beta)

    def final(i, _):
        r_old = r[now, i]
        x_last[i] = (x[i] + alpha_w * (inv[i] * r_old + beta_w * p[i]))[:, 0:nj]
        r_last[i] = (r_old - alpha_w * (w[i] + beta_w * s[i]))[:, 0:nj]
        return 0

    slabs(2, final, 0)
    rr, rw, rs, ww, ws, ss = reduce_wait(CG_ITERS, 6)
    scal_ref[last - 1] = line(rr)
    scal_ref[last] = line(rr - 2.0 * alpha * (rw + beta * rs) + alpha * alpha * (ww + 2.0 * beta * ws + beta * beta * ss))


def finish_kernel(scal, x, r, x_hbm, r_hbm, hist_hbm, hist, sem):
    copies = [pltpu.make_async_copy(x, x_hbm, sem.at[0]), pltpu.make_async_copy(r, r_hbm, sem.at[1]),
              pltpu.make_async_copy(hist, hist_hbm, sem.at[2])]
    copies[0].start()
    copies[1].start()
    for t in range(CG_ITERS):
        hist[t] = scal[t, 0, 0]
    copies[2].start()
    for copy in copies:
        copy.wait()


def solution(mesh):
    counts = (mesh.shape['gx'], mesh.shape['gy'], mesh.shape['gz'])
    grid_spec = P('gx', 'gy', 'gz')

    def local_solve(k_cell, k_ghost, f_rhs, u_init):
        ni, nj, nl = k_cell.shape
        flip = lambda a: jnp.swapaxes(a, 1, 2)
        slots = CG_ITERS + 3
        devices = counts[0] * counts[1] * counts[2]
        width = k_ghost.shape[2]
        any_spec = pl.BlockSpec(memory_space=pl.ANY)
        vm = lambda *shape: pltpu.VMEM(shape, F32)
        whole = vm(ni, nl, LANES)
        block = vm(ni, nl, nj)
        padded = vm(ni + 2, nl + 2 * PAD, LANES)
        dma = pltpu.SemaphoreType.DMA
        kept = pltpu.VMEM((ni, nl, nj), F32)
        vmem_spec = pl.BlockSpec(memory_space=pltpu.VMEM)
        x_last, r_last, scal = pl.pallas_call(
            functools.partial(solve_kernel, (ni, nl, nj), counts),
            out_shape=(kept, kept, pltpu.VMEM((CG_ITERS, 1, LANES), F32)),
            in_specs=[any_spec] * 4,
            out_specs=(vmem_spec,) * 3,
            scratch_shapes=[
                block, block, block, vm(nj, width), vm(ni, width), vm(ni, width), vm(-(-width // LANES) * LANES, LANES),
                vm(2, nl, LANES), vm(nl // 2, LANES), vm(2, ni, LANES),
                padded, padded, vm(ni + 1, nl, LANES), whole, whole, vm(ni, nl + 2 * PAD, LANES), whole,
                whole, vm(2, ni, nl, LANES), whole, whole, whole, whole, whole,
                vm(slots, nl // 2, LANES), vm(slots, 2, ni, LANES),
                vm(slots, 2, nl, LANES), vm(slots, nl // 2, LANES), vm(slots, 2, ni, LANES),
                vm(CG_ITERS + 1, 1, LANES), vm(CG_ITERS + 1, devices, 1, LANES),
                dma((slots, 2)), dma((slots,)), dma((slots, 2)), dma((slots, 2)), dma((slots,)), dma((slots, 2)),
                dma((CG_ITERS + 1,)), dma((CG_ITERS + 1,)), dma((6,)), pltpu.SemaphoreType.REGULAR((6,)),
            ],
            compiler_params=pltpu.CompilerParams(has_side_effects=True, collective_id=0, vmem_limit_bytes=28 << 20),
        )(*(pltpu.with_memory_space_constraint(a, pltpu.HBM) for a in (k_ghost, flip(k_cell), flip(f_rhs), flip(u_init))))
        out_block = jax.ShapeDtypeStruct((ni, nl, nj), F32)
        x_new, r_new, hist = pl.pallas_call(
            finish_kernel,
            out_shape=(out_block, out_block, jax.ShapeDtypeStruct((CG_ITERS,), F32)),
            in_specs=[vmem_spec] * 3,
            out_specs=(any_spec,) * 3,
            scratch_shapes=[pltpu.SMEM((CG_ITERS,), F32), dma((3,))],
            compiler_params=pltpu.CompilerParams(vmem_limit_bytes=28 << 20),
        )(scal, x_last, r_last)
        return flip(x_new), flip(r_new), hist

    return jax.shard_map(local_solve, mesh=mesh, in_specs=(grid_spec, P(), grid_spec, grid_spec),
                         out_specs=(grid_spec, grid_spec, P()), check_vma=False)
```

```python
import functools

import jax
import jax.numpy as jnp
from jax import lax
from jax.experimental import pallas as pl
from jax.experimental.pallas import tpu as pltpu
from jax.sharding import PartitionSpec as P

CG_ITERS = 8
LANES = 128
PAD = 8
GROUP = 6
COLUMNS = 48
UPDATE = 8
MESH = pl.DeviceIdType.MESH
F32 = jnp.float32


def solve_kernel(dims, counts, kg_hbm, k_hbm, f_hbm, u_hbm, x_last, r_last, scal_ref,
                 k_in, f_in, u_in, wall_x, wall_y, wall_z, wall_t, bx, by, bz,
                 kp, mp, cx, cy, cyh, cz, inv, x, r, w, s, z, p, n,
                 ys, zs, xr, yr, zr, red_s, red_r,
                 xs_sem, ys_sem, zs_sem, xr_sem, yr_sem, zr_sem, rs_sem, rr_sem, in_sem, near_sem):
    ni, nl, nj = dims
    ngx, ngy, ngz = counts
    half = nl // 2
    gx, gy, gz = lax.axis_index('gx'), lax.axis_index('gy'), lax.axis_index('gz')
    rows = pl.ds(PAD, nl)
    rows_dn = pl.ds(PAD - 1, nl)
    rows_up = pl.ds(PAD + 1, nl)
    lane = lax.broadcasted_iota(jnp.int32, (nl, LANES), 1)
    lane_i = lax.broadcasted_iota(jnp.int32, (ni, LANES), 1)
    lane_half = lax.broadcasted_iota(jnp.int32, (half, LANES), 1)
    lane_row = lax.broadcasted_iota(jnp.int32, (1, LANES), 1)
    inside = lane < nj
    has_xlo, has_xhi = gx > 0, gx < ngx - 1
    has_zlo, has_zhi = gz > 0, gz < ngz - 1
    face_lane = jnp.where(gy == 0, nj - 1, 0)
    y_low_wall, y_high_wall = gy == 0, gy > 0
    zero_slab = jnp.zeros((nl, LANES), F32)
    zero_acc = jnp.zeros((8, LANES), F32)
    others = ngx * ngy * ngz - 1

    def column_roll(slab, shift):
        return pltpu.roll(slab, shift + 2 * LANES, 1)

    def slabs(group, step, init):
        def body(g, carry):
            for k in range(group):
                carry = step(g * group + k, carry)
            return carry
        return lax.fori_loop(0, ni // group, body, init)

    def x_copy(ref, slot, up):
        src = ref.at[ni if up else 1, rows]
        return pltpu.make_async_remote_copy(
            src_ref=src, dst_ref=xr.at[slot, 0 if up else 1], send_sem=xs_sem.at[slot, 0 if up else 1],
            recv_sem=xr_sem.at[slot, 0 if up else 1], device_id=(gz, gy, gx + 1 if up else gx - 1), device_id_type=MESH)

    def z_copy(slot, up):
        return pltpu.make_async_remote_copy(
            src_ref=zs.at[slot, 0 if up else 1], dst_ref=zr.at[slot, 0 if up else 1],
            send_sem=zs_sem.at[slot, 0 if up else 1], recv_sem=zr_sem.at[slot, 0 if up else 1],
            device_id=(gz + 1 if up else gz - 1, gy, gx), device_id_type=MESH)

    def y_copy(slot):
        return pltpu.make_async_remote_copy(
            src_ref=ys.at[slot], dst_ref=yr.at[slot], send_sem=ys_sem.at[slot], recv_sem=yr_sem.at[slot],
            device_id=(gz, 1 - gy, gx), device_id_type=MESH)

    def pack_slab(slot, i, slab):
        zs[slot, 1, pl.ds(i, 1), :] = slab[0:1, :]
        zs[slot, 0, pl.ds(i, 1), :] = slab[nl - 1:nl, :]
        return column_roll(slab[0:half], i - face_lane), column_roll(slab[half:nl], i - face_lane + LANES // 2)

    def pack_rolls(ref, slot, i, behind=False):
        row = lax.max(i, 0) if behind else i
        return pack_slab(slot, row, ref[row + 1, rows, :])

    def pack(i, rolled, acc):
        acc = jnp.where(lane_half == i, rolled[0], acc)
        return jnp.where(lane_half == i + LANES // 2, rolled[1], acc)

    def packed_pass(ref, slot, step, init):
        def body(g, carry):
            state, acc = carry
            rolled = [pack_rolls(ref, slot, (g - 1) * GROUP + k, behind=True) for k in range(GROUP)]
            for k in range(GROUP):
                state = step(g * GROUP + k, state)
            for k in range(GROUP):
                acc = pack((g - 1) * GROUP + k, rolled[k], acc)
            return state, acc
        state, acc = lax.fori_loop(0, ni // GROUP, body, (init, jnp.zeros((half, LANES), F32)))
        rolled = [pack_rolls(ref, slot, ni - GROUP + k) for k in range(GROUP)]
        for k in range(GROUP):
            acc = pack(ni - GROUP + k, rolled[k], acc)
        ys[slot] = acc
        return state

    def scale_and_pack(slot):
        group = min(COLUMNS, ni)

        def body(g, acc):
            rolled = []
            for k in range(group):
                i = g * group + k
                m = inv[i] * w[i]
                mp[i + 1, rows, :] = m
                rolled.append(pack_slab(slot, i, m))
            for k in range(group):
                acc = pack(g * group + k, rolled[k], acc)
            return acc

        ys[slot] = lax.fori_loop(0, ni // group, body, jnp.zeros((half, LANES), F32))

    def exchange_start(ref, slot):
        y_copy(slot).start()
        pl.when(has_zlo)(lambda: z_copy(slot, False).start())
        pl.when(has_zhi)(lambda: z_copy(slot, True).start())
        pl.when(has_xlo)(lambda: x_copy(ref, slot, False).start())
        pl.when(has_xhi)(lambda: x_copy(ref, slot, True).start())

    def exchange_wait(ref, slot):
        @pl.when(has_xlo)
        def _():
            x_copy(ref, slot, False).wait_send()
            x_copy(ref, slot, True).wait_recv()

        @pl.when(has_xhi)
        def _():
            x_copy(ref, slot, True).wait_send()
            x_copy(ref, slot, False).wait_recv()

        @pl.when(has_zlo)
        def _():
            z_copy(slot, False).wait_send()
            z_copy(slot, True).wait_recv()

        @pl.when(has_zhi)
        def _():
            z_copy(slot, True).wait_send()
            z_copy(slot, False).wait_recv()

        y_copy(slot).wait()

    def add_rows(ref, layer, row):
        for i in range(ni):
            ref[i, row:row + 1, :] = ref[i, row:row + 1, :] + layer[i:i + 1, :]

    def add_columns(ref, packed):
        mask = lane == face_lane

        def step(g, _):
            columns = []
            for k in range(min(COLUMNS, ni)):
                i = g * min(COLUMNS, ni) + k
                columns.append((column_roll(packed, face_lane - i), column_roll(packed, face_lane - i - LANES // 2)))
            for k in range(min(COLUMNS, ni)):
                i = g * min(COLUMNS, ni) + k
                ref[i] = ref[i] + jnp.where(mask, jnp.concatenate(columns[k], axis=0), 0.0)
            return 0

        lax.fori_loop(0, ni // min(COLUMNS, ni), step, 0)

    def join_faces(ref, slot):
        y_copy(slot).wait()
        add_columns(n, by[...] * (ys[slot] - yr[slot]))

        @pl.when(has_xlo)
        def _():
            x_copy(ref, slot, False).wait_send()
            x_copy(ref, slot, True).wait_recv()
            n[0] = n[0] + bx[0] * (ref[1, rows, :] - xr[slot, 0])

        @pl.when(has_xhi)
        def _():
            x_copy(ref, slot, True).wait_send()
            x_copy(ref, slot, False).wait_recv()
            n[ni - 1] = n[ni - 1] + bx[1] * (ref[ni, rows, :] - xr[slot, 1])

        @pl.when(has_zlo)
        def _():
            z_copy(slot, False).wait_send()
            z_copy(slot, True).wait_recv()
            add_rows(n, bz[0] * (zs[slot, 1] - zr[slot, 0]), 0)

        @pl.when(has_zhi)
        def _():
            z_copy(slot, True).wait_send()
            z_copy(slot, False).wait_recv()
            add_rows(n, bz[1] * (zs[slot, 0] - zr[slot, 1]), nl - 1)

    def stencil(ref, diagonal=False):
        def step(i, carry):
            v, flux_x = carry
            above = ref[i + 2, rows, :]
            if diagonal:
                inv[i] = cx[i] + cx[i + 1] + cy[i] + cyh[i] + cz[i, rows, :] + cz[i, rows_up, :]
            flux_next = cx[i + 1] * (above - v)
            flux_zl = cz[i, rows, :] * (v - ref[i + 1, rows_dn, :])
            flux_zh = cz[i, rows_up, :] * (ref[i + 1, rows_up, :] - v)
            flux_yl = cy[i] * (v - pltpu.roll(v, 1, 1))
            flux_yh = cyh[i] * (pltpu.roll(v, LANES - 1, 1) - v)
            n[i] = (flux_x - flux_next) + (flux_yl - flux_yh) + (flux_zl - flux_zh)
            return above, flux_next

        first = ref[1, rows, :]
        slabs(GROUP, step, (first, cx[0] * (first - ref[0, rows, :])))

    def fold(slab):
        out = slab[0:8]
        for part in range(8, nl, 8):
            out = out + slab[part:part + 8]
        return out

    def reduce_row(slot, accs):
        row = jnp.zeros((1, LANES), F32)
        for q, acc in enumerate(accs):
            row = jnp.where(lane_row == q, jnp.sum(jnp.sum(acc, axis=0, keepdims=True), axis=1, keepdims=True), row)
        red_s[slot] = row
        red_r[slot, (gz * ngy + gy) * ngx + gx] = row

    def reduce_send(slot, planes):
        me = (gz * ngy + gy) * ngx + gx
        far, next_far = jnp.where(gz < 2, 3, 0), jnp.where(gz < 2, 2, 1)
        order = (far, next_far, 6 - gz - far - next_far, gz)
        for k in planes:
            z_to = order[k]
            for b in reversed(range(ngy)):
                for c in (2, 3, 1, 0):
                    copy = pltpu.make_async_remote_copy(
                        src_ref=red_s.at[slot], dst_ref=red_r.at[slot, me], send_sem=rs_sem.at[slot], recv_sem=rr_sem.at[slot],
                        device_id=(z_to, lax.rem(gy + b, ngy), lax.rem(gx + c, ngx)), device_id_type=MESH)
                    if b or c or k < ngz - 1:
                        copy.start()

    def reduce_wait(slot, count):
        whole = red_r.at[slot, pl.ds(0, others)]
        done = pltpu.make_async_remote_copy(
            src_ref=whole, dst_ref=whole, send_sem=rs_sem.at[slot], recv_sem=rr_sem.at[slot],
            device_id=(gz, gy, gx), device_id_type=MESH)
        done.wait_recv()
        done.wait_send()
        parts = [red_r[slot, device] for device in range(others + 1)]
        while len(parts) > 1:
            parts = [a + b for a, b in zip(parts[0::2], parts[1::2])]
        total = parts[0]
        return [jnp.sum(jnp.where(lane_row == q, total, 0.0), axis=1, keepdims=True) for q in range(count)]

    x_row, z_row = jnp.where(gx == 0, 0, 1), jnp.where(gz == 0, 4, 5)
    slabs_i = pl.ds(pl.multiple_of(gx * ni, 8), ni)
    inputs = [
        pltpu.make_async_copy(k_hbm, k_in, in_sem.at[0]),
        pltpu.make_async_copy(u_hbm, u_in, in_sem.at[1]),
        pltpu.make_async_copy(kg_hbm.at[x_row, pl.ds(pl.multiple_of(gy * nj, 8), nj)], wall_x, in_sem.at[2]),
        pltpu.make_async_copy(kg_hbm.at[2 + gy, slabs_i], wall_y, in_sem.at[3]),
        pltpu.make_async_copy(kg_hbm.at[z_row, slabs_i], wall_z, in_sem.at[4]),
        pltpu.make_async_copy(f_hbm, f_in, in_sem.at[5]),
    ]
    for copy in inputs[:5]:
        copy.start()

    def tell_neighbours(sem):
        tell = lambda *target: pl.semaphore_signal(sem, inc=1, device_id=target, device_id_type=MESH)
        pl.when(has_xlo)(lambda: tell(gz, gy, gx - 1))
        pl.when(has_xhi)(lambda: tell(gz, gy, gx + 1))
        pl.when(has_zlo)(lambda: tell(gz - 1, gy, gx))
        pl.when(has_zhi)(lambda: tell(gz + 1, gy, gx))
        tell(gz, 1 - gy, gx)

    neighbours = 5 - jnp.where(has_xlo, 0, 1) - jnp.where(has_xhi, 0, 1) - jnp.where(has_zlo, 0, 1) - jnp.where(has_zhi, 0, 1)
    rounds = (ngx - 1) + (ngy - 1) + (ngz - 1) - 1

    def next_round(k):
        pl.semaphore_wait(near_sem.at[k], neighbours)
        if k + 1 < rounds:
            tell_neighbours(near_sem.at[k + 1])

    barrier = pltpu.get_barrier_semaphore()
    tell_neighbours(barrier)

    for edge in (0, ni + 1):
        mp[edge] = jnp.zeros((nl + 2 * PAD, LANES), F32)
        kp[edge] = jnp.ones((nl + 2 * PAD, LANES), F32)

    def clear(i, _):
        mp[i + 1, pl.ds(0, PAD), :] = jnp.zeros((PAD, LANES), F32)
        mp[i + 1, pl.ds(PAD + nl, PAD), :] = jnp.zeros((PAD, LANES), F32)
        kp[i + 1, pl.ds(0, PAD), :] = jnp.ones((PAD, LANES), F32)
        kp[i + 1, pl.ds(PAD + nl, PAD), :] = jnp.ones((PAD, LANES), F32)
        mp[i + 1, rows, :] = zero_slab
        s[i] = zero_slab
        z[i] = zero_slab
        p[i] = zero_slab
        r[1, i] = zero_slab
        r[0, i] = zero_slab
        kp[i + 1, rows, :] = jnp.full((nl, LANES), 1.0, F32)
        return 0

    lax.fori_loop(0, ni, clear, 0)

    def load_k(i, _):
        kp[i + 1, rows, 0:nj] = k_in[i]
        return 0

    def load_u(i, _):
        mp[i + 1, rows, 0:nj] = u_in[i]
        return 0

    inputs[0].wait()
    inputs[5].start()
    packed_pass(kp, 0, load_k, 0)
    pl.semaphore_wait(barrier, neighbours)
    tell_neighbours(near_sem.at[0])
    exchange_start(kp, 0)
    inputs[1].wait()
    packed_pass(mp, 1, load_u, 0)
    exchange_start(mp, 1)
    next_round(0)

    for copy in inputs[2:5]:
        copy.wait()
    width = wall_x.shape[1]
    l_rows = pl.ds(pl.multiple_of(gz * nl, 8), nl)

    def flipped(wall, count):
        for start in range(0, width, LANES):
            size = min(LANES, width - start)
            block = jnp.concatenate([wall[:, start:start + size], jnp.ones((LANES - count, size), F32)], axis=0)
            wall_t[start:start + size, :] = block.T
        return wall_t[l_rows, :]

    x_wall = flipped(wall_x, nj)
    y_wall = flipped(wall_y, ni)
    if width > LANES:
        rest = jnp.concatenate([wall_z[:, LANES:width], jnp.ones((ni, 2 * LANES - width), F32)], axis=1)
        whole_z = wall_z[:, 0:LANES]
        turn = LANES - nj
        shifted = jnp.where(lane_i < turn, pltpu.roll(whole_z, turn, 1), pltpu.roll(rest, turn, 1))
    else:
        whole_z = jnp.concatenate([wall_z[...], jnp.ones((ni, LANES - width), F32)], axis=1)
        shifted = pltpu.roll(whole_z, LANES - nj, 1)
    z_wall = jnp.where(gy == 0, whole_z, shifted)

    def harmonic(left, right):
        return 2.0 * left * right / (left + right)

    next_round(1)

    in_i = lane_i < nj
    cx[0] = jnp.where(jnp.logical_and(inside, gx == 0), harmonic(x_wall, kp[1, rows, :]), 0.0)
    z_low = jnp.where(jnp.logical_and(in_i, gz == 0), harmonic(z_wall, zs[0, 1]), 0.0)
    z_high = jnp.where(jnp.logical_and(in_i, gz == ngz - 1), harmonic(zs[0, 0], z_wall), 0.0)
    y_low_mask = jnp.logical_and(inside, jnp.logical_or(lane > 0, y_low_wall))
    y_high_mask = jnp.logical_and(inside, jnp.logical_or(lane < nj - 1, y_high_wall))
    wall_lane = jnp.where(gy == 0, 0, nj)

    def coefs(i, _):
        here = kp[i + 1, rows, :]
        cx[i + 1] = jnp.where(inside, harmonic(here, kp[i + 2, rows, :]), 0.0)
        cz[i, rows_up, :] = jnp.where(inside, harmonic(here, kp[i + 1, rows_up, :]), 0.0)
        wall = column_roll(y_wall, wall_lane - i)
        low = jnp.where(jnp.logical_and(lane == 0, y_low_wall), wall, pltpu.roll(here, 1, 1))
        faces = harmonic(low, jnp.where(jnp.logical_and(lane == nj, y_high_wall), wall, here))
        cy[i] = jnp.where(y_low_mask, faces, 0.0)
        cyh[i] = jnp.where(y_high_mask, pltpu.roll(faces, LANES - 1, 1), 0.0)
        return 0

    slabs(GROUP, coefs, 0)
    next_round(2)
    cx[ni] = jnp.where(jnp.logical_and(inside, gx == ngx - 1), harmonic(kp[ni, rows, :], x_wall), 0.0)
    for i in range(ni):
        cz[i, PAD:PAD + 1, :] = z_low[i:i + 1, :]
        cz[i, PAD + nl:PAD + nl + 1, :] = z_high[i:i + 1, :]

    stencil(mp, diagonal=True)
    next_round(3)

    exchange_wait(kp, 0)

    @pl.when(has_xlo)
    def _():
        bx[0] = jnp.where(inside, harmonic(xr[0, 0], kp[1, rows, :]), 0.0)
        inv[0] = inv[0] + bx[0]

    @pl.when(has_xhi)
    def _():
        bx[1] = jnp.where(inside, harmonic(kp[ni, rows, :], xr[0, 1]), 0.0)
        inv[ni - 1] = inv[ni - 1] + bx[1]

    @pl.when(has_zlo)
    def _():
        bz[0] = jnp.where(in_i, harmonic(zr[0, 0], zs[0, 1]), 0.0)
        add_rows(inv, bz[0], 0)

    @pl.when(has_zhi)
    def _():
        bz[1] = jnp.where(in_i, harmonic(zs[0, 0], zr[0, 1]), 0.0)
        add_rows(inv, bz[1], nl - 1)

    y_face = jnp.where(lax.rem(lane_half, LANES // 2) < ni, harmonic(ys[0], yr[0]), 0.0)
    by[...] = y_face
    add_columns(inv, y_face)
    join_faces(mp, 1)
    inputs[5].wait()

    def first_residual(i, acc):
        iv = jnp.where(inside, 1.0 / jnp.where(inside, inv[i], 1.0), 0.0)
        inv[i] = iv
        x[i] = mp[i + 1, rows, :]
        r[0, i, :, 0:nj] = f_in[i]
        res = r[0, i] - n[i]
        r[0, i] = res
        u = res * iv
        mp[i + 1, rows, :] = u
        return acc + fold(res * u)

    gamma_acc = packed_pass(mp, 2, first_residual, zero_acc)
    exchange_start(mp, 2)
    next_round(4)
    stencil(mp)
    for k in range(5, rounds):
        next_round(k)
    join_faces(mp, 2)

    def first_w(i, acc):
        av = n[i]
        w[i] = av
        return acc + fold(av * mp[i + 1, rows, :])

    reduce_row(0, (gamma_acc, slabs(GROUP, first_w, zero_acc)))

    def scalars(t, sums, gamma_old, pap_old):
        gamma, delta, sigma = sums[0], sums[1], sums[2]
        beta = jnp.where(t == 0, 0.0, gamma / gamma_old)
        pap = delta + 2.0 * beta * sigma + beta * beta * pap_old
        return gamma, pap, beta, gamma / pap

    def wide(value):
        return jnp.broadcast_to(value, (nl, LANES))

    def advance_x(now, alpha, beta):
        alpha, beta = wide(alpha), wide(beta)

        def step(i, acc):
            p_new = inv[i] * r[1 - now, i] + beta * p[i]
            p[i] = p_new
            x[i] = x[i] + alpha * p_new
            return acc + fold(r[now, i] * r[now, i])
        return lax.fori_loop(0, ni, step, zero_acc)

    def iteration(t, carry):
        gamma_old, pap_old, alpha_old, beta_old = carry
        now = lax.rem(t, 2)
        reduce_send(t, range(0, ngz - 1))
        scale_and_pack(t + 3)
        exchange_start(mp, t + 3)
        reduce_send(t, (ngz - 1,))
        stencil(mp)
        rr_acc = advance_x(now, alpha_old, beta_old)
        join_faces(mp, t + 3)
        sums = reduce_wait(t, 4)
        gamma, pap, beta, alpha = scalars(t, sums, gamma_old, pap_old)

        alpha_w, beta_w = wide(alpha), wide(beta)

        def update(i, acc):
            iv = inv[i]
            w_old = w[i]
            z_new = n[i] + beta_w * z[i]
            s_new = w_old + beta_w * s[i]
            r_new = r[now, i] - alpha_w * s_new
            w_new = w_old - alpha_w * z_new
            u_new = iv * r_new
            z[i] = z_new
            s[i] = s_new
            r[1 - now, i] = r_new
            w[i] = w_new
            return acc[0] + fold(r_new * u_new), acc[1] + fold(w_new * u_new), acc[2] + fold(u_new * s_new)

        reduce_row(t + 1, slabs(UPDATE, update, (zero_acc,) * 3) + (rr_acc,))
        scal_ref[lax.rem(t + CG_ITERS - 2, CG_ITERS)] = jnp.broadcast_to(sums[3], (1, LANES))
        return gamma, pap, alpha, beta

    one = jnp.ones((1, 1), F32)
    last = CG_ITERS - 1
    gamma_old, pap_old, alpha_old, beta_old = lax.fori_loop(
        0, last, iteration, (one, one, 0.0 * one, 0.0 * one))

    now = last % 2
    reduce_send(last, range(ngz))

    def last_dots(i, acc):
        rv, sv = r[now, i], s[i]
        wv = w[i]
        pairs = ((rv, rv), (rv, wv), (rv, sv), (wv, wv), (wv, sv), (sv, sv))
        return tuple(a + fold(b * c) for a, (b, c) in zip(acc, pairs))

    reduce_row(CG_ITERS, slabs(3, last_dots, (zero_acc,) * 6))
    reduce_send(CG_ITERS, range(ngz))
    advance_x(now, alpha_old, beta_old)

    sums = reduce_wait(last, 4)
    line = lambda value: jnp.broadcast_to(value, (1, LANES))
    scal_ref[last - 2] = line(sums[3])
    gamma = sums[0]
    beta = gamma / gamma_old
    alpha = gamma / (sums[1] + 2.0 * beta * sums[2] + beta * beta * pap_old)
    alpha_w, beta_w = wide(alpha), wide(beta)

    def final(i, _):
        r_old = r[now, i]
        x_last[i] = (x[i] + alpha_w * (inv[i] * r_old + beta_w * p[i]))[:, 0:nj]
        r_last[i] = (r_old - alpha_w * (w[i] + beta_w * s[i]))[:, 0:nj]
        return 0

    slabs(2, final, 0)
    rr, rw, rs, ww, ws, ss = reduce_wait(CG_ITERS, 6)
    scal_ref[last - 1] = line(rr)
    scal_ref[last] = line(rr - 2.0 * alpha * (rw + beta * rs) + alpha * alpha * (ww + 2.0 * beta * ws + beta * beta * ss))


def finish_kernel(scal, x, r, x_hbm, r_hbm, hist_hbm, hist, sem):
    copies = [pltpu.make_async_copy(x, x_hbm, sem.at[0]), pltpu.make_async_copy(r, r_hbm, sem.at[1]),
              pltpu.make_async_copy(hist, hist_hbm, sem.at[2])]
    copies[0].start()
    copies[1].start()
    for t in range(CG_ITERS):
        hist[t] = scal[t, 0, 0]
    copies[2].start()
    for copy in copies:
        copy.wait()


def solution(mesh):
    counts = (mesh.shape['gx'], mesh.shape['gy'], mesh.shape['gz'])
    grid_spec = P('gx', 'gy', 'gz')

    def local_solve(k_cell, k_ghost, f_rhs, u_init):
        ni, nj, nl = k_cell.shape
        flip = lambda a: jnp.swapaxes(a, 1, 2)
        slots = CG_ITERS + 3
        devices = counts[0] * counts[1] * counts[2]
        width = k_ghost.shape[2]
        any_spec = pl.BlockSpec(memory_space=pl.ANY)
        vm = lambda *shape: pltpu.VMEM(shape, F32)
        whole = vm(ni, nl, LANES)
        block = vm(ni, nl, nj)
        padded = vm(ni + 2, nl + 2 * PAD, LANES)
        dma = pltpu.SemaphoreType.DMA
        kept = pltpu.VMEM((ni, nl, nj), F32)
        vmem_spec = pl.BlockSpec(memory_space=pltpu.VMEM)
        x_last, r_last, scal = pl.pallas_call(
            functools.partial(solve_kernel, (ni, nl, nj), counts),
            out_shape=(kept, kept, pltpu.VMEM((CG_ITERS, 1, LANES), F32)),
            in_specs=[any_spec] * 4,
            out_specs=(vmem_spec,) * 3,
            scratch_shapes=[
                block, block, block, vm(nj, width), vm(ni, width), vm(ni, width), vm(-(-width // LANES) * LANES, LANES),
                vm(2, nl, LANES), vm(nl // 2, LANES), vm(2, ni, LANES),
                padded, padded, vm(ni + 1, nl, LANES), whole, whole, vm(ni, nl + 2 * PAD, LANES), whole,
                whole, vm(2, ni, nl, LANES), whole, whole, whole, whole, whole,
                vm(slots, nl // 2, LANES), vm(slots, 2, ni, LANES),
                vm(slots, 2, nl, LANES), vm(slots, nl // 2, LANES), vm(slots, 2, ni, LANES),
                vm(CG_ITERS + 1, 1, LANES), vm(CG_ITERS + 1, devices, 1, LANES),
                dma((slots, 2)), dma((slots,)), dma((slots, 2)), dma((slots, 2)), dma((slots,)), dma((slots, 2)),
                dma((CG_ITERS + 1,)), dma((CG_ITERS + 1,)), dma((6,)), pltpu.SemaphoreType.REGULAR((6,)),
            ],
            compiler_params=pltpu.CompilerParams(has_side_effects=True, collective_id=0, vmem_limit_bytes=28 << 20),
        )(*(pltpu.with_memory_space_constraint(a, pltpu.HBM) for a in (k_ghost, flip(k_cell), flip(f_rhs), flip(u_init))))
        out_block = jax.ShapeDtypeStruct((ni, nl, nj), F32)
        x_new, r_new, hist = pl.pallas_call(
            finish_kernel,
            out_shape=(out_block, out_block, jax.ShapeDtypeStruct((CG_ITERS,), F32)),
            in_specs=[vmem_spec] * 3,
            out_specs=(any_spec,) * 3,
            scratch_shapes=[pltpu.SMEM((CG_ITERS,), F32), dma((3,))],
            compiler_params=pltpu.CompilerParams(vmem_limit_bytes=28 << 20),
        )(scal, x_last, r_last)
        return flip(x_new), flip(r_new), hist

    return jax.shard_map(local_solve, mesh=mesh, in_specs=(grid_spec, P(), grid_spec, grid_spec),
                         out_specs=(grid_spec, grid_spec, P()), check_vma=False)
```

```python
import functools

import jax
import jax.numpy as jnp
from jax import lax
from jax.experimental import pallas as pl
from jax.experimental.pallas import tpu as pltpu
from jax.sharding import PartitionSpec as P

CG_ITERS = 8
LANES = 128
PAD = 8
GROUP = 12
COLUMNS = 48
UPDATE = 8
MESH = pl.DeviceIdType.MESH
F32 = jnp.float32


def solve_kernel(dims, counts, kg_hbm, k_hbm, f_hbm, u_hbm, x_last, r_last, scal_ref,
                 k_in, f_in, u_in, wall_x, wall_y, wall_z, wall_t, bx, by, bz,
                 kp, mp, cx, cy, cyh, cz, inv, x, r, w, s, z, p, n,
                 ys, zs, xr, yr, zr, red_s, red_r,
                 xs_sem, ys_sem, zs_sem, xr_sem, yr_sem, zr_sem, rs_sem, rr_sem, in_sem, near_sem):
    ni, nl, nj = dims
    ngx, ngy, ngz = counts
    half = nl // 2
    gx, gy, gz = lax.axis_index('gx'), lax.axis_index('gy'), lax.axis_index('gz')
    rows = pl.ds(PAD, nl)
    rows_dn = pl.ds(PAD - 1, nl)
    rows_up = pl.ds(PAD + 1, nl)
    lane = lax.broadcasted_iota(jnp.int32, (nl, LANES), 1)
    lane_i = lax.broadcasted_iota(jnp.int32, (ni, LANES), 1)
    lane_half = lax.broadcasted_iota(jnp.int32, (half, LANES), 1)
    lane_row = lax.broadcasted_iota(jnp.int32, (1, LANES), 1)
    inside = lane < nj
    has_xlo, has_xhi = gx > 0, gx < ngx - 1
    has_zlo, has_zhi = gz > 0, gz < ngz - 1
    face_lane = jnp.where(gy == 0, nj - 1, 0)
    y_low_wall, y_high_wall = gy == 0, gy > 0
    zero_slab = jnp.zeros((nl, LANES), F32)
    zero_acc = jnp.zeros((8, LANES), F32)
    others = ngx * ngy * ngz - 1

    def column_roll(slab, shift):
        return pltpu.roll(slab, shift + 2 * LANES, 1)

    def slabs(group, step, init):
        def body(g, carry):
            for k in range(group):
                carry = step(g * group + k, carry)
            return carry
        return lax.fori_loop(0, ni // group, body, init)

    def x_copy(ref, slot, up):
        src = ref.at[ni if up else 1, rows]
        return pltpu.make_async_remote_copy(
            src_ref=src, dst_ref=xr.at[slot, 0 if up else 1], send_sem=xs_sem.at[slot, 0 if up else 1],
            recv_sem=xr_sem.at[slot, 0 if up else 1], device_id=(gz, gy, gx + 1 if up else gx - 1), device_id_type=MESH)

    def z_copy(slot, up):
        return pltpu.make_async_remote_copy(
            src_ref=zs.at[slot, 0 if up else 1], dst_ref=zr.at[slot, 0 if up else 1],
            send_sem=zs_sem.at[slot, 0 if up else 1], recv_sem=zr_sem.at[slot, 0 if up else 1],
            device_id=(gz + 1 if up else gz - 1, gy, gx), device_id_type=MESH)

    def y_copy(slot):
        return pltpu.make_async_remote_copy(
            src_ref=ys.at[slot], dst_ref=yr.at[slot], send_sem=ys_sem.at[slot], recv_sem=yr_sem.at[slot],
            device_id=(gz, 1 - gy, gx), device_id_type=MESH)

    def pack_slab(slot, i, slab):
        zs[slot, 1, pl.ds(i, 1), :] = slab[0:1, :]
        zs[slot, 0, pl.ds(i, 1), :] = slab[nl - 1:nl, :]
        return column_roll(slab[0:half], i - face_lane), column_roll(slab[half:nl], i - face_lane + LANES // 2)

    def pack_rolls(ref, slot, i, behind=False):
        row = lax.max(i, 0) if behind else i
        return pack_slab(slot, row, ref[row + 1, rows, :])

    def pack(i, rolled, acc):
        acc = jnp.where(lane_half == i, rolled[0], acc)
        return jnp.where(lane_half == i + LANES // 2, rolled[1], acc)

    def packed_pass(ref, slot, step, init):
        def body(g, carry):
            state, acc = carry
            rolled = [pack_rolls(ref, slot, (g - 1) * GROUP + k, behind=True) for k in range(GROUP)]
            for k in range(GROUP):
                state = step(g * GROUP + k, state)
            for k in range(GROUP):
                acc = pack((g - 1) * GROUP + k, rolled[k], acc)
            return state, acc
        state, acc = lax.fori_loop(0, ni // GROUP, body, (init, jnp.zeros((half, LANES), F32)))
        rolled = [pack_rolls(ref, slot, ni - GROUP + k) for k in range(GROUP)]
        for k in range(GROUP):
            acc = pack(ni - GROUP + k, rolled[k], acc)
        ys[slot] = acc
        return state

    def scale_and_pack(slot):
        group = min(COLUMNS, ni)

        def body(g, acc):
            rolled = []
            for k in range(group):
                i = g * group + k
                m = inv[i] * w[i]
                mp[i + 1, rows, :] = m
                rolled.append(pack_slab(slot, i, m))
            for k in range(group):
                acc = pack(g * group + k, rolled[k], acc)
            return acc

        ys[slot] = lax.fori_loop(0, ni // group, body, jnp.zeros((half, LANES), F32))

    def exchange_start(ref, slot):
        y_copy(slot).start()
        pl.when(has_zlo)(lambda: z_copy(slot, False).start())
        pl.when(has_zhi)(lambda: z_copy(slot, True).start())
        pl.when(has_xlo)(lambda: x_copy(ref, slot, False).start())
        pl.when(has_xhi)(lambda: x_copy(ref, slot, True).start())

    def exchange_wait(ref, slot):
        @pl.when(has_xlo)
        def _():
            x_copy(ref, slot, False).wait_send()
            x_copy(ref, slot, True).wait_recv()

        @pl.when(has_xhi)
        def _():
            x_copy(ref, slot, True).wait_send()
            x_copy(ref, slot, False).wait_recv()

        @pl.when(has_zlo)
        def _():
            z_copy(slot, False).wait_send()
            z_copy(slot, True).wait_recv()

        @pl.when(has_zhi)
        def _():
            z_copy(slot, True).wait_send()
            z_copy(slot, False).wait_recv()

        y_copy(slot).wait()

    def add_rows(ref, layer, row):
        for i in range(ni):
            ref[i, row:row + 1, :] = ref[i, row:row + 1, :] + layer[i:i + 1, :]

    def add_columns(ref, packed):
        mask = lane == face_lane

        def step(g, _):
            columns = []
            for k in range(min(COLUMNS, ni)):
                i = g * min(COLUMNS, ni) + k
                columns.append((column_roll(packed, face_lane - i), column_roll(packed, face_lane - i - LANES // 2)))
            for k in range(min(COLUMNS, ni)):
                i = g * min(COLUMNS, ni) + k
                ref[i] = ref[i] + jnp.where(mask, jnp.concatenate(columns[k], axis=0), 0.0)
            return 0

        lax.fori_loop(0, ni // min(COLUMNS, ni), step, 0)

    def join_faces(ref, slot):
        y_copy(slot).wait()
        add_columns(n, by[...] * (ys[slot] - yr[slot]))

        @pl.when(has_xlo)
        def _():
            x_copy(ref, slot, False).wait_send()
            x_copy(ref, slot, True).wait_recv()
            n[0] = n[0] + bx[0] * (ref[1, rows, :] - xr[slot, 0])

        @pl.when(has_xhi)
        def _():
            x_copy(ref, slot, True).wait_send()
            x_copy(ref, slot, False).wait_recv()
            n[ni - 1] = n[ni - 1] + bx[1] * (ref[ni, rows, :] - xr[slot, 1])

        @pl.when(has_zlo)
        def _():
            z_copy(slot, False).wait_send()
            z_copy(slot, True).wait_recv()
            add_rows(n, bz[0] * (zs[slot, 1] - zr[slot, 0]), 0)

        @pl.when(has_zhi)
        def _():
            z_copy(slot, True).wait_send()
            z_copy(slot, False).wait_recv()
            add_rows(n, bz[1] * (zs[slot, 0] - zr[slot, 1]), nl - 1)

    def stencil(ref, diagonal=False):
        def step(i, carry):
            v, flux_x = carry
            above = ref[i + 2, rows, :]
            if diagonal:
                inv[i] = cx[i] + cx[i + 1] + cy[i] + cyh[i] + cz[i, rows, :] + cz[i, rows_up, :]
            flux_next = cx[i + 1] * (above - v)
            flux_zl = cz[i, rows, :] * (v - ref[i + 1, rows_dn, :])
            flux_zh = cz[i, rows_up, :] * (ref[i + 1, rows_up, :] - v)
            flux_yl = cy[i] * (v - pltpu.roll(v, 1, 1))
            flux_yh = cyh[i] * (pltpu.roll(v, LANES - 1, 1) - v)
            n[i] = (flux_x - flux_next) + (flux_yl - flux_yh) + (flux_zl - flux_zh)
            return above, flux_next

        first = ref[1, rows, :]
        slabs(GROUP, step, (first, cx[0] * (first - ref[0, rows, :])))

    def fold(slab):
        out = slab[0:8]
        for part in range(8, nl, 8):
            out = out + slab[part:part + 8]
        return out

    def reduce_row(slot, accs):
        row = jnp.zeros((1, LANES), F32)
        for q, acc in enumerate(accs):
            row = jnp.where(lane_row == q, jnp.sum(jnp.sum(acc, axis=0, keepdims=True), axis=1, keepdims=True), row)
        red_s[slot] = row
        red_r[slot, (gz * ngy + gy) * ngx + gx] = row

    def reduce_send(slot, planes):
        me = (gz * ngy + gy) * ngx + gx
        far, next_far = jnp.where(gz < 2, 3, 0), jnp.where(gz < 2, 2, 1)
        order = (far, next_far, 6 - gz - far - next_far, gz)
        for k in planes:
            z_to = order[k]
            for b in reversed(range(ngy)):
                for c in (2, 3, 1, 0):
                    copy = pltpu.make_async_remote_copy(
                        src_ref=red_s.at[slot], dst_ref=red_r.at[slot, me], send_sem=rs_sem.at[slot], recv_sem=rr_sem.at[slot],
                        device_id=(z_to, lax.rem(gy + b, ngy), lax.rem(gx + c, ngx)), device_id_type=MESH)
                    if b or c or k < ngz - 1:
                        copy.start()

    def reduce_wait(slot, count):
        whole = red_r.at[slot, pl.ds(0, others)]
        done = pltpu.make_async_remote_copy(
            src_ref=whole, dst_ref=whole, send_sem=rs_sem.at[slot], recv_sem=rr_sem.at[slot],
            device_id=(gz, gy, gx), device_id_type=MESH)
        done.wait_recv()
        done.wait_send()
        parts = [red_r[slot, device] for device in range(others + 1)]
        while len(parts) > 1:
            parts = [a + b for a, b in zip(parts[0::2], parts[1::2])]
        total = parts[0]
        return [jnp.sum(jnp.where(lane_row == q, total, 0.0), axis=1, keepdims=True) for q in range(count)]

    x_row, z_row = jnp.where(gx == 0, 0, 1), jnp.where(gz == 0, 4, 5)
    slabs_i = pl.ds(pl.multiple_of(gx * ni, 8), ni)
    inputs = [
        pltpu.make_async_copy(k_hbm, k_in, in_sem.at[0]),
        pltpu.make_async_copy(u_hbm, u_in, in_sem.at[1]),
        pltpu.make_async_copy(kg_hbm.at[x_row, pl.ds(pl.multiple_of(gy * nj, 8), nj)], wall_x, in_sem.at[2]),
        pltpu.make_async_copy(kg_hbm.at[2 + gy, slabs_i], wall_y, in_sem.at[3]),
        pltpu.make_async_copy(kg_hbm.at[z_row, slabs_i], wall_z, in_sem.at[4]),
        pltpu.make_async_copy(f_hbm, f_in, in_sem.at[5]),
    ]
    for copy in inputs[:5]:
        copy.start()

    def tell_neighbours(sem):
        tell = lambda *target: pl.semaphore_signal(sem, inc=1, device_id=target, device_id_type=MESH)
        pl.when(has_xlo)(lambda: tell(gz, gy, gx - 1))
        pl.when(has_xhi)(lambda: tell(gz, gy, gx + 1))
        pl.when(has_zlo)(lambda: tell(gz - 1, gy, gx))
        pl.when(has_zhi)(lambda: tell(gz + 1, gy, gx))
        tell(gz, 1 - gy, gx)

    neighbours = 5 - jnp.where(has_xlo, 0, 1) - jnp.where(has_xhi, 0, 1) - jnp.where(has_zlo, 0, 1) - jnp.where(has_zhi, 0, 1)
    rounds = (ngx - 1) + (ngy - 1) + (ngz - 1) - 1

    def next_round(k):
        pl.semaphore_wait(near_sem.at[k], neighbours)
        if k + 1 < rounds:
            tell_neighbours(near_sem.at[k + 1])

    barrier = pltpu.get_barrier_semaphore()
    tell_neighbours(barrier)

    for edge in (0, ni + 1):
        mp[edge] = jnp.zeros((nl + 2 * PAD, LANES), F32)
        kp[edge] = jnp.ones((nl + 2 * PAD, LANES), F32)

    def clear(i, _):
        mp[i + 1, pl.ds(0, PAD), :] = jnp.zeros((PAD, LANES), F32)
        mp[i + 1, pl.ds(PAD + nl, PAD), :] = jnp.zeros((PAD, LANES), F32)
        kp[i + 1, pl.ds(0, PAD), :] = jnp.ones((PAD, LANES), F32)
        kp[i + 1, pl.ds(PAD + nl, PAD), :] = jnp.ones((PAD, LANES), F32)
        mp[i + 1, rows, :] = zero_slab
        s[i] = zero_slab
        z[i] = zero_slab
        p[i] = zero_slab
        r[1, i] = zero_slab
        r[0, i] = zero_slab
        kp[i + 1, rows, :] = jnp.full((nl, LANES), 1.0, F32)
        return 0

    lax.fori_loop(0, ni, clear, 0)

    def load_k(i, _):
        kp[i + 1, rows, 0:nj] = k_in[i]
        return 0

    def load_u(i, _):
        mp[i + 1, rows, 0:nj] = u_in[i]
        return 0

    inputs[0].wait()
    inputs[5].start()
    packed_pass(kp, 0, load_k, 0)
    pl.semaphore_wait(barrier, neighbours)
    tell_neighbours(near_sem.at[0])
    exchange_start(kp, 0)
    inputs[1].wait()
    packed_pass(mp, 1, load_u, 0)
    exchange_start(mp, 1)
    next_round(0)

    for copy in inputs[2:5]:
        copy.wait()
    width = wall_x.shape[1]
    l_rows = pl.ds(pl.multiple_of(gz * nl, 8), nl)

    def flipped(wall, count):
        for start in range(0, width, LANES):
            size = min(LANES, width - start)
            block = jnp.concatenate([wall[:, start:start + size], jnp.ones((LANES - count, size), F32)], axis=0)
            wall_t[start:start + size, :] = block.T
        return wall_t[l_rows, :]

    x_wall = flipped(wall_x, nj)
    y_wall = flipped(wall_y, ni)
    if width > LANES:
        rest = jnp.concatenate([wall_z[:, LANES:width], jnp.ones((ni, 2 * LANES - width), F32)], axis=1)
        whole_z = wall_z[:, 0:LANES]
        turn = LANES - nj
        shifted = jnp.where(lane_i < turn, pltpu.roll(whole_z, turn, 1), pltpu.roll(rest, turn, 1))
    else:
        whole_z = jnp.concatenate([wall_z[...], jnp.ones((ni, LANES - width), F32)], axis=1)
        shifted = pltpu.roll(whole_z, LANES - nj, 1)
    z_wall = jnp.where(gy == 0, whole_z, shifted)

    def harmonic(left, right):
        return 2.0 * left * right / (left + right)

    next_round(1)

    in_i = lane_i < nj
    cx[0] = jnp.where(jnp.logical_and(inside, gx == 0), harmonic(x_wall, kp[1, rows, :]), 0.0)
    z_low = jnp.where(jnp.logical_and(in_i, gz == 0), harmonic(z_wall, zs[0, 1]), 0.0)
    z_high = jnp.where(jnp.logical_and(in_i, gz == ngz - 1), harmonic(zs[0, 0], z_wall), 0.0)
    y_low_mask = jnp.logical_and(inside, jnp.logical_or(lane > 0, y_low_wall))
    y_high_mask = jnp.logical_and(inside, jnp.logical_or(lane < nj - 1, y_high_wall))
    wall_lane = jnp.where(gy == 0, 0, nj)

    def coefs(i, _):
        here = kp[i + 1, rows, :]
        cx[i + 1] = jnp.where(inside, harmonic(here, kp[i + 2, rows, :]), 0.0)
        cz[i, rows_up, :] = jnp.where(inside, harmonic(here, kp[i + 1, rows_up, :]), 0.0)
        wall = column_roll(y_wall, wall_lane - i)
        low = jnp.where(jnp.logical_and(lane == 0, y_low_wall), wall, pltpu.roll(here, 1, 1))
        faces = harmonic(low, jnp.where(jnp.logical_and(lane == nj, y_high_wall), wall, here))
        cy[i] = jnp.where(y_low_mask, faces, 0.0)
        cyh[i] = jnp.where(y_high_mask, pltpu.roll(faces, LANES - 1, 1), 0.0)
        return 0

    slabs(GROUP, coefs, 0)
    next_round(2)
    cx[ni] = jnp.where(jnp.logical_and(inside, gx == ngx - 1), harmonic(kp[ni, rows, :], x_wall), 0.0)
    for i in range(ni):
        cz[i, PAD:PAD + 1, :] = z_low[i:i + 1, :]
        cz[i, PAD + nl:PAD + nl + 1, :] = z_high[i:i + 1, :]

    stencil(mp, diagonal=True)
    next_round(3)

    exchange_wait(kp, 0)

    @pl.when(has_xlo)
    def _():
        bx[0] = jnp.where(inside, harmonic(xr[0, 0], kp[1, rows, :]), 0.0)
        inv[0] = inv[0] + bx[0]

    @pl.when(has_xhi)
    def _():
        bx[1] = jnp.where(inside, harmonic(kp[ni, rows, :], xr[0, 1]), 0.0)
        inv[ni - 1] = inv[ni - 1] + bx[1]

    @pl.when(has_zlo)
    def _():
        bz[0] = jnp.where(in_i, harmonic(zr[0, 0], zs[0, 1]), 0.0)
        add_rows(inv, bz[0], 0)

    @pl.when(has_zhi)
    def _():
        bz[1] = jnp.where(in_i, harmonic(zs[0, 0], zr[0, 1]), 0.0)
        add_rows(inv, bz[1], nl - 1)

    y_face = jnp.where(lax.rem(lane_half, LANES // 2) < ni, harmonic(ys[0], yr[0]), 0.0)
    by[...] = y_face
    add_columns(inv, y_face)
    join_faces(mp, 1)
    inputs[5].wait()

    def first_residual(i, acc):
        iv = jnp.where(inside, 1.0 / jnp.where(inside, inv[i], 1.0), 0.0)
        inv[i] = iv
        x[i] = mp[i + 1, rows, :]
        r[0, i, :, 0:nj] = f_in[i]
        res = r[0, i] - n[i]
        r[0, i] = res
        u = res * iv
        mp[i + 1, rows, :] = u
        return acc + fold(res * u)

    gamma_acc = packed_pass(mp, 2, first_residual, zero_acc)
    exchange_start(mp, 2)
    next_round(4)
    stencil(mp)
    for k in range(5, rounds):
        next_round(k)
    join_faces(mp, 2)

    def first_w(i, acc):
        av = n[i]
        w[i] = av
        return acc + fold(av * mp[i + 1, rows, :])

    reduce_row(0, (gamma_acc, slabs(GROUP, first_w, zero_acc)))

    def scalars(t, sums, gamma_old, pap_old):
        gamma, delta, sigma = sums[0], sums[1], sums[2]
        beta = jnp.where(t == 0, 0.0, gamma / gamma_old)
        pap = delta + 2.0 * beta * sigma + beta * beta * pap_old
        return gamma, pap, beta, gamma / pap

    def wide(value):
        return jnp.broadcast_to(value, (nl, LANES))

    def advance_x(now, alpha, beta):
        alpha, beta = wide(alpha), wide(beta)

        def step(i, acc):
            p_new = inv[i] * r[1 - now, i] + beta * p[i]
            p[i] = p_new
            x[i] = x[i] + alpha * p_new
            return acc + fold(r[now, i] * r[now, i])
        return lax.fori_loop(0, ni, step, zero_acc)

    def iteration(t, carry):
        gamma_old, pap_old, alpha_old, beta_old = carry
        now = lax.rem(t, 2)
        reduce_send(t, range(0, ngz - 1))
        scale_and_pack(t + 3)
        exchange_start(mp, t + 3)
        reduce_send(t, (ngz - 1,))
        stencil(mp)
        rr_acc = advance_x(now, alpha_old, beta_old)
        join_faces(mp, t + 3)
        sums = reduce_wait(t, 4)
        gamma, pap, beta, alpha = scalars(t, sums, gamma_old, pap_old)

        alpha_w, beta_w = wide(alpha), wide(beta)

        def update(i, acc):
            iv = inv[i]
            w_old = w[i]
            z_new = n[i] + beta_w * z[i]
            s_new = w_old + beta_w * s[i]
            r_new = r[now, i] - alpha_w * s_new
            w_new = w_old - alpha_w * z_new
            u_new = iv * r_new
            z[i] = z_new
            s[i] = s_new
            r[1 - now, i] = r_new
            w[i] = w_new
            return acc[0] + fold(r_new * u_new), acc[1] + fold(w_new * u_new), acc[2] + fold(u_new * s_new)

        reduce_row(t + 1, slabs(UPDATE, update, (zero_acc,) * 3) + (rr_acc,))
        scal_ref[lax.rem(t + CG_ITERS - 2, CG_ITERS)] = jnp.broadcast_to(sums[3], (1, LANES))
        return gamma, pap, alpha, beta

    one = jnp.ones((1, 1), F32)
    last = CG_ITERS - 1
    gamma_old, pap_old, alpha_old, beta_old = lax.fori_loop(
        0, last, iteration, (one, one, 0.0 * one, 0.0 * one))

    now = last % 2
    reduce_send(last, range(ngz))

    def last_dots(i, acc):
        rv, sv = r[now, i], s[i]
        wv = w[i]
        pairs = ((rv, rv), (rv, wv), (rv, sv), (wv, wv), (wv, sv), (sv, sv))
        return tuple(a + fold(b * c) for a, (b, c) in zip(acc, pairs))

    reduce_row(CG_ITERS, slabs(3, last_dots, (zero_acc,) * 6))
    reduce_send(CG_ITERS, range(ngz))
    advance_x(now, alpha_old, beta_old)

    sums = reduce_wait(last, 4)
    line = lambda value: jnp.broadcast_to(value, (1, LANES))
    scal_ref[last - 2] = line(sums[3])
    gamma = sums[0]
    beta = gamma / gamma_old
    alpha = gamma / (sums[1] + 2.0 * beta * sums[2] + beta * beta * pap_old)
    alpha_w, beta_w = wide(alpha), wide(beta)

    def final(i, _):
        r_old = r[now, i]
        x_last[i] = (x[i] + alpha_w * (inv[i] * r_old + beta_w * p[i]))[:, 0:nj]
        r_last[i] = (r_old - alpha_w * (w[i] + beta_w * s[i]))[:, 0:nj]
        return 0

    slabs(2, final, 0)
    rr, rw, rs, ww, ws, ss = reduce_wait(CG_ITERS, 6)
    scal_ref[last - 1] = line(rr)
    scal_ref[last] = line(rr - 2.0 * alpha * (rw + beta * rs) + alpha * alpha * (ww + 2.0 * beta * ws + beta * beta * ss))


def finish_kernel(scal, x, r, x_hbm, r_hbm, hist_hbm, hist, sem):
    copies = [pltpu.make_async_copy(x, x_hbm, sem.at[0]), pltpu.make_async_copy(r, r_hbm, sem.at[1]),
              pltpu.make_async_copy(hist, hist_hbm, sem.at[2])]
    copies[0].start()
    copies[1].start()
    for t in range(CG_ITERS):
        hist[t] = scal[t, 0, 0]
    copies[2].start()
    for copy in copies:
        copy.wait()


def solution(mesh):
    counts = (mesh.shape['gx'], mesh.shape['gy'], mesh.shape['gz'])
    grid_spec = P('gx', 'gy', 'gz')

    def local_solve(k_cell, k_ghost, f_rhs, u_init):
        ni, nj, nl = k_cell.shape
        flip = lambda a: jnp.swapaxes(a, 1, 2)
        slots = CG_ITERS + 3
        devices = counts[0] * counts[1] * counts[2]
        width = k_ghost.shape[2]
        any_spec = pl.BlockSpec(memory_space=pl.ANY)
        vm = lambda *shape: pltpu.VMEM(shape, F32)
        whole = vm(ni, nl, LANES)
        block = vm(ni, nl, nj)
        padded = vm(ni + 2, nl + 2 * PAD, LANES)
        dma = pltpu.SemaphoreType.DMA
        kept = pltpu.VMEM((ni, nl, nj), F32)
        vmem_spec = pl.BlockSpec(memory_space=pltpu.VMEM)
        x_last, r_last, scal = pl.pallas_call(
            functools.partial(solve_kernel, (ni, nl, nj), counts),
            out_shape=(kept, kept, pltpu.VMEM((CG_ITERS, 1, LANES), F32)),
            in_specs=[any_spec] * 4,
            out_specs=(vmem_spec,) * 3,
            scratch_shapes=[
                block, block, block, vm(nj, width), vm(ni, width), vm(ni, width), vm(-(-width // LANES) * LANES, LANES),
                vm(2, nl, LANES), vm(nl // 2, LANES), vm(2, ni, LANES),
                padded, padded, vm(ni + 1, nl, LANES), whole, whole, vm(ni, nl + 2 * PAD, LANES), whole,
                whole, vm(2, ni, nl, LANES), whole, whole, whole, whole, whole,
                vm(slots, nl // 2, LANES), vm(slots, 2, ni, LANES),
                vm(slots, 2, nl, LANES), vm(slots, nl // 2, LANES), vm(slots, 2, ni, LANES),
                vm(CG_ITERS + 1, 1, LANES), vm(CG_ITERS + 1, devices, 1, LANES),
                dma((slots, 2)), dma((slots,)), dma((slots, 2)), dma((slots, 2)), dma((slots,)), dma((slots, 2)),
                dma((CG_ITERS + 1,)), dma((CG_ITERS + 1,)), dma((6,)), pltpu.SemaphoreType.REGULAR((6,)),
            ],
            compiler_params=pltpu.CompilerParams(has_side_effects=True, collective_id=0, vmem_limit_bytes=28 << 20),
        )(*(pltpu.with_memory_space_constraint(a, pltpu.HBM) for a in (k_ghost, flip(k_cell), flip(f_rhs), flip(u_init))))
        out_block = jax.ShapeDtypeStruct((ni, nl, nj), F32)
        x_new, r_new, hist = pl.pallas_call(
            finish_kernel,
            out_shape=(out_block, out_block, jax.ShapeDtypeStruct((CG_ITERS,), F32)),
            in_specs=[vmem_spec] * 3,
            out_specs=(any_spec,) * 3,
            scratch_shapes=[pltpu.SMEM((CG_ITERS,), F32), dma((3,))],
            compiler_params=pltpu.CompilerParams(vmem_limit_bytes=28 << 20),
        )(scal, x_last, r_last)
        return flip(x_new), flip(r_new), hist

    return jax.shard_map(local_solve, mesh=mesh, in_specs=(grid_spec, P(), grid_spec, grid_spec),
                         out_specs=(grid_spec, grid_spec, P()), check_vma=False)
```

```python
import functools

import jax
import jax.numpy as jnp
from jax import lax
from jax.experimental import pallas as pl
from jax.experimental.pallas import tpu as pltpu
from jax.sharding import PartitionSpec as P

CG_ITERS = 8
LANES = 128
PAD = 8
GROUP = 6
COLUMNS = 48
UPDATE = 8
MESH = pl.DeviceIdType.MESH
F32 = jnp.float32


def solve_kernel(dims, counts, kg_hbm, k_hbm, f_hbm, u_hbm, x_last, r_last, scal_ref,
                 k_in, f_in, u_in, wall_x, wall_y, wall_z, wall_t, bx, by, bz,
                 kp, mp, cx, cy, cyh, cz, inv, x, r, w, s, z, p, n,
                 ys, zs, xr, yr, zr, red_s, red_r,
                 xs_sem, ys_sem, zs_sem, xr_sem, yr_sem, zr_sem, rs_sem, rr_sem, in_sem, near_sem):
    ni, nl, nj = dims
    ngx, ngy, ngz = counts
    half = nl // 2
    gx, gy, gz = lax.axis_index('gx'), lax.axis_index('gy'), lax.axis_index('gz')
    rows = pl.ds(PAD, nl)
    rows_dn = pl.ds(PAD - 1, nl)
    rows_up = pl.ds(PAD + 1, nl)
    lane = lax.broadcasted_iota(jnp.int32, (nl, LANES), 1)
    lane_i = lax.broadcasted_iota(jnp.int32, (ni, LANES), 1)
    lane_half = lax.broadcasted_iota(jnp.int32, (half, LANES), 1)
    lane_row = lax.broadcasted_iota(jnp.int32, (1, LANES), 1)
    inside = lane < nj
    has_xlo, has_xhi = gx > 0, gx < ngx - 1
    has_zlo, has_zhi = gz > 0, gz < ngz - 1
    face_lane = jnp.where(gy == 0, nj - 1, 0)
    y_low_wall, y_high_wall = gy == 0, gy > 0
    zero_slab = jnp.zeros((nl, LANES), F32)
    zero_acc = jnp.zeros((8, LANES), F32)
    others = ngx * ngy * ngz - 1

    def column_roll(slab, shift):
        return pltpu.roll(slab, shift + 2 * LANES, 1)

    def slabs(group, step, init):
        def body(g, carry):
            for k in range(group):
                carry = step(g * group + k, carry)
            return carry
        return lax.fori_loop(0, ni // group, body, init)

    def x_copy(ref, slot, up):
        src = ref.at[ni if up else 1, rows]
        return pltpu.make_async_remote_copy(
            src_ref=src, dst_ref=xr.at[slot, 0 if up else 1], send_sem=xs_sem.at[slot, 0 if up else 1],
            recv_sem=xr_sem.at[slot, 0 if up else 1], device_id=(gz, gy, gx + 1 if up else gx - 1), device_id_type=MESH)

    def z_copy(slot, up):
        return pltpu.make_async_remote_copy(
            src_ref=zs.at[slot, 0 if up else 1], dst_ref=zr.at[slot, 0 if up else 1],
            send_sem=zs_sem.at[slot, 0 if up else 1], recv_sem=zr_sem.at[slot, 0 if up else 1],
            device_id=(gz + 1 if up else gz - 1, gy, gx), device_id_type=MESH)

    def y_copy(slot):
        return pltpu.make_async_remote_copy(
            src_ref=ys.at[slot], dst_ref=yr.at[slot], send_sem=ys_sem.at[slot], recv_sem=yr_sem.at[slot],
            device_id=(gz, 1 - gy, gx), device_id_type=MESH)

    def pack_slab(slot, i, slab):
        zs[slot, 1, pl.ds(i, 1), :] = slab[0:1, :]
        zs[slot, 0, pl.ds(i, 1), :] = slab[nl - 1:nl, :]
        return column_roll(slab[0:half], i - face_lane), column_roll(slab[half:nl], i - face_lane + LANES // 2)

    def pack_rolls(ref, slot, i, behind=False):
        row = lax.max(i, 0) if behind else i
        return pack_slab(slot, row, ref[row + 1, rows, :])

    def pack(i, rolled, acc):
        acc = jnp.where(lane_half == i, rolled[0], acc)
        return jnp.where(lane_half == i + LANES // 2, rolled[1], acc)

    def packed_pass(ref, slot, step, init):
        def body(g, carry):
            state, acc = carry
            rolled = [pack_rolls(ref, slot, (g - 1) * GROUP + k, behind=True) for k in range(GROUP)]
            for k in range(GROUP):
                state = step(g * GROUP + k, state)
            for k in range(GROUP):
                acc = pack((g - 1) * GROUP + k, rolled[k], acc)
            return state, acc
        state, acc = lax.fori_loop(0, ni // GROUP, body, (init, jnp.zeros((half, LANES), F32)))
        rolled = [pack_rolls(ref, slot, ni - GROUP + k) for k in range(GROUP)]
        for k in range(GROUP):
            acc = pack(ni - GROUP + k, rolled[k], acc)
        ys[slot] = acc
        return state

    def scale_and_pack(slot):
        group = min(COLUMNS, ni)

        def body(g, acc):
            rolled = []
            for k in range(group):
                i = g * group + k
                m = inv[i] * w[i]
                mp[i + 1, rows, :] = m
                rolled.append(pack_slab(slot, i, m))
            for k in range(group):
                acc = pack(g * group + k, rolled[k], acc)
            return acc

        ys[slot] = lax.fori_loop(0, ni // group, body, jnp.zeros((half, LANES), F32))

    def exchange_start(ref, slot):
        y_copy(slot).start()
        pl.when(has_zlo)(lambda: z_copy(slot, False).start())
        pl.when(has_zhi)(lambda: z_copy(slot, True).start())
        pl.when(has_xlo)(lambda: x_copy(ref, slot, False).start())
        pl.when(has_xhi)(lambda: x_copy(ref, slot, True).start())

    def exchange_wait(ref, slot):
        @pl.when(has_xlo)
        def _():
            x_copy(ref, slot, False).wait_send()
            x_copy(ref, slot, True).wait_recv()

        @pl.when(has_xhi)
        def _():
            x_copy(ref, slot, True).wait_send()
            x_copy(ref, slot, False).wait_recv()

        @pl.when(has_zlo)
        def _():
            z_copy(slot, False).wait_send()
            z_copy(slot, True).wait_recv()

        @pl.when(has_zhi)
        def _():
            z_copy(slot, True).wait_send()
            z_copy(slot, False).wait_recv()

        y_copy(slot).wait()

    def add_rows(ref, layer, row):
        for i in range(ni):
            ref[i, row:row + 1, :] = ref[i, row:row + 1, :] + layer[i:i + 1, :]

    def add_columns(ref, packed):
        mask = lane == face_lane

        def step(g, _):
            columns = []
            for k in range(min(COLUMNS, ni)):
                i = g * min(COLUMNS, ni) + k
                columns.append((column_roll(packed, face_lane - i), column_roll(packed, face_lane - i - LANES // 2)))
            for k in range(min(COLUMNS, ni)):
                i = g * min(COLUMNS, ni) + k
                ref[i] = ref[i] + jnp.where(mask, jnp.concatenate(columns[k], axis=0), 0.0)
            return 0

        lax.fori_loop(0, ni // min(COLUMNS, ni), step, 0)

    def join_faces(ref, slot):
        y_copy(slot).wait()
        add_columns(n, by[...] * (ys[slot] - yr[slot]))

        @pl.when(has_xlo)
        def _():
            x_copy(ref, slot, False).wait_send()
            x_copy(ref, slot, True).wait_recv()
            n[0] = n[0] + bx[0] * (ref[1, rows, :] - xr[slot, 0])

        @pl.when(has_xhi)
        def _():
            x_copy(ref, slot, True).wait_send()
            x_copy(ref, slot, False).wait_recv()
            n[ni - 1] = n[ni - 1] + bx[1] * (ref[ni, rows, :] - xr[slot, 1])

        @pl.when(has_zlo)
        def _():
            z_copy(slot, False).wait_send()
            z_copy(slot, True).wait_recv()
            add_rows(n, bz[0] * (zs[slot, 1] - zr[slot, 0]), 0)

        @pl.when(has_zhi)
        def _():
            z_copy(slot, True).wait_send()
            z_copy(slot, False).wait_recv()
            add_rows(n, bz[1] * (zs[slot, 0] - zr[slot, 1]), nl - 1)

    def stencil(ref, diagonal=False):
        def step(i, carry):
            v, flux_x = carry
            above = ref[i + 2, rows, :]
            if diagonal:
                inv[i] = cx[i] + cx[i + 1] + cy[i] + cyh[i] + cz[i, rows, :] + cz[i, rows_up, :]
            flux_next = cx[i + 1] * (above - v)
            flux_zl = cz[i, rows, :] * (v - ref[i + 1, rows_dn, :])
            flux_zh = cz[i, rows_up, :] * (ref[i + 1, rows_up, :] - v)
            flux_yl = cy[i] * (v - pltpu.roll(v, 1, 1))
            flux_yh = cyh[i] * (pltpu.roll(v, LANES - 1, 1) - v)
            n[i] = (flux_x - flux_next) + (flux_yl - flux_yh) + (flux_zl - flux_zh)
            return above, flux_next

        first = ref[1, rows, :]
        slabs(GROUP, step, (first, cx[0] * (first - ref[0, rows, :])))

    def fold(slab):
        out = slab[0:8]
        for part in range(8, nl, 8):
            out = out + slab[part:part + 8]
        return out

    def reduce_row(slot, accs):
        row = jnp.zeros((1, LANES), F32)
        for q, acc in enumerate(accs):
            row = jnp.where(lane_row == q, jnp.sum(jnp.sum(acc, axis=0, keepdims=True), axis=1, keepdims=True), row)
        red_s[slot] = row
        red_r[slot, (gz * ngy + gy) * ngx + gx] = row

    def reduce_send(slot, planes):
        me = (gz * ngy + gy) * ngx + gx
        far, next_far = jnp.where(gz < 2, 3, 0), jnp.where(gz < 2, 2, 1)
        order = (far, next_far, 6 - gz - far - next_far, gz)
        for k in planes:
            z_to = order[k]
            for b in reversed(range(ngy)):
                for c in (2, 3, 1, 0):
                    copy = pltpu.make_async_remote_copy(
                        src_ref=red_s.at[slot], dst_ref=red_r.at[slot, me], send_sem=rs_sem.at[slot], recv_sem=rr_sem.at[slot],
                        device_id=(z_to, lax.rem(gy + b, ngy), lax.rem(gx + c, ngx)), device_id_type=MESH)
                    if b or c or k < ngz - 1:
                        copy.start()

    def reduce_wait(slot, count):
        whole = red_r.at[slot, pl.ds(0, others)]
        done = pltpu.make_async_remote_copy(
            src_ref=whole, dst_ref=whole, send_sem=rs_sem.at[slot], recv_sem=rr_sem.at[slot],
            device_id=(gz, gy, gx), device_id_type=MESH)
        done.wait_recv()
        done.wait_send()
        parts = [red_r[slot, device] for device in range(others + 1)]
        while len(parts) > 1:
            parts = [a + b for a, b in zip(parts[0::2], parts[1::2])]
        total = parts[0]
        return [jnp.sum(jnp.where(lane_row == q, total, 0.0), axis=1, keepdims=True) for q in range(count)]

    x_row, z_row = jnp.where(gx == 0, 0, 1), jnp.where(gz == 0, 4, 5)
    slabs_i = pl.ds(pl.multiple_of(gx * ni, 8), ni)
    inputs = [
        pltpu.make_async_copy(k_hbm, k_in, in_sem.at[0]),
        pltpu.make_async_copy(u_hbm, u_in, in_sem.at[1]),
        pltpu.make_async_copy(kg_hbm.at[x_row, pl.ds(pl.multiple_of(gy * nj, 8), nj)], wall_x, in_sem.at[2]),
        pltpu.make_async_copy(kg_hbm.at[2 + gy, slabs_i], wall_y, in_sem.at[3]),
        pltpu.make_async_copy(kg_hbm.at[z_row, slabs_i], wall_z, in_sem.at[4]),
        pltpu.make_async_copy(f_hbm, f_in, in_sem.at[5]),
    ]
    for copy in inputs[:5]:
        copy.start()

    def tell_neighbours(sem):
        tell = lambda *target: pl.semaphore_signal(sem, inc=1, device_id=target, device_id_type=MESH)
        pl.when(has_xlo)(lambda: tell(gz, gy, gx - 1))
        pl.when(has_xhi)(lambda: tell(gz, gy, gx + 1))
        pl.when(has_zlo)(lambda: tell(gz - 1, gy, gx))
        pl.when(has_zhi)(lambda: tell(gz + 1, gy, gx))
        tell(gz, 1 - gy, gx)

    neighbours = 5 - jnp.where(has_xlo, 0, 1) - jnp.where(has_xhi, 0, 1) - jnp.where(has_zlo, 0, 1) - jnp.where(has_zhi, 0, 1)
    rounds = (ngx - 1) + (ngy - 1) + (ngz - 1) - 1

    def next_round(k):
        pl.semaphore_wait(near_sem.at[k], neighbours)
        if k + 1 < rounds:
            tell_neighbours(near_sem.at[k + 1])

    barrier = pltpu.get_barrier_semaphore()
    tell_neighbours(barrier)

    for edge in (0, ni + 1):
        mp[edge] = jnp.zeros((nl + 2 * PAD, LANES), F32)
        kp[edge] = jnp.ones((nl + 2 * PAD, LANES), F32)

    def clear(i, _):
        mp[i + 1, pl.ds(0, PAD), :] = jnp.zeros((PAD, LANES), F32)
        mp[i + 1, pl.ds(PAD + nl, PAD), :] = jnp.zeros((PAD, LANES), F32)
        kp[i + 1, pl.ds(0, PAD), :] = jnp.ones((PAD, LANES), F32)
        kp[i + 1, pl.ds(PAD + nl, PAD), :] = jnp.ones((PAD, LANES), F32)
        mp[i + 1, rows, :] = zero_slab
        s[i] = zero_slab
        z[i] = zero_slab
        p[i] = zero_slab
        r[1, i] = zero_slab
        r[0, i] = zero_slab
        kp[i + 1, rows, :] = jnp.full((nl, LANES), 1.0, F32)
        return 0

    lax.fori_loop(0, ni, clear, 0)

    def load_k(i, _):
        kp[i + 1, rows, 0:nj] = k_in[i]
        return 0

    def load_u(i, _):
        mp[i + 1, rows, 0:nj] = u_in[i]
        return 0

    inputs[0].wait()
    inputs[5].start()
    packed_pass(kp, 0, load_k, 0)
    pl.semaphore_wait(barrier, neighbours)
    tell_neighbours(near_sem.at[0])
    exchange_start(kp, 0)
    inputs[1].wait()
    packed_pass(mp, 1, load_u, 0)
    exchange_start(mp, 1)
    next_round(0)

    for copy in inputs[2:5]:
        copy.wait()
    width = wall_x.shape[1]
    l_rows = pl.ds(pl.multiple_of(gz * nl, 8), nl)

    def flipped(wall, count):
        for start in range(0, width, LANES):
            size = min(LANES, width - start)
            block = jnp.concatenate([wall[:, start:start + size], jnp.ones((LANES - count, size), F32)], axis=0)
            wall_t[start:start + size, :] = block.T
        return wall_t[l_rows, :]

    x_wall = flipped(wall_x, nj)
    y_wall = flipped(wall_y, ni)
    if width > LANES:
        rest = jnp.concatenate([wall_z[:, LANES:width], jnp.ones((ni, 2 * LANES - width), F32)], axis=1)
        whole_z = wall_z[:, 0:LANES]
        turn = LANES - nj
        shifted = jnp.where(lane_i < turn, pltpu.roll(whole_z, turn, 1), pltpu.roll(rest, turn, 1))
    else:
        whole_z = jnp.concatenate([wall_z[...], jnp.ones((ni, LANES - width), F32)], axis=1)
        shifted = pltpu.roll(whole_z, LANES - nj, 1)
    z_wall = jnp.where(gy == 0, whole_z, shifted)

    def harmonic(left, right):
        return 2.0 * left * right / (left + right)

    next_round(1)

    in_i = lane_i < nj
    cx[0] = jnp.where(jnp.logical_and(inside, gx == 0), harmonic(x_wall, kp[1, rows, :]), 0.0)
    z_low = jnp.where(jnp.logical_and(in_i, gz == 0), harmonic(z_wall, zs[0, 1]), 0.0)
    z_high = jnp.where(jnp.logical_and(in_i, gz == ngz - 1), harmonic(zs[0, 0], z_wall), 0.0)
    y_low_mask = jnp.logical_and(inside, jnp.logical_or(lane > 0, y_low_wall))
    y_high_mask = jnp.logical_and(inside, jnp.logical_or(lane < nj - 1, y_high_wall))
    wall_lane = jnp.where(gy == 0, 0, nj)

    def coefs(i, _):
        here = kp[i + 1, rows, :]
        cx[i + 1] = jnp.where(inside, harmonic(here, kp[i + 2, rows, :]), 0.0)
        cz[i, rows_up, :] = jnp.where(inside, harmonic(here, kp[i + 1, rows_up, :]), 0.0)
        wall = column_roll(y_wall, wall_lane - i)
        low = jnp.where(jnp.logical_and(lane == 0, y_low_wall), wall, pltpu.roll(here, 1, 1))
        faces = harmonic(low, jnp.where(jnp.logical_and(lane == nj, y_high_wall), wall, here))
        cy[i] = jnp.where(y_low_mask, faces, 0.0)
        cyh[i] = jnp.where(y_high_mask, pltpu.roll(faces, LANES - 1, 1), 0.0)
        return 0

    slabs(GROUP, coefs, 0)
    next_round(2)
    cx[ni] = jnp.where(jnp.logical_and(inside, gx == ngx - 1), harmonic(kp[ni, rows, :], x_wall), 0.0)
    for i in range(ni):
        cz[i, PAD:PAD + 1, :] = z_low[i:i + 1, :]
        cz[i, PAD + nl:PAD + nl + 1, :] = z_high[i:i + 1, :]

    stencil(mp, diagonal=True)
    next_round(3)

    exchange_wait(kp, 0)

    @pl.when(has_xlo)
    def _():
        bx[0] = jnp.where(inside, harmonic(xr[0, 0], kp[1, rows, :]), 0.0)
        inv[0] = inv[0] + bx[0]

    @pl.when(has_xhi)
    def _():
        bx[1] = jnp.where(inside, harmonic(kp[ni, rows, :], xr[0, 1]), 0.0)
        inv[ni - 1] = inv[ni - 1] + bx[1]

    @pl.when(has_zlo)
    def _():
        bz[0] = jnp.where(in_i, harmonic(zr[0, 0], zs[0, 1]), 0.0)
        add_rows(inv, bz[0], 0)

    @pl.when(has_zhi)
    def _():
        bz[1] = jnp.where(in_i, harmonic(zs[0, 0], zr[0, 1]), 0.0)
        add_rows(inv, bz[1], nl - 1)

    y_face = jnp.where(lax.rem(lane_half, LANES // 2) < ni, harmonic(ys[0], yr[0]), 0.0)
    by[...] = y_face
    add_columns(inv, y_face)
    join_faces(mp, 1)
    inputs[5].wait()

    def first_residual(i, acc):
        iv = jnp.where(inside, 1.0 / jnp.where(inside, inv[i], 1.0), 0.0)
        inv[i] = iv
        x[i] = mp[i + 1, rows, :]
        r[0, i, :, 0:nj] = f_in[i]
        res = r[0, i] - n[i]
        r[0, i] = res
        u = res * iv
        mp[i + 1, rows, :] = u
        return acc + fold(res * u)

    gamma_acc = packed_pass(mp, 2, first_residual, zero_acc)
    exchange_start(mp, 2)
    next_round(4)
    stencil(mp)
    for k in range(5, rounds):
        next_round(k)
    join_faces(mp, 2)

    def first_w(i, acc):
        av = n[i]
        w[i] = av
        return acc + fold(av * mp[i + 1, rows, :])

    reduce_row(0, (gamma_acc, slabs(GROUP, first_w, zero_acc)))

    def scalars(t, sums, gamma_old, pap_old):
        gamma, delta, sigma = sums[0], sums[1], sums[2]
        beta = jnp.where(t == 0, 0.0, gamma / gamma_old)
        pap = delta + 2.0 * beta * sigma + beta * beta * pap_old
        return gamma, pap, beta, gamma / pap

    def wide(value):
        return jnp.broadcast_to(value, (nl, LANES))

    def advance_x(now, alpha, beta):
        alpha, beta = wide(alpha), wide(beta)

        def step(i, acc):
            p_new = inv[i] * r[1 - now, i] + beta * p[i]
            p[i] = p_new
            x[i] = x[i] + alpha * p_new
            return acc + fold(r[now, i] * r[now, i])
        return lax.fori_loop(0, ni, step, zero_acc)

    def iteration(t, carry):
        gamma_old, pap_old, alpha_old, beta_old = carry
        now = lax.rem(t, 2)
        reduce_send(t, range(0, ngz // 2))
        scale_and_pack(t + 3)
        exchange_start(mp, t + 3)
        reduce_send(t, range(ngz // 2, ngz))
        stencil(mp)
        rr_acc = advance_x(now, alpha_old, beta_old)
        join_faces(mp, t + 3)
        sums = reduce_wait(t, 4)
        gamma, pap, beta, alpha = scalars(t, sums, gamma_old, pap_old)

        alpha_w, beta_w = wide(alpha), wide(beta)

        def update(i, acc):
            iv = inv[i]
            w_old = w[i]
            z_new = n[i] + beta_w * z[i]
            s_new = w_old + beta_w * s[i]
            r_new = r[now, i] - alpha_w * s_new
            w_new = w_old - alpha_w * z_new
            u_new = iv * r_new
            z[i] = z_new
            s[i] = s_new
            r[1 - now, i] = r_new
            w[i] = w_new
            return acc[0] + fold(r_new * u_new), acc[1] + fold(w_new * u_new), acc[2] + fold(u_new * s_new)

        reduce_row(t + 1, slabs(UPDATE, update, (zero_acc,) * 3) + (rr_acc,))
        scal_ref[lax.rem(t + CG_ITERS - 2, CG_ITERS)] = jnp.broadcast_to(sums[3], (1, LANES))
        return gamma, pap, alpha, beta

    one = jnp.ones((1, 1), F32)
    last = CG_ITERS - 1
    gamma_old, pap_old, alpha_old, beta_old = lax.fori_loop(
        0, last, iteration, (one, one, 0.0 * one, 0.0 * one))

    now = last % 2
    reduce_send(last, range(ngz))

    def last_dots(i, acc):
        rv, sv = r[now, i], s[i]
        wv = w[i]
        pairs = ((rv, rv), (rv, wv), (rv, sv), (wv, wv), (wv, sv), (sv, sv))
        return tuple(a + fold(b * c) for a, (b, c) in zip(acc, pairs))

    reduce_row(CG_ITERS, slabs(3, last_dots, (zero_acc,) * 6))
    reduce_send(CG_ITERS, range(ngz))
    advance_x(now, alpha_old, beta_old)

    sums = reduce_wait(last, 4)
    line = lambda value: jnp.broadcast_to(value, (1, LANES))
    scal_ref[last - 2] = line(sums[3])
    gamma = sums[0]
    beta = gamma / gamma_old
    alpha = gamma / (sums[1] + 2.0 * beta * sums[2] + beta * beta * pap_old)
    alpha_w, beta_w = wide(alpha), wide(beta)

    def final(i, _):
        r_old = r[now, i]
        x_last[i] = (x[i] + alpha_w * (inv[i] * r_old + beta_w * p[i]))[:, 0:nj]
        r_last[i] = (r_old - alpha_w * (w[i] + beta_w * s[i]))[:, 0:nj]
        return 0

    slabs(2, final, 0)
    rr, rw, rs, ww, ws, ss = reduce_wait(CG_ITERS, 6)
    scal_ref[last - 1] = line(rr)
    scal_ref[last] = line(rr - 2.0 * alpha * (rw + beta * rs) + alpha * alpha * (ww + 2.0 * beta * ws + beta * beta * ss))


def finish_kernel(scal, x, r, x_hbm, r_hbm, hist_hbm, hist, sem):
    copies = [pltpu.make_async_copy(x, x_hbm, sem.at[0]), pltpu.make_async_copy(r, r_hbm, sem.at[1]),
              pltpu.make_async_copy(hist, hist_hbm, sem.at[2])]
    copies[0].start()
    copies[1].start()
    for t in range(CG_ITERS):
        hist[t] = scal[t, 0, 0]
    copies[2].start()
    for copy in copies:
        copy.wait()


def solution(mesh):
    counts = (mesh.shape['gx'], mesh.shape['gy'], mesh.shape['gz'])
    grid_spec = P('gx', 'gy', 'gz')

    def local_solve(k_cell, k_ghost, f_rhs, u_init):
        ni, nj, nl = k_cell.shape
        flip = lambda a: jnp.swapaxes(a, 1, 2)
        slots = CG_ITERS + 3
        devices = counts[0] * counts[1] * counts[2]
        width = k_ghost.shape[2]
        any_spec = pl.BlockSpec(memory_space=pl.ANY)
        vm = lambda *shape: pltpu.VMEM(shape, F32)
        whole = vm(ni, nl, LANES)
        block = vm(ni, nl, nj)
        padded = vm(ni + 2, nl + 2 * PAD, LANES)
        dma = pltpu.SemaphoreType.DMA
        kept = pltpu.VMEM((ni, nl, nj), F32)
        vmem_spec = pl.BlockSpec(memory_space=pltpu.VMEM)
        x_last, r_last, scal = pl.pallas_call(
            functools.partial(solve_kernel, (ni, nl, nj), counts),
            out_shape=(kept, kept, pltpu.VMEM((CG_ITERS, 1, LANES), F32)),
            in_specs=[any_spec] * 4,
            out_specs=(vmem_spec,) * 3,
            scratch_shapes=[
                block, block, block, vm(nj, width), vm(ni, width), vm(ni, width), vm(-(-width // LANES) * LANES, LANES),
                vm(2, nl, LANES), vm(nl // 2, LANES), vm(2, ni, LANES),
                padded, padded, vm(ni + 1, nl, LANES), whole, whole, vm(ni, nl + 2 * PAD, LANES), whole,
                whole, vm(2, ni, nl, LANES), whole, whole, whole, whole, whole,
                vm(slots, nl // 2, LANES), vm(slots, 2, ni, LANES),
                vm(slots, 2, nl, LANES), vm(slots, nl // 2, LANES), vm(slots, 2, ni, LANES),
                vm(CG_ITERS + 1, 1, LANES), vm(CG_ITERS + 1, devices, 1, LANES),
                dma((slots, 2)), dma((slots,)), dma((slots, 2)), dma((slots, 2)), dma((slots,)), dma((slots, 2)),
                dma((CG_ITERS + 1,)), dma((CG_ITERS + 1,)), dma((6,)), pltpu.SemaphoreType.REGULAR((6,)),
            ],
            compiler_params=pltpu.CompilerParams(has_side_effects=True, collective_id=0, vmem_limit_bytes=28 << 20),
        )(*(pltpu.with_memory_space_constraint(a, pltpu.HBM) for a in (k_ghost, flip(k_cell), flip(f_rhs), flip(u_init))))
        out_block = jax.ShapeDtypeStruct((ni, nl, nj), F32)
        x_new, r_new, hist = pl.pallas_call(
            finish_kernel,
            out_shape=(out_block, out_block, jax.ShapeDtypeStruct((CG_ITERS,), F32)),
            in_specs=[vmem_spec] * 3,
            out_specs=(any_spec,) * 3,
            scratch_shapes=[pltpu.SMEM((CG_ITERS,), F32), dma((3,))],
            compiler_params=pltpu.CompilerParams(vmem_limit_bytes=28 << 20),
        )(scal, x_last, r_last)
        return flip(x_new), flip(r_new), hist

    return jax.shard_map(local_solve, mesh=mesh, in_specs=(grid_spec, P(), grid_spec, grid_spec),
                         out_specs=(grid_spec, grid_spec, P()), check_vma=False)
```
